32 devices in a mesh: dp: 8 (over y, x, core), shard: 4 (over z).
Axes of the slice: x: 2, y: 2, z: 4, core: 2. Of those that a mesh axis runs over, the one named last changes fastest.
Arguments:
- hidden_in: bfloat16 [16384, 960], P(('dp', 'shard')), may hold values from -6 to 6
- out_grad: bfloat16 [16384, 960], P(('dp', 'shard')), may hold values from -6 to 6
- seg_ids: int32 [8, 2048], P('dp'), may hold values from 0 to 11, as said below
- doc_start: int32 [16384], P(('dp', 'shard')), may hold values from 0 to 2047, as said below
- norm_gains: float32 [2, 960], replicated, may hold values from 0.5 to 1.5
- heads_weight: float32 [960, 1600], P('shard', 'dp'), may hold values from -0.1875 to 0.1875
- output_weight: float32 [960, 960], P('shard', 'dp'), may hold values from -1 to 1
- expand_weight: float32 [960, 5120], P('shard', 'dp'), may hold values from -0.1875 to 0.1875
- down_weight: float32 [2560, 960], P('shard', 'dp'), may hold values from -0.125 to 0.125
- gains_first: float32 [2, 960], replicated, may hold values from -80 to 80
- gains_second: float32 [2, 960], replicated, may hold values from 983.04 to 3932.16
- heads_first: float32 [960, 1600], P('shard', 'dp'), may hold values from -56 to 56
- heads_second: float32 [960, 1600], P('shard', 'dp'), may hold values from 819.2 to 3276.8
- output_first: float32 [960, 960], P('shard', 'dp'), may hold values from -12 to 12
- output_second: float32 [960, 960], P('shard', 'dp'), may hold values from 32.768 to 131.072
- expand_first: float32 [960, 5120], P('shard', 'dp'), may hold values from -40 to 40
- expand_second: float32 [960, 5120], P('shard', 'dp'), may hold values from 98.304 to 393.216
- down_first: float32 [2560, 960], P('shard', 'dp'), may hold values from -64 to 64
- down_second: float32 [2560, 960], P('shard', 'dp'), may hold values from 147.456 to 589.824
Outputs:
- hidden_out: bfloat16 [16384, 960], P(('dp', 'shard'))
- input_grad: float32 [16384, 960], P(('dp', 'shard'))
- gains_grad: float32 [2, 960], replicated
- heads_grad: float32 [960, 1600], P('shard', 'dp')
- output_grad: float32 [960, 960], P('shard', 'dp')
- expand_grad: float32 [960, 5120], P('shard', 'dp')
- down_grad: float32 [2560, 960], P('shard', 'dp')
- gains_new: float32 [2, 960], replicated
- heads_new: float32 [960, 1600], P('shard', 'dp')
- output_new: float32 [960, 960], P('shard', 'dp')
- expand_new: float32 [960, 5120], P('shard', 'dp')
- down_new: float32 [2560, 960], P('shard', 'dp')
- gains_first_new: float32 [2, 960], replicated
- gains_second_new: float32 [2, 960], replicated
- heads_first_new: float32 [960, 1600], P('shard', 'dp')
- heads_second_new: float32 [960, 1600], P('shard', 'dp')
- output_first_new: float32 [960, 960], P('shard', 'dp')
- output_second_new: float32 [960, 960], P('shard', 'dp')
- expand_first_new: float32 [960, 5120], P('shard', 'dp')
- expand_second_new: float32 [960, 5120], P('shard', 'dp')
- down_first_new: float32 [2560, 960], P('shard', 'dp')
- down_second_new: float32 [2560, 960], P('shard', 'dp')
The draws below stay inside these ranges and needn't reach their ends.
Inputs may be any that keep to these rules, and one draw needn't show every extreme that they name: `seg_ids`: each row is one sequence; ids are 0 at its first token and rise by one at each document's first token. Every document has at most 2000 tokens, and every one but the first and last of its sequence at least 204. Some sequence holds a document of exactly 2000 tokens, and some sequence reaches the largest id. `doc_start`: agrees with seg_ids: for each token, the position within its sequence of the first token with the same id.
All inputs are finite; a program needn't handle non-finite values.
Results may differ from the reference program's by a relative error of at most 0.014.
Values may be sent and summed in bfloat16 or wider, within the bound.
A program may use at most 256 MiB of HBM per device.

```python
import math
import jax
import jax.numpy as jnp
from jax import lax

D = 960
QUERY_HEADS = 15
KEY_VALUE_HEADS = 5
HEAD_SIZE = 64
FF = 2560
ADAM_STEP = 10
QKV = 1600
SEQ = 2048
SEQS = 8
TOKENS = 16384
DOC_LO = 204
DOC_HI = 2000


def document_layout(key):
    middle_count = (SEQ - 2) // DOC_LO
    doc_count = middle_count + 2
    base_key = jax.random.fold_in(key, 11)
    first_lengths = jax.random.randint(jax.random.fold_in(base_key, 1), (SEQS, 1), 1, DOC_HI + 1, dtype=jnp.int32)
    later_lengths = jax.random.randint(jax.random.fold_in(base_key, 2), (SEQS, doc_count - 1), DOC_LO, DOC_HI + 1, dtype=jnp.int32)
    random_rows = jnp.concatenate([first_lengths, later_lengths], axis=1)
    slack = SEQ - 2 - middle_count * DOC_LO
    extra = jax.random.randint(jax.random.fold_in(base_key, 3), (1,), 0, slack + 1, dtype=jnp.int32)
    picked = jax.random.randint(jax.random.fold_in(base_key, 4), (1,), 0, middle_count, dtype=jnp.int32)
    columns = jnp.arange(middle_count, dtype=jnp.int32)
    dense_middle = DOC_LO + (slack - extra) * (columns == picked).astype(jnp.int32)
    dense_row = jnp.concatenate([1 + extra, dense_middle, jnp.ones((1,), jnp.int32)])
    offset = jax.random.randint(jax.random.fold_in(base_key, 5), (1,), 0, SEQ - DOC_HI + 1, dtype=jnp.int32)
    long_row = jnp.concatenate([offset, jnp.full((1,), DOC_HI, jnp.int32), jnp.full((doc_count - 2,), SEQ, jnp.int32)])
    dense_seq = jax.random.randint(jax.random.fold_in(base_key, 6), (), 0, SEQS, dtype=jnp.int32)
    long_seq = (dense_seq + 1 + jax.random.randint(jax.random.fold_in(base_key, 7), (), 0, SEQS - 1, dtype=jnp.int32)) % SEQS
    row_index = jnp.arange(SEQS, dtype=jnp.int32)[:, None]
    lengths = jnp.where(row_index == dense_seq, dense_row[None, :], jnp.where(row_index == long_seq, long_row[None, :], random_rows))
    doc_ends = jnp.cumsum(lengths, axis=1)
    doc_starts = doc_ends - lengths
    places = jnp.arange(SEQ, dtype=jnp.int32)
    passed = doc_ends[:, None, :] <= places[None, :, None]
    raw_index = jnp.sum(passed.astype(jnp.int32), axis=2)
    segment = jnp.sum((passed & (lengths[:, None, :] > 0)).astype(jnp.int32), axis=2)
    first_pos = jnp.take_along_axis(doc_starts, raw_index, axis=1)
    return (segment.astype(jnp.int32), first_pos.astype(jnp.int32))


def draw_seg_ids(key, part):
    segment, first_pos = document_layout(key)
    return segment


def draw_doc_start(key, part):
    segment, first_pos = document_layout(key)
    return first_pos.reshape(TOKENS)


def with_spikes(values, own_key, source, target, shards_of, factor):
    def block_of(dim):
        return (jnp.arange(values.shape[dim]) // (values.shape[dim] // shards_of)).reshape((-1,) + (1,) * (values.ndim - 1 - dim))

    first = jax.random.permutation(own_key, shards_of)[block_of(target)]
    second = (block_of(target) + shards_of // 2) % shards_of
    return jnp.where((block_of(source) == first) | (block_of(source) == second), factor * values, values)


def steps_of(own_key, extent, pieces, least, high):
    level = 1.0
    for axis_at, parts in pieces:
        draws = jax.random.uniform(jax.random.fold_in(jax.random.fold_in(own_key, 6), axis_at), (parts,), jnp.float32, least / len(pieces), high / len(pieces))
        level = level * jnp.repeat(jnp.exp(draws), extent[axis_at] // parts).reshape((-1,) + (1,) * (len(extent) - 1 - axis_at))
    return level


def gaussian(stream_key, shape, spread, limit, split=(), kind=jnp.bfloat16):
    entries = jax.random.normal(stream_key, shape, jnp.float32) * spread
    if len(split) > 0:
        entries = steps_of(stream_key, shape, split, -0.22, 0.18) * entries
    return jnp.clip(entries, min=-limit, max=limit).astype(kind)


def bell_draw_with(rng, dims, scale, most, pieces, heavy, kind=jnp.bfloat16):
    drawn = scale * jax.random.normal(rng, dims, jnp.float32)
    if pieces:
        drawn = drawn * steps_of(rng, dims, pieces, -0.22, 0.18)
    return jnp.clip(with_spikes(drawn, jax.random.fold_in(rng, 3), *heavy), -most, most).astype(kind)


def setup_inputs(seed: int = 0) -> dict:
    key_list = jax.random.split(jax.random.key(seed), 20)
    hidden_in = gaussian(key_list[0], (TOKENS, D), 1.0, 6.0, ((0, 32),))
    out_grad = bell_draw_with(key_list[1], (TOKENS, D), 1.0, 6.0, ((0, 32),), (0, 1, 32, 2.75))
    seg_ids = draw_seg_ids(jax.random.fold_in(key_list[19], 71), 0)
    doc_start = draw_doc_start(jax.random.fold_in(key_list[19], 71), 0)
    norm_gains = jnp.clip(1.0 + 0.1 * jax.random.normal(key_list[4], (2, D), jnp.float32), 0.5, 1.5)
    heads_weight = gaussian(key_list[5], (D, QKV), D ** -0.5, 0.1875, ((0, 4), (1, 8)), jnp.float32)
    output_weight = gaussian(key_list[6], (QUERY_HEADS * HEAD_SIZE, D), 32 ** -0.5, 1.0, ((0, 4), (1, 8)), jnp.float32)
    expand_weight = gaussian(key_list[7], (D, 2 * FF), D ** -0.5, 0.1875, ((0, 4), (1, 8)), jnp.float32)
    down_weight = gaussian(key_list[8], (FF, D), FF ** -0.5, 0.125, ((0, 4), (1, 8)), jnp.float32)
    gains_first = gaussian(key_list[9], (2, D), (0.1 * TOKENS ** 0.5), 80.0, (), jnp.float32)
    gains_second = jnp.clip(jnp.exp(jax.random.uniform(key_list[10], (2, D), jnp.float32, math.log(983.04), math.log(3932.16))), 983.04, 3932.16)
    heads_first = gaussian(key_list[11], (D, QKV), (0.075 * TOKENS ** 0.5), 56.0, ((0, 4), (1, 8)), jnp.float32)
    heads_second = jnp.clip(jnp.exp(math.log(3276.8) - 1.3862944 * jax.random.uniform(key_list[12], (D, QKV), jnp.float32) ** steps_of(key_list[12], (D, QKV), ((0, 4), (1, 8)), -0.2, 0.2)), 819.2, 3276.8)
    output_first = gaussian(key_list[13], (QUERY_HEADS * HEAD_SIZE, D), (0.015 * TOKENS ** 0.5), 12.0, ((0, 4), (1, 8)), jnp.float32)
    output_second = jnp.clip(jnp.exp(math.log(131.072) - 1.3862944 * jax.random.uniform(key_list[14], (QUERY_HEADS * HEAD_SIZE, D), jnp.float32) ** steps_of(key_list[14], (QUERY_HEADS * HEAD_SIZE, D), ((0, 4), (1, 8)), -0.2, 0.2)), 32.768, 131.072)
    expand_first = gaussian(key_list[15], (D, 2 * FF), (0.05 * TOKENS ** 0.5), 40.0, ((0, 4), (1, 8)), jnp.float32)
    expand_second = jnp.clip(jnp.exp(math.log(393.216) - 1.3862944 * jax.random.uniform(key_list[16], (D, 2 * FF), jnp.float32) ** steps_of(key_list[16], (D, 2 * FF), ((0, 4), (1, 8)), -0.2, 0.2)), 98.304, 393.216)
    down_first = gaussian(key_list[17], (FF, D), (0.09 * TOKENS ** 0.5), 64.0, ((0, 4), (1, 8)), jnp.float32)
    down_second = jnp.clip(jnp.exp(math.log(589.824) - 1.3862944 * jax.random.uniform(key_list[18], (FF, D), jnp.float32) ** steps_of(key_list[18], (FF, D), ((0, 4), (1, 8)), -0.2, 0.2)), 147.456, 589.824)
    return dict(hidden_in=hidden_in, out_grad=out_grad, seg_ids=seg_ids, doc_start=doc_start, norm_gains=norm_gains, heads_weight=heads_weight, output_weight=output_weight, expand_weight=expand_weight, down_weight=down_weight, gains_first=gains_first, gains_second=gains_second, heads_first=heads_first, heads_second=heads_second, output_first=output_first, output_second=output_second, expand_first=expand_first, expand_second=expand_second, down_first=down_first, down_second=down_second)


norm_epsilon = 1e-05
beta_one = 0.9
beta_two = 0.95
adam_epsilon = 1e-08
matrix_rate = 0.03
output_rate = 0.15
gain_rate = 0.5
decay_rate = 0.1

def rounded_wide(values):
    return lax.optimization_barrier(values.astype(jnp.bfloat16)).astype(jnp.float32)

def rotary_tables(relative):
    half_width = HEAD_SIZE // 2
    freq_table = jnp.power(10000.0, -jnp.arange(half_width).astype(jnp.float32) / half_width)
    angle_table = relative.astype(jnp.float32)[:, None] * freq_table[None, :]
    return (jnp.cos(angle_table), jnp.sin(angle_table))

def apply_rotary(values, cosine_table, sine_table):
    half_width = HEAD_SIZE // 2
    first_half = values[..., :half_width]
    second_half = values[..., half_width:]
    cos_part = cosine_table[:, None, :]
    sin_part = sine_table[:, None, :]
    return jnp.concatenate([first_half * cos_part - second_half * sin_part, second_half * cos_part + first_half * sin_part], axis=-1)

def reverse_rotary(values, cosine_table, sine_table):
    half_width = HEAD_SIZE // 2
    first_half = values[..., :half_width]
    second_half = values[..., half_width:]
    cos_part = cosine_table[:, None, :]
    sin_part = sine_table[:, None, :]
    return jnp.concatenate([first_half * cos_part + second_half * sin_part, second_half * cos_part - first_half * sin_part], axis=-1)

def rms_forward(values, gain):
    inverse = lax.rsqrt(lax.optimization_barrier(jnp.mean(values * values, axis=-1, keepdims=True)) + norm_epsilon)
    normed = values * inverse
    return (normed, inverse, (normed * gain).astype(jnp.bfloat16))

def rms_backward(upstream, normed, inverse, gain):
    scaled = upstream * gain
    gain_term = lax.optimization_barrier(jnp.sum(upstream * normed, axis=0))
    back = inverse * (scaled - normed * lax.optimization_barrier(jnp.mean(scaled * normed, axis=-1, keepdims=True)))
    return (back, gain_term)

def adamw(weight, grad, first, second, rate, decay):
    first_new = beta_one * first + (1.0 - beta_one) * grad
    second_new = beta_two * second + (1.0 - beta_two) * grad * grad
    first_hat = first_new / (1.0 - beta_one ** ADAM_STEP)
    second_hat = second_new / (1.0 - beta_two ** ADAM_STEP)
    weight_new = weight - rate * (first_hat / (jnp.sqrt(second_hat) + adam_epsilon) + decay * weight)
    return (weight_new, first_new, second_new)

def attend_forward(queries, packed, allowed):
    group_width = QUERY_HEADS // KEY_VALUE_HEADS
    key_total_width = KEY_VALUE_HEADS * HEAD_SIZE
    outputs = []
    logsums = []
    for group_of_head in range(KEY_VALUE_HEADS):
        query_group = queries[:, group_of_head * group_width:(group_of_head + 1) * group_width, :].astype(jnp.float32)
        key_group = packed[:, group_of_head * HEAD_SIZE:(group_of_head + 1) * HEAD_SIZE].astype(jnp.float32)
        value_group = packed[:, key_total_width + group_of_head * HEAD_SIZE:key_total_width + (group_of_head + 1) * HEAD_SIZE].astype(jnp.float32)
        scores = jnp.einsum('qhd,kd->hqk', query_group, key_group) * HEAD_SIZE ** (-0.5)
        exponent = jnp.where(allowed[None], jnp.exp(scores), 0.0)
        totals = lax.optimization_barrier(jnp.sum(exponent, axis=-1))
        probs = rounded_wide(exponent / totals[..., None])
        outputs.append(jnp.einsum('hqk,kd->qhd', probs, value_group))
        logsums.append(jnp.log(totals))
    return (jnp.concatenate(outputs, axis=1), jnp.concatenate(logsums, axis=0))

def attend_backward(queries, packed, allowed, logsums, attended, attended_grad):
    group_width = QUERY_HEADS // KEY_VALUE_HEADS
    key_total_width = KEY_VALUE_HEADS * HEAD_SIZE
    row_delta = lax.optimization_barrier(jnp.sum(attended_grad.astype(jnp.float32) * attended.astype(jnp.float32), axis=-1))
    query_grads = []
    key_grads = []
    value_grads = []
    for group_of_head in range(KEY_VALUE_HEADS):
        lower_head = group_of_head * group_width
        upper_head = lower_head + group_width
        query_group = queries[:, lower_head:upper_head, :].astype(jnp.float32)
        grad_group = attended_grad[:, lower_head:upper_head, :].astype(jnp.float32)
        key_group = packed[:, group_of_head * HEAD_SIZE:(group_of_head + 1) * HEAD_SIZE].astype(jnp.float32)
        value_group = packed[:, key_total_width + group_of_head * HEAD_SIZE:key_total_width + (group_of_head + 1) * HEAD_SIZE].astype(jnp.float32)
        scores = jnp.einsum('qhd,kd->hqk', query_group, key_group) * HEAD_SIZE ** (-0.5)
        probs = jnp.where(allowed[None], jnp.exp(scores - logsums[lower_head:upper_head][..., None]), 0.0)
        probs_half = rounded_wide(probs)
        prob_grad = jnp.einsum('qhd,kd->hqk', grad_group, value_group)
        score_grad = rounded_wide(probs * (prob_grad - jnp.transpose(row_delta[:, lower_head:upper_head])[..., None]) * HEAD_SIZE ** (-0.5))
        query_grads.append(jnp.einsum('hqk,kd->qhd', score_grad, key_group))
        key_grads.append(jnp.einsum('hqk,qhd->kd', score_grad, query_group))
        value_grads.append(jnp.einsum('hqk,qhd->kd', probs_half, grad_group))
    return (jnp.concatenate(query_grads, axis=1), jnp.concatenate(key_grads + value_grads, axis=1))

def sequence_pass(params, tokens, cotangent, seg_row, start_row):
    norm_gains, heads_half, output_half, expand_half, down_half = params
    count_of_rows = tokens.shape[0]
    query_total_width = QUERY_HEADS * HEAD_SIZE
    key_total_width = KEY_VALUE_HEADS * HEAD_SIZE
    positions = jnp.arange(count_of_rows).astype(jnp.int32)
    cosine_table, sine_table = rotary_tables(positions - start_row)
    allowed = (seg_row[:, None] == seg_row[None, :]) & (positions[None, :] <= positions[:, None])
    gain_one = norm_gains[0]
    gain_two = norm_gains[1]
    inputs = tokens.astype(jnp.float32)
    normed_one, inverse_one, hidden_one = rms_forward(inputs, gain_one)
    projected_rows = jnp.dot(hidden_one, heads_half, preferred_element_type=jnp.float32)
    queries = apply_rotary(projected_rows[:, :query_total_width].reshape(count_of_rows, QUERY_HEADS, HEAD_SIZE), cosine_table, sine_table).astype(jnp.bfloat16)
    key_rotated = apply_rotary(projected_rows[:, query_total_width:query_total_width + key_total_width].reshape(count_of_rows, KEY_VALUE_HEADS, HEAD_SIZE), cosine_table, sine_table).astype(jnp.bfloat16)
    values = projected_rows[:, query_total_width + key_total_width:].astype(jnp.bfloat16)
    packed = jnp.concatenate([key_rotated.reshape(count_of_rows, key_total_width), values], axis=1)
    attended, logsums = attend_forward(queries, packed, allowed)
    attended_half = attended.astype(jnp.bfloat16)
    attended_flat = attended_half.reshape(count_of_rows, query_total_width)
    residual = inputs + jnp.dot(attended_flat, output_half, preferred_element_type=jnp.float32)
    normed_two, inverse_two, hidden_two = rms_forward(residual, gain_two)
    gate_up = jnp.dot(hidden_two, expand_half, preferred_element_type=jnp.float32)
    gate_part = gate_up[:, :FF]
    up_part = gate_up[:, FF:]
    sigmoid_gate = jax.nn.sigmoid(gate_part)
    silu_gate = gate_part * sigmoid_gate
    mixed_act = (silu_gate * up_part).astype(jnp.bfloat16)
    hidden_out = (residual + jnp.dot(mixed_act, down_half, preferred_element_type=jnp.float32)).astype(jnp.bfloat16)
    upstream = cotangent.astype(jnp.float32)
    mixed_grad = jnp.dot(cotangent, down_half.T, preferred_element_type=jnp.float32)
    down_term = jnp.dot(mixed_act.T, cotangent, preferred_element_type=jnp.float32)
    gate_grad = mixed_grad * up_part * sigmoid_gate * (1.0 + gate_part * (1.0 - sigmoid_gate))
    up_grad = mixed_grad * silu_gate
    expand_delta = jnp.concatenate([gate_grad, up_grad], axis=1).astype(jnp.bfloat16)
    expand_term = jnp.dot(hidden_two.T, expand_delta, preferred_element_type=jnp.float32)
    hidden_two_grad = jnp.dot(expand_delta, expand_half.T, preferred_element_type=jnp.float32)
    residual_back, gain_two_term = rms_backward(hidden_two_grad, normed_two, inverse_two, gain_two)
    residual_grad = upstream + residual_back
    residual_delta = residual_grad.astype(jnp.bfloat16)
    output_term = jnp.dot(attended_flat.T, residual_delta, preferred_element_type=jnp.float32)
    attended_grad = jnp.dot(residual_delta, output_half.T, preferred_element_type=jnp.float32).astype(jnp.bfloat16).reshape(count_of_rows, QUERY_HEADS, HEAD_SIZE)
    query_grad, packed_gradient = attend_backward(queries, packed, allowed, logsums, attended_half, attended_grad)
    key_backward = reverse_rotary(packed_gradient[:, :key_total_width].reshape(count_of_rows, KEY_VALUE_HEADS, HEAD_SIZE), cosine_table, sine_table).reshape(count_of_rows, key_total_width)
    query_back = reverse_rotary(query_grad, cosine_table, sine_table).reshape(count_of_rows, query_total_width)
    heads_delta = jnp.concatenate([query_back, key_backward, packed_gradient[:, key_total_width:]], axis=1).astype(jnp.bfloat16)
    heads_term = jnp.dot(hidden_one.T, heads_delta, preferred_element_type=jnp.float32)
    hidden_one_grad = jnp.dot(heads_delta, heads_half.T, preferred_element_type=jnp.float32)
    input_back, gain_one_term = rms_backward(hidden_one_grad, normed_one, inverse_one, gain_one)
    input_grad = residual_grad + input_back
    gain_terms = jnp.stack([gain_one_term, gain_two_term], axis=0)
    return (hidden_out, input_grad, (gain_terms, heads_term, output_term, expand_term, down_term))

def reference(hidden_in, out_grad, seg_ids, doc_start, norm_gains, heads_weight, output_weight, expand_weight, down_weight, gains_first, gains_second, heads_first, heads_second, output_first, output_second, expand_first, expand_second, down_first, down_second):
    params = (norm_gains, heads_weight.astype(jnp.bfloat16), output_weight.astype(jnp.bfloat16), expand_weight.astype(jnp.bfloat16), down_weight.astype(jnp.bfloat16))
    initial = (jnp.zeros((2, D), jnp.float32), jnp.zeros(heads_weight.shape, jnp.float32), jnp.zeros(output_weight.shape, jnp.float32), jnp.zeros(expand_weight.shape, jnp.float32), jnp.zeros(down_weight.shape, jnp.float32))

    def one_sequence(totals, inputs):
        tokens, cotangent, seg_row, start_row = inputs
        out_rows, grad_rows, terms = sequence_pass(params, tokens, cotangent, seg_row, start_row)
        summed = tuple((total + term for total, term in zip(totals, terms)))
        return (summed, (out_rows, grad_rows))
    sums, stacked = lax.scan(one_sequence, initial, (hidden_in.reshape(SEQS, SEQ, D), out_grad.reshape(SEQS, SEQ, D), seg_ids, doc_start.reshape(SEQS, SEQ)))
    hidden_out = stacked[0].reshape(TOKENS, D)
    input_grad = stacked[1].reshape(TOKENS, D)
    gains_grad, heads_grad, output_grad, expand_grad, down_grad = sums
    gains_new, gains_first_new, gains_second_new = adamw(norm_gains, gains_grad, gains_first, gains_second, gain_rate, 0.0)
    heads_new, heads_first_new, heads_second_new = adamw(heads_weight, heads_grad, heads_first, heads_second, matrix_rate, decay_rate)
    output_new, output_first_new, output_second_new = adamw(output_weight, output_grad, output_first, output_second, output_rate, decay_rate)
    expand_new, expand_first_new, expand_second_new = adamw(expand_weight, expand_grad, expand_first, expand_second, matrix_rate, decay_rate)
    down_new, down_first_new, down_second_new = adamw(down_weight, down_grad, down_first, down_second, matrix_rate, decay_rate)
    return (hidden_out, input_grad, gains_grad, heads_grad, output_grad, expand_grad, down_grad, gains_new, heads_new, output_new, expand_new, down_new, gains_first_new, gains_second_new, heads_first_new, heads_second_new, output_first_new, output_second_new, expand_first_new, expand_second_new, down_first_new, down_second_new)
```

```python
import functools
import math

import jax
import jax.numpy as jnp
from jax import lax
from jax.experimental import pallas as pl
from jax.experimental.pallas import tpu as pltpu
from jax.sharding import PartitionSpec as P

MESH = pl.DeviceIdType.MESH
ANY = pl.BlockSpec(memory_space=pl.ANY)
VMEM = pl.BlockSpec(memory_space=pltpu.VMEM)


class Grid:
    def __init__(self, mesh):
        self.nd = mesh.shape["dp"]
        self.nz = mesh.shape["shard"]
        self.nx = math.isqrt(self.nd // 2)
        self.ny = self.nd // 2 // self.nx
        assert self.nx == self.ny and self.nx * self.ny * 2 == self.nd

    def dp(self, y, x, c):
        return (y * self.nx + x) * 2 + c


class Here:
    def __init__(self, grid):
        self.grid = grid
        d = lax.axis_index("dp")
        self.z = lax.axis_index("shard")
        self.d = d
        self.c = lax.rem(d, 2)
        self.x = lax.rem(d // 2, grid.nx)
        self.y = d // (2 * grid.nx)
        g = grid
        self.xs = [lax.rem(self.x + k, g.nx) for k in range(1, g.nx)]
        self.ys = [lax.rem(self.y + k, g.ny) for k in range(1, g.ny)]
        self.zs = [lax.rem(self.z + k, g.nz) for k in range(1, g.nz)]
        self.partner = (g.dp(self.y, self.x, 1 - self.c), self.z)

    def on_x(self, x):
        return (self.grid.dp(self.y, x, self.c), self.z)

    def on_y(self, y):
        return (self.grid.dp(y, self.x, self.c), self.z)

    def on_z(self, z):
        return (self.d, z)

    def peers(self):
        return (
            [self.partner]
            + [self.on_x(x) for x in self.xs]
            + [self.on_y(y) for y in self.ys]
            + [self.on_z(z) for z in self.zs]
        )


def greet(peers):
    barrier = pltpu.get_barrier_semaphore()
    for peer in peers:
        pl.semaphore_signal(barrier, inc=1, device_id=peer, device_id_type=MESH)
    pl.semaphore_wait(barrier, len(peers))


def send(src, dst, send_sem, recv_sem, device):
    pltpu.make_async_remote_copy(
        src_ref=src,
        dst_ref=dst,
        send_sem=send_sem,
        recv_sem=recv_sem,
        device_id=device,
        device_id_type=MESH,
    ).start()


def wait_bytes(ref, sem):
    pltpu.make_async_copy(ref, ref, sem).wait()


def half_rows(rows):
    return max(16, int(rows / 32 + 0.5) * 16)


class Gather:
    def __init__(self, here, shard, out, sems, z_major):
        self.h, self.shard, self.out, self.sems, self.z_major = here, shard, out, sems, z_major
        self.rows = shard.shape[0]
        self.cut = half_rows(self.rows)

    def column(self, d, half=None):
        rows = {None: slice(None), 0: pl.ds(0, self.cut), 1: pl.ds(self.cut, self.rows - self.cut)}[half]
        if self.z_major:
            return self.out.at[:, d, rows]
        return self.out.at[d, :, rows]

    def block(self, d, z):
        return self.out.at[z, d] if self.z_major else self.out.at[d, z]

    def columns(self, count):
        return self.out.at[:, pl.ds(0, count)] if self.z_major else self.out.at[pl.ds(0, count)]

    def blocks(self, count):
        return self.out.at[pl.ds(0, count), 0] if self.z_major else self.out.at[0, pl.ds(0, count)]

    def stage_z(self):
        h, s = self.h, self.sems
        for z in h.zs:
            send(self.shard, self.block(h.d, h.z), s.at[0], s.at[1], h.on_z(z))
        self.own = pltpu.make_async_copy(self.shard, self.block(h.d, h.z), s.at[8])
        self.own.start()

    def stage_one(self):
        h, s = self.h, self.sems
        wait_bytes(self.blocks(len(h.zs)), s.at[1])
        self.own.wait()
        for x in h.xs:
            send(self.column(h.d, 0), self.column(h.d, 0), s.at[2], s.at[3], h.on_x(x))
        for y in h.ys:
            send(self.column(h.d, 1), self.column(h.d, 1), s.at[2], s.at[3], h.on_y(y))
        send(self.column(h.d), self.column(h.d), s.at[6], s.at[7], h.partner)

    def stage_two(self):
        h, s, g = self.h, self.sems, self.h.grid
        wait_bytes(self.columns(len(h.xs)), s.at[3])
        for y in h.ys:
            for x in [h.x] + h.xs:
                col = self.column(g.dp(h.y, x, h.c), 0)
                send(col, col, s.at[4], s.at[5], h.on_y(y))
        for x in h.xs:
            for y in [h.y] + h.ys:
                col = self.column(g.dp(y, h.x, h.c), 1)
                send(col, col, s.at[4], s.at[5], h.on_x(x))
        for x in h.xs:
            col = self.column(g.dp(h.y, x, h.c), 0)
            send(col, col, s.at[6], s.at[7], h.partner)
        for y in h.ys:
            col = self.column(g.dp(y, h.x, h.c), 1)
            send(col, col, s.at[6], s.at[7], h.partner)

    def stage_three(self):
        h, s, g = self.h, self.sems, self.h.grid
        wait_bytes(self.columns(g.nx * len(h.ys)), s.at[5])
        for y in h.ys:
            for x in [h.x] + h.xs:
                col = self.column(g.dp(y, x, h.c), 0)
                send(col, col, s.at[6], s.at[7], h.partner)
        for x in h.xs:
            for y in [h.y] + h.ys:
                col = self.column(g.dp(y, x, h.c), 1)
                send(col, col, s.at[6], s.at[7], h.partner)

    def arrive(self):
        g = self.h.grid
        wait_bytes(self.columns(g.nd // 2), self.sems.at[7])

    def drain(self):
        h, s, g = self.h, self.sems, self.h.grid
        wait_bytes(self.blocks(len(h.zs)), s.at[0])
        wait_bytes(self.columns(len(h.xs)), s.at[2])
        wait_bytes(self.columns(g.nx * len(h.ys)), s.at[4])
        wait_bytes(self.columns(g.nd // 2), s.at[6])


GATHER_SEMS = 9


def gather_kernel(grid, z_majors, *refs):
    n = len(z_majors)
    shards, outs, sems = refs[:n], refs[n : 2 * n], refs[2 * n]
    here = Here(grid)
    greet(here.peers())
    jobs = [Gather(here, shards[i], outs[i], sems.at[i], z_majors[i]) for i in range(n)]
    for job in jobs:
        job.stage_z()
    for step in range(n + 2):
        if step < n:
            jobs[step].stage_one()
        if 0 <= step - 1 < n:
            jobs[step - 1].stage_two()
        if 0 <= step - 2 < n:
            jobs[step - 2].stage_three()
    for job in jobs:
        job.arrive()
        job.drain()


def gather_weights(grid, shards, z_majors, collective_id):
    shapes = []
    for shard, z_major in zip(shards, z_majors):
        lead = (grid.nz, grid.nd) if z_major else (grid.nd, grid.nz)
        shapes.append(jax.ShapeDtypeStruct(lead + shard.shape, shard.dtype))
    return pl.pallas_call(
        functools.partial(gather_kernel, grid, tuple(z_majors)),
        out_shape=shapes,
        in_specs=[VMEM] * len(shards),
        out_specs=[ANY] * len(shards),
        scratch_shapes=[pltpu.SemaphoreType.DMA((len(shards), GATHER_SEMS))],
        compiler_params=pltpu.CompilerParams(collective_id=collective_id, has_side_effects=True),
        name="gather_weights",
    )(*shards)


class Reduce:
    def __init__(self, here, terms, result, bufs, sems, z_major):
        self.h, self.terms, self.result, self.sems, self.z_major = here, terms, result, sems, z_major
        self.own, self.other, self.one_a, self.one_b, self.two_a, self.two_b, self.last = bufs
        self.rows = self.own.shape[-2]
        self.cut = half_rows(self.rows)

    @staticmethod
    def scratch(grid, rows, cols, z_major):
        cut = half_rows(rows)
        ny, nx, nz = grid.ny, grid.nx, grid.nz
        full = (nz, ny, nx) if z_major else (ny, nx, nz)
        row = (nz, nx) if z_major else (nx, nz)
        bf = jnp.bfloat16
        return [
            pltpu.VMEM(full + (rows, cols), bf),
            pltpu.VMEM(full + (rows, cols), bf),
            pltpu.VMEM((ny,) + row + (cut, cols), bf),
            pltpu.VMEM((nx,) + row + (rows - cut, cols), bf),
            pltpu.VMEM((nx, nz, cut, cols), bf),
            pltpu.VMEM((ny, nz, rows - cut, cols), bf),
            pltpu.VMEM((nz, rows, cols), bf),
        ]

    def span(self, half):
        return {None: slice(None), 0: pl.ds(0, self.cut), 1: pl.ds(self.cut, self.rows - self.cut)}[half]

    def at(self, y, x, z, half):
        y, x, z = (slice(None) if v is None else v for v in (y, x, z))
        return (z, y, x, self.span(half)) if self.z_major else (y, x, z, self.span(half))

    def side(self, c):
        return self.terms.at[:, :, :, c] if self.z_major else self.terms.at[:, :, c]

    def stage_core(self):
        h, s = self.h, self.sems
        send(self.side(1 - h.c), self.other, s.at[0], s.at[1], h.partner)
        self.load = pltpu.make_async_copy(self.side(h.c), self.own, s.at[8])
        self.load.start()

    def add_loop(self, shape, body):
        total = math.prod(shape)

        def step(i, carry):
            place = []
            rest = i
            for size in reversed(shape):
                place.append(lax.rem(rest, size))
                rest = rest // size
            body(tuple(reversed(place)))
            return carry

        lax.fori_loop(0, total, step, 0)

    def stage_one(self):
        h, s, g = self.h, self.sems, self.h.grid
        self.load.wait()
        wait_bytes(self.other, s.at[1])

        def body(place):
            total = self.own[place].astype(jnp.float32) + self.other[place].astype(jnp.float32)
            self.own[place] = total.astype(jnp.bfloat16)

        self.add_loop(self.own.shape[:3], body)
        for y in h.ys:
            send(self.own.at[self.at(y, None, None, 0)], self.one_a.at[h.y], s.at[2], s.at[3], h.on_y(y))
        for x in h.xs:
            send(self.own.at[self.at(None, x, None, 1)], self.one_b.at[h.x], s.at[9], s.at[10], h.on_x(x))

    def stage_two(self):
        h, s, g = self.h, self.sems, self.h.grid
        wait_bytes(self.one_a.at[pl.ds(0, g.ny - 1)], s.at[3])
        wait_bytes(self.one_b.at[pl.ds(0, g.nx - 1)], s.at[10])

        def body_a(place):
            where = (place[1], place[0]) if self.z_major else place
            spot = self.at(h.y, where[0], where[1], 0)
            total = self.own[spot].astype(jnp.float32)
            for y in h.ys:
                total += self.one_a[(y,) + place].astype(jnp.float32)
            self.own[spot] = total.astype(jnp.bfloat16)

        self.add_loop(self.one_a.shape[1:3], body_a)

        def body_b(place):
            where = (place[1], place[0]) if self.z_major else place
            spot = self.at(where[0], h.x, where[1], 1)
            total = self.own[spot].astype(jnp.float32)
            for x in h.xs:
                total += self.one_b[(x,) + place].astype(jnp.float32)
            self.own[spot] = total.astype(jnp.bfloat16)

        self.add_loop(self.one_b.shape[1:3], body_b)
        for x in h.xs:
            send(self.own.at[self.at(h.y, x, None, 0)], self.two_a.at[h.x], s.at[4], s.at[5], h.on_x(x))
        for y in h.ys:
            send(self.own.at[self.at(y, h.x, None, 1)], self.two_b.at[h.y], s.at[11], s.at[12], h.on_y(y))

    def stage_three(self):
        h, s, g = self.h, self.sems, self.h.grid
        wait_bytes(self.two_a.at[pl.ds(0, g.nx - 1)], s.at[5])
        wait_bytes(self.two_b.at[pl.ds(0, g.ny - 1)], s.at[12])

        def body(place):
            (z,) = place
            spot = self.at(h.y, h.x, z, 0)
            total = self.own[spot].astype(jnp.float32)
            for x in h.xs:
                total += self.two_a[x, z].astype(jnp.float32)
            self.own[spot] = total.astype(jnp.bfloat16)
            spot = self.at(h.y, h.x, z, 1)
            total = self.own[spot].astype(jnp.float32)
            for y in h.ys:
                total += self.two_b[y, z].astype(jnp.float32)
            self.own[spot] = total.astype(jnp.bfloat16)

        self.add_loop((g.nz,), body)
        for z in h.zs:
            send(self.own.at[self.at(h.y, h.x, z, None)], self.last.at[h.z], s.at[6], s.at[7], h.on_z(z))

    def finish(self):
        h, s, g = self.h, self.sems, self.h.grid
        wait_bytes(self.last.at[pl.ds(0, g.nz - 1)], s.at[7])
        total = self.own[self.at(h.y, h.x, h.z, None)].astype(jnp.float32)
        for z in h.zs:
            total += self.last[z].astype(jnp.float32)
        self.result[...] = total

    def drain(self):
        g, s = self.h.grid, self.sems
        wait_bytes(self.other, s.at[0])
        wait_bytes(self.one_a.at[pl.ds(0, g.ny - 1)], s.at[2])
        wait_bytes(self.one_b.at[pl.ds(0, g.nx - 1)], s.at[9])
        wait_bytes(self.two_a.at[pl.ds(0, g.nx - 1)], s.at[4])
        wait_bytes(self.two_b.at[pl.ds(0, g.ny - 1)], s.at[11])
        wait_bytes(self.last.at[pl.ds(0, g.nz - 1)], s.at[6])


REDUCE_SEMS = 13
REDUCE_BUFS = 7


class Share:
    def __init__(self, here, value, result, bufs, sems):
        self.h, self.value, self.result, self.sems = here, value, result, sems
        self.bufs = bufs

    @staticmethod
    def scratch(grid, shape):
        return [pltpu.VMEM((n,) + shape, jnp.float32) for n in (2, grid.nx, grid.ny, grid.nz)]

    def axis(self, k):
        h = self.h
        return (
            (h.c, [h.partner], 2),
            (h.x, [h.on_x(x) for x in h.xs], h.grid.nx),
            (h.y, [h.on_y(y) for y in h.ys], h.grid.ny),
            (h.z, [h.on_z(z) for z in h.zs], h.grid.nz),
        )[k]

    def start(self, k):
        me, peers, n = self.axis(k)
        self.bufs[k][me] = self.value[...] if k == 0 else self.total
        for peer in peers:
            send(self.bufs[k].at[me], self.bufs[k].at[me], self.sems.at[2 * k], self.sems.at[2 * k + 1], peer)

    def end(self, k):
        me, peers, n = self.axis(k)
        wait_bytes(self.bufs[k].at[pl.ds(0, n - 1)], self.sems.at[2 * k + 1])
        total = self.bufs[k][0]
        for i in range(1, n):
            total = total + self.bufs[k][i]
        self.total = total
        if k == 3:
            self.result[...] = total

    def drain(self):
        for k in range(4):
            n = self.axis(k)[2]
            wait_bytes(self.bufs[k].at[pl.ds(0, n - 1)], self.sems.at[2 * k])


SHARE_SEMS = 8


def reduce_kernel(grid, z_majors, shared, *refs):
    n = len(z_majors)
    terms, refs = refs[:n], refs[n:]
    value, refs = (refs[0], refs[1:]) if shared else (None, refs)
    results, refs = refs[:n], refs[n:]
    value_sum, refs = (refs[0], refs[1:]) if shared else (None, refs)
    here = Here(grid)
    greet(here.peers())
    jobs = []
    for i in range(n):
        bufs, refs = refs[:REDUCE_BUFS], refs[REDUCE_BUFS:]
        jobs.append((bufs, i))
    sems, refs = refs[0], refs[1:]
    jobs = [Reduce(here, terms[i], results[i], bufs, sems.at[i], z_majors[i]) for bufs, i in jobs]
    share = None
    if shared:
        share = Share(here, value, value_sum, refs[:4], refs[4])
        share.start(0)
    for job in jobs:
        job.stage_core()
    for step in range(n + 3):
        if step < n:
            jobs[step].stage_one()
        if 0 <= step - 1 < n:
            jobs[step - 1].stage_two()
        if 0 <= step - 2 < n:
            jobs[step - 2].stage_three()
        if 0 <= step - 3 < n:
            jobs[step - 3].finish()
        if share is not None and step < 4:
            share.end(step)
            if step < 3:
                share.start(step + 1)
    if share is not None:
        for step in range(n + 3, 4):
            share.end(step)
            if step < 3:
                share.start(step + 1)
        share.drain()
    for job in jobs:
        job.drain()


def reduce_grads(grid, terms, z_majors, value, collective_id):
    split, shapes, scratch = [], [], []
    for term, z_major in zip(terms, z_majors):
        rows, cols = term.shape[-2:]
        lead = (grid.ny, grid.nx, 2)
        lead = (grid.nz,) + lead if z_major else lead + (grid.nz,)
        split.append(term.reshape(lead + (rows, cols)))
        shapes.append(jax.ShapeDtypeStruct((rows, cols), jnp.float32))
        scratch += Reduce.scratch(grid, rows, cols, z_major)
    n = len(terms)
    scratch.append(pltpu.SemaphoreType.DMA((n, REDUCE_SEMS)))
    shared = value is not None
    if shared:
        shapes.append(jax.ShapeDtypeStruct(value.shape, jnp.float32))
        scratch += Share.scratch(grid, value.shape)
        scratch.append(pltpu.SemaphoreType.DMA((SHARE_SEMS,)))
    return pl.pallas_call(
        functools.partial(reduce_kernel, grid, tuple(z_majors), shared),
        out_shape=shapes,
        in_specs=[ANY] * n + [VMEM] * shared,
        out_specs=[VMEM] * len(shapes),
        scratch_shapes=scratch,
        compiler_params=pltpu.CompilerParams(
            collective_id=collective_id, has_side_effects=True, vmem_limit_bytes=62 << 20
        ),
        name="reduce_grads",
    )(*split, *([value] if shared else []))


QUERY_HEADS = 15
KEY_VALUE_HEADS = 5
HEAD_SIZE = 64
FF = 2560
ADAM_STEP = 10


norm_epsilon = 1e-05
beta_one = 0.9
beta_two = 0.95
adam_epsilon = 1e-08
matrix_rate = 0.03
output_rate = 0.15
gain_rate = 0.5
decay_rate = 0.1


def rotary_tables(relative):
    half_width = HEAD_SIZE // 2
    freq_table = jnp.power(10000.0, -jnp.arange(half_width).astype(jnp.float32) / half_width)
    angle_table = relative.astype(jnp.float32)[:, None] * freq_table[None, :]
    return (jnp.cos(angle_table), jnp.sin(angle_table))


def apply_rotary(values, cosine_table, sine_table):
    half_width = HEAD_SIZE // 2
    first_half = values[..., :half_width]
    second_half = values[..., half_width:]
    cos_part = cosine_table[:, None, :]
    sin_part = sine_table[:, None, :]
    return jnp.concatenate(
        [
            first_half * cos_part - second_half * sin_part,
            second_half * cos_part + first_half * sin_part,
        ],
        axis=-1,
    )


def reverse_rotary(values, cosine_table, sine_table):
    half_width = HEAD_SIZE // 2
    first_half = values[..., :half_width]
    second_half = values[..., half_width:]
    cos_part = cosine_table[:, None, :]
    sin_part = sine_table[:, None, :]
    return jnp.concatenate(
        [
            first_half * cos_part + second_half * sin_part,
            second_half * cos_part - first_half * sin_part,
        ],
        axis=-1,
    )


def rms_forward(values, gain):
    inverse = lax.rsqrt(jnp.mean(values * values, axis=-1, keepdims=True) + norm_epsilon)
    normed = values * inverse
    return (normed, inverse, (normed * gain).astype(jnp.bfloat16))


def rms_backward(upstream, normed, inverse, gain):
    scaled = upstream * gain
    gain_term = jnp.sum(upstream * normed, axis=0)
    back = inverse * (scaled - normed * jnp.mean(scaled * normed, axis=-1, keepdims=True))
    return (back, gain_term)


def times_transposed(left, right):
    return lax.dot_general(
        left, right, (((1,), (1,)), ((), ())), preferred_element_type=jnp.float32
    )


def transposed_times(left, right):
    return lax.dot_general(
        left, right, (((0,), (0,)), ((), ())), preferred_element_type=jnp.float32
    )


def adamw(weight, grad, first, second, rate, decay):
    first_new = beta_one * first + (1.0 - beta_one) * grad
    second_new = beta_two * second + (1.0 - beta_two) * grad * grad
    first_hat = first_new / (1.0 - beta_one**ADAM_STEP)
    second_hat = second_new / (1.0 - beta_two**ADAM_STEP)
    weight_new = weight - rate * (
        first_hat / (jnp.sqrt(second_hat) + adam_epsilon) + decay * weight
    )
    return (weight_new, first_new, second_new)


def attend_forward(queries, all_keys, allowed):
    group_width = QUERY_HEADS // KEY_VALUE_HEADS
    key_total_width = KEY_VALUE_HEADS * HEAD_SIZE
    outputs = []
    logsums = []
    for group_of_head in range(KEY_VALUE_HEADS):
        query_group = queries[:, group_of_head * group_width : (group_of_head + 1) * group_width, :]
        key_group = all_keys[:, group_of_head * HEAD_SIZE : (group_of_head + 1) * HEAD_SIZE]
        value_group = all_keys[
            :,
            key_total_width
            + group_of_head * HEAD_SIZE : key_total_width
            + (group_of_head + 1) * HEAD_SIZE,
        ]
        scores = jnp.einsum(
            "qhd,kd->hqk", query_group, key_group, preferred_element_type=jnp.float32
        ) * HEAD_SIZE ** (-0.5)
        exponent = jnp.where(allowed[None], jnp.exp(scores), 0.0)
        totals = jnp.sum(exponent, axis=-1)
        probs = (exponent / totals[..., None]).astype(jnp.bfloat16)
        outputs.append(
            jnp.einsum("hqk,kd->qhd", probs, value_group, preferred_element_type=jnp.float32)
        )
        logsums.append(jnp.log(totals))
    return (jnp.concatenate(outputs, axis=1), jnp.concatenate(logsums, axis=0))


def attend_backward(queries, all_keys, allowed, logsums, attended, attended_grad):
    group_width = QUERY_HEADS // KEY_VALUE_HEADS
    key_total_width = KEY_VALUE_HEADS * HEAD_SIZE
    row_delta = jnp.sum(attended_grad.astype(jnp.float32) * attended.astype(jnp.float32), axis=-1)
    query_grads = []
    key_grads = []
    value_grads = []
    for group_of_head in range(KEY_VALUE_HEADS):
        lower_head = group_of_head * group_width
        upper_head = lower_head + group_width
        query_group = queries[:, lower_head:upper_head, :]
        grad_group = attended_grad[:, lower_head:upper_head, :]
        key_group = all_keys[:, group_of_head * HEAD_SIZE : (group_of_head + 1) * HEAD_SIZE]
        value_group = all_keys[
            :,
            key_total_width
            + group_of_head * HEAD_SIZE : key_total_width
            + (group_of_head + 1) * HEAD_SIZE,
        ]
        scores = jnp.einsum(
            "qhd,kd->hqk", query_group, key_group, preferred_element_type=jnp.float32
        ) * HEAD_SIZE ** (-0.5)
        probs = jnp.where(
            allowed[None], jnp.exp(scores - logsums[lower_head:upper_head][..., None]), 0.0
        )
        probs_half = probs.astype(jnp.bfloat16)
        prob_grad = jnp.einsum(
            "qhd,kd->hqk", grad_group, value_group, preferred_element_type=jnp.float32
        )
        score_grad = (
            probs
            * (prob_grad - jnp.transpose(row_delta[:, lower_head:upper_head])[..., None])
            * HEAD_SIZE ** (-0.5)
        ).astype(jnp.bfloat16)
        query_grads.append(
            jnp.einsum("hqk,kd->qhd", score_grad, key_group, preferred_element_type=jnp.float32)
        )
        key_grads.append(
            jnp.einsum("hqk,qhd->kd", score_grad, query_group, preferred_element_type=jnp.float32)
        )
        value_grads.append(
            jnp.einsum("hqk,qhd->kd", probs_half, grad_group, preferred_element_type=jnp.float32)
        )
    return (jnp.concatenate(query_grads, axis=1), jnp.concatenate(key_grads + value_grads, axis=1))


Z_MAJOR = (True, True, False, True)


def local(
    grid,
    hidden_in,
    out_grad,
    seg_ids,
    doc_start,
    norm_gains,
    heads_weight,
    output_weight,
    expand_weight,
    down_weight,
    gains_first,
    gains_second,
    heads_first,
    heads_second,
    output_first,
    output_second,
    expand_first,
    expand_second,
    down_first,
    down_second,
):
    count_of_rows = hidden_in.shape[0]
    query_total_width = QUERY_HEADS * HEAD_SIZE
    key_total_width = KEY_VALUE_HEADS * HEAD_SIZE
    heads_stack, output_stack, expand_stack, down_stack = gather_weights(
        grid,
        [
            heads_weight.astype(jnp.bfloat16).T,
            output_weight.astype(jnp.bfloat16).T,
            expand_weight.astype(jnp.bfloat16),
            down_weight.astype(jnp.bfloat16).T,
        ],
        Z_MAJOR,
        1,
    )
    heads_half = heads_stack.transpose(0, 3, 1, 2).reshape(-1, heads_weight.shape[1] * grid.nd)
    output_half = output_stack.transpose(0, 3, 1, 2).reshape(-1, output_weight.shape[1] * grid.nd)
    expand_half = expand_stack.transpose(1, 2, 0, 3).reshape(-1, expand_weight.shape[1] * grid.nd)
    down_half = down_stack.transpose(0, 3, 1, 2).reshape(-1, down_weight.shape[1] * grid.nd)
    first_row = lax.axis_index("shard") * count_of_rows
    positions = first_row + jnp.arange(count_of_rows, dtype=jnp.int32)
    cosine_table, sine_table = rotary_tables(positions - doc_start)
    seg_row = seg_ids[0]
    seg_query = lax.dynamic_slice_in_dim(seg_row, first_row, count_of_rows)
    key_places = jnp.arange(seg_row.shape[0], dtype=jnp.int32)
    allowed = (seg_query[:, None] == seg_row[None, :]) & (key_places[None, :] <= positions[:, None])
    gain_one = norm_gains[0]
    gain_two = norm_gains[1]
    inputs = hidden_in.astype(jnp.float32)
    normed_one, inverse_one, hidden_one = rms_forward(inputs, gain_one)
    projected_rows = jnp.dot(hidden_one, heads_half, preferred_element_type=jnp.float32)
    queries = apply_rotary(
        projected_rows[:, :query_total_width].reshape(count_of_rows, QUERY_HEADS, HEAD_SIZE),
        cosine_table,
        sine_table,
    ).astype(jnp.bfloat16)
    key_rotated = apply_rotary(
        projected_rows[:, query_total_width : query_total_width + key_total_width].reshape(
            count_of_rows, KEY_VALUE_HEADS, HEAD_SIZE
        ),
        cosine_table,
        sine_table,
    ).astype(jnp.bfloat16)
    values = projected_rows[:, query_total_width + key_total_width :].astype(jnp.bfloat16)
    packed = jnp.concatenate([key_rotated.reshape(count_of_rows, key_total_width), values], axis=1)
    all_keys = lax.all_gather(packed, "shard", axis=0, tiled=True)
    attended, logsums = attend_forward(queries, all_keys, allowed)
    attended_half = attended.astype(jnp.bfloat16)
    attended_flat = attended_half.reshape(count_of_rows, query_total_width)
    residual = inputs + jnp.dot(attended_flat, output_half, preferred_element_type=jnp.float32)
    normed_two, inverse_two, hidden_two = rms_forward(residual, gain_two)
    gate_up = jnp.dot(hidden_two, expand_half, preferred_element_type=jnp.float32)
    gate_part = gate_up[:, :FF]
    up_part = gate_up[:, FF:]
    sigmoid_gate = jax.nn.sigmoid(gate_part)
    silu_gate = gate_part * sigmoid_gate
    mixed_act = (silu_gate * up_part).astype(jnp.bfloat16)
    hidden_out = (
        residual + jnp.dot(mixed_act, down_half, preferred_element_type=jnp.float32)
    ).astype(jnp.bfloat16)
    upstream = out_grad.astype(jnp.float32)
    mixed_grad = times_transposed(out_grad, down_half)
    down_term = transposed_times(mixed_act, out_grad)
    gate_grad = mixed_grad * up_part * sigmoid_gate * (1.0 + gate_part * (1.0 - sigmoid_gate))
    up_grad = mixed_grad * silu_gate
    expand_delta = jnp.concatenate([gate_grad, up_grad], axis=1).astype(jnp.bfloat16)
    expand_term = transposed_times(hidden_two, expand_delta)
    hidden_two_grad = times_transposed(expand_delta, expand_half)
    residual_back, gain_two_term = rms_backward(hidden_two_grad, normed_two, inverse_two, gain_two)
    residual_grad = upstream + residual_back
    residual_delta = residual_grad.astype(jnp.bfloat16)
    output_term = transposed_times(attended_flat, residual_delta)
    attended_grad = (
        times_transposed(residual_delta, output_half)
        .astype(jnp.bfloat16)
        .reshape(count_of_rows, QUERY_HEADS, HEAD_SIZE)
    )
    query_grad, packed_terms = attend_backward(
        queries, all_keys, allowed, logsums, attended_half, attended_grad
    )
    packed_gradient = lax.psum_scatter(packed_terms, "shard", scatter_dimension=0, tiled=True)
    key_backward = reverse_rotary(
        packed_gradient[:, :key_total_width].reshape(count_of_rows, KEY_VALUE_HEADS, HEAD_SIZE),
        cosine_table,
        sine_table,
    ).reshape(count_of_rows, key_total_width)
    query_back = reverse_rotary(query_grad, cosine_table, sine_table).reshape(
        count_of_rows, query_total_width
    )
    heads_delta = jnp.concatenate(
        [query_back, key_backward, packed_gradient[:, key_total_width:]], axis=1
    ).astype(jnp.bfloat16)
    heads_term = transposed_times(hidden_one, heads_delta)
    hidden_one_grad = times_transposed(heads_delta, heads_half)
    input_back, gain_one_term = rms_backward(hidden_one_grad, normed_one, inverse_one, gain_one)
    input_grad = residual_grad + input_back
    def stacked(term, z_major):
        rows, cols = term.shape[0] // grid.nz, term.shape[1] // grid.nd
        term = term.astype(jnp.bfloat16).reshape(grid.nz, rows, grid.nd, cols)
        return term.transpose(0, 2, 3, 1) if z_major else term.transpose(2, 0, 1, 3)

    down_grad, expand_grad, output_grad, heads_grad, gains_grad = reduce_grads(
        grid,
        [stacked(down_term, True), stacked(expand_term, False), stacked(output_term, True), stacked(heads_term, True)],
        (True, False, True, True),
        jnp.stack([gain_one_term, gain_two_term], axis=0),
        2,
    )
    heads_grad, output_grad, down_grad = heads_grad.T, output_grad.T, down_grad.T
    gains_new, gains_first_new, gains_second_new = adamw(
        norm_gains, gains_grad, gains_first, gains_second, gain_rate, 0.0
    )
    heads_new, heads_first_new, heads_second_new = adamw(
        heads_weight, heads_grad, heads_first, heads_second, matrix_rate, decay_rate
    )
    output_new, output_first_new, output_second_new = adamw(
        output_weight, output_grad, output_first, output_second, output_rate, decay_rate
    )
    expand_new, expand_first_new, expand_second_new = adamw(
        expand_weight, expand_grad, expand_first, expand_second, matrix_rate, decay_rate
    )
    down_new, down_first_new, down_second_new = adamw(
        down_weight, down_grad, down_first, down_second, matrix_rate, decay_rate
    )
    return (
        hidden_out,
        input_grad,
        gains_grad,
        heads_grad,
        output_grad,
        expand_grad,
        down_grad,
        gains_new,
        heads_new,
        output_new,
        expand_new,
        down_new,
        gains_first_new,
        gains_second_new,
        heads_first_new,
        heads_second_new,
        output_first_new,
        output_second_new,
        expand_first_new,
        expand_second_new,
        down_first_new,
        down_second_new,
    )


def solution(mesh):
    return jax.shard_map(
        functools.partial(local, Grid(mesh)),
        mesh=mesh,
        in_specs=(
            P(("dp", "shard"), None),
            P(("dp", "shard"), None),
            P("dp", None),
            P(("dp", "shard")),
            P(),
            P("shard", "dp"),
            P("shard", "dp"),
            P("shard", "dp"),
            P("shard", "dp"),
            P(),
            P(),
            P("shard", "dp"),
            P("shard", "dp"),
            P("shard", "dp"),
            P("shard", "dp"),
            P("shard", "dp"),
            P("shard", "dp"),
            P("shard", "dp"),
            P("shard", "dp"),
        ),
        out_specs=(
            P(("dp", "shard"), None),
            P(("dp", "shard"), None),
            P(),
            P("shard", "dp"),
            P("shard", "dp"),
            P("shard", "dp"),
            P("shard", "dp"),
            P(),
            P("shard", "dp"),
            P("shard", "dp"),
            P("shard", "dp"),
            P("shard", "dp"),
            P(),
            P(),
            P("shard", "dp"),
            P("shard", "dp"),
            P("shard", "dp"),
            P("shard", "dp"),
            P("shard", "dp"),
            P("shard", "dp"),
            P("shard", "dp"),
            P("shard", "dp"),
        ),
        check_vma=False,
    )
```

```python
import functools
import math

import jax
import jax.numpy as jnp
from jax import lax
from jax.experimental import pallas as pl
from jax.experimental.pallas import tpu as pltpu
from jax.sharding import PartitionSpec as P

MESH = pl.DeviceIdType.MESH
ANY = pl.BlockSpec(memory_space=pl.ANY)
VMEM = pl.BlockSpec(memory_space=pltpu.VMEM)


class Grid:
    def __init__(self, mesh):
        self.nd = mesh.shape["dp"]
        self.nz = mesh.shape["shard"]
        self.nx = math.isqrt(self.nd // 2)
        self.ny = self.nd // 2 // self.nx
        assert self.nx == self.ny and self.nx * self.ny * 2 == self.nd

    def dp(self, y, x, c):
        return (y * self.nx + x) * 2 + c


class Here:
    def __init__(self, grid):
        self.grid = grid
        d = lax.axis_index("dp")
        self.z = lax.axis_index("shard")
        self.d = d
        self.c = lax.rem(d, 2)
        self.x = lax.rem(d // 2, grid.nx)
        self.y = d // (2 * grid.nx)
        g = grid
        self.xs = [lax.rem(self.x + k, g.nx) for k in range(1, g.nx)]
        self.ys = [lax.rem(self.y + k, g.ny) for k in range(1, g.ny)]
        self.zs = [lax.rem(self.z + k, g.nz) for k in range(1, g.nz)]
        self.partner = (g.dp(self.y, self.x, 1 - self.c), self.z)

    def on_x(self, x):
        return (self.grid.dp(self.y, x, self.c), self.z)

    def on_y(self, y):
        return (self.grid.dp(y, self.x, self.c), self.z)

    def on_z(self, z):
        return (self.d, z)

    def peers(self):
        return (
            [self.partner]
            + [self.on_x(x) for x in self.xs]
            + [self.on_y(y) for y in self.ys]
            + [self.on_z(z) for z in self.zs]
        )


def greet(peers):
    barrier = pltpu.get_barrier_semaphore()
    for peer in peers:
        pl.semaphore_signal(barrier, inc=1, device_id=peer, device_id_type=MESH)
    pl.semaphore_wait(barrier, len(peers))


def send(src, dst, send_sem, recv_sem, device):
    pltpu.make_async_remote_copy(
        src_ref=src,
        dst_ref=dst,
        send_sem=send_sem,
        recv_sem=recv_sem,
        device_id=device,
        device_id_type=MESH,
    ).start()


def wait_bytes(ref, sem):
    pltpu.make_async_copy(ref, ref, sem).wait()


def half_rows(rows):
    return max(16, int(rows / 32 + 0.5) * 16)


class Gather:
    def __init__(self, here, shard, out, sems, z_major):
        self.h, self.shard, self.out, self.sems, self.z_major = here, shard, out, sems, z_major
        self.rows = shard.shape[0]
        self.cut = half_rows(self.rows)

    def column(self, d, half=None):
        rows = {None: slice(None), 0: pl.ds(0, self.cut), 1: pl.ds(self.cut, self.rows - self.cut)}[half]
        if self.z_major:
            return self.out.at[:, d, rows]
        return self.out.at[d, :, rows]

    def block(self, d, z):
        return self.out.at[z, d] if self.z_major else self.out.at[d, z]

    def columns(self, count):
        return self.out.at[:, pl.ds(0, count)] if self.z_major else self.out.at[pl.ds(0, count)]

    def blocks(self, count):
        return self.out.at[pl.ds(0, count), 0] if self.z_major else self.out.at[0, pl.ds(0, count)]

    def stage_z(self):
        h, s = self.h, self.sems
        for z in h.zs:
            send(self.shard, self.block(h.d, h.z), s.at[0], s.at[1], h.on_z(z))
        self.own = pltpu.make_async_copy(self.shard, self.block(h.d, h.z), s.at[8])
        self.own.start()

    def stage_one(self):
        h, s = self.h, self.sems
        wait_bytes(self.blocks(len(h.zs)), s.at[1])
        self.own.wait()
        for x in h.xs:
            send(self.column(h.d, 0), self.column(h.d, 0), s.at[2], s.at[3], h.on_x(x))
        for y in h.ys:
            send(self.column(h.d, 1), self.column(h.d, 1), s.at[2], s.at[3], h.on_y(y))
        send(self.column(h.d), self.column(h.d), s.at[6], s.at[7], h.partner)

    def stage_two(self):
        h, s, g = self.h, self.sems, self.h.grid
        wait_bytes(self.columns(len(h.xs)), s.at[3])
        for y in h.ys:
            for x in [h.x] + h.xs:
                col = self.column(g.dp(h.y, x, h.c), 0)
                send(col, col, s.at[4], s.at[5], h.on_y(y))
        for x in h.xs:
            for y in [h.y] + h.ys:
                col = self.column(g.dp(y, h.x, h.c), 1)
                send(col, col, s.at[4], s.at[5], h.on_x(x))
        for x in h.xs:
            col = self.column(g.dp(h.y, x, h.c), 0)
            send(col, col, s.at[6], s.at[7], h.partner)
        for y in h.ys:
            col = self.column(g.dp(y, h.x, h.c), 1)
            send(col, col, s.at[6], s.at[7], h.partner)

    def stage_three(self):
        h, s, g = self.h, self.sems, self.h.grid
        wait_bytes(self.columns(g.nx * len(h.ys)), s.at[5])
        for y in h.ys:
            for x in [h.x] + h.xs:
                col = self.column(g.dp(y, x, h.c), 0)
                send(col, col, s.at[6], s.at[7], h.partner)
        for x in h.xs:
            for y in [h.y] + h.ys:
                col = self.column(g.dp(y, x, h.c), 1)
                send(col, col, s.at[6], s.at[7], h.partner)

    def arrive(self):
        g = self.h.grid
        wait_bytes(self.columns(g.nd // 2), self.sems.at[7])

    def drain(self):
        h, s, g = self.h, self.sems, self.h.grid
        wait_bytes(self.blocks(len(h.zs)), s.at[0])
        wait_bytes(self.columns(len(h.xs)), s.at[2])
        wait_bytes(self.columns(g.nx * len(h.ys)), s.at[4])
        wait_bytes(self.columns(g.nd // 2), s.at[6])


GATHER_SEMS = 9


def gather_kernel(grid, z_majors, *refs):
    n = len(z_majors)
    shards, outs, sems = refs[:n], refs[n : 2 * n], refs[2 * n]
    here = Here(grid)
    greet(here.peers())
    jobs = [Gather(here, shards[i], outs[i], sems.at[i], z_majors[i]) for i in range(n)]
    for job in jobs:
        job.stage_z()
    for step in range(n + 2):
        if step < n:
            jobs[step].stage_one()
        if 0 <= step - 1 < n:
            jobs[step - 1].stage_two()
        if 0 <= step - 2 < n:
            jobs[step - 2].stage_three()
    for job in jobs:
        job.arrive()
        job.drain()


def gather_weights(grid, shards, z_majors, collective_id):
    shapes = []
    for shard, z_major in zip(shards, z_majors):
        lead = (grid.nz, grid.nd) if z_major else (grid.nd, grid.nz)
        shapes.append(jax.ShapeDtypeStruct(lead + shard.shape, shard.dtype))
    return pl.pallas_call(
        functools.partial(gather_kernel, grid, tuple(z_majors)),
        out_shape=shapes,
        in_specs=[VMEM] * len(shards),
        out_specs=[ANY] * len(shards),
        scratch_shapes=[pltpu.SemaphoreType.DMA((len(shards), GATHER_SEMS))],
        compiler_params=pltpu.CompilerParams(collective_id=collective_id, has_side_effects=True),
        name="gather_weights",
    )(*shards)


class Reduce:
    def __init__(self, here, terms, result, bufs, sems, z_major):
        self.h, self.terms, self.result, self.sems, self.z_major = here, terms, result, sems, z_major
        self.own, self.other, self.one_a, self.one_b, self.two_a, self.two_b, self.last = bufs
        self.rows = self.own.shape[-2]
        self.cut = half_rows(self.rows)

    @staticmethod
    def scratch(grid, rows, cols, z_major):
        cut = half_rows(rows)
        ny, nx, nz = grid.ny, grid.nx, grid.nz
        full = (nz, ny, nx) if z_major else (ny, nx, nz)
        row = (nz, nx) if z_major else (nx, nz)
        bf = jnp.bfloat16
        return [
            pltpu.VMEM(full + (rows, cols), bf),
            pltpu.VMEM(full + (rows, cols), bf),
            pltpu.VMEM((ny,) + row + (cut, cols), bf),
            pltpu.VMEM((nx,) + row + (rows - cut, cols), bf),
            pltpu.VMEM((nx, nz, cut, cols), bf),
            pltpu.VMEM((ny, nz, rows - cut, cols), bf),
            pltpu.VMEM((nz, rows, cols), bf),
        ]

    def span(self, half):
        return {None: slice(None), 0: pl.ds(0, self.cut), 1: pl.ds(self.cut, self.rows - self.cut)}[half]

    def at(self, y, x, z, half):
        y, x, z = (slice(None) if v is None else v for v in (y, x, z))
        return (z, y, x, self.span(half)) if self.z_major else (y, x, z, self.span(half))

    def side(self, c):
        return self.terms.at[:, :, :, c] if self.z_major else self.terms.at[:, :, c]

    def stage_core(self):
        h, s = self.h, self.sems
        send(self.side(1 - h.c), self.other, s.at[0], s.at[1], h.partner)
        self.load = pltpu.make_async_copy(self.side(h.c), self.own, s.at[8])
        self.load.start()

    def add_loop(self, shape, body):
        total = math.prod(shape)

        def step(i, carry):
            place = []
            rest = i
            for size in reversed(shape):
                place.append(lax.rem(rest, size))
                rest = rest // size
            body(tuple(reversed(place)))
            return carry

        lax.fori_loop(0, total, step, 0)

    def stage_one(self):
        h, s, g = self.h, self.sems, self.h.grid
        self.load.wait()
        wait_bytes(self.other, s.at[1])

        def body(place):
            total = self.own[place].astype(jnp.float32) + self.other[place].astype(jnp.float32)
            self.own[place] = total.astype(jnp.bfloat16)

        self.add_loop(self.own.shape[:3], body)
        for y in h.ys:
            send(self.own.at[self.at(y, None, None, 0)], self.one_a.at[h.y], s.at[2], s.at[3], h.on_y(y))
        for x in h.xs:
            send(self.own.at[self.at(None, x, None, 1)], self.one_b.at[h.x], s.at[9], s.at[10], h.on_x(x))

    def stage_two(self):
        h, s, g = self.h, self.sems, self.h.grid
        wait_bytes(self.one_a.at[pl.ds(0, g.ny - 1)], s.at[3])
        wait_bytes(self.one_b.at[pl.ds(0, g.nx - 1)], s.at[10])

        def body_a(place):
            where = (place[1], place[0]) if self.z_major else place
            spot = self.at(h.y, where[0], where[1], 0)
            total = self.own[spot].astype(jnp.float32)
            for y in h.ys:
                total += self.one_a[(y,) + place].astype(jnp.float32)
            self.own[spot] = total.astype(jnp.bfloat16)

        self.add_loop(self.one_a.shape[1:3], body_a)

        def body_b(place):
            where = (place[1], place[0]) if self.z_major else place
            spot = self.at(where[0], h.x, where[1], 1)
            total = self.own[spot].astype(jnp.float32)
            for x in h.xs:
                total += self.one_b[(x,) + place].astype(jnp.float32)
            self.own[spot] = total.astype(jnp.bfloat16)

        self.add_loop(self.one_b.shape[1:3], body_b)
        for x in h.xs:
            send(self.own.at[self.at(h.y, x, None, 0)], self.two_a.at[h.x], s.at[4], s.at[5], h.on_x(x))
        for y in h.ys:
            send(self.own.at[self.at(y, h.x, None, 1)], self.two_b.at[h.y], s.at[11], s.at[12], h.on_y(y))

    def stage_three(self):
        h, s, g = self.h, self.sems, self.h.grid
        wait_bytes(self.two_a.at[pl.ds(0, g.nx - 1)], s.at[5])
        wait_bytes(self.two_b.at[pl.ds(0, g.ny - 1)], s.at[12])

        def body(place):
            (z,) = place
            spot = self.at(h.y, h.x, z, 0)
            total = self.own[spot].astype(jnp.float32)
            for x in h.xs:
                total += self.two_a[x, z].astype(jnp.float32)
            self.own[spot] = total.astype(jnp.bfloat16)
            spot = self.at(h.y, h.x, z, 1)
            total = self.own[spot].astype(jnp.float32)
            for y in h.ys:
                total += self.two_b[y, z].astype(jnp.float32)
            self.own[spot] = total.astype(jnp.bfloat16)

        self.add_loop((g.nz,), body)
        for z in h.zs:
            send(self.own.at[self.at(h.y, h.x, z, None)], self.last.at[h.z], s.at[6], s.at[7], h.on_z(z))

    def finish(self):
        h, s, g = self.h, self.sems, self.h.grid
        wait_bytes(self.last.at[pl.ds(0, g.nz - 1)], s.at[7])
        total = self.own[self.at(h.y, h.x, h.z, None)].astype(jnp.float32)
        for z in h.zs:
            total += self.last[z].astype(jnp.float32)
        self.result[...] = total

    def drain(self):
        g, s = self.h.grid, self.sems
        wait_bytes(self.other, s.at[0])
        wait_bytes(self.one_a.at[pl.ds(0, g.ny - 1)], s.at[2])
        wait_bytes(self.one_b.at[pl.ds(0, g.nx - 1)], s.at[9])
        wait_bytes(self.two_a.at[pl.ds(0, g.nx - 1)], s.at[4])
        wait_bytes(self.two_b.at[pl.ds(0, g.ny - 1)], s.at[11])
        wait_bytes(self.last.at[pl.ds(0, g.nz - 1)], s.at[6])


REDUCE_SEMS = 13
REDUCE_BUFS = 7


class Share:
    def __init__(self, here, value, result, bufs, sems):
        self.h, self.value, self.result, self.sems = here, value, result, sems
        self.bufs = bufs

    @staticmethod
    def scratch(grid, shape):
        return [pltpu.VMEM((n,) + shape, jnp.float32) for n in (2, grid.nx, grid.ny, grid.nz)]

    def axis(self, k):
        h = self.h
        return (
            (h.c, [h.partner], 2),
            (h.x, [h.on_x(x) for x in h.xs], h.grid.nx),
            (h.y, [h.on_y(y) for y in h.ys], h.grid.ny),
            (h.z, [h.on_z(z) for z in h.zs], h.grid.nz),
        )[k]

    def start(self, k):
        me, peers, n = self.axis(k)
        self.bufs[k][me] = self.value[...] if k == 0 else self.total
        for peer in peers:
            send(self.bufs[k].at[me], self.bufs[k].at[me], self.sems.at[2 * k], self.sems.at[2 * k + 1], peer)

    def end(self, k):
        me, peers, n = self.axis(k)
        wait_bytes(self.bufs[k].at[pl.ds(0, n - 1)], self.sems.at[2 * k + 1])
        total = self.bufs[k][0]
        for i in range(1, n):
            total = total + self.bufs[k][i]
        self.total = total
        if k == 3:
            self.result[...] = total

    def drain(self):
        for k in range(4):
            n = self.axis(k)[2]
            wait_bytes(self.bufs[k].at[pl.ds(0, n - 1)], self.sems.at[2 * k])


SHARE_SEMS = 8


def reduce_kernel(grid, z_majors, shared, *refs):
    n = len(z_majors)
    terms, refs = refs[:n], refs[n:]
    value, refs = (refs[0], refs[1:]) if shared else (None, refs)
    results, refs = refs[:n], refs[n:]
    value_sum, refs = (refs[0], refs[1:]) if shared else (None, refs)
    here = Here(grid)
    greet(here.peers())
    jobs = []
    for i in range(n):
        bufs, refs = refs[:REDUCE_BUFS], refs[REDUCE_BUFS:]
        jobs.append((bufs, i))
    sems, refs = refs[0], refs[1:]
    jobs = [Reduce(here, terms[i], results[i], bufs, sems.at[i], z_majors[i]) for bufs, i in jobs]
    share = None
    if shared:
        share = Share(here, value, value_sum, refs[:4], refs[4])
        share.start(0)
    for job in jobs:
        job.stage_core()
    for step in range(n + 3):
        if step < n:
            jobs[step].stage_one()
        if 0 <= step - 1 < n:
            jobs[step - 1].stage_two()
        if 0 <= step - 2 < n:
            jobs[step - 2].stage_three()
        if 0 <= step - 3 < n:
            jobs[step - 3].finish()
        if share is not None and step < 4:
            share.end(step)
            if step < 3:
                share.start(step + 1)
    if share is not None:
        for step in range(n + 3, 4):
            share.end(step)
            if step < 3:
                share.start(step + 1)
        share.drain()
    for job in jobs:
        job.drain()


def reduce_grads(grid, terms, z_majors, value, collective_id):
    split, shapes, scratch = [], [], []
    for term, z_major in zip(terms, z_majors):
        rows, cols = term.shape[-2:]
        lead = (grid.ny, grid.nx, 2)
        lead = (grid.nz,) + lead if z_major else lead + (grid.nz,)
        split.append(term.reshape(lead + (rows, cols)))
        shapes.append(jax.ShapeDtypeStruct((rows, cols), jnp.float32))
        scratch += Reduce.scratch(grid, rows, cols, z_major)
    n = len(terms)
    scratch.append(pltpu.SemaphoreType.DMA((n, REDUCE_SEMS)))
    shared = value is not None
    if shared:
        shapes.append(jax.ShapeDtypeStruct(value.shape, jnp.float32))
        scratch += Share.scratch(grid, value.shape)
        scratch.append(pltpu.SemaphoreType.DMA((SHARE_SEMS,)))
    return pl.pallas_call(
        functools.partial(reduce_kernel, grid, tuple(z_majors), shared),
        out_shape=shapes,
        in_specs=[ANY] * n + [VMEM] * shared,
        out_specs=[VMEM] * len(shapes),
        scratch_shapes=scratch,
        compiler_params=pltpu.CompilerParams(
            collective_id=collective_id, has_side_effects=True, vmem_limit_bytes=62 << 20
        ),
        name="reduce_grads",
    )(*split, *([value] if shared else []))


D = 960
QUERY_HEADS = 15
KEY_VALUE_HEADS = 5
GROUP = QUERY_HEADS // KEY_VALUE_HEADS
HEAD = 64
FF = 2560
QKV = (QUERY_HEADS + 2 * KEY_VALUE_HEADS) * HEAD
ADAM_STEP = 10
DOCS = 16
HIDE = -1e30
VALUE_SCALE = 2.0**-9

norm_epsilon = 1e-05
beta_one = 0.9
beta_two = 0.95
adam_epsilon = 1e-08
matrix_rate = 0.03
output_rate = 0.15
gain_rate = 0.5
decay_rate = 0.1

f32 = jnp.float32
bf16 = jnp.bfloat16
DEPTH = 4
SLICE = D // DEPTH


def mm(a, b):
    return lax.dot_general(a, b, (((1,), (0,)), ((), ())), preferred_element_type=f32)


def mm_nt(a, b):
    return lax.dot_general(a, b, (((1,), (1,)), ((), ())), preferred_element_type=f32)


def mm_tn(a, b):
    return lax.dot_general(a, b, (((0,), (0,)), ((), ())), preferred_element_type=f32)


def lanes_below(shape, n):
    return lax.broadcasted_iota(jnp.int32, shape, len(shape) - 1) < n


def inverse_rms(ref):
    total = jnp.zeros((1, ref.shape[1]), f32)
    for k in range(DEPTH):
        x = ref[pl.ds(k * SLICE, SLICE)].astype(f32)
        total += jnp.sum(x * x, axis=0, keepdims=True)
    return lax.rsqrt(total * (1.0 / D) + norm_epsilon)


def three_pieces(row):
    hi = row.astype(bf16).astype(f32)
    mid = (row - hi).astype(bf16).astype(f32)
    low = row - hi - mid
    place = lax.broadcasted_iota(jnp.int32, (16, row.shape[1]), 0)
    block = jnp.where(place == 0, hi, jnp.where(place == 1, mid, jnp.where(place == 2, low, 0.0)))
    return block.astype(bf16)


class KeyChain:
    def __init__(self, here, kv, sems):
        self.h, self.kv, self.sems = here, kv, sems

    def up(self, slot):
        h = self.h
        to = lax.rem(h.z + 1, h.grid.nz)

        @pl.when(h.z < h.grid.nz - 1)
        def _():
            send(self.kv.at[slot], self.kv.at[slot], self.sems.at[0, slot], self.sems.at[1, slot], h.on_z(to))

    def take(self, slot):
        wait_bytes(self.kv.at[slot], self.sems.at[1, slot])
        self.up(slot)

    def drain(self):
        h = self.h
        for s in range(h.grid.nz):

            @pl.when(jnp.logical_and(h.z >= s, h.z < h.grid.nz - 1))
            def _():
                wait_bytes(self.kv.at[h.z - s], self.sems.at[0, h.z - s])


def front_kernel(grid, z_majors, *refs):
    n = len(z_majors)
    shards, refs = refs[:n], refs[n:]
    heads, x, gain, cos, sin, qext, kext = refs[:7]
    refs = refs[7:]
    outs, refs = refs[:n], refs[n:]
    qx, kv, att, lse = refs[:4]
    h1, proj, kx, vt, acc, sems, kv_sems = refs[4:]
    here = Here(grid)
    tokens = x.shape[1]
    half = tokens // 2
    greet(here.peers())
    jobs = [Gather(here, shards[i], outs[i], sems.at[i], z_majors[i]) for i in range(n)]
    for job in jobs[:-1]:
        job.stage_z()

    inverse = inverse_rms(x)
    for k in range(DEPTH):
        rows = pl.ds(k * SLICE, SLICE)
        h1[rows] = (x[rows].astype(f32) * inverse * gain[rows]).astype(bf16)

    part = QKV // 5

    def project(m, carry):
        rows = pl.ds(pl.multiple_of(m * part, 16), part)
        total = mm(heads[0, rows], h1[pl.ds(0, SLICE)])
        for k in range(1, DEPTH):
            total += mm(heads[k, rows], h1[pl.ds(k * SLICE, SLICE)])
        proj[rows] = total
        return carry

    lax.fori_loop(0, 5, project, 0)

    def turned(h):
        base = h * HEAD
        a = proj[pl.ds(pl.multiple_of(base, 8), HEAD // 2)]
        b = proj[pl.ds(pl.multiple_of(base + HEAD // 2, 8), HEAD // 2)]
        c, s = cos[...], sin[...]
        return a * c - b * s, b * c + a * s

    def keys(g, carry):
        a, b = turned(QUERY_HEADS + g)
        v = proj[pl.ds(pl.multiple_of((QUERY_HEADS + KEY_VALUE_HEADS + g) * HEAD, 8), HEAD)]
        both = jnp.concatenate([a, b, v], axis=0)
        kv[here.z, g] = both.T.astype(bf16)
        return carry

    lax.fori_loop(0, KEY_VALUE_HEADS, keys, 0)
    chain = KeyChain(here, kv, kv_sems)
    chain.up(here.z)
    jobs[-1].stage_z()

    def queries(h, carry):
        a, b = turned(h)
        scale = HEAD**-0.5
        qx[h, pl.ds(0, 32)] = (a.astype(bf16).astype(f32) * scale).astype(bf16)
        qx[h, pl.ds(32, 32)] = (b.astype(bf16).astype(f32) * scale).astype(bf16)
        qx[h, pl.ds(64, 64)] = qext[...]
        return carry

    lax.fori_loop(0, QUERY_HEADS, queries, 0)

    def prepare(slot):
        ext = kext[pl.ds(pl.multiple_of(slot * tokens, 16), tokens)]

        def body(g, carry):
            block = kv[slot, g]
            kx[g] = jnp.where(lanes_below(block.shape, HEAD), block, ext)
            turned_block = block.astype(f32).T
            vt[g, pl.ds(0, 16)] = jnp.ones((16, tokens), bf16)
            vt[g, pl.ds(16, HEAD)] = (turned_block[HEAD:] * VALUE_SCALE).astype(bf16)
            return carry

        lax.fori_loop(0, KEY_VALUE_HEADS, body, 0)

    def below(key, query):
        row = lax.broadcasted_iota(jnp.int32, (half, half), 0)
        col = lax.broadcasted_iota(jnp.int32, (half, half), 1)
        return row <= col

    def diagonal():
        prepare(here.z)

        def body(g, carry):
            for i in range(GROUP):
                h = g * GROUP + i
                mask = below(0, 0)
                s = mm(kx[g, pl.ds(0, half)], qx[h])
                low = jnp.exp(jnp.where(mask, s[:, :half], HIDE)).astype(bf16)
                high = jnp.exp(s[:, half:]).astype(bf16)
                acc[h, :, pl.ds(0, half)] = mm(vt[g, :, pl.ds(0, half)], low)
                total = mm(vt[g, :, pl.ds(0, half)], high)
                s = mm(kx[g, pl.ds(half, half)], qx[h, :, pl.ds(half, half)])
                p = jnp.exp(jnp.where(mask, s, HIDE)).astype(bf16)
                acc[h, :, pl.ds(half, half)] = total + mm(vt[g, :, pl.ds(half, half)], p)
            return carry

        lax.fori_loop(0, KEY_VALUE_HEADS, body, 0)

    def whole(slot):
        prepare(slot)

        def body(g, carry):
            for i in range(GROUP):
                h = g * GROUP + i
                total = acc[h]
                for k in range(2):
                    s = mm(kx[g, pl.ds(k * half, half)], qx[h])
                    total += mm(vt[g, :, pl.ds(k * half, half)], jnp.exp(s).astype(bf16))
                acc[h] = total
            return carry

        lax.fori_loop(0, KEY_VALUE_HEADS, body, 0)

    def earlier(s):
        @pl.when(here.z >= s)
        def _():
            chain.take(here.z - s)
            whole(here.z - s)

    ticks = []
    for step in range(n + 2):
        if step < n:
            ticks.append(jobs[step].stage_one)
        if 0 <= step - 1 < n:
            ticks.append(jobs[step - 1].stage_two)
        if 0 <= step - 2 < n:
            ticks.append(jobs[step - 2].stage_three)
    diagonal()
    steps = grid.nz - 1
    share = -(-len(ticks) // (steps + 1))
    for s in range(1, grid.nz):
        for tick in ticks[(s - 1) * share : s * share]:
            tick()
        earlier(s)
    for tick in ticks[steps * share :]:
        tick()

    def close(h, carry):
        totals = acc[h, pl.ds(0, 1)]
        scale = (1.0 / VALUE_SCALE) / totals
        att[pl.ds(pl.multiple_of(h * HEAD, 16), HEAD)] = (acc[h, pl.ds(16, HEAD)] * scale).astype(bf16)
        lse[h] = jnp.log(totals)
        return carry

    lax.fori_loop(0, QUERY_HEADS, close, 0)
    for job in jobs:
        job.arrive()
        job.drain()
    chain.drain()


def front(grid, shards, z_majors, heads, x, gain, cos, sin, qext, kext, collective_id):
    tokens = x.shape[1]
    shapes = []
    for shard, z_major in zip(shards, z_majors):
        lead = (grid.nz, grid.nd) if z_major else (grid.nd, grid.nz)
        shapes.append(jax.ShapeDtypeStruct(lead + shard.shape, shard.dtype))
    n = len(shards)
    shapes += [
        jax.ShapeDtypeStruct((QUERY_HEADS, 128, tokens), bf16),
        jax.ShapeDtypeStruct((grid.nz, KEY_VALUE_HEADS, tokens, 128), bf16),
        jax.ShapeDtypeStruct((D, tokens), bf16),
        jax.ShapeDtypeStruct((QUERY_HEADS, 1, tokens), f32),
    ]
    return pl.pallas_call(
        functools.partial(front_kernel, grid, tuple(z_majors)),
        out_shape=shapes,
        in_specs=[VMEM] * (n + 7),
        out_specs=[ANY] * n + [VMEM] * 4,
        scratch_shapes=[
            pltpu.VMEM((D, tokens), bf16),
            pltpu.VMEM((QKV, tokens), f32),
            pltpu.VMEM((KEY_VALUE_HEADS, tokens, 128), bf16),
            pltpu.VMEM((KEY_VALUE_HEADS, 80, tokens), bf16),
            pltpu.VMEM((QUERY_HEADS, 80, tokens), f32),
            pltpu.SemaphoreType.DMA((n, GATHER_SEMS)),
            pltpu.SemaphoreType.DMA((2, grid.nz)),
        ],
        compiler_params=pltpu.CompilerParams(
            collective_id=collective_id, has_side_effects=True, vmem_limit_bytes=60 << 20
        ),
        name="front",
    )(*shards, heads, x, gain, cos, sin, qext, kext)


def middle_kernel(blocks, att, wo, x, ogt, gain, eg, eu, dn, out, rg, gsum, dexp, ddn, dwo, dot, delta,
                  res, inv, h2, h2t, og, acc_o, acc_h, mixed, dgate, dup):
    f = pl.program_id(0)
    tokens = x.shape[1]
    half = tokens // 2

    @pl.when(f == 0)
    def _():
        total = jnp.zeros((1, tokens), f32)
        for m in range(DEPTH):
            rows = pl.ds(m * SLICE, SLICE)
            r = x[rows].astype(f32)
            for k in range(DEPTH):
                r += mm(wo[k, rows], att[pl.ds(k * SLICE, SLICE)])
            res[rows] = r
            total += jnp.sum(r * r, axis=0, keepdims=True)
        inverse = lax.rsqrt(total * (1.0 / D) + norm_epsilon)
        inv[...] = inverse
        for m in range(DEPTH):
            rows = pl.ds(m * SLICE, SLICE)
            h2t[rows] = (res[rows] * inverse * gain[rows]).astype(bf16)
        h2[...] = h2t[...].astype(f32).T.astype(bf16)
        og[...] = ogt[...].astype(f32).T.astype(bf16)
        acc_o[...] = jnp.zeros_like(acc_o)
        acc_h[...] = jnp.zeros_like(acc_h)

    def activate(i, carry):
        rows = pl.ds(pl.multiple_of(i * 128, 128), 128)
        gate = mm(h2[rows], eg[...])
        up = mm(h2[rows], eu[...])
        back = mm(og[rows], dn[...])
        s = 1.0 / (1.0 + jnp.exp(-gate))
        silu = gate * s
        mixed[rows] = (silu * up).astype(bf16)
        dgate[rows] = (back * up * s * (1.0 + gate * (1.0 - s))).astype(bf16)
        dup[rows] = (back * silu).astype(bf16)
        return carry

    lax.fori_loop(0, tokens // 128, activate, 0)
    for m in range(DEPTH):
        rows = pl.ds(m * SLICE, SLICE)
        acc_o[rows] += mm_nt(dn[rows], mixed[...])
        acc_h[rows] += mm_nt(eg[rows], dgate[...]) + mm_nt(eu[rows], dup[...])
        dexp[0, rows] = mm(h2t[rows], dgate[...]).astype(bf16)
        dexp[1, rows] = mm(h2t[rows], dup[...]).astype(bf16)
        ddn[rows] = mm(ogt[rows], mixed[...]).astype(bf16)

    @pl.when(f == blocks - 1)
    def _():
        inverse = inv[...]
        total = jnp.zeros((1, tokens), f32)
        for m in range(DEPTH):
            rows = pl.ds(m * SLICE, SLICE)
            out[rows] = (res[rows] + acc_o[rows]).astype(bf16)
            normed = res[rows] * inverse
            up = acc_h[rows]
            gsum[rows] = jnp.sum(up * normed, axis=1, keepdims=True)
            total += jnp.sum(up * gain[rows] * normed, axis=0, keepdims=True)
        mean = total * (1.0 / D)
        for m in range(DEPTH):
            rows = pl.ds(m * SLICE, SLICE)
            normed = res[rows] * inverse
            r = ogt[rows].astype(f32) + inverse * (acc_h[rows] * gain[rows] - normed * mean)
            rg[rows] = r
            h2t[rows] = r.astype(bf16)
        for k in range(DEPTH):
            rows = pl.ds(k * SLICE, SLICE)
            dwo[k] = mm_nt(h2t[...], att[rows]).astype(bf16)
            dot[rows] = mm_tn(wo[k], h2t[...]).astype(bf16)

        def rows_of(h, carry):
            rows = pl.ds(pl.multiple_of(h * HEAD, 16), HEAD)
            delta[h] = jnp.sum(dot[rows].astype(f32) * att[rows].astype(f32), axis=0, keepdims=True)
            return carry

        lax.fori_loop(0, QUERY_HEADS, rows_of, 0)


def middle(att, wo, x, ogt, gain, expand, down):
    tokens = x.shape[1]
    blocks, _, width = down.shape
    full = pl.BlockSpec(memory_space=pltpu.VMEM)

    def spec(offset):
        return pl.BlockSpec((None, D, width), lambda f: (f + offset, 0, 0))

    return pl.pallas_call(
        functools.partial(middle_kernel, blocks),
        grid=(blocks,),
        out_shape=[
            jax.ShapeDtypeStruct((D, tokens), bf16),
            jax.ShapeDtypeStruct((D, tokens), f32),
            jax.ShapeDtypeStruct((D, 1), f32),
            jax.ShapeDtypeStruct((2, blocks, D, width), bf16),
            jax.ShapeDtypeStruct((blocks, D, width), bf16),
            jax.ShapeDtypeStruct((DEPTH, D, SLICE), bf16),
            jax.ShapeDtypeStruct((D, tokens), bf16),
            jax.ShapeDtypeStruct((QUERY_HEADS, 1, tokens), f32),
        ],
        in_specs=[full] * 5 + [spec(0), spec(blocks), spec(0)],
        out_specs=[
            full,
            full,
            full,
            pl.BlockSpec((2, None, D, width), lambda f: (0, f, 0, 0)),
            spec(0),
            full,
            full,
            full,
        ],
        scratch_shapes=[
            pltpu.VMEM((D, tokens), f32),
            pltpu.VMEM((1, tokens), f32),
            pltpu.VMEM((tokens, D), bf16),
            pltpu.VMEM((D, tokens), bf16),
            pltpu.VMEM((tokens, D), bf16),
            pltpu.VMEM((D, tokens), f32),
            pltpu.VMEM((D, tokens), f32),
            pltpu.VMEM((tokens, width), bf16),
            pltpu.VMEM((tokens, width), bf16),
            pltpu.VMEM((tokens, width), bf16),
        ],
        compiler_params=pltpu.CompilerParams(vmem_limit_bytes=62 << 20),
        name="middle",
    )(att, wo, x, ogt, gain, expand, expand, down)


class GradChain:
    def __init__(self, here, part, sent, got, sems):
        self.h, self.part, self.sent, self.got, self.sems = here, part, sent, got, sems

    def summed(self, slot, write):
        h = self.h

        @pl.when(h.z < h.grid.nz - 1)
        def _():
            wait_bytes(self.got.at[slot], self.sems.at[1, slot])

            def body(g, carry):
                write(g, self.part[slot, g] + self.got[slot, g].astype(f32))
                return carry

            lax.fori_loop(0, KEY_VALUE_HEADS, body, 0)

        @pl.when(h.z == h.grid.nz - 1)
        def _():
            def body(g, carry):
                write(g, self.part[slot, g])
                return carry

            lax.fori_loop(0, KEY_VALUE_HEADS, body, 0)

    def relay(self, slot):
        h = self.h

        @pl.when(slot < h.z)
        def _():
            def write(g, value):
                self.sent[slot, g] = value.astype(bf16)

            self.summed(slot, write)
            to = lax.rem(h.z + h.grid.nz - 1, h.grid.nz)
            send(self.sent.at[slot], self.got.at[slot], self.sems.at[0, slot], self.sems.at[1, slot], h.on_z(to))

    def drain(self):
        h = self.h
        for slot in range(h.grid.nz - 1):

            @pl.when(slot < h.z)
            def _():
                wait_bytes(self.sent.at[slot], self.sems.at[0, slot])


def back_kernel(grid, z_majors, *refs):
    n = len(z_majors)
    terms, refs = refs[:n], refs[n:]
    qx_in, lse, dot, delta, kv, kext, cos, sin = refs[:8]
    refs = refs[8:]
    results, refs = refs[:n], refs[n:]
    hd, refs = refs[0], refs[1:]
    jobs = []
    here = Here(grid)
    for i in range(n):
        jobs.append(refs[:REDUCE_BUFS])
        refs = refs[REDUCE_BUFS:]
    qx, dox, kx, vx, kt, dq, part, sent, got, sems, kv_sems = refs
    jobs = [Reduce(here, terms[i], results[i], jobs[i], sems.at[i], z_majors[i]) for i in range(n)]
    tokens = dot.shape[1]
    half = tokens // 2
    greet(here.peers())
    for job in jobs:
        job.stage_core()
    ticks = []
    for step in range(n + 3):
        if step < n:
            ticks.append(jobs[step].stage_one)
        if 0 <= step - 1 < n:
            ticks.append(jobs[step - 1].stage_two)
        if 0 <= step - 2 < n:
            ticks.append(jobs[step - 2].stage_three)
        if 0 <= step - 3 < n:
            ticks.append(jobs[step - 3].finish)

    def gather_queries(h, carry):
        qx[h, pl.ds(0, 80)] = qx_in[h, pl.ds(0, 80)]
        qx[h, pl.ds(80, 16)] = three_pieces(-lse[h])
        qx[h, pl.ds(96, 32)] = jnp.zeros((32, tokens), bf16)
        dox[h, pl.ds(0, 16)] = three_pieces(-delta[h])
        dox[h, pl.ds(16, 48)] = jnp.zeros((48, tokens), bf16)
        dox[h, pl.ds(64, 64)] = dot[pl.ds(pl.multiple_of(h * HEAD, 16), HEAD)]
        dq[h] = jnp.zeros((HEAD, tokens), f32)
        return carry

    lax.fori_loop(0, QUERY_HEADS, gather_queries, 0)

    def prepare(slot):
        ext = kext[pl.ds(pl.multiple_of(slot * tokens, 16), tokens)]

        def body(g, carry):
            block = kv[slot, g]
            low = lanes_below(block.shape, HEAD)
            kx[g] = jnp.where(low, block, ext)
            ones = jnp.where(lanes_below(block.shape, 3), 1.0, 0.0).astype(bf16)
            vx[g] = jnp.where(low, ones, block)
            kt[g] = block.astype(f32).T[:HEAD].astype(bf16)
            return carry

        lax.fori_loop(0, KEY_VALUE_HEADS, body, 0)

    def tile(g, h, k, queries, masked):
        keys = pl.ds(k * half, half)
        start, count = queries
        cols = pl.ds(start, count)
        s = mm(kx[g, keys], qx[h, :, cols])
        if masked:
            row = lax.broadcasted_iota(jnp.int32, s.shape, 0) + k * half
            col = lax.broadcasted_iota(jnp.int32, s.shape, 1) + start
            s = jnp.where(row <= col, s, HIDE)
        p = jnp.exp(s)
        ds = (p * mm(vx[g, keys], dox[h, :, cols])).astype(bf16)
        dq[h, :, cols] += mm(kt[g, :, keys], ds)
        dk = mm_nt(ds, qx[h, :, cols])
        dv = mm_nt(p.astype(bf16), dox[h, :, cols])
        return jnp.where(lanes_below(dk.shape, HEAD), dk, dv)

    def whole(slot):
        prepare(slot)

        def body(g, carry):
            for k in range(2):
                total = tile(g, g * GROUP, k, (0, tokens), False)
                for i in range(1, GROUP):
                    total += tile(g, g * GROUP + i, k, (0, tokens), False)
                part[slot, g, pl.ds(k * half, half)] = total
            return carry

        lax.fori_loop(0, KEY_VALUE_HEADS, body, 0)

    def diagonal():
        prepare(here.z)

        def body(g, carry):
            for k in range(2):
                span = (k * half, tokens - k * half)
                total = tile(g, g * GROUP, k, span, True)
                for i in range(1, GROUP):
                    total += tile(g, g * GROUP + i, k, span, True)
                part[here.z, g, pl.ds(k * half, half)] = total
            return carry

        lax.fori_loop(0, KEY_VALUE_HEADS, body, 0)

    chain = GradChain(here, part, sent, got, kv_sems)
    steps = grid.nz
    share = -(-len(ticks) // (steps + 1))
    for slot in range(grid.nz - 1):
        for tick in ticks[slot * share : (slot + 1) * share]:
            tick()

        @pl.when(slot < here.z)
        def _():
            whole(slot)

        if slot > 0:
            chain.relay(slot - 1)
    for tick in ticks[(steps - 1) * share : steps * share]:
        tick()
    diagonal()
    chain.relay(grid.nz - 2)
    for tick in ticks[steps * share :]:
        tick()

    def turn_back(a, b):
        c, s = cos[...], sin[...]
        return a * c + b * s, b * c - a * s

    def queries(h, carry):
        scale = HEAD**-0.5
        a, b = turn_back(dq[h, pl.ds(0, 32)] * scale, dq[h, pl.ds(32, 32)] * scale)
        hd[pl.ds(pl.multiple_of(h * HEAD, 16), 32)] = a.astype(bf16)
        hd[pl.ds(pl.multiple_of(h * HEAD + 32, 16), 32)] = b.astype(bf16)
        return carry

    lax.fori_loop(0, QUERY_HEADS, queries, 0)

    def write(g, value):
        turned = value.T
        a, b = turn_back(turned[:32], turned[32:64])
        base = (QUERY_HEADS + g) * HEAD
        hd[pl.ds(pl.multiple_of(base, 16), 32)] = a.astype(bf16)
        hd[pl.ds(pl.multiple_of(base + 32, 16), 32)] = b.astype(bf16)
        base = (QUERY_HEADS + KEY_VALUE_HEADS + g) * HEAD
        hd[pl.ds(pl.multiple_of(base, 16), HEAD)] = turned[64:].astype(bf16)

    chain.summed(here.z, write)
    chain.drain()
    for job in jobs:
        job.drain()


def split_terms(grid, terms, z_majors):
    split = []
    for term, z_major in zip(terms, z_majors):
        lead = (grid.ny, grid.nx, 2)
        lead = (grid.nz,) + lead if z_major else lead + (grid.nz,)
        split.append(term.reshape(lead + term.shape[-2:]))
    return split


def back(grid, terms, z_majors, qx, lse, dot, delta, kv, kext, cos, sin, collective_id):
    tokens = dot.shape[1]
    n = len(terms)
    scratch, shapes = [], []
    for term, z_major in zip(terms, z_majors):
        rows, cols = term.shape[-2:]
        shapes.append(jax.ShapeDtypeStruct((rows, cols), f32))
        scratch += Reduce.scratch(grid, rows, cols, z_major)
    shapes.append(jax.ShapeDtypeStruct((QKV, tokens), bf16))
    blocks = (grid.nz, KEY_VALUE_HEADS, tokens, 128)
    scratch += [
        pltpu.VMEM((QUERY_HEADS, 128, tokens), bf16),
        pltpu.VMEM((QUERY_HEADS, 128, tokens), bf16),
        pltpu.VMEM((KEY_VALUE_HEADS, tokens, 128), bf16),
        pltpu.VMEM((KEY_VALUE_HEADS, tokens, 128), bf16),
        pltpu.VMEM((KEY_VALUE_HEADS, HEAD, tokens), bf16),
        pltpu.VMEM((QUERY_HEADS, HEAD, tokens), f32),
        pltpu.VMEM(blocks, f32),
        pltpu.VMEM((grid.nz - 1,) + blocks[1:], bf16),
        pltpu.VMEM(blocks, bf16),
        pltpu.SemaphoreType.DMA((n, REDUCE_SEMS)),
        pltpu.SemaphoreType.DMA((2, grid.nz)),
    ]
    return pl.pallas_call(
        functools.partial(back_kernel, grid, tuple(z_majors)),
        out_shape=shapes,
        in_specs=[ANY] * n + [VMEM] * 8,
        out_specs=[VMEM] * (n + 1),
        scratch_shapes=scratch,
        compiler_params=pltpu.CompilerParams(
            collective_id=collective_id, has_side_effects=True, vmem_limit_bytes=63 << 20
        ),
        name="back",
    )(*split_terms(grid, terms, z_majors), qx, lse, dot, delta, kv, kext, cos, sin)


def ending_kernel(hd, heads, x, gain, rg, ig, gsum, dheads, h1, og, inv):
    tokens = x.shape[1]
    inverse = inverse_rms(x)
    for k in range(DEPTH):
        rows = pl.ds(k * SLICE, SLICE)
        normed = x[rows].astype(f32) * inverse
        h1[rows] = (normed * gain[rows]).astype(bf16)
    for k in range(DEPTH):
        rows = pl.ds(k * SLICE, SLICE)
        for m in range(5):
            part = pl.ds(m * (QKV // 5), QKV // 5)
            dheads[k, part] = mm_nt(hd[part], h1[rows]).astype(bf16)
        og[rows] = mm_tn(heads[k], hd[...])
    total = jnp.zeros((1, tokens), f32)
    for k in range(DEPTH):
        rows = pl.ds(k * SLICE, SLICE)
        normed = x[rows].astype(f32) * inverse
        gsum[rows] = jnp.sum(og[rows] * normed, axis=1, keepdims=True)
        total += jnp.sum(og[rows] * gain[rows] * normed, axis=0, keepdims=True)
    mean = total * (1.0 / D)
    for k in range(DEPTH):
        rows = pl.ds(k * SLICE, SLICE)
        normed = x[rows].astype(f32) * inverse
        ig[rows] = rg[rows] + inverse * (og[rows] * gain[rows] - normed * mean)


def ending(hd, heads, x, gain, rg):
    tokens = x.shape[1]
    return pl.pallas_call(
        ending_kernel,
        out_shape=[
            jax.ShapeDtypeStruct((D, tokens), f32),
            jax.ShapeDtypeStruct((D, 1), f32),
            jax.ShapeDtypeStruct((DEPTH, QKV, SLICE), bf16),
        ],
        in_specs=[VMEM] * 5,
        out_specs=[VMEM] * 3,
        scratch_shapes=[
            pltpu.VMEM((D, tokens), bf16),
            pltpu.VMEM((D, tokens), f32),
            pltpu.VMEM((1, tokens), f32),
        ],
        compiler_params=pltpu.CompilerParams(vmem_limit_bytes=60 << 20),
        name="ending",
    )(hd, heads, x, gain, rg)


def adamw(weight, grad, first, second, rate, decay):
    first_new = beta_one * first + (1.0 - beta_one) * grad
    second_new = beta_two * second + (1.0 - beta_two) * grad * grad
    first_hat = first_new / (1.0 - beta_one**ADAM_STEP)
    second_hat = second_new / (1.0 - beta_two**ADAM_STEP)
    weight_new = weight - rate * (
        first_hat / (jnp.sqrt(second_hat) + adam_epsilon) + decay * weight
    )
    return (weight_new, first_new, second_new)


EXPAND_BLOCKS = 8


def local(
    grid,
    hidden_in,
    out_grad,
    seg_ids,
    doc_start,
    norm_gains,
    heads_weight,
    output_weight,
    expand_weight,
    down_weight,
    gains_first,
    gains_second,
    heads_first,
    heads_second,
    output_first,
    output_second,
    expand_first,
    expand_second,
    down_first,
    down_second,
):
    tokens = hidden_in.shape[0]
    first_row = lax.axis_index("shard") * tokens
    positions = first_row + jnp.arange(tokens, dtype=jnp.int32)
    freq = jnp.power(10000.0, -jnp.arange(HEAD // 2).astype(f32) / (HEAD // 2))
    angle = (positions - doc_start).astype(f32)[None, :] * freq[:, None]
    cos, sin = jnp.cos(angle), jnp.sin(angle)
    seg_row = seg_ids[0]
    seg_query = lax.dynamic_slice_in_dim(seg_row, first_row, tokens)
    doc = jnp.arange(HEAD, dtype=jnp.int32)
    qext = jnp.where((doc[:, None] < DOCS) & (seg_query[None, :] == doc[:, None]), HIDE, 0.0).astype(bf16)
    lane = jnp.arange(128, dtype=jnp.int32) - HEAD
    other_doc = (lane[None, :] >= 0) & (lane[None, :] < DOCS) & (seg_row[:, None] != lane[None, :])
    kext = jnp.where(other_doc | ((lane >= DOCS) & (lane < DOCS + 3))[None, :], 1.0, 0.0).astype(bf16)
    x, ogt = hidden_in.T, out_grad.T
    gain_one, gain_two = norm_gains[0][:, None], norm_gains[1][:, None]

    (heads_stack,) = gather_weights(grid, [heads_weight.astype(bf16).T], (True,), 1)
    heads = heads_stack.reshape(DEPTH, QKV, SLICE)
    shards = [output_weight.astype(bf16).T, down_weight.astype(bf16).T, expand_weight.astype(bf16)]
    z_majors = (True, True, False)
    output_stack, down_stack, expand_stack, qx, kv, att, lse = front(
        grid, shards, z_majors, heads, x, gain_one, cos, sin, qext, kext, 2
    )
    wo = output_stack.reshape(DEPTH, D, SLICE)
    down = down_stack.reshape(DEPTH, D, FF // DEPTH)
    expand = expand_stack.reshape(grid.nd, D, 2 * FF // grid.nd)
    pieces = grid.nd // EXPAND_BLOCKS
    if pieces > 1:
        expand = expand.reshape(EXPAND_BLOCKS, pieces, D, -1).transpose(0, 2, 1, 3)
        expand = expand.reshape(EXPAND_BLOCKS, D, 2 * FF // EXPAND_BLOCKS)
    out, rg, gain_two_term, dexpand, ddn, dwo, dot, delta = middle(att, wo, x, ogt, gain_two, expand, down)
    if pieces > 1:
        dexpand = dexpand.reshape(EXPAND_BLOCKS, D, pieces, -1).transpose(0, 2, 1, 3)
    terms = [
        ddn.reshape(down_stack.shape),
        dexpand.reshape(expand_stack.shape),
        dwo.reshape(output_stack.shape),
    ]
    down_grad, expand_grad, output_grad, hd = back(
        grid, terms, (True, False, True), qx, lse, dot, delta, kv, kext, cos, sin, 3
    )
    ig, gain_one_term, dheads = ending(hd, heads, x, gain_one, rg)
    heads_grad, gains_grad = reduce_grads(
        grid,
        [dheads.reshape(heads_stack.shape)],
        (True,),
        jnp.concatenate([gain_one_term, gain_two_term], axis=1).T,
        4,
    )
    heads_grad, output_grad, down_grad = heads_grad.T, output_grad.T, down_grad.T
    hidden_out, input_grad = out.T, ig.T
    gains_new, gains_first_new, gains_second_new = adamw(
        norm_gains, gains_grad, gains_first, gains_second, gain_rate, 0.0
    )
    heads_new, heads_first_new, heads_second_new = adamw(
        heads_weight, heads_grad, heads_first, heads_second, matrix_rate, decay_rate
    )
    output_new, output_first_new, output_second_new = adamw(
        output_weight, output_grad, output_first, output_second, output_rate, decay_rate
    )
    expand_new, expand_first_new, expand_second_new = adamw(
        expand_weight, expand_grad, expand_first, expand_second, matrix_rate, decay_rate
    )
    down_new, down_first_new, down_second_new = adamw(
        down_weight, down_grad, down_first, down_second, matrix_rate, decay_rate
    )
    return (
        hidden_out,
        input_grad,
        gains_grad,
        heads_grad,
        output_grad,
        expand_grad,
        down_grad,
        gains_new,
        heads_new,
        output_new,
        expand_new,
        down_new,
        gains_first_new,
        gains_second_new,
        heads_first_new,
        heads_second_new,
        output_first_new,
        output_second_new,
        expand_first_new,
        expand_second_new,
        down_first_new,
        down_second_new,
    )


def solution(mesh):
    return jax.shard_map(
        functools.partial(local, Grid(mesh)),
        mesh=mesh,
        in_specs=(
            P(("dp", "shard"), None),
            P(("dp", "shard"), None),
            P("dp", None),
            P(("dp", "shard")),
            P(),
            P("shard", "dp"),
            P("shard", "dp"),
            P("shard", "dp"),
            P("shard", "dp"),
            P(),
            P(),
            P("shard", "dp"),
            P("shard", "dp"),
            P("shard", "dp"),
            P("shard", "dp"),
            P("shard", "dp"),
            P("shard", "dp"),
            P("shard", "dp"),
            P("shard", "dp"),
        ),
        out_specs=(
            P(("dp", "shard"), None),
            P(("dp", "shard"), None),
            P(),
            P("shard", "dp"),
            P("shard", "dp"),
            P("shard", "dp"),
            P("shard", "dp"),
            P(),
            P("shard", "dp"),
            P("shard", "dp"),
            P("shard", "dp"),
            P("shard", "dp"),
            P(),
            P(),
            P("shard", "dp"),
            P("shard", "dp"),
            P("shard", "dp"),
            P("shard", "dp"),
            P("shard", "dp"),
            P("shard", "dp"),
            P("shard", "dp"),
            P("shard", "dp"),
        ),
        check_vma=False,
    )
```

```python
import functools
import math

import jax
import jax.numpy as jnp
from jax import lax
from jax.experimental import pallas as pl
from jax.experimental.pallas import tpu as pltpu
from jax.sharding import PartitionSpec as P

MESH = pl.DeviceIdType.MESH
ANY = pl.BlockSpec(memory_space=pl.ANY)
VMEM = pl.BlockSpec(memory_space=pltpu.VMEM)


class Grid:
    def __init__(self, mesh):
        self.nd = mesh.shape["dp"]
        self.nz = mesh.shape["shard"]
        self.nx = math.isqrt(self.nd // 2)
        self.ny = self.nd // 2 // self.nx
        assert self.nx == self.ny and self.nx * self.ny * 2 == self.nd

    def dp(self, y, x, c):
        return (y * self.nx + x) * 2 + c


class Here:
    def __init__(self, grid):
        self.grid = grid
        d = lax.axis_index("dp")
        self.z = lax.axis_index("shard")
        self.d = d
        self.c = lax.rem(d, 2)
        self.x = lax.rem(d // 2, grid.nx)
        self.y = d // (2 * grid.nx)
        g = grid
        self.xs = [lax.rem(self.x + k, g.nx) for k in range(1, g.nx)]
        self.ys = [lax.rem(self.y + k, g.ny) for k in range(1, g.ny)]
        self.zs = [lax.rem(self.z + k, g.nz) for k in range(1, g.nz)]
        self.partner = (g.dp(self.y, self.x, 1 - self.c), self.z)

    def on_x(self, x):
        return (self.grid.dp(self.y, x, self.c), self.z)

    def on_y(self, y):
        return (self.grid.dp(y, self.x, self.c), self.z)

    def on_z(self, z):
        return (self.d, z)

    def peers(self):
        return (
            [self.partner]
            + [self.on_x(x) for x in self.xs]
            + [self.on_y(y) for y in self.ys]
            + [self.on_z(z) for z in self.zs]
        )


def greet(peers):
    barrier = pltpu.get_barrier_semaphore()
    for peer in peers:
        pl.semaphore_signal(barrier, inc=1, device_id=peer, device_id_type=MESH)
    pl.semaphore_wait(barrier, len(peers))


def send(src, dst, send_sem, recv_sem, device):
    pltpu.make_async_remote_copy(
        src_ref=src,
        dst_ref=dst,
        send_sem=send_sem,
        recv_sem=recv_sem,
        device_id=device,
        device_id_type=MESH,
    ).start()


def wait_bytes(ref, sem):
    pltpu.make_async_copy(ref, ref, sem).wait()


def half_rows(rows):
    return max(16, int(rows / 32 + 0.5) * 16)


def chunks_of(rows, size=64):
    starts = list(range(0, rows, size))
    if len(starts) > 1 and rows - starts[-1] < size // 2:
        starts.pop()
    return [(start, stop - start) for start, stop in zip(starts, starts[1:] + [rows])]


class Gather:
    def __init__(self, here, shard, out, sems, z_major, rows):
        self.h, self.shard, self.out, self.sems, self.z_major = here, shard, out, sems, z_major
        self.start, self.rows = rows
        self.cut = half_rows(self.rows)

    def span(self, half=None):
        if half is None:
            return pl.ds(self.start, self.rows)
        return pl.ds(self.start, self.cut) if half == 0 else pl.ds(self.start + self.cut, self.rows - self.cut)

    def column(self, d, half=None):
        return self.out.at[:, d, self.span(half)] if self.z_major else self.out.at[d, :, self.span(half)]

    def block(self, d, z):
        return self.out.at[z, d, self.span()] if self.z_major else self.out.at[d, z, self.span()]

    def columns(self, count):
        some = pl.ds(0, count)
        return self.out.at[:, some, self.span()] if self.z_major else self.out.at[some, :, self.span()]

    def blocks(self, count):
        some = pl.ds(0, count)
        return self.out.at[some, 0, self.span()] if self.z_major else self.out.at[0, some, self.span()]

    def own(self):
        h = self.h
        return pltpu.make_async_copy(self.shard.at[self.span()], self.block(h.d, h.z), self.sems.at[8])

    def stage_z(self):
        h, s = self.h, self.sems
        for z in h.zs:
            send(self.shard.at[self.span()], self.block(h.d, h.z), s.at[0], s.at[1], h.on_z(z))
        self.own().start()

    def stage_one(self):
        h, s = self.h, self.sems
        wait_bytes(self.blocks(len(h.zs)), s.at[1])
        self.own().wait()
        for x in h.xs:
            send(self.column(h.d, 0), self.column(h.d, 0), s.at[2], s.at[3], h.on_x(x))
        for y in h.ys:
            send(self.column(h.d, 1), self.column(h.d, 1), s.at[2], s.at[3], h.on_y(y))
        send(self.column(h.d), self.column(h.d), s.at[6], s.at[7], h.partner)

    def stage_two(self):
        h, s, g = self.h, self.sems, self.h.grid
        wait_bytes(self.columns(len(h.xs)), s.at[3])
        for y in h.ys:
            for x in [h.x] + h.xs:
                col = self.column(g.dp(h.y, x, h.c), 0)
                send(col, col, s.at[4], s.at[5], h.on_y(y))
        for x in h.xs:
            for y in [h.y] + h.ys:
                col = self.column(g.dp(y, h.x, h.c), 1)
                send(col, col, s.at[4], s.at[5], h.on_x(x))
        for x in h.xs:
            col = self.column(g.dp(h.y, x, h.c), 0)
            send(col, col, s.at[6], s.at[7], h.partner)
        for y in h.ys:
            col = self.column(g.dp(y, h.x, h.c), 1)
            send(col, col, s.at[6], s.at[7], h.partner)

    def stage_three(self):
        h, s, g = self.h, self.sems, self.h.grid
        wait_bytes(self.columns(g.nx * len(h.ys)), s.at[5])
        for y in h.ys:
            for x in [h.x] + h.xs:
                col = self.column(g.dp(y, x, h.c), 0)
                send(col, col, s.at[6], s.at[7], h.partner)
        for x in h.xs:
            for y in [h.y] + h.ys:
                col = self.column(g.dp(y, x, h.c), 1)
                send(col, col, s.at[6], s.at[7], h.partner)

    def arrive(self):
        g = self.h.grid
        wait_bytes(self.columns(g.nd // 2), self.sems.at[7])

    def drain(self):
        h, s, g = self.h, self.sems, self.h.grid
        wait_bytes(self.blocks(len(h.zs)), s.at[0])
        wait_bytes(self.columns(len(h.xs)), s.at[2])
        wait_bytes(self.columns(g.nx * len(h.ys)), s.at[4])
        wait_bytes(self.columns(g.nd // 2), s.at[6])

    stages = ("stage_z", "stage_one", "stage_two", "stage_three")


def pipelined(jobs, ahead=0):
    ticks = [getattr(job, job.stages[0]) for job in jobs[:ahead]]
    depth = len(jobs[0].stages) if jobs else 0
    for step in range(len(jobs) + depth - 1):
        for k in range(depth):
            i = step - k
            if 0 <= i < len(jobs) and not (k == 0 and i < ahead):
                ticks.append(getattr(jobs[i], jobs[i].stages[k]))
    return ticks


def chunk_list(shards, leads=None):
    pieces = []
    for i, shard in enumerate(shards):
        if leads is not None and leads[i]:
            pieces += [(i, k, (0, shard.shape[-2])) for k in leads[i]]
        else:
            pieces += [(i, None, rows) for rows in chunks_of(shard.shape[-2])]
    return pieces


def piece_of(ref, lead):
    return ref if lead is None else ref.at[lead]


def gather_jobs(here, shards, outs, sems, z_majors, pieces):
    return [
        Gather(here, piece_of(shards[i], lead), piece_of(outs[i], lead), sems.at[k], z_majors[i], rows)
        for k, (i, lead, rows) in enumerate(pieces)
    ]


GATHER_SEMS = 9


def gather_kernel(grid, z_majors, pieces, *refs):
    n = len(z_majors)
    shards, outs, sems = refs[:n], refs[n : 2 * n], refs[2 * n]
    here = Here(grid)
    greet(here.peers())
    jobs = gather_jobs(here, shards, outs, sems, z_majors, pieces)
    for tick in pipelined(jobs, len(jobs)):
        tick()
    for job in jobs:
        job.arrive()
        job.drain()


def gather_weights(grid, shards, z_majors, collective_id):
    shapes = []
    for shard, z_major in zip(shards, z_majors):
        lead = (grid.nz, grid.nd) if z_major else (grid.nd, grid.nz)
        shapes.append(jax.ShapeDtypeStruct(lead + shard.shape, shard.dtype))
    pieces = chunk_list(shards)
    return pl.pallas_call(
        functools.partial(gather_kernel, grid, tuple(z_majors), pieces),
        out_shape=shapes,
        in_specs=[VMEM] * len(shards),
        out_specs=[ANY] * len(shards),
        scratch_shapes=[pltpu.SemaphoreType.DMA((len(pieces), GATHER_SEMS))],
        compiler_params=pltpu.CompilerParams(collective_id=collective_id, has_side_effects=True),
        name="gather_weights",
    )(*shards)


class Reduce:
    def __init__(self, here, terms, result, bufs, sems, z_major, rows):
        self.h, self.terms, self.result, self.sems, self.z_major = here, terms, result, sems, z_major
        self.own, self.other, self.one_a, self.one_b, self.two_a, self.two_b, self.last = bufs
        self.start, self.rows = rows
        self.cut = half_rows(self.rows)

    @staticmethod
    def scratch(grid, rows, cols, z_major):
        cut = half_rows(rows)
        ny, nx, nz = grid.ny, grid.nx, grid.nz
        full = (nz, ny, nx) if z_major else (ny, nx, nz)
        row = (nz, nx) if z_major else (nx, nz)
        bf = jnp.bfloat16
        return [
            pltpu.VMEM(full + (rows, cols), bf),
            pltpu.VMEM(full + (rows, cols), bf),
            pltpu.VMEM((ny,) + row + (cut, cols), bf),
            pltpu.VMEM((nx,) + row + (rows - cut, cols), bf),
            pltpu.VMEM((nx, nz, cut, cols), bf),
            pltpu.VMEM((ny, nz, rows - cut, cols), bf),
            pltpu.VMEM((nz, rows, cols), bf),
        ]

    def span(self, half):
        return {None: slice(None), 0: pl.ds(0, self.cut), 1: pl.ds(self.cut, self.rows - self.cut)}[half]

    def at(self, y, x, z, half):
        y, x, z = (slice(None) if v is None else v for v in (y, x, z))
        return (z, y, x, self.span(half)) if self.z_major else (y, x, z, self.span(half))

    def side(self, c):
        rows = pl.ds(self.start, self.rows)
        return self.terms.at[:, :, :, c, rows] if self.z_major else self.terms.at[:, :, c, :, rows]

    def load(self):
        return pltpu.make_async_copy(self.side(self.h.c), self.own, self.sems.at[8])

    def stage_core(self):
        h, s = self.h, self.sems
        send(self.side(1 - h.c), self.other, s.at[0], s.at[1], h.partner)
        self.load().start()

    def add_loop(self, shape, body):
        total = math.prod(shape)

        def step(i, carry):
            place = []
            rest = i
            for size in reversed(shape):
                place.append(lax.rem(rest, size))
                rest = rest // size
            body(tuple(reversed(place)))
            return carry

        lax.fori_loop(0, total, step, 0)

    def stage_one(self):
        h, s, g = self.h, self.sems, self.h.grid
        self.load().wait()
        wait_bytes(self.other, s.at[1])

        def body(place):
            self.own[place] = self.own[place] + self.other[place]

        self.add_loop(self.own.shape[:3], body)
        for y in h.ys:
            send(self.own.at[self.at(y, None, None, 0)], self.one_a.at[h.y], s.at[2], s.at[3], h.on_y(y))
        for x in h.xs:
            send(self.own.at[self.at(None, x, None, 1)], self.one_b.at[h.x], s.at[9], s.at[10], h.on_x(x))

    def stage_two(self):
        h, s, g = self.h, self.sems, self.h.grid
        wait_bytes(self.one_a.at[pl.ds(0, g.ny - 1)], s.at[3])
        wait_bytes(self.one_b.at[pl.ds(0, g.nx - 1)], s.at[10])

        def body_a(place):
            where = (place[1], place[0]) if self.z_major else place
            spot = self.at(h.y, where[0], where[1], 0)
            total = self.own[spot].astype(jnp.float32)
            for y in h.ys:
                total += self.one_a[(y,) + place].astype(jnp.float32)
            self.own[spot] = total.astype(jnp.bfloat16)

        self.add_loop(self.one_a.shape[1:3], body_a)

        def body_b(place):
            where = (place[1], place[0]) if self.z_major else place
            spot = self.at(where[0], h.x, where[1], 1)
            total = self.own[spot].astype(jnp.float32)
            for x in h.xs:
                total += self.one_b[(x,) + place].astype(jnp.float32)
            self.own[spot] = total.astype(jnp.bfloat16)

        self.add_loop(self.one_b.shape[1:3], body_b)
        for x in h.xs:
            send(self.own.at[self.at(h.y, x, None, 0)], self.two_a.at[h.x], s.at[4], s.at[5], h.on_x(x))
        for y in h.ys:
            send(self.own.at[self.at(y, h.x, None, 1)], self.two_b.at[h.y], s.at[11], s.at[12], h.on_y(y))

    def stage_three(self):
        h, s, g = self.h, self.sems, self.h.grid
        wait_bytes(self.two_a.at[pl.ds(0, g.nx - 1)], s.at[5])
        wait_bytes(self.two_b.at[pl.ds(0, g.ny - 1)], s.at[12])

        def body(place):
            (z,) = place
            spot = self.at(h.y, h.x, z, 0)
            total = self.own[spot].astype(jnp.float32)
            for x in h.xs:
                total += self.two_a[x, z].astype(jnp.float32)
            self.own[spot] = total.astype(jnp.bfloat16)
            spot = self.at(h.y, h.x, z, 1)
            total = self.own[spot].astype(jnp.float32)
            for y in h.ys:
                total += self.two_b[y, z].astype(jnp.float32)
            self.own[spot] = total.astype(jnp.bfloat16)

        self.add_loop((g.nz,), body)
        for z in h.zs:
            send(self.own.at[self.at(h.y, h.x, z, None)], self.last.at[h.z], s.at[6], s.at[7], h.on_z(z))

    def finish(self):
        h, s, g = self.h, self.sems, self.h.grid
        wait_bytes(self.last.at[pl.ds(0, g.nz - 1)], s.at[7])
        total = self.own[self.at(h.y, h.x, h.z, None)].astype(jnp.float32)
        for z in h.zs:
            total += self.last[z].astype(jnp.float32)
        self.result[pl.ds(self.start, self.rows)] = total

    stages = ("stage_core", "stage_one", "stage_two", "stage_three", "finish")

    def drain(self):
        g, s = self.h.grid, self.sems
        wait_bytes(self.other, s.at[0])
        wait_bytes(self.one_a.at[pl.ds(0, g.ny - 1)], s.at[2])
        wait_bytes(self.one_b.at[pl.ds(0, g.nx - 1)], s.at[9])
        wait_bytes(self.two_a.at[pl.ds(0, g.nx - 1)], s.at[4])
        wait_bytes(self.two_b.at[pl.ds(0, g.ny - 1)], s.at[11])
        wait_bytes(self.last.at[pl.ds(0, g.nz - 1)], s.at[6])


REDUCE_SEMS = 13
REDUCE_BUFS = 7


class Share:
    def __init__(self, here, value, result, bufs, sems):
        self.h, self.value, self.result, self.sems = here, value, result, sems
        self.bufs = bufs

    @staticmethod
    def scratch(grid, shape):
        return [pltpu.VMEM((n,) + shape, jnp.float32) for n in (2, grid.nx, grid.ny, grid.nz)]

    def axis(self, k):
        h = self.h
        return (
            (h.c, [h.partner], 2),
            (h.x, [h.on_x(x) for x in h.xs], h.grid.nx),
            (h.y, [h.on_y(y) for y in h.ys], h.grid.ny),
            (h.z, [h.on_z(z) for z in h.zs], h.grid.nz),
        )[k]

    def start(self, k):
        me, peers, n = self.axis(k)
        self.bufs[k][me] = self.value[...] if k == 0 else self.total
        for peer in peers:
            send(self.bufs[k].at[me], self.bufs[k].at[me], self.sems.at[2 * k], self.sems.at[2 * k + 1], peer)

    def end(self, k):
        me, peers, n = self.axis(k)
        wait_bytes(self.bufs[k].at[pl.ds(0, n - 1)], self.sems.at[2 * k + 1])
        total = self.bufs[k][0]
        for i in range(1, n):
            total = total + self.bufs[k][i]
        self.total = total
        if k == 3:
            self.result[...] = total

    def drain(self):
        for k in range(4):
            n = self.axis(k)[2]
            wait_bytes(self.bufs[k].at[pl.ds(0, n - 1)], self.sems.at[2 * k])


SHARE_SEMS = 8


def reduce_kernel(grid, z_majors, pieces, shared, *refs):
    n = len(z_majors)
    terms, refs = refs[:n], refs[n:]
    value, refs = (refs[0], refs[1:]) if shared else (None, refs)
    results, refs = refs[:n], refs[n:]
    value_sum, refs = (refs[0], refs[1:]) if shared else (None, refs)
    here = Here(grid)
    greet(here.peers())
    jobs, refs = reduce_jobs(here, terms, results, refs, z_majors, pieces)
    share = None
    if shared:
        share = Share(here, value, value_sum, refs[:4], refs[4])
        share.start(0)
    ticks = pipelined(jobs, len(jobs))
    for k, tick in enumerate(ticks):
        tick()
        if share is not None and k >= len(jobs) and k - len(jobs) < 4:
            step = k - len(jobs)
            share.end(step)
            if step < 3:
                share.start(step + 1)
    if share is not None:
        share.drain()
    for job in jobs:
        job.drain()


def reduce_jobs(here, terms, results, refs, z_majors, pieces):
    n = len(pieces)
    sems = refs[n * REDUCE_BUFS]
    jobs = []
    for k, (i, lead, rows) in enumerate(pieces):
        bufs = refs[k * REDUCE_BUFS : (k + 1) * REDUCE_BUFS]
        term, result = piece_of(terms[i], lead), piece_of(results[i], lead)
        jobs.append(Reduce(here, term, result, bufs, sems.at[k], z_majors[i], rows))
    return jobs, refs[n * REDUCE_BUFS + 1 :]


def reduce_scratch(grid, terms, z_majors, pieces):
    scratch = []
    for i, _, (_, rows) in pieces:
        scratch += Reduce.scratch(grid, rows, terms[i].shape[-1], z_majors[i])
    return scratch + [pltpu.SemaphoreType.DMA((max(len(pieces), 1), REDUCE_SEMS))]


def split_terms(grid, terms, z_majors):
    split = []
    for term, z_major in zip(terms, z_majors):
        lead = (grid.ny, grid.nx, 2)
        lead = (grid.nz,) + lead if z_major else lead + (grid.nz,)
        split.append(term.reshape(term.shape[:-4] + lead + term.shape[-2:]))
    return split


def reduce_grads(grid, terms, z_majors, value, collective_id):
    shapes = [jax.ShapeDtypeStruct(term.shape[-2:], jnp.float32) for term in terms]
    pieces = chunk_list(terms)
    scratch = reduce_scratch(grid, terms, z_majors, pieces)
    n = len(terms)
    shared = value is not None
    if shared:
        shapes.append(jax.ShapeDtypeStruct(value.shape, jnp.float32))
        scratch += Share.scratch(grid, value.shape)
        scratch.append(pltpu.SemaphoreType.DMA((SHARE_SEMS,)))
    return pl.pallas_call(
        functools.partial(reduce_kernel, grid, tuple(z_majors), pieces, shared),
        out_shape=shapes,
        in_specs=[ANY] * n + [VMEM] * shared,
        out_specs=[VMEM] * len(shapes),
        scratch_shapes=scratch,
        compiler_params=pltpu.CompilerParams(
            collective_id=collective_id, has_side_effects=True, vmem_limit_bytes=62 << 20
        ),
        name="reduce_grads",
    )(*split_terms(grid, terms, z_majors), *([value] if shared else []))


D = 960
QUERY_HEADS = 15
KEY_VALUE_HEADS = 5
GROUP = QUERY_HEADS // KEY_VALUE_HEADS
HEAD = 64
FF = 2560
QKV = (QUERY_HEADS + 2 * KEY_VALUE_HEADS) * HEAD
ADAM_STEP = 10
DOCS = 16
HIDE = -1e30
VALUE_SCALE = 2.0**-9

norm_epsilon = 1e-05
beta_one = 0.9
beta_two = 0.95
adam_epsilon = 1e-08
matrix_rate = 0.03
output_rate = 0.15
gain_rate = 0.5
decay_rate = 0.1

f32 = jnp.float32
bf16 = jnp.bfloat16
DEPTH = 4
SLICE = D // DEPTH


def mm(a, b):
    return lax.dot_general(a, b, (((1,), (0,)), ((), ())), preferred_element_type=f32)


def mm_nt(a, b):
    return lax.dot_general(a, b, (((1,), (1,)), ((), ())), preferred_element_type=f32)


def mm_tn(a, b):
    return lax.dot_general(a, b, (((0,), (0,)), ((), ())), preferred_element_type=f32)


def lanes_below(shape, n):
    return lax.broadcasted_iota(jnp.int32, shape, len(shape) - 1) < n


def inverse_rms(ref):
    total = jnp.zeros((1, ref.shape[1]), f32)
    for k in range(DEPTH):
        x = ref[pl.ds(k * SLICE, SLICE)].astype(f32)
        total += jnp.sum(x * x, axis=0, keepdims=True)
    return lax.rsqrt(total * (1.0 / D) + norm_epsilon)


def three_pieces(row):
    hi = row.astype(bf16).astype(f32)
    mid = (row - hi).astype(bf16).astype(f32)
    low = row - hi - mid
    place = lax.broadcasted_iota(jnp.int32, (16, row.shape[1]), 0)
    block = jnp.where(place == 0, hi, jnp.where(place == 1, mid, jnp.where(place == 2, low, 0.0)))
    return block.astype(bf16)


class KeyChain:
    def __init__(self, here, kv, sems):
        self.h, self.kv, self.sems = here, kv, sems

    def up(self, slot):
        h = self.h
        to = lax.rem(h.z + 1, h.grid.nz)

        @pl.when(h.z < h.grid.nz - 1)
        def _():
            send(self.kv.at[slot], self.kv.at[slot], self.sems.at[0, slot], self.sems.at[1, slot], h.on_z(to))

    def take(self, slot):
        wait_bytes(self.kv.at[slot], self.sems.at[1, slot])
        self.up(slot)

    def drain(self):
        h = self.h
        for s in range(h.grid.nz):

            @pl.when(jnp.logical_and(h.z >= s, h.z < h.grid.nz - 1))
            def _():
                wait_bytes(self.kv.at[h.z - s], self.sems.at[0, h.z - s])


def front_kernel(grid, z_majors, pieces, *refs):
    n = len(z_majors)
    shards, refs = refs[:n], refs[n:]
    heads, x, gain, cos, sin, qext, kext = refs[:7]
    refs = refs[7:]
    outs, refs = refs[:n], refs[n:]
    qx, qn, kv, att = refs[:4]
    h1, proj, kx, vt, acc, sems, kv_sems = refs[4:]
    here = Here(grid)
    tokens = x.shape[1]
    half = tokens // 2
    greet(here.peers())
    jobs = gather_jobs(here, shards, outs, sems, z_majors, pieces)
    ticks = pipelined(jobs, 3)
    for tick in ticks[:3]:
        tick()

    inverse = inverse_rms(x)
    for k in range(DEPTH):
        rows = pl.ds(k * SLICE, SLICE)
        h1[rows] = (x[rows].astype(f32) * inverse * gain[rows]).astype(bf16)

    part = QKV // 5

    def project(m, carry):
        rows = pl.ds(pl.multiple_of(m * part, 16), part)
        total = mm(heads[0, rows], h1[pl.ds(0, SLICE)])
        for k in range(1, DEPTH):
            total += mm(heads[k, rows], h1[pl.ds(k * SLICE, SLICE)])
        proj[rows] = total
        return carry

    lax.fori_loop(0, 5, project, 0)

    def turned(h):
        base = h * HEAD
        a = proj[pl.ds(pl.multiple_of(base, 8), HEAD // 2)]
        b = proj[pl.ds(pl.multiple_of(base + HEAD // 2, 8), HEAD // 2)]
        c, s = cos[...], sin[...]
        return a * c - b * s, b * c + a * s

    def keys(g, carry):
        a, b = turned(QUERY_HEADS + g)
        v = proj[pl.ds(pl.multiple_of((QUERY_HEADS + KEY_VALUE_HEADS + g) * HEAD, 8), HEAD)]
        both = jnp.concatenate([a, b, v], axis=0)
        kv[here.z, g] = both.T.astype(bf16)
        return carry

    lax.fori_loop(0, KEY_VALUE_HEADS, keys, 0)
    chain = KeyChain(here, kv, kv_sems)
    chain.up(here.z)

    def queries(h, carry):
        a, b = turned(h)
        scale = HEAD**-0.5
        qx[h, pl.ds(0, 32)] = (a.astype(bf16).astype(f32) * scale).astype(bf16)
        qx[h, pl.ds(32, 32)] = (b.astype(bf16).astype(f32) * scale).astype(bf16)
        qx[h, pl.ds(64, 64)] = qext[...]
        qn[h] = qx[h].astype(f32).T.astype(bf16)
        return carry

    lax.fori_loop(0, QUERY_HEADS, queries, 0)

    def prepare(slot):
        ext = kext[pl.ds(pl.multiple_of(slot * tokens, 16), tokens)]

        def body(g, carry):
            block = kv[slot, g]
            kx[g] = jnp.where(lanes_below(block.shape, HEAD), block, ext)
            turned_block = block.astype(f32).T
            vt[g, pl.ds(0, 16)] = jnp.ones((16, tokens), bf16)
            vt[g, pl.ds(16, HEAD)] = (turned_block[HEAD:] * VALUE_SCALE).astype(bf16)
            return carry

        lax.fori_loop(0, KEY_VALUE_HEADS, body, 0)

    def below(shape, shift):
        return lax.broadcasted_iota(jnp.int32, shape, 0) <= lax.broadcasted_iota(jnp.int32, shape, 1) + shift

    def diagonal(g):
        for i in range(GROUP):
            h = g * GROUP + i
            s = mm(kx[g, pl.ds(0, half)], qx[h, :, pl.ds(0, half)])
            p = jnp.exp(jnp.where(below(s.shape, 0), s, HIDE)).astype(bf16)
            acc[h, :, pl.ds(0, half)] = mm(vt[g, :, pl.ds(0, half)], p)
            s = mm(kx[g], qx[h, :, pl.ds(half, half)])
            p = jnp.exp(jnp.where(below(s.shape, half), s, HIDE)).astype(bf16)
            acc[h, :, pl.ds(half, half)] = mm(vt[g], p)

    def whole(g):
        for i in range(GROUP):
            h = g * GROUP + i
            for k in range(2):
                cols = pl.ds(k * half, half)
                p = jnp.exp(mm(kx[g], qx[h, :, cols])).astype(bf16)
                acc[h, :, cols] += mm(vt[g], p)

    ticks = ticks[3:]

    def micro(t, carry):
        s = t // KEY_VALUE_HEADS
        g = lax.rem(t, KEY_VALUE_HEADS)

        @pl.when(s <= here.z)
        def _():
            slot = here.z - s

            @pl.when(g == 0)
            def _():
                @pl.when(s > 0)
                def _():
                    chain.take(slot)

                prepare(slot)

            @pl.when(s == 0)
            def _():
                diagonal(g)

            @pl.when(s > 0)
            def _():
                whole(g)

        for k, tick in enumerate(ticks):
            pl.when(t == k * micros // len(ticks))(tick)
        return carry

    micros = grid.nz * KEY_VALUE_HEADS
    lax.fori_loop(0, micros, micro, 0)

    def close(h, carry):
        totals = acc[h, pl.ds(0, 1)]
        scale = (1.0 / VALUE_SCALE) / totals
        att[pl.ds(pl.multiple_of(h * HEAD, 16), HEAD)] = (acc[h, pl.ds(16, HEAD)] * scale).astype(bf16)
        qx[h, pl.ds(HEAD + DOCS, 16)] = three_pieces(-jnp.log(totals))
        return carry

    lax.fori_loop(0, QUERY_HEADS, close, 0)
    for job in jobs:
        job.arrive()
        job.drain()
    chain.drain()


def front(grid, shards, z_majors, leads, heads, x, gain, cos, sin, qext, kext, collective_id):
    tokens = x.shape[1]
    shapes = []
    for shard, z_major, chosen in zip(shards, z_majors, leads):
        lead = (grid.nz, grid.nd) if z_major else (grid.nd, grid.nz)
        lead = (len(chosen),) + lead if chosen else lead
        shapes.append(jax.ShapeDtypeStruct(lead + shard.shape[-2:], shard.dtype))
    n = len(shards)
    pieces = chunk_list(shards, leads)
    shapes += [
        jax.ShapeDtypeStruct((QUERY_HEADS, 128, tokens), bf16),
        jax.ShapeDtypeStruct((QUERY_HEADS, tokens, 128), bf16),
        jax.ShapeDtypeStruct((grid.nz, KEY_VALUE_HEADS, tokens, 128), bf16),
        jax.ShapeDtypeStruct((D, tokens), bf16),
    ]
    return pl.pallas_call(
        functools.partial(front_kernel, grid, tuple(z_majors), pieces),
        out_shape=shapes,
        in_specs=[VMEM] * (n + 7),
        out_specs=[ANY] * n + [VMEM] * 4,
        scratch_shapes=[
            pltpu.VMEM((D, tokens), bf16),
            pltpu.VMEM((QKV, tokens), f32),
            pltpu.VMEM((KEY_VALUE_HEADS, tokens, 128), bf16),
            pltpu.VMEM((KEY_VALUE_HEADS, 80, tokens), bf16),
            pltpu.VMEM((QUERY_HEADS, 80, tokens), f32),
            pltpu.SemaphoreType.DMA((max(len(pieces), 1), GATHER_SEMS)),
            pltpu.SemaphoreType.DMA((2, grid.nz)),
        ],
        compiler_params=pltpu.CompilerParams(
            collective_id=collective_id, has_side_effects=True, vmem_limit_bytes=60 << 20
        ),
        name="front",
    )(*shards, heads, x, gain, cos, sin, qext, kext)


STEPS = 5
WIDTH = 128
PARTS = 6


def middle_kernel(grid, ready, summed, *refs):
    att, wo, x, ogt, gain, exp_in, dn_in = refs[:7]
    refs = refs[7:]
    late = STEPS - ready
    if late:
        shard, refs = refs[0], refs[1:]
    out, rg, gsum, dwo, dox, dexp, ddn = refs[:7]
    refs = refs[7:]
    if late:
        exp_late, refs = refs[0], refs[1:]
    if summed:
        gexp, refs = refs[0], refs[1:]
    (res, inv, h2, h2t, og, acc_o, acc_h, mixed, dgate, dup, wg, wu, wd, sg, sd, w_sems, o_sems) = refs[:17]
    refs = refs[17:]
    tokens = x.shape[1]
    half = 2 * WIDTH
    schedule = {}
    gathers, sums = [], []
    if late or summed:
        here = Here(grid)
        greet(here.peers())
    if late:
        pieces = [(0, k, (0, SLICE)) for k in range(late)]
        g_sems, refs = refs[0], refs[1:]
        gathers = [
            Gather(here, shard.at[ready + k], exp_late.at[k], g_sems.at[k], False, (0, SLICE)) for k in range(late)
        ]
        for job in gathers:
            job.stage_z()
        for k, job in enumerate(gathers):
            for i, stage in enumerate(job.stages[1:]):
                schedule.setdefault(5 * i + 2 * k, []).append(getattr(job, stage))
            schedule.setdefault((ready + k - 1) * PARTS + 1, []).append(job.arrive)
    if summed:
        pieces = [(0, k, (0, SLICE)) for k in range(summed)]
        sums, refs = reduce_jobs(here, [dexp], [gexp], refs, (False,), pieces)
        for k, job in enumerate(sums):
            for i, stage in enumerate(job.stages):
                place = min((k + 1) * PARTS + 3 + 4 * i, STEPS * PARTS - 1)
                schedule.setdefault(place, []).append(getattr(job, stage))

    def fetch_from(source, index, step, slot, go):
        for d in range(4):
            lanes = pl.ds(d * WIDTH, WIDTH)
            go(pltpu.make_async_copy(source.at[index, d], wg.at[slot, :, :, lanes], w_sems.at[slot, 0]))
            go(pltpu.make_async_copy(source.at[index, 4 + d], wu.at[slot, :, :, lanes], w_sems.at[slot, 1]))
            columns = pl.ds(pl.multiple_of(step * WIDTH, WIDTH), WIDTH)
            go(pltpu.make_async_copy(dn_in.at[d, :, columns], wd.at[slot, :, lanes], w_sems.at[slot, 2]))

    def fetch(step):
        slot = lax.rem(step, 2)

        @pl.when(step < ready)
        def _():
            fetch_from(exp_in, step, step, slot, lambda copy: copy.start())

        if late:

            @pl.when(step >= ready)
            def _():
                fetch_from(exp_late, step - ready, step, slot, lambda copy: copy.start())

    def put_expand(step, go):
        for k in range(2):
            for d in range(4):
                lanes = pl.ds(d * WIDTH, WIDTH)
                to = dexp.at[step, 4 * k + d] if not sums_split else dexp.at[(step,) + sums_place(4 * k + d)]
                go(pltpu.make_async_copy(sg.at[k, :, :, lanes], to, o_sems.at[0]))

    def put_down(step, go):
        for d in range(4):
            columns = pl.ds(pl.multiple_of(step * WIDTH, WIDTH), WIDTH)
            go(pltpu.make_async_copy(sd.at[:, pl.ds(d * WIDTH, WIDTH)], ddn.at[d, :, columns], o_sems.at[1]))

    sums_split = len(dexp.shape) == 7

    def sums_place(d):
        return (d // (2 * grid.nx), d // 2 % grid.nx, d % 2)

    fetch(jnp.int32(0))
    total = jnp.zeros((1, tokens), f32)
    for m in range(DEPTH):
        rows = pl.ds(m * SLICE, SLICE)
        r = x[rows].astype(f32)
        for k in range(DEPTH):
            r += mm(wo[k, rows], att[pl.ds(k * SLICE, SLICE)])
        res[rows] = r
        total += jnp.sum(r * r, axis=0, keepdims=True)
    inverse = lax.rsqrt(total * (1.0 / D) + norm_epsilon)
    inv[...] = inverse
    for m in range(DEPTH):
        rows = pl.ds(m * SLICE, SLICE)
        h2t[rows] = (res[rows] * inverse * gain[rows]).astype(bf16)
    h2[...] = h2t[...].astype(f32).T.astype(bf16)
    og[...] = ogt[...].astype(f32).T.astype(bf16)
    acc_o[...] = jnp.zeros_like(acc_o)
    acc_h[...] = jnp.zeros_like(acc_h)

    def activate(slot, k):
        cols = pl.ds(k * half, half)
        gate = mm(h2[...], wg[slot, :, :, cols].reshape(D, half))
        up = mm(h2[...], wu[slot, :, :, cols].reshape(D, half))
        back = mm(og[...], wd[slot, :, cols])
        s = 1.0 / (1.0 + jnp.exp(-gate))
        silu = gate * s
        mixed[:, cols] = (silu * up).astype(bf16)
        dgate[:, cols] = (back * up * s * (1.0 + gate * (1.0 - s))).astype(bf16)
        dup[:, cols] = (back * silu).astype(bf16)

    def micro(t, carry):
        step = t // PARTS
        part = lax.rem(t, PARTS)
        slot = lax.rem(step, 2)

        for place, ticks in schedule.items():

            @pl.when(t == place)
            def _():
                for tick in ticks:
                    tick()

        @pl.when(part == 0)
        def _():
            wait_bytes(wg.at[slot], w_sems.at[slot, 0])
            wait_bytes(wu.at[slot], w_sems.at[slot, 1])
            wait_bytes(wd.at[slot], w_sems.at[slot, 2])
            activate(slot, 0)

        @pl.when(part == 1)
        def _():
            @pl.when(step > 0)
            def _():
                wait_bytes(sg, o_sems.at[0])
                wait_bytes(sd, o_sems.at[1])

            pl.when(step + 1 < STEPS)(lambda: fetch(step + 1))
            activate(slot, 1)

        @pl.when(part == 2)
        def _():
            acc_o[...] += mm_nt(wd[slot], mixed[...])

        @pl.when(part == 3)
        def _():
            for m in range(DEPTH):
                sg[0, m] = mm(h2t[pl.ds(m * SLICE, SLICE)], dgate[...]).astype(bf16)
                sg[1, m] = mm(h2t[pl.ds(m * SLICE, SLICE)], dup[...]).astype(bf16)
            put_expand(step, lambda copy: copy.start())

        @pl.when(part == 4)
        def _():
            sd[...] = mm(ogt[...], mixed[...]).astype(bf16)
            put_down(step, lambda copy: copy.start())

        @pl.when(part == 5)
        def _():
            acc_h[...] += mm_nt(wg[slot].reshape(D, 2 * half), dgate[...])
            acc_h[...] += mm_nt(wu[slot].reshape(D, 2 * half), dup[...])

        return carry

    lax.fori_loop(0, STEPS * PARTS, micro, 0)
    wait_bytes(sg, o_sems.at[0])
    wait_bytes(sd, o_sems.at[1])
    inverse = inv[...]
    total = jnp.zeros((1, tokens), f32)
    for m in range(DEPTH):
        rows = pl.ds(m * SLICE, SLICE)
        out[rows] = (res[rows] + acc_o[rows]).astype(bf16)
        normed = res[rows] * inverse
        up = acc_h[rows]
        gsum[rows] = jnp.sum(up * normed, axis=1, keepdims=True)
        total += jnp.sum(up * gain[rows] * normed, axis=0, keepdims=True)
    mean = total * (1.0 / D)
    for m in range(DEPTH):
        rows = pl.ds(m * SLICE, SLICE)
        normed = res[rows] * inverse
        r = ogt[rows].astype(f32) + inverse * (acc_h[rows] * gain[rows] - normed * mean)
        rg[rows] = r
        h2t[rows] = r.astype(bf16)
    for k in range(DEPTH):
        rows = pl.ds(k * SLICE, SLICE)
        dwo[k] = mm_nt(h2t[...], att[rows]).astype(bf16)
        acc_h[rows] = mm_tn(wo[k], h2t[...])

    def rows_of(h, carry):
        rows = pl.ds(pl.multiple_of(h * HEAD, 16), HEAD)
        grad = acc_h[rows].astype(bf16)
        dox[h, pl.ds(HEAD, HEAD)] = grad
        delta = jnp.sum(grad.astype(f32) * att[rows].astype(f32), axis=0, keepdims=True)
        dox[h, pl.ds(0, 16)] = three_pieces(-delta)
        dox[h, pl.ds(16, 48)] = jnp.zeros((48, tokens), bf16)
        return carry

    lax.fori_loop(0, QUERY_HEADS, rows_of, 0)
    for job in gathers + sums:
        job.drain()


def middle(grid, att, wo, x, ogt, gain, expand, down, shard, summed, collective_id):
    tokens = x.shape[1]
    ready = expand.shape[0]
    late = STEPS - ready
    blocks = expand.shape[1:]
    if summed:
        grads = (STEPS, grid.ny, grid.nx, 2) + blocks[1:]
    else:
        grads = (STEPS,) + blocks
    shapes = [
        jax.ShapeDtypeStruct((D, tokens), bf16),
        jax.ShapeDtypeStruct((D, tokens), f32),
        jax.ShapeDtypeStruct((D, 1), f32),
        jax.ShapeDtypeStruct((DEPTH, D, SLICE), bf16),
        jax.ShapeDtypeStruct((QUERY_HEADS, 128, tokens), bf16),
        jax.ShapeDtypeStruct(grads, bf16),
        jax.ShapeDtypeStruct(down.shape, bf16),
    ]
    out_specs = [VMEM] * 5 + [ANY] * 2
    inputs = [att, wo, x, ogt, gain, expand, down]
    in_specs = [VMEM] * 5 + [ANY] * 2
    scratch = [
        pltpu.VMEM((D, tokens), f32),
        pltpu.VMEM((1, tokens), f32),
        pltpu.VMEM((tokens, D), bf16),
        pltpu.VMEM((D, tokens), bf16),
        pltpu.VMEM((tokens, D), bf16),
        pltpu.VMEM((D, tokens), f32),
        pltpu.VMEM((D, tokens), f32),
        pltpu.VMEM((tokens, 4 * WIDTH), bf16),
        pltpu.VMEM((tokens, 4 * WIDTH), bf16),
        pltpu.VMEM((tokens, 4 * WIDTH), bf16),
        pltpu.VMEM((2, DEPTH, SLICE, 4 * WIDTH), bf16),
        pltpu.VMEM((2, DEPTH, SLICE, 4 * WIDTH), bf16),
        pltpu.VMEM((2, D, 4 * WIDTH), bf16),
        pltpu.VMEM((2, DEPTH, SLICE, 4 * WIDTH), bf16),
        pltpu.VMEM((D, 4 * WIDTH), bf16),
        pltpu.SemaphoreType.DMA((2, 3)),
        pltpu.SemaphoreType.DMA((2,)),
    ]
    if late:
        inputs.append(shard)
        in_specs.append(VMEM)
        shapes.append(jax.ShapeDtypeStruct((late,) + blocks, bf16))
        out_specs.append(ANY)
        scratch.append(pltpu.SemaphoreType.DMA((late, GATHER_SEMS)))
    if summed:
        shapes.append(jax.ShapeDtypeStruct((summed,) + blocks[2:], f32))
        out_specs.append(VMEM)
        pieces = [(0, k, (0, SLICE)) for k in range(summed)]
        term = jax.ShapeDtypeStruct(blocks, bf16)
        scratch += reduce_scratch(grid, [term], (False,), pieces)
    params = dict(collective_id=collective_id, has_side_effects=True) if late or summed else {}
    return pl.pallas_call(
        functools.partial(middle_kernel, grid, ready, summed),
        out_shape=shapes,
        in_specs=in_specs,
        out_specs=out_specs,
        scratch_shapes=scratch,
        compiler_params=pltpu.CompilerParams(vmem_limit_bytes=62 << 20, **params),
        name="middle",
    )(*inputs)


class GradChain:
    def __init__(self, here, part, sent, got, sems):
        self.h, self.part, self.sent, self.got, self.sems = here, part, sent, got, sems

    def summed(self, slot, g, write):
        h = self.h

        @pl.when(h.z < h.grid.nz - 1)
        def _():
            wait_bytes(self.got.at[slot, g], self.sems.at[1, slot, g])
            write(g, self.part[slot, g] + self.got[slot, g].astype(f32))

        @pl.when(h.z == h.grid.nz - 1)
        def _():
            write(g, self.part[slot, g])

    def relay(self, slot, g):
        h = self.h

        def write(g, value):
            self.sent[slot, g] = value.astype(bf16)

        self.summed(slot, g, write)
        to = lax.rem(h.z + h.grid.nz - 1, h.grid.nz)
        sems = self.sems
        send(self.sent.at[slot, g], self.got.at[slot, g], sems.at[0, slot, g], sems.at[1, slot, g], h.on_z(to))

    def drain(self):
        h = self.h

        def body(t, carry):
            slot, g = t // KEY_VALUE_HEADS, lax.rem(t, KEY_VALUE_HEADS)
            wait_bytes(self.sent.at[slot, g], self.sems.at[0, slot, g])
            return carry

        lax.fori_loop(0, h.z * KEY_VALUE_HEADS, body, 0)


def back_kernel(grid, z_majors, pieces, *refs):
    n = len(z_majors)
    terms, refs = refs[:n], refs[n:]
    qx, qn, dox, kv, kext, cos, sin = refs[:7]
    refs = refs[7:]
    results, refs = refs[:n], refs[n:]
    hd, refs = refs[0], refs[1:]
    here = Here(grid)
    jobs, refs = reduce_jobs(here, terms, results, refs, z_majors, pieces)
    don, kx, vx, kt, dq, part, sent, got, kv_sems = refs
    tokens = dox.shape[2]
    half = tokens // 2
    greet(here.peers())
    ticks = pipelined(jobs, len(jobs))
    for tick in ticks[: len(jobs)]:
        tick()
    ticks = ticks[len(jobs) :]

    def gather_queries(h, carry):
        dq[h] = jnp.zeros((HEAD, tokens), f32)
        don[h] = dox[h].astype(f32).T.astype(bf16)
        return carry

    lax.fori_loop(0, QUERY_HEADS, gather_queries, 0)

    def prepare(slot):
        ext = kext[pl.ds(pl.multiple_of(slot * tokens, 16), tokens)]

        def body(g, carry):
            block = kv[slot, g]
            low = lanes_below(block.shape, HEAD)
            kx[g] = jnp.where(low, block, ext)
            ones = jnp.where(lanes_below(block.shape, 3), 1.0, 0.0).astype(bf16)
            vx[g] = jnp.where(low, ones, block)
            kt[g] = block.astype(f32).T[:HEAD].astype(bf16)
            return carry

        lax.fori_loop(0, KEY_VALUE_HEADS, body, 0)

    def tile(g, h, count, k, masked):
        keys, cols = pl.ds(0, count), pl.ds(k * half, half)
        s = mm(kx[g, keys], qx[h, :, cols])
        if masked:
            row = lax.broadcasted_iota(jnp.int32, s.shape, 0)
            col = lax.broadcasted_iota(jnp.int32, s.shape, 1) + k * half
            s = jnp.where(row <= col, s, HIDE)
        p = jnp.exp(s)
        ds = (p * mm(vx[g, keys], dox[h, :, cols])).astype(bf16)
        dq[h, :, cols] += mm(kt[g, :, keys], ds)
        dk = mm(ds, qn[h, cols])
        dv = mm(p.astype(bf16), don[h, cols])
        return jnp.where(lanes_below(dk.shape, HEAD), dk, dv)

    def whole(slot, g):
        total = None
        for i in range(GROUP):
            for k in range(2):
                new = tile(g, g * GROUP + i, tokens, k, False)
                total = new if total is None else total + new
        part[slot, g] = total

    def diagonal(g):
        total = None
        for i in range(GROUP):
            new = tile(g, g * GROUP + i, tokens, 1, True)
            total = new if total is None else total + new
        part[here.z, g] = total
        total = part[here.z, g, pl.ds(0, half)]
        for i in range(GROUP):
            total += tile(g, g * GROUP + i, half, 0, True)
        part[here.z, g, pl.ds(0, half)] = total

    chain = GradChain(here, part, sent, got, kv_sems)
    micros = grid.nz * KEY_VALUE_HEADS
    top = here.z == grid.nz - 1

    def micro(t, carry):
        slot = t // KEY_VALUE_HEADS
        g = lax.rem(t, KEY_VALUE_HEADS)

        @pl.when(slot <= here.z)
        def _():
            pl.when(g == 0)(lambda: prepare(slot))

            @pl.when(slot < here.z)
            def _():
                whole(slot, g)
                pl.when(top)(lambda: chain.relay(slot, g))

            pl.when(slot == here.z)(lambda: diagonal(g))

        @pl.when(jnp.logical_and(jnp.logical_not(top), jnp.logical_and(slot >= 1, slot <= here.z)))
        def _():
            chain.relay(slot - 1, g)

        for k, tick in enumerate(ticks):
            pl.when(t == k * micros // len(ticks))(tick)
        return carry

    lax.fori_loop(0, micros, micro, 0)

    def turn_back(a, b):
        c, s = cos[...], sin[...]
        return a * c + b * s, b * c - a * s

    def queries(h, carry):
        scale = HEAD**-0.5
        a, b = turn_back(dq[h, pl.ds(0, 32)] * scale, dq[h, pl.ds(32, 32)] * scale)
        hd[pl.ds(pl.multiple_of(h * HEAD, 16), 32)] = a.astype(bf16)
        hd[pl.ds(pl.multiple_of(h * HEAD + 32, 16), 32)] = b.astype(bf16)
        return carry

    lax.fori_loop(0, QUERY_HEADS, queries, 0)

    def write(g, value):
        turned = value.T
        a, b = turn_back(turned[:32], turned[32:64])
        base = (QUERY_HEADS + g) * HEAD
        hd[pl.ds(pl.multiple_of(base, 16), 32)] = a.astype(bf16)
        hd[pl.ds(pl.multiple_of(base + 32, 16), 32)] = b.astype(bf16)
        base = (QUERY_HEADS + KEY_VALUE_HEADS + g) * HEAD
        hd[pl.ds(pl.multiple_of(base, 16), HEAD)] = turned[64:].astype(bf16)

    def close(g, carry):
        chain.summed(here.z, g, write)
        return carry

    lax.fori_loop(0, KEY_VALUE_HEADS, close, 0)
    chain.drain()
    for job in jobs:
        job.drain()


def back(grid, terms, z_majors, leads, qx, qn, dox, kv, kext, cos, sin, collective_id):
    tokens = dox.shape[2]
    n = len(terms)
    pieces = chunk_list(terms, leads)
    shapes = []
    for term, chosen in zip(terms, leads):
        lead = (term.shape[0],) if chosen else ()
        shapes.append(jax.ShapeDtypeStruct(lead + term.shape[-2:], f32))
    scratch = reduce_scratch(grid, terms, z_majors, pieces)
    shapes.append(jax.ShapeDtypeStruct((QKV, tokens), bf16))
    blocks = (grid.nz, KEY_VALUE_HEADS, tokens, 128)
    scratch += [
        pltpu.VMEM((QUERY_HEADS, tokens, 128), bf16),
        pltpu.VMEM((KEY_VALUE_HEADS, tokens, 128), bf16),
        pltpu.VMEM((KEY_VALUE_HEADS, tokens, 128), bf16),
        pltpu.VMEM((KEY_VALUE_HEADS, HEAD, tokens), bf16),
        pltpu.VMEM((QUERY_HEADS, HEAD, tokens), f32),
        pltpu.VMEM(blocks, f32),
        pltpu.VMEM((grid.nz - 1,) + blocks[1:], bf16),
        pltpu.VMEM(blocks, bf16),
        pltpu.SemaphoreType.DMA((2, grid.nz, KEY_VALUE_HEADS)),
    ]
    return pl.pallas_call(
        functools.partial(back_kernel, grid, tuple(z_majors), pieces),
        out_shape=shapes,
        in_specs=[ANY] * n + [VMEM] * 7,
        out_specs=[VMEM] * (n + 1),
        scratch_shapes=scratch,
        compiler_params=pltpu.CompilerParams(
            collective_id=collective_id, has_side_effects=True, vmem_limit_bytes=63 << 20
        ),
        name="back",
    )(*split_terms(grid, terms, z_majors), qx, qn, dox, kv, kext, cos, sin)


def adamw(weight, grad, first, second, rate, decay):
    first_new = beta_one * first + (1.0 - beta_one) * grad
    second_new = beta_two * second + (1.0 - beta_two) * grad * grad
    first_hat = first_new / (1.0 - beta_one**ADAM_STEP)
    second_hat = second_new / (1.0 - beta_two**ADAM_STEP)
    weight_new = weight - rate * (
        first_hat / (jnp.sqrt(second_hat) + adam_epsilon) + decay * weight
    )
    return (weight_new, first_new, second_new)


def finish_kernel(grid, pieces, *refs):
    hd, heads, x, gain, rg, gain_two, ig, gheads, ggains, h1, og, flat, wide, terms, value = refs[:15]
    here = Here(grid)
    greet(here.peers())
    jobs, refs = reduce_jobs(here, [terms], [gheads], refs[15:], (True,), pieces)
    share = Share(here, value, ggains, refs[:4], refs[4])
    tokens = x.shape[1]
    inverse = inverse_rms(x)
    for k in range(DEPTH):
        rows = pl.ds(k * SLICE, SLICE)
        h1[rows] = (x[rows].astype(f32) * inverse * gain[rows]).astype(bf16)
    rows = terms.shape[-2]
    for k in range(DEPTH):
        flat[...] = mm_nt(hd[...], h1[pl.ds(k * SLICE, SLICE)])
        for d in range(grid.nd):
            place = (k, d // (2 * grid.nx), d // 2 % grid.nx, d % 2)
            terms[place] = flat[pl.ds(d * rows, rows)].astype(bf16)
    ticks = pipelined(jobs, len(jobs))
    for tick in ticks[: len(jobs)]:
        tick()
    ticks = ticks[len(jobs) :]

    def turn(count=1):
        for _ in range(count):
            if ticks:
                ticks.pop(0)()

    for k in range(DEPTH):
        og[pl.ds(k * SLICE, SLICE)] = mm_tn(heads[k], hd[...])
        if k == 1:
            turn()
    turn()
    total = jnp.zeros((1, tokens), f32)
    for k in range(DEPTH):
        rows = pl.ds(k * SLICE, SLICE)
        normed = x[rows].astype(f32) * inverse
        column = jnp.sum(og[rows] * normed, axis=1, keepdims=True)
        place = lax.broadcasted_iota(jnp.int32, (SLICE, 128), 1)
        wide[rows] = jnp.where(place == 0, column, jnp.where(place == 1, gain_two[rows], 0.0))
        total += jnp.sum(og[rows] * gain[rows] * normed, axis=0, keepdims=True)
    value[...] = wide[...].T[:8]
    share.start(0)
    turn()
    mean = total * (1.0 / D)
    for k in range(DEPTH):
        rows = pl.ds(k * SLICE, SLICE)
        normed = x[rows].astype(f32) * inverse
        ig[rows] = rg[rows] + inverse * (og[rows] * gain[rows] - normed * mean)
    turn()
    for k in range(4):
        share.end(k)
        if k < 3:
            share.start(k + 1)
        turn(2)
    turn(len(ticks))
    share.drain()
    for job in jobs:
        job.drain()


def finish(grid, hd, heads, x, gain, rg, gain_two, collective_id):
    tokens = x.shape[1]
    rows = QKV // grid.nd
    term = jax.ShapeDtypeStruct((rows, SLICE), bf16)
    pieces = chunk_list([term])
    scratch = [
        pltpu.VMEM((D, tokens), bf16),
        pltpu.VMEM((D, tokens), f32),
        pltpu.VMEM((QKV, SLICE), f32),
        pltpu.VMEM((D, 128), f32),
        pltpu.VMEM((grid.nz, grid.ny, grid.nx, 2, rows, SLICE), bf16),
        pltpu.VMEM((8, D), f32),
    ]
    scratch += reduce_scratch(grid, [term], (True,), pieces)
    scratch += Share.scratch(grid, (8, D))
    scratch.append(pltpu.SemaphoreType.DMA((SHARE_SEMS,)))
    return pl.pallas_call(
        functools.partial(finish_kernel, grid, pieces),
        out_shape=[
            jax.ShapeDtypeStruct((D, tokens), f32),
            jax.ShapeDtypeStruct((rows, SLICE), f32),
            jax.ShapeDtypeStruct((8, D), f32),
        ],
        in_specs=[VMEM] * 6,
        out_specs=[VMEM] * 3,
        scratch_shapes=scratch,
        compiler_params=pltpu.CompilerParams(
            collective_id=collective_id, has_side_effects=True, vmem_limit_bytes=62 << 20
        ),
        name="finish",
    )(hd, heads, x, gain, rg, gain_two)


READY = 3
SUMMED = 1


def local(
    grid,
    hidden_in,
    out_grad,
    seg_ids,
    doc_start,
    norm_gains,
    heads_weight,
    output_weight,
    expand_weight,
    down_weight,
    gains_first,
    gains_second,
    heads_first,
    heads_second,
    output_first,
    output_second,
    expand_first,
    expand_second,
    down_first,
    down_second,
):
    tokens = hidden_in.shape[0]
    first_row = lax.axis_index("shard") * tokens
    positions = first_row + jnp.arange(tokens, dtype=jnp.int32)
    freq = jnp.power(10000.0, -jnp.arange(HEAD // 2).astype(f32) / (HEAD // 2))
    angle = (positions - doc_start).astype(f32)[None, :] * freq[:, None]
    cos, sin = jnp.cos(angle), jnp.sin(angle)
    seg_row = seg_ids[0]
    seg_query = lax.dynamic_slice_in_dim(seg_row, first_row, tokens)
    doc = jnp.arange(HEAD, dtype=jnp.int32)
    qext = jnp.where((doc[:, None] < DOCS) & (seg_query[None, :] == doc[:, None]), HIDE, 0.0).astype(bf16)
    lane = jnp.arange(128, dtype=jnp.int32) - HEAD
    other_doc = (lane[None, :] >= 0) & (lane[None, :] < DOCS) & (seg_row[:, None] != lane[None, :])
    kext = jnp.where(other_doc | ((lane >= DOCS) & (lane < DOCS + 3))[None, :], 1.0, 0.0).astype(bf16)
    x, ogt = hidden_in.T, out_grad.T
    gain_one, gain_two = norm_gains[0][:, None], norm_gains[1][:, None]

    (heads_stack,) = gather_weights(grid, [heads_weight.astype(bf16).T], (True,), 1)
    heads = heads_stack.reshape(DEPTH, QKV, SLICE)
    expand_half = expand_weight.astype(bf16)
    stepped = expand_half.shape[1] == STEPS * WIDTH
    if stepped:
        shard = expand_half.reshape(SLICE, STEPS, WIDTH).transpose(1, 0, 2)
        leads = [None, None, list(range(READY))]
    else:
        shard, leads = expand_half, [None, None, None]
    shards = [output_weight.astype(bf16).T, down_weight.astype(bf16).T, shard]
    output_stack, down_stack, expand_stack, qx, qn, kv, att = front(
        grid, shards, (True, True, False), leads, heads, x, gain_one, cos, sin, qext, kext, 2
    )
    wo = output_stack.reshape(DEPTH, D, SLICE)
    down = down_stack.reshape(DEPTH, D, FF // DEPTH)
    blocks = (8, DEPTH, SLICE)
    if stepped:
        late = middle(grid, att, wo, x, ogt, gain_two, expand_stack, down, shard, SUMMED, 5)
        out, rg, gain_two_term, dwo, dox, dexpand, ddn, _, early_exp = late
    else:
        expand = expand_stack.transpose(1, 2, 0, 3).reshape(DEPTH, SLICE, 8, STEPS, WIDTH)
        expand = expand.transpose(3, 2, 0, 1, 4)
        out, rg, gain_two_term, dwo, dox, dexpand, ddn = middle(
            grid, att, wo, x, ogt, gain_two, expand, down, None, 0, 5
        )
        early_exp = None
        dexpand = dexpand.transpose(2, 3, 1, 0, 4).reshape(DEPTH, SLICE, grid.nd, -1).transpose(2, 0, 1, 3)
    if stepped:
        dexpand = dexpand.reshape((STEPS, grid.nd, grid.nz, SLICE, WIDTH))
    terms = [ddn.reshape(down_stack.shape), dexpand, dwo.reshape(output_stack.shape)]
    leads = [None, list(range(SUMMED, STEPS)) if stepped else None, None]
    down_grad, late_exp, output_grad, hd = back(
        grid, terms, (True, False, True), leads, qx, qn, dox, kv, kext, cos, sin, 3
    )
    ig, heads_grad, gains_grad = finish(grid, hd, heads, x, gain_one, rg, gain_two_term, 4)
    if stepped:
        steps = [(early_exp if k < SUMMED else late_exp)[k] for k in range(STEPS)]
        expand_grad = jnp.concatenate(steps, axis=1)
    else:
        expand_grad = late_exp
    heads_grad, output_grad, down_grad, gains_grad = heads_grad.T, output_grad.T, down_grad.T, gains_grad[:2]
    hidden_out, input_grad = out.T, ig.T
    gains_new, gains_first_new, gains_second_new = adamw(
        norm_gains, gains_grad, gains_first, gains_second, gain_rate, 0.0
    )
    heads_new, heads_first_new, heads_second_new = adamw(
        heads_weight, heads_grad, heads_first, heads_second, matrix_rate, decay_rate
    )
    output_new, output_first_new, output_second_new = adamw(
        output_weight, output_grad, output_first, output_second, output_rate, decay_rate
    )
    expand_new, expand_first_new, expand_second_new = adamw(
        expand_weight, expand_grad, expand_first, expand_second, matrix_rate, decay_rate
    )
    down_new, down_first_new, down_second_new = adamw(
        down_weight, down_grad, down_first, down_second, matrix_rate, decay_rate
    )
    return (
        hidden_out,
        input_grad,
        gains_grad,
        heads_grad,
        output_grad,
        expand_grad,
        down_grad,
        gains_new,
        heads_new,
        output_new,
        expand_new,
        down_new,
        gains_first_new,
        gains_second_new,
        heads_first_new,
        heads_second_new,
        output_first_new,
        output_second_new,
        expand_first_new,
        expand_second_new,
        down_first_new,
        down_second_new,
    )


def solution(mesh):
    return jax.shard_map(
        functools.partial(local, Grid(mesh)),
        mesh=mesh,
        in_specs=(
            P(("dp", "shard"), None),
            P(("dp", "shard"), None),
            P("dp", None),
            P(("dp", "shard")),
            P(),
            P("shard", "dp"),
            P("shard", "dp"),
            P("shard", "dp"),
            P("shard", "dp"),
            P(),
            P(),
            P("shard", "dp"),
            P("shard", "dp"),
            P("shard", "dp"),
            P("shard", "dp"),
            P("shard", "dp"),
            P("shard", "dp"),
            P("shard", "dp"),
            P("shard", "dp"),
        ),
        out_specs=(
            P(("dp", "shard"), None),
            P(("dp", "shard"), None),
            P(),
            P("shard", "dp"),
            P("shard", "dp"),
            P("shard", "dp"),
            P("shard", "dp"),
            P(),
            P("shard", "dp"),
            P("shard", "dp"),
            P("shard", "dp"),
            P("shard", "dp"),
            P(),
            P(),
            P("shard", "dp"),
            P("shard", "dp"),
            P("shard", "dp"),
            P("shard", "dp"),
            P("shard", "dp"),
            P("shard", "dp"),
            P("shard", "dp"),
            P("shard", "dp"),
        ),
        check_vma=False,
    )
```

```python
import functools
import math

import jax
import jax.numpy as jnp
from jax import lax
from jax.experimental import pallas as pl
from jax.experimental.pallas import tpu as pltpu
from jax.sharding import PartitionSpec as P

MESH = pl.DeviceIdType.MESH
ANY = pl.BlockSpec(memory_space=pl.ANY)
VMEM = pl.BlockSpec(memory_space=pltpu.VMEM)


class Grid:
    def __init__(self, mesh):
        self.nd = mesh.shape["dp"]
        self.nz = mesh.shape["shard"]
        self.nx = math.isqrt(self.nd // 2)
        self.ny = self.nd // 2 // self.nx
        assert self.nx == self.ny and self.nx * self.ny * 2 == self.nd

    def dp(self, y, x, c):
        return (y * self.nx + x) * 2 + c


class Here:
    def __init__(self, grid):
        self.grid = grid
        d = lax.axis_index("dp")
        self.z = lax.axis_index("shard")
        self.d = d
        self.c = lax.rem(d, 2)
        self.x = lax.rem(d // 2, grid.nx)
        self.y = d // (2 * grid.nx)
        g = grid
        self.xs = [lax.rem(self.x + k, g.nx) for k in range(1, g.nx)]
        self.ys = [lax.rem(self.y + k, g.ny) for k in range(1, g.ny)]
        self.zs = [lax.rem(self.z + k, g.nz) for k in range(1, g.nz)]
        self.partner = (g.dp(self.y, self.x, 1 - self.c), self.z)

    def on_x(self, x):
        return (self.grid.dp(self.y, x, self.c), self.z)

    def on_y(self, y):
        return (self.grid.dp(y, self.x, self.c), self.z)

    def on_z(self, z):
        return (self.d, z)

    def peers(self):
        return (
            [self.partner]
            + [self.on_x(x) for x in self.xs]
            + [self.on_y(y) for y in self.ys]
            + [self.on_z(z) for z in self.zs]
        )


def greet(peers):
    barrier = pltpu.get_barrier_semaphore()
    for peer in peers:
        pl.semaphore_signal(barrier, inc=1, device_id=peer, device_id_type=MESH)
    pl.semaphore_wait(barrier, len(peers))


def send(src, dst, send_sem, recv_sem, device):
    pltpu.make_async_remote_copy(
        src_ref=src,
        dst_ref=dst,
        send_sem=send_sem,
        recv_sem=recv_sem,
        device_id=device,
        device_id_type=MESH,
    ).start()


def wait_bytes(ref, sem):
    pltpu.make_async_copy(ref, ref, sem).wait()


def half_rows(rows):
    return max(16, int(rows / 32 + 0.5) * 16)


def chunks_of(rows, size=64):
    starts = list(range(0, rows, size))
    if len(starts) > 1 and rows - starts[-1] < size // 2:
        starts.pop()
    return [(start, stop - start) for start, stop in zip(starts, starts[1:] + [rows])]


class Gather:
    def __init__(self, here, shard, out, sems, z_major, rows):
        self.h, self.shard, self.out, self.sems, self.z_major = here, shard, out, sems, z_major
        self.start, self.rows = rows
        self.cut = half_rows(self.rows)

    def span(self, half=None):
        if half is None:
            return pl.ds(self.start, self.rows)
        return pl.ds(self.start, self.cut) if half == 0 else pl.ds(self.start + self.cut, self.rows - self.cut)

    def column(self, d, half=None):
        return self.out.at[:, d, self.span(half)] if self.z_major else self.out.at[d, :, self.span(half)]

    def block(self, d, z):
        return self.out.at[z, d, self.span()] if self.z_major else self.out.at[d, z, self.span()]

    def columns(self, count):
        some = pl.ds(0, count)
        return self.out.at[:, some, self.span()] if self.z_major else self.out.at[some, :, self.span()]

    def blocks(self, count):
        some = pl.ds(0, count)
        return self.out.at[some, 0, self.span()] if self.z_major else self.out.at[0, some, self.span()]

    def own(self):
        h = self.h
        return pltpu.make_async_copy(self.shard.at[self.span()], self.block(h.d, h.z), self.sems.at[8])

    def stage_z(self):
        h, s = self.h, self.sems
        for z in h.zs:
            send(self.shard.at[self.span()], self.block(h.d, h.z), s.at[0], s.at[1], h.on_z(z))
        self.own().start()

    def await_z(self):
        wait_bytes(self.blocks(len(self.h.zs)), self.sems.at[1])

    def drain_z(self):
        wait_bytes(self.blocks(len(self.h.zs)), self.sems.at[0])

    def stage_one(self):
        h, s = self.h, self.sems
        self.await_z()
        self.own().wait()
        for x in h.xs:
            send(self.column(h.d, 0), self.column(h.d, 0), s.at[2], s.at[3], h.on_x(x))
        for y in h.ys:
            send(self.column(h.d, 1), self.column(h.d, 1), s.at[2], s.at[3], h.on_y(y))
        send(self.column(h.d), self.column(h.d), s.at[6], s.at[7], h.partner)

    def stage_two(self):
        h, s, g = self.h, self.sems, self.h.grid
        wait_bytes(self.columns(len(h.xs)), s.at[3])
        for y in h.ys:
            for x in [h.x] + h.xs:
                col = self.column(g.dp(h.y, x, h.c), 0)
                send(col, col, s.at[4], s.at[5], h.on_y(y))
        for x in h.xs:
            for y in [h.y] + h.ys:
                col = self.column(g.dp(y, h.x, h.c), 1)
                send(col, col, s.at[4], s.at[5], h.on_x(x))
        for x in h.xs:
            col = self.column(g.dp(h.y, x, h.c), 0)
            send(col, col, s.at[6], s.at[7], h.partner)
        for y in h.ys:
            col = self.column(g.dp(y, h.x, h.c), 1)
            send(col, col, s.at[6], s.at[7], h.partner)

    def stage_three(self):
        h, s, g = self.h, self.sems, self.h.grid
        wait_bytes(self.columns(g.nx * len(h.ys)), s.at[5])
        for y in h.ys:
            for x in [h.x] + h.xs:
                col = self.column(g.dp(y, x, h.c), 0)
                send(col, col, s.at[6], s.at[7], h.partner)
        for x in h.xs:
            for y in [h.y] + h.ys:
                col = self.column(g.dp(y, x, h.c), 1)
                send(col, col, s.at[6], s.at[7], h.partner)

    def arrive(self):
        g = self.h.grid
        wait_bytes(self.columns(g.nd // 2), self.sems.at[7])

    def drain(self):
        h, s, g = self.h, self.sems, self.h.grid
        self.drain_z()
        wait_bytes(self.columns(len(h.xs)), s.at[2])
        wait_bytes(self.columns(g.nx * len(h.ys)), s.at[4])
        wait_bytes(self.columns(g.nd // 2), s.at[6])

    stages = ("stage_z", "stage_one", "stage_two", "stage_three")


class ColumnGather(Gather):
    def own(self):
        return pltpu.make_async_copy(self.shard.at[:, self.span()], self.column(self.h.d), self.sems.at[8])

    def stage_z(self):
        self.own().start()

    def await_z(self):
        pass

    def drain_z(self):
        pass


class Spread:
    def __init__(self, here, shard, out, sems):
        self.h, self.shard, self.out, self.sems = here, shard, out, sems

    def own(self):
        return pltpu.make_async_copy(self.shard, self.out.at[self.h.z], self.sems.at[2])

    def begin(self):
        h, s = self.h, self.sems
        for z in h.zs:
            send(self.shard, self.out.at[h.z], s.at[0], s.at[1], h.on_z(z))
        self.own().start()

    def end(self):
        some = self.out.at[pl.ds(0, len(self.h.zs))]
        wait_bytes(some, self.sems.at[1])
        wait_bytes(some, self.sems.at[0])
        self.own().wait()


def pipelined(jobs, ahead=0):
    ticks = [getattr(job, job.stages[0]) for job in jobs[:ahead]]
    depth = max((len(job.stages) for job in jobs), default=0)
    for step in range(len(jobs) + depth - 1):
        for k in range(depth):
            i = step - k
            if 0 <= i < len(jobs) and k < len(jobs[i].stages) and not (k == 0 and i < ahead):
                ticks.append(getattr(jobs[i], jobs[i].stages[k]))
    return ticks


def chunk_list(shards, leads=None):
    pieces = []
    for i, shard in enumerate(shards):
        if leads is not None and leads[i]:
            pieces += [(i, k, (0, shard.shape[-2])) for k in leads[i]]
        else:
            pieces += [(i, None, rows) for rows in chunks_of(shard.shape[-2])]
    return pieces


def piece_of(ref, lead):
    return ref if lead is None else ref.at[lead]


def gather_jobs(here, shards, outs, sems, z_majors, pieces):
    jobs = []
    for k, (i, lead, rows) in enumerate(pieces):
        kind = ColumnGather if lead is None and len(shards[i].shape) == 3 else Gather
        job = kind(here, piece_of(shards[i], lead), piece_of(outs[i], lead), sems.at[k], z_majors[i], rows)
        jobs.append(job)
    return jobs


GATHER_SEMS = 9


def gather_kernel(grid, z_majors, pieces, spreads, *refs):
    n = len(z_majors)
    shards, refs = refs[:n], refs[n:]
    singles, refs = refs[:spreads], refs[spreads:]
    outs, refs = refs[:n], refs[n:]
    columns, refs = refs[:spreads], refs[spreads:]
    sems, spread_sems = refs
    here = Here(grid)
    greet(here.peers())
    jobs = gather_jobs(here, shards, outs, sems, z_majors, pieces)
    ticks = pipelined(jobs, len(jobs))
    for tick in ticks[: len(jobs)]:
        tick()
    others = [Spread(here, singles[k], columns[k], spread_sems.at[k]) for k in range(spreads)]
    for other in others:
        other.begin()
    for tick in ticks[len(jobs) :]:
        tick()
    for job in jobs:
        job.arrive()
        job.drain()
    for other in others:
        other.end()


def gather_weights(grid, shards, z_majors, singles, collective_id):
    shapes = []
    for shard, z_major in zip(shards, z_majors):
        lead = (grid.nz, grid.nd) if z_major else (grid.nd, grid.nz)
        shapes.append(jax.ShapeDtypeStruct(lead + shard.shape, shard.dtype))
    for single in singles:
        shapes.append(jax.ShapeDtypeStruct((grid.nz,) + single.shape, single.dtype))
    pieces = chunk_list(shards)
    return pl.pallas_call(
        functools.partial(gather_kernel, grid, tuple(z_majors), pieces, len(singles)),
        out_shape=shapes,
        in_specs=[VMEM] * (len(shards) + len(singles)),
        out_specs=[ANY] * len(shapes),
        scratch_shapes=[
            pltpu.SemaphoreType.DMA((len(pieces), GATHER_SEMS)),
            pltpu.SemaphoreType.DMA((len(singles), 3)),
        ],
        compiler_params=pltpu.CompilerParams(collective_id=collective_id, has_side_effects=True),
        name="gather_weights",
    )(*shards, *singles)


class Reduce:
    def __init__(self, here, terms, result, bufs, sems, z_major, rows):
        self.h, self.terms, self.result, self.sems, self.z_major = here, terms, result, sems, z_major
        self.own, self.other, self.one_a, self.one_b, self.two_a, self.two_b, self.last = bufs
        self.start, self.rows = rows
        self.cut = half_rows(self.rows)

    @staticmethod
    def scratch(grid, rows, cols, z_major):
        cut = half_rows(rows)
        ny, nx, nz = grid.ny, grid.nx, grid.nz
        full = (nz, ny, nx) if z_major else (ny, nx, nz)
        row = (nz, nx) if z_major else (nx, nz)
        bf = jnp.bfloat16
        return [
            pltpu.VMEM(full + (rows, cols), bf),
            pltpu.VMEM(full + (rows, cols), bf),
            pltpu.VMEM((ny,) + row + (cut, cols), bf),
            pltpu.VMEM((nx,) + row + (rows - cut, cols), bf),
            pltpu.VMEM((nx, nz, cut, cols), bf),
            pltpu.VMEM((ny, nz, rows - cut, cols), bf),
            pltpu.VMEM((nz, rows, cols), bf),
        ]

    def span(self, half):
        return {None: slice(None), 0: pl.ds(0, self.cut), 1: pl.ds(self.cut, self.rows - self.cut)}[half]

    def at(self, y, x, z, half):
        y, x, z = (slice(None) if v is None else v for v in (y, x, z))
        return (z, y, x, self.span(half)) if self.z_major else (y, x, z, self.span(half))

    def side(self, c):
        rows = pl.ds(self.start, self.rows)
        return self.terms.at[:, :, :, c, rows] if self.z_major else self.terms.at[:, :, c, :, rows]

    def load(self):
        return pltpu.make_async_copy(self.side(self.h.c), self.own, self.sems.at[8])

    def stage_core(self):
        h, s = self.h, self.sems
        send(self.side(1 - h.c), self.other, s.at[0], s.at[1], h.partner)
        self.load().start()

    def add_loop(self, shape, body):
        total = math.prod(shape)

        def step(i, carry):
            place = []
            rest = i
            for size in reversed(shape):
                place.append(lax.rem(rest, size))
                rest = rest // size
            body(tuple(reversed(place)))
            return carry

        lax.fori_loop(0, total, step, 0)

    def stage_one(self):
        h, s, g = self.h, self.sems, self.h.grid
        self.load().wait()
        wait_bytes(self.other, s.at[1])

        def body(place):
            self.own[place] = self.own[place] + self.other[place]

        self.add_loop(self.own.shape[:3], body)
        for y in h.ys:
            send(self.own.at[self.at(y, None, None, 0)], self.one_a.at[h.y], s.at[2], s.at[3], h.on_y(y))
        for x in h.xs:
            send(self.own.at[self.at(None, x, None, 1)], self.one_b.at[h.x], s.at[9], s.at[10], h.on_x(x))

    def stage_two(self):
        h, s, g = self.h, self.sems, self.h.grid
        wait_bytes(self.one_a.at[pl.ds(0, g.ny - 1)], s.at[3])
        wait_bytes(self.one_b.at[pl.ds(0, g.nx - 1)], s.at[10])

        def body_a(place):
            where = (place[1], place[0]) if self.z_major else place
            spot = self.at(h.y, where[0], where[1], 0)
            total = self.own[spot].astype(jnp.float32)
            for y in h.ys:
                total += self.one_a[(y,) + place].astype(jnp.float32)
            self.own[spot] = total.astype(jnp.bfloat16)

        self.add_loop(self.one_a.shape[1:3], body_a)

        def body_b(place):
            where = (place[1], place[0]) if self.z_major else place
            spot = self.at(where[0], h.x, where[1], 1)
            total = self.own[spot].astype(jnp.float32)
            for x in h.xs:
                total += self.one_b[(x,) + place].astype(jnp.float32)
            self.own[spot] = total.astype(jnp.bfloat16)

        self.add_loop(self.one_b.shape[1:3], body_b)
        for x in h.xs:
            send(self.own.at[self.at(h.y, x, None, 0)], self.two_a.at[h.x], s.at[4], s.at[5], h.on_x(x))
        for y in h.ys:
            send(self.own.at[self.at(y, h.x, None, 1)], self.two_b.at[h.y], s.at[11], s.at[12], h.on_y(y))

    def stage_three(self):
        h, s, g = self.h, self.sems, self.h.grid
        wait_bytes(self.two_a.at[pl.ds(0, g.nx - 1)], s.at[5])
        wait_bytes(self.two_b.at[pl.ds(0, g.ny - 1)], s.at[12])

        def body(place):
            (z,) = place
            spot = self.at(h.y, h.x, z, 0)
            total = self.own[spot].astype(jnp.float32)
            for x in h.xs:
                total += self.two_a[x, z].astype(jnp.float32)
            self.own[spot] = total.astype(jnp.bfloat16)
            spot = self.at(h.y, h.x, z, 1)
            total = self.own[spot].astype(jnp.float32)
            for y in h.ys:
                total += self.two_b[y, z].astype(jnp.float32)
            self.own[spot] = total.astype(jnp.bfloat16)

        self.add_loop((g.nz,), body)
        for z in h.zs:
            send(self.own.at[self.at(h.y, h.x, z, None)], self.last.at[h.z], s.at[6], s.at[7], h.on_z(z))

    def finish(self):
        h, s, g = self.h, self.sems, self.h.grid
        wait_bytes(self.last.at[pl.ds(0, g.nz - 1)], s.at[7])
        total = self.own[self.at(h.y, h.x, h.z, None)].astype(jnp.float32)
        for z in h.zs:
            total += self.last[z].astype(jnp.float32)
        self.result[pl.ds(self.start, self.rows)] = total

    stages = ("stage_core", "stage_one", "stage_two", "stage_three", "finish")

    def drain_z(self):
        wait_bytes(self.last.at[pl.ds(0, self.h.grid.nz - 1)], self.sems.at[6])

    def drain(self):
        g, s = self.h.grid, self.sems
        wait_bytes(self.other, s.at[0])
        wait_bytes(self.one_a.at[pl.ds(0, g.ny - 1)], s.at[2])
        wait_bytes(self.one_b.at[pl.ds(0, g.nx - 1)], s.at[9])
        wait_bytes(self.two_a.at[pl.ds(0, g.nx - 1)], s.at[4])
        wait_bytes(self.two_b.at[pl.ds(0, g.ny - 1)], s.at[11])
        self.drain_z()


class ColumnReduce(Reduce):
    stages = ("stage_core", "stage_one", "stage_two", "stage_three")

    def stage_three(self):
        h, s, g = self.h, self.sems, self.h.grid
        wait_bytes(self.two_a.at[pl.ds(0, g.nx - 1)], s.at[5])
        wait_bytes(self.two_b.at[pl.ds(0, g.ny - 1)], s.at[12])

        def body(place):
            (z,) = place
            total = self.own[self.at(h.y, h.x, z, 0)].astype(jnp.float32)
            for x in h.xs:
                total += self.two_a[x, z].astype(jnp.float32)
            self.result[z, pl.ds(self.start, self.cut)] = total.astype(jnp.bfloat16)
            total = self.own[self.at(h.y, h.x, z, 1)].astype(jnp.float32)
            for y in h.ys:
                total += self.two_b[y, z].astype(jnp.float32)
            self.result[z, pl.ds(self.start + self.cut, self.rows - self.cut)] = total.astype(jnp.bfloat16)

        self.add_loop((g.nz,), body)

    def drain_z(self):
        pass


class Collect:
    def __init__(self, here, column, last, sems):
        self.h, self.column, self.last, self.sems = here, column, last, sems

    def begin(self):
        h, s = self.h, self.sems
        for z in h.zs:
            send(self.column.at[z], self.last.at[h.z], s.at[0], s.at[1], h.on_z(z))

    def end(self):
        h = self.h
        wait_bytes(self.last.at[pl.ds(0, len(h.zs))], self.sems.at[1])
        total = self.column[h.z].astype(jnp.float32)
        for z in h.zs:
            total += self.last[z].astype(jnp.float32)
        return total

    def drain(self):
        wait_bytes(self.last.at[pl.ds(0, len(self.h.zs))], self.sems.at[0])


REDUCE_SEMS = 13
REDUCE_BUFS = 7


class Share:
    def __init__(self, here, value, result, bufs, sems):
        self.h, self.value, self.result, self.sems = here, value, result, sems
        self.bufs = bufs

    @staticmethod
    def scratch(grid, shape):
        return [pltpu.VMEM((n,) + shape, jnp.float32) for n in (2, grid.nx, grid.ny, grid.nz)]

    def axis(self, k):
        h = self.h
        return (
            (h.c, [h.partner], 2),
            (h.x, [h.on_x(x) for x in h.xs], h.grid.nx),
            (h.y, [h.on_y(y) for y in h.ys], h.grid.ny),
            (h.z, [h.on_z(z) for z in h.zs], h.grid.nz),
        )[k]

    def start(self, k):
        me, peers, n = self.axis(k)
        self.bufs[k][me] = self.value[...] if k == 0 else self.total
        for peer in peers:
            send(self.bufs[k].at[me], self.bufs[k].at[me], self.sems.at[2 * k], self.sems.at[2 * k + 1], peer)

    def end(self, k):
        me, peers, n = self.axis(k)
        wait_bytes(self.bufs[k].at[pl.ds(0, n - 1)], self.sems.at[2 * k + 1])
        total = self.bufs[k][0]
        for i in range(1, n):
            total = total + self.bufs[k][i]
        self.total = total
        if k == 3:
            self.result[...] = total

    def drain(self):
        for k in range(4):
            n = self.axis(k)[2]
            wait_bytes(self.bufs[k].at[pl.ds(0, n - 1)], self.sems.at[2 * k])


SHARE_SEMS = 8


def reduce_kernel(grid, z_majors, pieces, shared, *refs):
    n = len(z_majors)
    terms, refs = refs[:n], refs[n:]
    value, refs = (refs[0], refs[1:]) if shared else (None, refs)
    results, refs = refs[:n], refs[n:]
    value_sum, refs = (refs[0], refs[1:]) if shared else (None, refs)
    here = Here(grid)
    greet(here.peers())
    jobs, refs = reduce_jobs(here, terms, results, refs, z_majors, pieces)
    share = None
    if shared:
        share = Share(here, value, value_sum, refs[:4], refs[4])
        share.start(0)
    ticks = pipelined(jobs, len(jobs))
    for k, tick in enumerate(ticks):
        tick()
        if share is not None and k >= len(jobs) and k - len(jobs) < 4:
            step = k - len(jobs)
            share.end(step)
            if step < 3:
                share.start(step + 1)
    if share is not None:
        share.drain()
    for job in jobs:
        job.drain()


def reduce_jobs(here, terms, results, refs, z_majors, pieces):
    n = len(pieces)
    sems = refs[n * REDUCE_BUFS]
    jobs = []
    for k, (i, lead, rows) in enumerate(pieces):
        bufs = refs[k * REDUCE_BUFS : (k + 1) * REDUCE_BUFS]
        term, result, kind = piece_of(terms[i], lead), results[i], Reduce
        deep = len(result.shape) == 3
        if lead is None:
            kind = ColumnReduce if deep else Reduce
        else:
            width = term.shape[-1]
            result = result.at[lead] if deep else result.at[:, pl.ds(lead * width, width)]
        jobs.append(kind(here, term, result, bufs, sems.at[k], z_majors[i], rows))
    return jobs, refs[n * REDUCE_BUFS + 1 :]


def reduce_scratch(grid, terms, z_majors, pieces):
    scratch = []
    for i, _, (_, rows) in pieces:
        scratch += Reduce.scratch(grid, rows, terms[i].shape[-1], z_majors[i])
    return scratch + [pltpu.SemaphoreType.DMA((max(len(pieces), 1), REDUCE_SEMS))]


def split_terms(grid, terms, z_majors):
    split = []
    for term, z_major in zip(terms, z_majors):
        lead = (grid.ny, grid.nx, 2)
        lead = (grid.nz,) + lead if z_major else lead + (grid.nz,)
        split.append(term.reshape(term.shape[:-4] + lead + term.shape[-2:]))
    return split


def reduce_grads(grid, terms, z_majors, value, collective_id):
    shapes = [jax.ShapeDtypeStruct(term.shape[-2:], jnp.float32) for term in terms]
    pieces = chunk_list(terms)
    scratch = reduce_scratch(grid, terms, z_majors, pieces)
    n = len(terms)
    shared = value is not None
    if shared:
        shapes.append(jax.ShapeDtypeStruct(value.shape, jnp.float32))
        scratch += Share.scratch(grid, value.shape)
        scratch.append(pltpu.SemaphoreType.DMA((SHARE_SEMS,)))
    return pl.pallas_call(
        functools.partial(reduce_kernel, grid, tuple(z_majors), pieces, shared),
        out_shape=shapes,
        in_specs=[ANY] * n + [VMEM] * shared,
        out_specs=[VMEM] * len(shapes),
        scratch_shapes=scratch,
        compiler_params=pltpu.CompilerParams(
            collective_id=collective_id, has_side_effects=True, vmem_limit_bytes=62 << 20
        ),
        name="reduce_grads",
    )(*split_terms(grid, terms, z_majors), *([value] if shared else []))


D = 960
QUERY_HEADS = 15
KEY_VALUE_HEADS = 5
GROUP = QUERY_HEADS // KEY_VALUE_HEADS
HEAD = 64
FF = 2560
QKV = (QUERY_HEADS + 2 * KEY_VALUE_HEADS) * HEAD
ADAM_STEP = 10
DOCS = 16
HIDE = -1e30
VALUE_SCALE = 2.0**-9

norm_epsilon = 1e-05
beta_one = 0.9
beta_two = 0.95
adam_epsilon = 1e-08
matrix_rate = 0.03
output_rate = 0.15
gain_rate = 0.5
decay_rate = 0.1

f32 = jnp.float32
bf16 = jnp.bfloat16
DEPTH = 4
SLICE = D // DEPTH


def mm(a, b):
    return lax.dot_general(a, b, (((1,), (0,)), ((), ())), preferred_element_type=f32)


def mm_nt(a, b):
    return lax.dot_general(a, b, (((1,), (1,)), ((), ())), preferred_element_type=f32)


def mm_tn(a, b):
    return lax.dot_general(a, b, (((0,), (0,)), ((), ())), preferred_element_type=f32)


def lanes_below(shape, n):
    return lax.broadcasted_iota(jnp.int32, shape, len(shape) - 1) < n


def inverse_rms(ref):
    total = jnp.zeros((1, ref.shape[1]), f32)
    for k in range(DEPTH):
        x = ref[pl.ds(k * SLICE, SLICE)].astype(f32)
        total += jnp.sum(x * x, axis=0, keepdims=True)
    return lax.rsqrt(total * (1.0 / D) + norm_epsilon)


def three_pieces(row):
    hi = row.astype(bf16).astype(f32)
    mid = (row - hi).astype(bf16).astype(f32)
    low = row - hi - mid
    place = lax.broadcasted_iota(jnp.int32, (16, row.shape[1]), 0)
    block = jnp.where(place == 0, hi, jnp.where(place == 1, mid, jnp.where(place == 2, low, 0.0)))
    return block.astype(bf16)


class KeyChain:
    def __init__(self, here, kv, sems):
        self.h, self.kv, self.sems = here, kv, sems

    def up(self, slot):
        h = self.h
        to = lax.rem(h.z + 1, h.grid.nz)

        @pl.when(h.z < h.grid.nz - 1)
        def _():
            send(self.kv.at[slot], self.kv.at[slot], self.sems.at[0, slot], self.sems.at[1, slot], h.on_z(to))

    def take(self, slot):
        wait_bytes(self.kv.at[slot], self.sems.at[1, slot])
        self.up(slot)

    def drain(self):
        h = self.h
        for s in range(h.grid.nz):

            @pl.when(jnp.logical_and(h.z >= s, h.z < h.grid.nz - 1))
            def _():
                wait_bytes(self.kv.at[h.z - s], self.sems.at[0, h.z - s])


def front_kernel(grid, z_majors, pieces, *refs):
    n = len(z_majors)
    shards, refs = refs[:n], refs[n:]
    heads, x, gain, cos, sin, qext, kext = refs[:7]
    refs = refs[7:]
    outs, refs = refs[:n], refs[n:]
    qx, qn, kv, att = refs[:4]
    h1, proj, kx, vt, acc, sems, kv_sems = refs[4:]
    here = Here(grid)
    tokens = x.shape[1]
    half = tokens // 2
    greet(here.peers())
    jobs = gather_jobs(here, shards, outs, sems, z_majors, pieces)
    ticks = pipelined(jobs, 3)
    for tick in ticks[:3]:
        tick()

    inverse = inverse_rms(x)
    for k in range(DEPTH):
        rows = pl.ds(k * SLICE, SLICE)
        h1[rows] = (x[rows].astype(f32) * inverse * gain[rows]).astype(bf16)

    part = QKV // 5

    def project(m, carry):
        rows = pl.ds(pl.multiple_of(m * part, 16), part)
        total = mm(heads[0, rows], h1[pl.ds(0, SLICE)])
        for k in range(1, DEPTH):
            total += mm(heads[k, rows], h1[pl.ds(k * SLICE, SLICE)])
        proj[rows] = total
        return carry

    lax.fori_loop(0, 5, project, 0)

    def turned(h):
        base = h * HEAD
        a = proj[pl.ds(pl.multiple_of(base, 8), HEAD // 2)]
        b = proj[pl.ds(pl.multiple_of(base + HEAD // 2, 8), HEAD // 2)]
        c, s = cos[...], sin[...]
        return a * c - b * s, b * c + a * s

    def keys(g, carry):
        a, b = turned(QUERY_HEADS + g)
        v = proj[pl.ds(pl.multiple_of((QUERY_HEADS + KEY_VALUE_HEADS + g) * HEAD, 8), HEAD)]
        both = jnp.concatenate([a, b, v], axis=0)
        kv[here.z, g] = both.T.astype(bf16)
        return carry

    lax.fori_loop(0, KEY_VALUE_HEADS, keys, 0)
    chain = KeyChain(here, kv, kv_sems)
    chain.up(here.z)

    def queries(h, carry):
        a, b = turned(h)
        scale = HEAD**-0.5
        qx[h, pl.ds(0, 32)] = (a.astype(bf16).astype(f32) * scale).astype(bf16)
        qx[h, pl.ds(32, 32)] = (b.astype(bf16).astype(f32) * scale).astype(bf16)
        qx[h, pl.ds(64, 64)] = qext[...]
        qn[h] = qx[h].astype(f32).T.astype(bf16)
        return carry

    lax.fori_loop(0, QUERY_HEADS, queries, 0)

    def prepare(slot):
        ext = kext[pl.ds(pl.multiple_of(slot * tokens, 16), tokens)]

        def body(g, carry):
            block = kv[slot, g]
            kx[g] = jnp.where(lanes_below(block.shape, HEAD), block, ext)
            turned_block = block.astype(f32).T
            vt[g, pl.ds(0, 16)] = jnp.ones((16, tokens), bf16)
            vt[g, pl.ds(16, HEAD)] = (turned_block[HEAD:] * VALUE_SCALE).astype(bf16)
            return carry

        lax.fori_loop(0, KEY_VALUE_HEADS, body, 0)

    def below(shape, shift):
        return lax.broadcasted_iota(jnp.int32, shape, 0) <= lax.broadcasted_iota(jnp.int32, shape, 1) + shift

    def diagonal(g):
        for i in range(GROUP):
            h = g * GROUP + i
            s = mm(kx[g, pl.ds(0, half)], qx[h, :, pl.ds(0, half)])
            p = jnp.exp(jnp.where(below(s.shape, 0), s, HIDE)).astype(bf16)
            acc[h, :, pl.ds(0, half)] = mm(vt[g, :, pl.ds(0, half)], p)
            s = mm(kx[g], qx[h, :, pl.ds(half, half)])
            p = jnp.exp(jnp.where(below(s.shape, half), s, HIDE)).astype(bf16)
            acc[h, :, pl.ds(half, half)] = mm(vt[g], p)

    def whole(g):
        for i in range(GROUP):
            h = g * GROUP + i
            for k in range(2):
                cols = pl.ds(k * half, half)
                p = jnp.exp(mm(kx[g], qx[h, :, cols])).astype(bf16)
                acc[h, :, cols] += mm(vt[g], p)

    ticks = ticks[3:]

    def micro(t, carry):
        s = t // KEY_VALUE_HEADS
        g = lax.rem(t, KEY_VALUE_HEADS)

        @pl.when(s <= here.z)
        def _():
            slot = here.z - s

            @pl.when(g == 0)
            def _():
                @pl.when(s > 0)
                def _():
                    chain.take(slot)

                prepare(slot)

            @pl.when(s == 0)
            def _():
                diagonal(g)

            @pl.when(s > 0)
            def _():
                whole(g)

        for k, tick in enumerate(ticks):
            pl.when(t == k * micros // len(ticks))(tick)
        return carry

    micros = grid.nz * KEY_VALUE_HEADS
    lax.fori_loop(0, micros, micro, 0)

    def close(h, carry):
        totals = acc[h, pl.ds(0, 1)]
        scale = (1.0 / VALUE_SCALE) / totals
        att[pl.ds(pl.multiple_of(h * HEAD, 16), HEAD)] = (acc[h, pl.ds(16, HEAD)] * scale).astype(bf16)
        qx[h, pl.ds(HEAD + DOCS, 16)] = three_pieces(-jnp.log(totals))
        return carry

    lax.fori_loop(0, QUERY_HEADS, close, 0)
    for job in jobs:
        job.arrive()
        job.drain()
    chain.drain()


def front(grid, shards, z_majors, leads, heads, x, gain, cos, sin, qext, kext, collective_id):
    tokens = x.shape[1]
    shapes = []
    for shard, z_major, chosen in zip(shards, z_majors, leads):
        lead = (grid.nz, grid.nd) if z_major else (grid.nd, grid.nz)
        lead = (len(chosen),) + lead if chosen else lead
        shapes.append(jax.ShapeDtypeStruct(lead + shard.shape[-2:], shard.dtype))
    n = len(shards)
    pieces = chunk_list(shards, leads)
    shapes += [
        jax.ShapeDtypeStruct((QUERY_HEADS, 128, tokens), bf16),
        jax.ShapeDtypeStruct((QUERY_HEADS, tokens, 128), bf16),
        jax.ShapeDtypeStruct((grid.nz, KEY_VALUE_HEADS, tokens, 128), bf16),
        jax.ShapeDtypeStruct((D, tokens), bf16),
    ]
    return pl.pallas_call(
        functools.partial(front_kernel, grid, tuple(z_majors), pieces),
        out_shape=shapes,
        in_specs=[VMEM] * (n + 7),
        out_specs=[ANY] * n + [VMEM] * 4,
        scratch_shapes=[
            pltpu.VMEM((D, tokens), bf16),
            pltpu.VMEM((QKV, tokens), f32),
            pltpu.VMEM((KEY_VALUE_HEADS, tokens, 128), bf16),
            pltpu.VMEM((KEY_VALUE_HEADS, 80, tokens), bf16),
            pltpu.VMEM((QUERY_HEADS, 80, tokens), f32),
            pltpu.SemaphoreType.DMA((max(len(pieces), 1), GATHER_SEMS)),
            pltpu.SemaphoreType.DMA((2, grid.nz)),
        ],
        compiler_params=pltpu.CompilerParams(
            collective_id=collective_id, has_side_effects=True, vmem_limit_bytes=60 << 20
        ),
        name="front",
    )(*shards, heads, x, gain, cos, sin, qext, kext)


STEPS = 5
WIDTH = 128
PARTS = 6


def middle_kernel(grid, ready, summed, *refs):
    att, wo, x, ogt, gain, exp_in, dn_in = refs[:7]
    refs = refs[7:]
    late = STEPS - ready
    if late:
        shard, refs = refs[0], refs[1:]
    out, rg, gsum, dwo, dox, dexp, ddn = refs[:7]
    refs = refs[7:]
    if late:
        exp_late, refs = refs[0], refs[1:]
    if summed:
        gexp, refs = refs[0], refs[1:]
    (res, inv, h2, h2t, og, acc_o, acc_h, mixed, dgate, dup, wg, wu, wd, sg, sd, w_sems, o_sems) = refs[:17]
    refs = refs[17:]
    tokens = x.shape[1]
    half = 2 * WIDTH
    schedule = {}
    gathers, sums = [], []
    if late or summed:
        here = Here(grid)
        greet(here.peers())
    if late:
        pieces = [(0, k, (0, SLICE)) for k in range(late)]
        g_sems, refs = refs[0], refs[1:]
        gathers = [
            Gather(here, shard.at[ready + k], exp_late.at[k], g_sems.at[k], False, (0, SLICE)) for k in range(late)
        ]
        for job in gathers:
            job.stage_z()
        for k, job in enumerate(gathers):
            for i, stage in enumerate(job.stages[1:]):
                schedule.setdefault(5 * i + 2 * k, []).append(getattr(job, stage))
            schedule.setdefault((ready + k - 1) * PARTS + 1, []).append(job.arrive)
    if summed:
        pieces = [(0, k, (0, SLICE)) for k in range(summed)]
        sums, refs = reduce_jobs(here, [dexp], [gexp], refs, (False,), pieces)
        for k, job in enumerate(sums):
            for i, stage in enumerate(job.stages):
                place = min((k + 1) * PARTS + 2 + 5 * i, STEPS * PARTS - 1)
                schedule.setdefault(place, []).append(getattr(job, stage))

    def fetch_from(source, index, step, slot, go):
        for d in range(4):
            lanes = pl.ds(d * WIDTH, WIDTH)
            go(pltpu.make_async_copy(source.at[index, d], wg.at[slot, :, :, lanes], w_sems.at[slot, 0]))
            go(pltpu.make_async_copy(source.at[index, 4 + d], wu.at[slot, :, :, lanes], w_sems.at[slot, 1]))
            columns = pl.ds(pl.multiple_of(step * WIDTH, WIDTH), WIDTH)
            go(pltpu.make_async_copy(dn_in.at[d, :, columns], wd.at[slot, :, lanes], w_sems.at[slot, 2]))

    def fetch(step):
        slot = lax.rem(step, 2)

        @pl.when(step < ready)
        def _():
            fetch_from(exp_in, step, step, slot, lambda copy: copy.start())

        if late:

            @pl.when(step >= ready)
            def _():
                fetch_from(exp_late, step - ready, step, slot, lambda copy: copy.start())

    def put_expand(step, go):
        for k in range(2):
            for d in range(4):
                lanes = pl.ds(d * WIDTH, WIDTH)
                to = dexp.at[step, 4 * k + d] if not sums_split else dexp.at[(step,) + sums_place(4 * k + d)]
                go(pltpu.make_async_copy(sg.at[k, :, :, lanes], to, o_sems.at[0]))

    def put_down(step, go):
        for d in range(4):
            columns = pl.ds(pl.multiple_of(step * WIDTH, WIDTH), WIDTH)
            go(pltpu.make_async_copy(sd.at[:, pl.ds(d * WIDTH, WIDTH)], ddn.at[d, :, columns], o_sems.at[1]))

    sums_split = len(dexp.shape) == 7

    def sums_place(d):
        return (d // (2 * grid.nx), d // 2 % grid.nx, d % 2)

    fetch(jnp.int32(0))
    total = jnp.zeros((1, tokens), f32)
    for m in range(DEPTH):
        rows = pl.ds(m * SLICE, SLICE)
        r = x[rows].astype(f32)
        for k in range(DEPTH):
            r += mm(wo[k, rows], att[pl.ds(k * SLICE, SLICE)])
        res[rows] = r
        total += jnp.sum(r * r, axis=0, keepdims=True)
    inverse = lax.rsqrt(total * (1.0 / D) + norm_epsilon)
    inv[...] = inverse
    for m in range(DEPTH):
        rows = pl.ds(m * SLICE, SLICE)
        h2t[rows] = (res[rows] * inverse * gain[rows]).astype(bf16)
    h2[...] = h2t[...].astype(f32).T.astype(bf16)
    og[...] = ogt[...].astype(f32).T.astype(bf16)
    acc_o[...] = jnp.zeros_like(acc_o)
    acc_h[...] = jnp.zeros_like(acc_h)

    def activate(slot, k):
        cols = pl.ds(k * half, half)
        gate = mm(h2[...], wg[slot, :, :, cols].reshape(D, half))
        up = mm(h2[...], wu[slot, :, :, cols].reshape(D, half))
        back = mm(og[...], wd[slot, :, cols])
        s = 1.0 / (1.0 + jnp.exp(-gate))
        silu = gate * s
        mixed[:, cols] = (silu * up).astype(bf16)
        dgate[:, cols] = (back * up * s * (1.0 + gate * (1.0 - s))).astype(bf16)
        dup[:, cols] = (back * silu).astype(bf16)

    def micro(t, carry):
        step = t // PARTS
        part = lax.rem(t, PARTS)
        slot = lax.rem(step, 2)

        for place, ticks in schedule.items():

            @pl.when(t == place)
            def _():
                for tick in ticks:
                    tick()

        @pl.when(part == 0)
        def _():
            wait_bytes(wg.at[slot], w_sems.at[slot, 0])
            wait_bytes(wu.at[slot], w_sems.at[slot, 1])
            wait_bytes(wd.at[slot], w_sems.at[slot, 2])
            activate(slot, 0)

        @pl.when(part == 1)
        def _():
            @pl.when(step > 0)
            def _():
                wait_bytes(sg, o_sems.at[0])
                wait_bytes(sd, o_sems.at[1])

            pl.when(step + 1 < STEPS)(lambda: fetch(step + 1))
            activate(slot, 1)

        @pl.when(part == 2)
        def _():
            acc_o[...] += mm_nt(wd[slot], mixed[...])

        @pl.when(part == 3)
        def _():
            for m in range(DEPTH):
                sg[0, m] = mm(h2t[pl.ds(m * SLICE, SLICE)], dgate[...]).astype(bf16)
                sg[1, m] = mm(h2t[pl.ds(m * SLICE, SLICE)], dup[...]).astype(bf16)
            put_expand(step, lambda copy: copy.start())

        @pl.when(part == 4)
        def _():
            sd[...] = mm(ogt[...], mixed[...]).astype(bf16)
            put_down(step, lambda copy: copy.start())

        @pl.when(part == 5)
        def _():
            acc_h[...] += mm_nt(wg[slot].reshape(D, 2 * half), dgate[...])
            acc_h[...] += mm_nt(wu[slot].reshape(D, 2 * half), dup[...])

        return carry

    lax.fori_loop(0, STEPS * PARTS, micro, 0)
    wait_bytes(sg, o_sems.at[0])
    wait_bytes(sd, o_sems.at[1])
    inverse = inv[...]
    total = jnp.zeros((1, tokens), f32)
    for m in range(DEPTH):
        rows = pl.ds(m * SLICE, SLICE)
        out[rows] = (res[rows] + acc_o[rows]).astype(bf16)
        normed = res[rows] * inverse
        up = acc_h[rows]
        gsum[rows] = jnp.sum(up * normed, axis=1, keepdims=True)
        total += jnp.sum(up * gain[rows] * normed, axis=0, keepdims=True)
    mean = total * (1.0 / D)
    for m in range(DEPTH):
        rows = pl.ds(m * SLICE, SLICE)
        normed = res[rows] * inverse
        r = ogt[rows].astype(f32) + inverse * (acc_h[rows] * gain[rows] - normed * mean)
        rg[rows] = r
        h2t[rows] = r.astype(bf16)
    for k in range(DEPTH):
        rows = pl.ds(k * SLICE, SLICE)
        dwo[k] = mm_nt(h2t[...], att[rows]).astype(bf16)
        acc_h[rows] = mm_tn(wo[k], h2t[...])

    def rows_of(h, carry):
        rows = pl.ds(pl.multiple_of(h * HEAD, 16), HEAD)
        grad = acc_h[rows].astype(bf16)
        dox[h, pl.ds(HEAD, HEAD)] = grad
        delta = jnp.sum(grad.astype(f32) * att[rows].astype(f32), axis=0, keepdims=True)
        dox[h, pl.ds(0, 16)] = three_pieces(-delta)
        dox[h, pl.ds(16, 48)] = jnp.zeros((48, tokens), bf16)
        return carry

    lax.fori_loop(0, QUERY_HEADS, rows_of, 0)
    for job in gathers + sums:
        job.drain()


def middle(grid, att, wo, x, ogt, gain, expand, down, shard, summed, collective_id):
    tokens = x.shape[1]
    ready = expand.shape[0]
    late = STEPS - ready
    blocks = expand.shape[1:]
    if summed:
        grads = (STEPS, grid.ny, grid.nx, 2) + blocks[1:]
    else:
        grads = (STEPS,) + blocks
    shapes = [
        jax.ShapeDtypeStruct((D, tokens), bf16),
        jax.ShapeDtypeStruct((D, tokens), f32),
        jax.ShapeDtypeStruct((D, 1), f32),
        jax.ShapeDtypeStruct((DEPTH, D, SLICE), bf16),
        jax.ShapeDtypeStruct((QUERY_HEADS, 128, tokens), bf16),
        jax.ShapeDtypeStruct(grads, bf16),
        jax.ShapeDtypeStruct(down.shape, bf16),
    ]
    out_specs = [VMEM] * 5 + [ANY] * 2
    inputs = [att, wo, x, ogt, gain, expand, down]
    in_specs = [VMEM] * 5 + [ANY] * 2
    scratch = [
        pltpu.VMEM((D, tokens), f32),
        pltpu.VMEM((1, tokens), f32),
        pltpu.VMEM((tokens, D), bf16),
        pltpu.VMEM((D, tokens), bf16),
        pltpu.VMEM((tokens, D), bf16),
        pltpu.VMEM((D, tokens), f32),
        pltpu.VMEM((D, tokens), f32),
        pltpu.VMEM((tokens, 4 * WIDTH), bf16),
        pltpu.VMEM((tokens, 4 * WIDTH), bf16),
        pltpu.VMEM((tokens, 4 * WIDTH), bf16),
        pltpu.VMEM((2, DEPTH, SLICE, 4 * WIDTH), bf16),
        pltpu.VMEM((2, DEPTH, SLICE, 4 * WIDTH), bf16),
        pltpu.VMEM((2, D, 4 * WIDTH), bf16),
        pltpu.VMEM((2, DEPTH, SLICE, 4 * WIDTH), bf16),
        pltpu.VMEM((D, 4 * WIDTH), bf16),
        pltpu.SemaphoreType.DMA((2, 3)),
        pltpu.SemaphoreType.DMA((2,)),
    ]
    if late:
        inputs.append(shard)
        in_specs.append(VMEM)
        shapes.append(jax.ShapeDtypeStruct((late,) + blocks, bf16))
        out_specs.append(ANY)
        scratch.append(pltpu.SemaphoreType.DMA((late, GATHER_SEMS)))
    if summed:
        shapes.append(jax.ShapeDtypeStruct((summed,) + blocks[2:], f32))
        out_specs.append(VMEM)
        pieces = [(0, k, (0, SLICE)) for k in range(summed)]
        term = jax.ShapeDtypeStruct(blocks, bf16)
        scratch += reduce_scratch(grid, [term], (False,), pieces)
    params = dict(collective_id=collective_id, has_side_effects=True) if late or summed else {}
    return pl.pallas_call(
        functools.partial(middle_kernel, grid, ready, summed),
        out_shape=shapes,
        in_specs=in_specs,
        out_specs=out_specs,
        scratch_shapes=scratch,
        compiler_params=pltpu.CompilerParams(vmem_limit_bytes=62 << 20, **params),
        name="middle",
    )(*inputs)


class GradChain:
    def __init__(self, here, part, sent, got, sems):
        self.h, self.part, self.sent, self.got, self.sems = here, part, sent, got, sems

    def summed(self, slot, g, write):
        h = self.h

        @pl.when(h.z < h.grid.nz - 1)
        def _():
            wait_bytes(self.got.at[slot, g], self.sems.at[1, slot, g])
            write(g, self.part[slot, g] + self.got[slot, g].astype(f32))

        @pl.when(h.z == h.grid.nz - 1)
        def _():
            write(g, self.part[slot, g])

    def relay(self, slot, g):
        h = self.h

        def write(g, value):
            self.sent[slot, g] = value.astype(bf16)

        self.summed(slot, g, write)
        to = lax.rem(h.z + h.grid.nz - 1, h.grid.nz)
        sems = self.sems
        send(self.sent.at[slot, g], self.got.at[slot, g], sems.at[0, slot, g], sems.at[1, slot, g], h.on_z(to))

    def drain(self):
        h = self.h

        def body(t, carry):
            slot, g = t // KEY_VALUE_HEADS, lax.rem(t, KEY_VALUE_HEADS)
            wait_bytes(self.sent.at[slot, g], self.sems.at[0, slot, g])
            return carry

        lax.fori_loop(0, h.z * KEY_VALUE_HEADS, body, 0)


def back_kernel(grid, z_majors, pieces, early, *refs):
    n = len(z_majors)
    terms, refs = refs[:n], refs[n:]
    qx, qn, dox, kv, kext, cos, sin = refs[:7]
    refs = refs[7:]
    if early:
        first, refs = refs[0], refs[1:]
    results, refs = refs[:n], refs[n:]
    for k in range(early):
        results[1][:, pl.ds(k * WIDTH, WIDTH)] = first[k]
    hd, refs = refs[0], refs[1:]
    here = Here(grid)
    jobs, refs = reduce_jobs(here, terms, results, refs, z_majors, pieces)
    don, kx, vx, kt, dq, part, sent, got, kv_sems = refs
    tokens = dox.shape[2]
    half = tokens // 2
    greet(here.peers())
    ticks = pipelined(jobs, len(jobs))
    for tick in ticks[: len(jobs)]:
        tick()
    ticks = ticks[len(jobs) :]

    def gather_queries(h, carry):
        dq[h] = jnp.zeros((HEAD, tokens), f32)
        don[h] = dox[h].astype(f32).T.astype(bf16)
        return carry

    lax.fori_loop(0, QUERY_HEADS, gather_queries, 0)

    def prepare(slot):
        ext = kext[pl.ds(pl.multiple_of(slot * tokens, 16), tokens)]

        def body(g, carry):
            block = kv[slot, g]
            low = lanes_below(block.shape, HEAD)
            kx[g] = jnp.where(low, block, ext)
            ones = jnp.where(lanes_below(block.shape, 3), 1.0, 0.0).astype(bf16)
            vx[g] = jnp.where(low, ones, block)
            kt[g] = block.astype(f32).T[:HEAD].astype(bf16)
            return carry

        lax.fori_loop(0, KEY_VALUE_HEADS, body, 0)

    def tile(g, h, count, k, masked):
        keys, cols = pl.ds(0, count), pl.ds(k * half, half)
        s = mm(kx[g, keys], qx[h, :, cols])
        if masked:
            row = lax.broadcasted_iota(jnp.int32, s.shape, 0)
            col = lax.broadcasted_iota(jnp.int32, s.shape, 1) + k * half
            s = jnp.where(row <= col, s, HIDE)
        p = jnp.exp(s)
        ds = (p * mm(vx[g, keys], dox[h, :, cols])).astype(bf16)
        dq[h, :, cols] += mm(kt[g, :, keys], ds)
        dk = mm(ds, qn[h, cols])
        dv = mm(p.astype(bf16), don[h, cols])
        return jnp.where(lanes_below(dk.shape, HEAD), dk, dv)

    def whole(slot, g):
        total = None
        for i in range(GROUP):
            for k in range(2):
                new = tile(g, g * GROUP + i, tokens, k, False)
                total = new if total is None else total + new
        part[slot, g] = total

    def diagonal(g):
        total = None
        for i in range(GROUP):
            new = tile(g, g * GROUP + i, tokens, 1, True)
            total = new if total is None else total + new
        part[here.z, g] = total
        total = part[here.z, g, pl.ds(0, half)]
        for i in range(GROUP):
            total += tile(g, g * GROUP + i, half, 0, True)
        part[here.z, g, pl.ds(0, half)] = total

    chain = GradChain(here, part, sent, got, kv_sems)
    micros = grid.nz * KEY_VALUE_HEADS
    top = here.z == grid.nz - 1

    def micro(t, carry):
        slot = t // KEY_VALUE_HEADS
        g = lax.rem(t, KEY_VALUE_HEADS)

        @pl.when(slot <= here.z)
        def _():
            pl.when(g == 0)(lambda: prepare(slot))

            @pl.when(slot < here.z)
            def _():
                whole(slot, g)
                pl.when(top)(lambda: chain.relay(slot, g))

            pl.when(slot == here.z)(lambda: diagonal(g))

        @pl.when(jnp.logical_and(jnp.logical_not(top), jnp.logical_and(slot >= 1, slot <= here.z)))
        def _():
            chain.relay(slot - 1, g)

        for k, tick in enumerate(ticks):
            pl.when(t == k * micros // len(ticks))(tick)
        return carry

    lax.fori_loop(0, micros, micro, 0)

    def turn_back(a, b):
        c, s = cos[...], sin[...]
        return a * c + b * s, b * c - a * s

    def queries(h, carry):
        scale = HEAD**-0.5
        a, b = turn_back(dq[h, pl.ds(0, 32)] * scale, dq[h, pl.ds(32, 32)] * scale)
        hd[pl.ds(pl.multiple_of(h * HEAD, 16), 32)] = a.astype(bf16)
        hd[pl.ds(pl.multiple_of(h * HEAD + 32, 16), 32)] = b.astype(bf16)
        return carry

    lax.fori_loop(0, QUERY_HEADS, queries, 0)

    def write(g, value):
        turned = value.T
        a, b = turn_back(turned[:32], turned[32:64])
        base = (QUERY_HEADS + g) * HEAD
        hd[pl.ds(pl.multiple_of(base, 16), 32)] = a.astype(bf16)
        hd[pl.ds(pl.multiple_of(base + 32, 16), 32)] = b.astype(bf16)
        base = (QUERY_HEADS + KEY_VALUE_HEADS + g) * HEAD
        hd[pl.ds(pl.multiple_of(base, 16), HEAD)] = turned[64:].astype(bf16)

    def close(g, carry):
        chain.summed(here.z, g, write)
        return carry

    lax.fori_loop(0, KEY_VALUE_HEADS, close, 0)
    chain.drain()
    for job in jobs:
        job.drain()


def back(grid, terms, z_majors, leads, early, qx, qn, dox, kv, kext, cos, sin, collective_id):
    tokens = dox.shape[2]
    n = len(terms)
    pieces = chunk_list(terms, leads)
    shapes = []
    for k, (term, chosen) in enumerate(zip(terms, leads)):
        rows, cols = term.shape[-2:]
        if k == 1:
            shapes.append(jax.ShapeDtypeStruct((rows, cols * term.shape[0] if chosen else cols), f32))
        else:
            shapes.append(jax.ShapeDtypeStruct((grid.nz, rows, cols), bf16))
    scratch = reduce_scratch(grid, terms, z_majors, pieces)
    shapes.append(jax.ShapeDtypeStruct((QKV, tokens), bf16))
    blocks = (grid.nz, KEY_VALUE_HEADS, tokens, 128)
    scratch += [
        pltpu.VMEM((QUERY_HEADS, tokens, 128), bf16),
        pltpu.VMEM((KEY_VALUE_HEADS, tokens, 128), bf16),
        pltpu.VMEM((KEY_VALUE_HEADS, tokens, 128), bf16),
        pltpu.VMEM((KEY_VALUE_HEADS, HEAD, tokens), bf16),
        pltpu.VMEM((QUERY_HEADS, HEAD, tokens), f32),
        pltpu.VMEM(blocks, f32),
        pltpu.VMEM((grid.nz - 1,) + blocks[1:], bf16),
        pltpu.VMEM(blocks, bf16),
        pltpu.SemaphoreType.DMA((2, grid.nz, KEY_VALUE_HEADS)),
    ]
    return pl.pallas_call(
        functools.partial(back_kernel, grid, tuple(z_majors), pieces, 0 if early is None else early.shape[0]),
        out_shape=shapes,
        in_specs=[ANY] * n + [VMEM] * (7 + (early is not None)),
        out_specs=[VMEM] * (n + 1),
        scratch_shapes=scratch,
        compiler_params=pltpu.CompilerParams(
            collective_id=collective_id, has_side_effects=True, vmem_limit_bytes=63 << 20
        ),
        name="back",
    )(*split_terms(grid, terms, z_majors), qx, qn, dox, kv, kext, cos, sin, *([] if early is None else [early]))


def adamw(weight, grad, first, second, rate, decay):
    first_new = beta_one * first + (1.0 - beta_one) * grad
    second_new = beta_two * second + (1.0 - beta_two) * grad * grad
    first_hat = first_new / (1.0 - beta_one**ADAM_STEP)
    second_hat = second_new / (1.0 - beta_two**ADAM_STEP)
    weight_new = weight - rate * (
        first_hat / (jnp.sqrt(second_hat) + adam_epsilon) + decay * weight
    )
    return (weight_new, first_new, second_new)


def finish_kernel(grid, pieces, *refs):
    hd, heads, x, gain, rg, gain_two, down, output, ig, gheads, ggains, gdown, goutput = refs[:13]
    h1, og, flat, wide, terms, value, last_down, last_output, last_sems = refs[13:22]
    here = Here(grid)
    greet(here.peers())
    columns = [Collect(here, down, last_down, last_sems.at[0]), Collect(here, output, last_output, last_sems.at[1])]
    for column in columns:
        column.begin()
    jobs, refs = reduce_jobs(here, [terms], [gheads], refs[22:], (True,), pieces)
    share = Share(here, value, ggains, refs[:4], refs[4])
    tokens = x.shape[1]
    inverse = inverse_rms(x)
    for k in range(DEPTH):
        rows = pl.ds(k * SLICE, SLICE)
        h1[rows] = (x[rows].astype(f32) * inverse * gain[rows]).astype(bf16)
    rows = terms.shape[-2]
    for k in range(DEPTH):
        flat[...] = mm_nt(hd[...], h1[pl.ds(k * SLICE, SLICE)])
        for d in range(grid.nd):
            place = (k, d // (2 * grid.nx), d // 2 % grid.nx, d % 2)
            terms[place] = flat[pl.ds(d * rows, rows)].astype(bf16)
    ticks = pipelined(jobs, len(jobs))
    for tick in ticks[: len(jobs)]:
        tick()
    ticks = ticks[len(jobs) :]

    def turn(count=1):
        for _ in range(count):
            if ticks:
                ticks.pop(0)()

    for k in range(DEPTH):
        og[pl.ds(k * SLICE, SLICE)] = mm_tn(heads[k], hd[...])
        if k == 1:
            turn()
    turn()
    total = jnp.zeros((1, tokens), f32)
    for k in range(DEPTH):
        rows = pl.ds(k * SLICE, SLICE)
        normed = x[rows].astype(f32) * inverse
        sums = jnp.sum(og[rows] * normed, axis=1, keepdims=True)
        place = lax.broadcasted_iota(jnp.int32, (SLICE, 128), 1)
        wide[rows] = jnp.where(place == 0, sums, jnp.where(place == 1, gain_two[rows], 0.0))
        total += jnp.sum(og[rows] * gain[rows] * normed, axis=0, keepdims=True)
    value[...] = wide[...].T[:8]
    share.start(0)
    turn()
    mean = total * (1.0 / D)
    for k in range(DEPTH):
        rows = pl.ds(k * SLICE, SLICE)
        normed = x[rows].astype(f32) * inverse
        ig[rows] = rg[rows] + inverse * (og[rows] * gain[rows] - normed * mean)
    turn()
    gdown[...] = columns[0].end()
    goutput[...] = columns[1].end().T
    for k in range(4):
        share.end(k)
        if k < 3:
            share.start(k + 1)
        turn(2)
    turn(len(ticks))
    share.drain()
    for job in jobs + columns:
        job.drain()


def finish(grid, hd, heads, x, gain, rg, gain_two, down, output, collective_id):
    tokens = x.shape[1]
    rows = QKV // grid.nd
    term = jax.ShapeDtypeStruct((rows, SLICE), bf16)
    pieces = chunk_list([term])
    scratch = [
        pltpu.VMEM((D, tokens), bf16),
        pltpu.VMEM((D, tokens), f32),
        pltpu.VMEM((QKV, SLICE), f32),
        pltpu.VMEM((D, 128), f32),
        pltpu.VMEM((grid.nz, grid.ny, grid.nx, 2, rows, SLICE), bf16),
        pltpu.VMEM((8, D), f32),
        pltpu.VMEM(down.shape, bf16),
        pltpu.VMEM(output.shape, bf16),
        pltpu.SemaphoreType.DMA((2, 2)),
    ]
    scratch += reduce_scratch(grid, [term], (True,), pieces)
    scratch += Share.scratch(grid, (8, D))
    scratch.append(pltpu.SemaphoreType.DMA((SHARE_SEMS,)))
    return pl.pallas_call(
        functools.partial(finish_kernel, grid, pieces),
        out_shape=[
            jax.ShapeDtypeStruct((D, tokens), f32),
            jax.ShapeDtypeStruct((rows, SLICE), f32),
            jax.ShapeDtypeStruct((8, D), f32),
            jax.ShapeDtypeStruct(down.shape[1:], f32),
            jax.ShapeDtypeStruct(output.shape[:0:-1], f32),
        ],
        in_specs=[VMEM] * 8,
        out_specs=[VMEM] * 5,
        scratch_shapes=scratch,
        compiler_params=pltpu.CompilerParams(
            collective_id=collective_id, has_side_effects=True, vmem_limit_bytes=62 << 20
        ),
        name="finish",
    )(hd, heads, x, gain, rg, gain_two, down, output)


READY = 4
SUMMED = 1


def local(
    grid,
    hidden_in,
    out_grad,
    seg_ids,
    doc_start,
    norm_gains,
    heads_weight,
    output_weight,
    expand_weight,
    down_weight,
    gains_first,
    gains_second,
    heads_first,
    heads_second,
    output_first,
    output_second,
    expand_first,
    expand_second,
    down_first,
    down_second,
):
    tokens = hidden_in.shape[0]
    first_row = lax.axis_index("shard") * tokens
    positions = first_row + jnp.arange(tokens, dtype=jnp.int32)
    freq = jnp.power(10000.0, -jnp.arange(HEAD // 2).astype(f32) / (HEAD // 2))
    angle = (positions - doc_start).astype(f32)[None, :] * freq[:, None]
    cos, sin = jnp.cos(angle), jnp.sin(angle)
    seg_row = seg_ids[0]
    seg_query = lax.dynamic_slice_in_dim(seg_row, first_row, tokens)
    doc = jnp.arange(HEAD, dtype=jnp.int32)
    qext = jnp.where((doc[:, None] < DOCS) & (seg_query[None, :] == doc[:, None]), HIDE, 0.0).astype(bf16)
    lane = jnp.arange(128, dtype=jnp.int32) - HEAD
    other_doc = (lane[None, :] >= 0) & (lane[None, :] < DOCS) & (seg_row[:, None] != lane[None, :])
    kext = jnp.where(other_doc | ((lane >= DOCS) & (lane < DOCS + 3))[None, :], 1.0, 0.0).astype(bf16)
    x, ogt = hidden_in.T, out_grad.T
    gain_one, gain_two = norm_gains[0][:, None], norm_gains[1][:, None]

    singles = [output_weight.astype(bf16).T, down_weight.astype(bf16).T]
    heads_stack, *columns = gather_weights(grid, [heads_weight.astype(bf16).T], (True,), singles, 1)
    heads = heads_stack.reshape(DEPTH, QKV, SLICE)
    expand_half = expand_weight.astype(bf16)
    stepped = expand_half.shape[1] == STEPS * WIDTH
    if stepped:
        shard = expand_half.reshape(SLICE, STEPS, WIDTH).transpose(1, 0, 2)
        leads = [None, None, list(range(READY))]
    else:
        shard, leads = expand_half, [None, None, None]
    shards = [*columns, shard]
    output_stack, down_stack, expand_stack, qx, qn, kv, att = front(
        grid, shards, (True, True, False), leads, heads, x, gain_one, cos, sin, qext, kext, 2
    )
    wo = output_stack.reshape(DEPTH, D, SLICE)
    down = down_stack.reshape(DEPTH, D, FF // DEPTH)
    blocks = (8, DEPTH, SLICE)
    if stepped:
        late = middle(grid, att, wo, x, ogt, gain_two, expand_stack, down, shard, SUMMED, 5)
        out, rg, gain_two_term, dwo, dox, dexpand, ddn, _, early_exp = late
    else:
        expand = expand_stack.transpose(1, 2, 0, 3).reshape(DEPTH, SLICE, 8, STEPS, WIDTH)
        expand = expand.transpose(3, 2, 0, 1, 4)
        out, rg, gain_two_term, dwo, dox, dexpand, ddn = middle(
            grid, att, wo, x, ogt, gain_two, expand, down, None, 0, 5
        )
        early_exp = None
        dexpand = dexpand.transpose(2, 3, 1, 0, 4).reshape(DEPTH, SLICE, grid.nd, -1).transpose(2, 0, 1, 3)
    if stepped:
        dexpand = dexpand.reshape((STEPS, grid.nd, grid.nz, SLICE, WIDTH))
    terms = [ddn.reshape(down_stack.shape), dexpand, dwo.reshape(output_stack.shape)]
    leads = [None, list(range(SUMMED, STEPS)) if stepped else None, None]
    down_column, expand_grad, output_column, hd = back(
        grid, terms, (True, False, True), leads, early_exp, qx, qn, dox, kv, kext, cos, sin, 3
    )
    ig, heads_grad, gains_grad, down_grad, output_grad = finish(
        grid, hd, heads, x, gain_one, rg, gain_two_term, down_column, output_column, 4
    )
    heads_grad, down_grad, gains_grad = heads_grad.T, down_grad.T, gains_grad[:2]
    hidden_out, input_grad = out.T, ig.T
    gains_new, gains_first_new, gains_second_new = adamw(
        norm_gains, gains_grad, gains_first, gains_second, gain_rate, 0.0
    )
    heads_new, heads_first_new, heads_second_new = adamw(
        heads_weight, heads_grad, heads_first, heads_second, matrix_rate, decay_rate
    )
    output_new, output_first_new, output_second_new = adamw(
        output_weight, output_grad, output_first, output_second, output_rate, decay_rate
    )
    expand_new, expand_first_new, expand_second_new = adamw(
        expand_weight, expand_grad, expand_first, expand_second, matrix_rate, decay_rate
    )
    down_new, down_first_new, down_second_new = adamw(
        down_weight, down_grad, down_first, down_second, matrix_rate, decay_rate
    )
    return (
        hidden_out,
        input_grad,
        gains_grad,
        heads_grad,
        output_grad,
        expand_grad,
        down_grad,
        gains_new,
        heads_new,
        output_new,
        expand_new,
        down_new,
        gains_first_new,
        gains_second_new,
        heads_first_new,
        heads_second_new,
        output_first_new,
        output_second_new,
        expand_first_new,
        expand_second_new,
        down_first_new,
        down_second_new,
    )


def solution(mesh):
    return jax.shard_map(
        functools.partial(local, Grid(mesh)),
        mesh=mesh,
        in_specs=(
            P(("dp", "shard"), None),
            P(("dp", "shard"), None),
            P("dp", None),
            P(("dp", "shard")),
            P(),
            P("shard", "dp"),
            P("shard", "dp"),
            P("shard", "dp"),
            P("shard", "dp"),
            P(),
            P(),
            P("shard", "dp"),
            P("shard", "dp"),
            P("shard", "dp"),
            P("shard", "dp"),
            P("shard", "dp"),
            P("shard", "dp"),
            P("shard", "dp"),
            P("shard", "dp"),
        ),
        out_specs=(
            P(("dp", "shard"), None),
            P(("dp", "shard"), None),
            P(),
            P("shard", "dp"),
            P("shard", "dp"),
            P("shard", "dp"),
            P("shard", "dp"),
            P(),
            P("shard", "dp"),
            P("shard", "dp"),
            P("shard", "dp"),
            P("shard", "dp"),
            P(),
            P(),
            P("shard", "dp"),
            P("shard", "dp"),
            P("shard", "dp"),
            P("shard", "dp"),
            P("shard", "dp"),
            P("shard", "dp"),
            P("shard", "dp"),
            P("shard", "dp"),
        ),
        check_vma=False,
    )
```

```python
import functools
import math

import jax
import jax.numpy as jnp
from jax import lax
from jax.experimental import pallas as pl
from jax.experimental.pallas import tpu as pltpu
from jax.sharding import PartitionSpec as P

MESH = pl.DeviceIdType.MESH
ANY = pl.BlockSpec(memory_space=pl.ANY)
VMEM = pl.BlockSpec(memory_space=pltpu.VMEM)


class Grid:
    def __init__(self, mesh):
        self.nd = mesh.shape["dp"]
        self.nz = mesh.shape["shard"]
        self.nx = math.isqrt(self.nd // 2)
        self.ny = self.nd // 2 // self.nx
        assert self.nx == self.ny and self.nx * self.ny * 2 == self.nd

    def dp(self, y, x, c):
        return (y * self.nx + x) * 2 + c


class Here:
    def __init__(self, grid):
        self.grid = grid
        d = lax.axis_index("dp")
        self.z = lax.axis_index("shard")
        self.d = d
        self.c = lax.rem(d, 2)
        self.x = lax.rem(d // 2, grid.nx)
        self.y = d // (2 * grid.nx)
        g = grid
        self.xs = [lax.rem(self.x + k, g.nx) for k in range(1, g.nx)]
        self.ys = [lax.rem(self.y + k, g.ny) for k in range(1, g.ny)]
        self.zs = [lax.rem(self.z + k, g.nz) for k in range(1, g.nz)]
        self.partner = (g.dp(self.y, self.x, 1 - self.c), self.z)

    def on_x(self, x):
        return (self.grid.dp(self.y, x, self.c), self.z)

    def on_y(self, y):
        return (self.grid.dp(y, self.x, self.c), self.z)

    def on_z(self, z):
        return (self.d, z)

    def peers(self):
        return (
            [self.partner]
            + [self.on_x(x) for x in self.xs]
            + [self.on_y(y) for y in self.ys]
            + [self.on_z(z) for z in self.zs]
        )


def greet(peers):
    barrier = pltpu.get_barrier_semaphore()
    for peer in peers:
        pl.semaphore_signal(barrier, inc=1, device_id=peer, device_id_type=MESH)
    pl.semaphore_wait(barrier, len(peers))


def send(src, dst, send_sem, recv_sem, device):
    pltpu.make_async_remote_copy(
        src_ref=src,
        dst_ref=dst,
        send_sem=send_sem,
        recv_sem=recv_sem,
        device_id=device,
        device_id_type=MESH,
    ).start()


def wait_bytes(ref, sem):
    pltpu.make_async_copy(ref, ref, sem).wait()


def half_rows(rows):
    return max(16, int(rows / 32 + 0.5) * 16)


def chunks_of(rows, size=64):
    starts = list(range(0, rows, size))
    if len(starts) > 1 and rows - starts[-1] < size // 2:
        starts.pop()
    return [(start, stop - start) for start, stop in zip(starts, starts[1:] + [rows])]


class Gather:
    def __init__(self, here, shard, out, sems, z_major, rows):
        self.h, self.shard, self.out, self.sems, self.z_major = here, shard, out, sems, z_major
        self.start, self.rows = rows
        self.cut = half_rows(self.rows)

    def span(self, half=None):
        if half is None:
            return pl.ds(self.start, self.rows)
        return pl.ds(self.start, self.cut) if half == 0 else pl.ds(self.start + self.cut, self.rows - self.cut)

    def column(self, d, half=None):
        return self.out.at[:, d, self.span(half)] if self.z_major else self.out.at[d, :, self.span(half)]

    def block(self, d, z):
        return self.out.at[z, d, self.span()] if self.z_major else self.out.at[d, z, self.span()]

    def columns(self, count):
        some = pl.ds(0, count)
        return self.out.at[:, some, self.span()] if self.z_major else self.out.at[some, :, self.span()]

    def blocks(self, count):
        some = pl.ds(0, count)
        return self.out.at[some, 0, self.span()] if self.z_major else self.out.at[0, some, self.span()]

    def own(self):
        h = self.h
        return pltpu.make_async_copy(self.shard.at[self.span()], self.block(h.d, h.z), self.sems.at[8])

    def stage_z(self):
        h, s = self.h, self.sems
        for z in h.zs:
            send(self.shard.at[self.span()], self.block(h.d, h.z), s.at[0], s.at[1], h.on_z(z))
        self.own().start()

    def await_z(self):
        wait_bytes(self.blocks(len(self.h.zs)), self.sems.at[1])

    def drain_z(self):
        wait_bytes(self.blocks(len(self.h.zs)), self.sems.at[0])

    def stage_one(self):
        h, s = self.h, self.sems
        self.await_z()
        self.own().wait()
        for x in h.xs:
            send(self.column(h.d, 0), self.column(h.d, 0), s.at[2], s.at[3], h.on_x(x))
        for y in h.ys:
            send(self.column(h.d, 1), self.column(h.d, 1), s.at[2], s.at[3], h.on_y(y))
        send(self.column(h.d), self.column(h.d), s.at[6], s.at[7], h.partner)

    def stage_two(self):
        h, s, g = self.h, self.sems, self.h.grid
        wait_bytes(self.columns(len(h.xs)), s.at[3])
        for y in h.ys:
            for x in [h.x] + h.xs:
                col = self.column(g.dp(h.y, x, h.c), 0)
                send(col, col, s.at[4], s.at[5], h.on_y(y))
        for x in h.xs:
            for y in [h.y] + h.ys:
                col = self.column(g.dp(y, h.x, h.c), 1)
                send(col, col, s.at[4], s.at[5], h.on_x(x))
        for x in h.xs:
            col = self.column(g.dp(h.y, x, h.c), 0)
            send(col, col, s.at[6], s.at[7], h.partner)
        for y in h.ys:
            col = self.column(g.dp(y, h.x, h.c), 1)
            send(col, col, s.at[6], s.at[7], h.partner)

    def stage_three(self):
        h, s, g = self.h, self.sems, self.h.grid
        wait_bytes(self.columns(g.nx * len(h.ys)), s.at[5])
        for y in h.ys:
            for x in [h.x] + h.xs:
                col = self.column(g.dp(y, x, h.c), 0)
                send(col, col, s.at[6], s.at[7], h.partner)
        for x in h.xs:
            for y in [h.y] + h.ys:
                col = self.column(g.dp(y, x, h.c), 1)
                send(col, col, s.at[6], s.at[7], h.partner)

    def arrive(self):
        g = self.h.grid
        wait_bytes(self.columns(g.nd // 2), self.sems.at[7])

    def drain(self):
        h, s, g = self.h, self.sems, self.h.grid
        self.drain_z()
        wait_bytes(self.columns(len(h.xs)), s.at[2])
        wait_bytes(self.columns(g.nx * len(h.ys)), s.at[4])
        wait_bytes(self.columns(g.nd // 2), s.at[6])

    stages = ("stage_z", "stage_one", "stage_two", "stage_three")


class ColumnGather(Gather):
    def own(self):
        return pltpu.make_async_copy(self.shard.at[:, self.span()], self.column(self.h.d), self.sems.at[8])

    def stage_z(self):
        self.own().start()

    def await_z(self):
        pass

    def drain_z(self):
        pass


class Spread:
    def __init__(self, here, shard, out, sems):
        self.h, self.shard, self.out, self.sems = here, shard, out, sems

    def own(self):
        return pltpu.make_async_copy(self.shard, self.out.at[self.h.z], self.sems.at[2])

    def begin(self):
        h, s = self.h, self.sems
        for z in h.zs:
            send(self.shard, self.out.at[h.z], s.at[0], s.at[1], h.on_z(z))
        self.own().start()

    def end(self):
        some = self.out.at[pl.ds(0, len(self.h.zs))]
        wait_bytes(some, self.sems.at[1])
        wait_bytes(some, self.sems.at[0])
        self.own().wait()


def pipelined(jobs, ahead=0):
    ticks = [getattr(job, job.stages[0]) for job in jobs[:ahead]]
    depth = max((len(job.stages) for job in jobs), default=0)
    for step in range(len(jobs) + depth - 1):
        for k in range(depth):
            i = step - k
            if 0 <= i < len(jobs) and k < len(jobs[i].stages) and not (k == 0 and i < ahead):
                ticks.append(getattr(jobs[i], jobs[i].stages[k]))
    return ticks


def chunk_list(shards, leads=None):
    pieces = []
    for i, shard in enumerate(shards):
        if leads is not None and leads[i]:
            pieces += [(i, k, (0, shard.shape[-2])) for k in leads[i]]
        else:
            pieces += [(i, None, rows) for rows in chunks_of(shard.shape[-2])]
    return pieces


def piece_of(ref, lead):
    return ref if lead is None else ref.at[lead]


def gather_jobs(here, shards, outs, sems, z_majors, pieces):
    jobs = []
    for k, (i, lead, rows) in enumerate(pieces):
        kind = ColumnGather if lead is None and len(shards[i].shape) == 3 else Gather
        job = kind(here, piece_of(shards[i], lead), piece_of(outs[i], lead), sems.at[k], z_majors[i], rows)
        jobs.append(job)
    return jobs


GATHER_SEMS = 9


def gather_kernel(grid, z_majors, pieces, turns, *refs):
    n, spreads = len(z_majors), len(turns) - len(z_majors)
    given, refs = refs[: n + spreads], refs[n + spreads :]
    outs, refs = refs[:n], refs[n:]
    columns, refs = refs[:spreads], refs[spreads:]
    rounded, (sems, spread_sems) = refs[: n + spreads], refs[n + spreads :]
    for source, half, turn in zip(given, rounded, turns):
        half[...] = (source[...].T if turn else source[...]).astype(jnp.bfloat16)
    shards, singles = rounded[:n], rounded[n:]
    here = Here(grid)
    greet(here.peers())
    jobs = gather_jobs(here, shards, outs, sems, z_majors, pieces)
    ticks = pipelined(jobs, len(jobs))
    for tick in ticks[: len(jobs)]:
        tick()
    others = [Spread(here, singles[k], columns[k], spread_sems.at[k]) for k in range(spreads)]
    for other in others:
        other.begin()
    for tick in ticks[len(jobs) :]:
        tick()
    for job in jobs:
        job.arrive()
        job.drain()
    for other in others:
        other.end()


def gather_weights(grid, shards, z_majors, singles, turns, collective_id):
    blocks = []
    for value, turn in zip([*shards, *singles], turns):
        blocks.append(jax.ShapeDtypeStruct(value.shape[::-1] if turn else value.shape, jnp.bfloat16))
    n = len(shards)
    shapes = []
    for block, z_major in zip(blocks, z_majors):
        lead = (grid.nz, grid.nd) if z_major else (grid.nd, grid.nz)
        shapes.append(jax.ShapeDtypeStruct(lead + block.shape, block.dtype))
    for block in blocks[n:]:
        shapes.append(jax.ShapeDtypeStruct((grid.nz,) + block.shape, block.dtype))
    pieces = chunk_list(blocks[:n])
    return pl.pallas_call(
        functools.partial(gather_kernel, grid, tuple(z_majors), pieces, tuple(turns)),
        out_shape=shapes,
        in_specs=[VMEM] * len(blocks),
        out_specs=[ANY] * len(shapes),
        scratch_shapes=[pltpu.VMEM(block.shape, block.dtype) for block in blocks]
        + [
            pltpu.SemaphoreType.DMA((len(pieces), GATHER_SEMS)),
            pltpu.SemaphoreType.DMA((len(singles), 3)),
        ],
        compiler_params=pltpu.CompilerParams(collective_id=collective_id, has_side_effects=True),
        name="gather_weights",
    )(*shards, *singles)


class Reduce:
    def __init__(self, here, terms, result, bufs, sems, z_major, rows):
        self.h, self.terms, self.result, self.sems, self.z_major = here, terms, result, sems, z_major
        self.own, self.other, self.one_a, self.one_b, self.two_a, self.two_b, self.last = bufs
        self.start, self.rows = rows
        self.cut = half_rows(self.rows)

    @staticmethod
    def scratch(grid, rows, cols, z_major):
        cut = half_rows(rows)
        ny, nx, nz = grid.ny, grid.nx, grid.nz
        full = (nz, ny, nx) if z_major else (ny, nx, nz)
        row = (nz, nx) if z_major else (nx, nz)
        bf = jnp.bfloat16
        return [
            pltpu.VMEM(full + (rows, cols), bf),
            pltpu.VMEM(full + (rows, cols), bf),
            pltpu.VMEM((ny,) + row + (cut, cols), bf),
            pltpu.VMEM((nx,) + row + (rows - cut, cols), bf),
            pltpu.VMEM((nx, nz, cut, cols), bf),
            pltpu.VMEM((ny, nz, rows - cut, cols), bf),
            pltpu.VMEM((nz, rows, cols), bf),
        ]

    def span(self, half):
        return {None: slice(None), 0: pl.ds(0, self.cut), 1: pl.ds(self.cut, self.rows - self.cut)}[half]

    def at(self, y, x, z, half):
        y, x, z = (slice(None) if v is None else v for v in (y, x, z))
        return (z, y, x, self.span(half)) if self.z_major else (y, x, z, self.span(half))

    def side(self, c):
        rows = pl.ds(self.start, self.rows)
        return self.terms.at[:, :, :, c, rows] if self.z_major else self.terms.at[:, :, c, :, rows]

    def load(self):
        return pltpu.make_async_copy(self.side(self.h.c), self.own, self.sems.at[8])

    def stage_core(self):
        h, s = self.h, self.sems
        send(self.side(1 - h.c), self.other, s.at[0], s.at[1], h.partner)
        self.load().start()

    def add_loop(self, shape, body):
        total = math.prod(shape)

        def step(i, carry):
            place = []
            rest = i
            for size in reversed(shape):
                place.append(lax.rem(rest, size))
                rest = rest // size
            body(tuple(reversed(place)))
            return carry

        lax.fori_loop(0, total, step, 0)

    def stage_one(self):
        h, s, g = self.h, self.sems, self.h.grid
        self.load().wait()
        wait_bytes(self.other, s.at[1])

        def body(place):
            self.own[place] = self.own[place] + self.other[place]

        self.add_loop(self.own.shape[:3], body)
        for y in h.ys:
            send(self.own.at[self.at(y, None, None, 0)], self.one_a.at[h.y], s.at[2], s.at[3], h.on_y(y))
        for x in h.xs:
            send(self.own.at[self.at(None, x, None, 1)], self.one_b.at[h.x], s.at[9], s.at[10], h.on_x(x))

    def stage_two(self):
        h, s, g = self.h, self.sems, self.h.grid
        wait_bytes(self.one_a.at[pl.ds(0, g.ny - 1)], s.at[3])
        wait_bytes(self.one_b.at[pl.ds(0, g.nx - 1)], s.at[10])

        def body_a(place):
            where = (place[1], place[0]) if self.z_major else place
            spot = self.at(h.y, where[0], where[1], 0)
            total = self.own[spot].astype(jnp.float32)
            for y in h.ys:
                total += self.one_a[(y,) + place].astype(jnp.float32)
            self.own[spot] = total.astype(jnp.bfloat16)

        self.add_loop(self.one_a.shape[1:3], body_a)

        def body_b(place):
            where = (place[1], place[0]) if self.z_major else place
            spot = self.at(where[0], h.x, where[1], 1)
            total = self.own[spot].astype(jnp.float32)
            for x in h.xs:
                total += self.one_b[(x,) + place].astype(jnp.float32)
            self.own[spot] = total.astype(jnp.bfloat16)

        self.add_loop(self.one_b.shape[1:3], body_b)
        for x in h.xs:
            send(self.own.at[self.at(h.y, x, None, 0)], self.two_a.at[h.x], s.at[4], s.at[5], h.on_x(x))
        for y in h.ys:
            send(self.own.at[self.at(y, h.x, None, 1)], self.two_b.at[h.y], s.at[11], s.at[12], h.on_y(y))

    def stage_three(self):
        h, s, g = self.h, self.sems, self.h.grid
        wait_bytes(self.two_a.at[pl.ds(0, g.nx - 1)], s.at[5])
        wait_bytes(self.two_b.at[pl.ds(0, g.ny - 1)], s.at[12])

        def body(place):
            (z,) = place
            spot = self.at(h.y, h.x, z, 0)
            total = self.own[spot].astype(jnp.float32)
            for x in h.xs:
                total += self.two_a[x, z].astype(jnp.float32)
            self.own[spot] = total.astype(jnp.bfloat16)
            spot = self.at(h.y, h.x, z, 1)
            total = self.own[spot].astype(jnp.float32)
            for y in h.ys:
                total += self.two_b[y, z].astype(jnp.float32)
            self.own[spot] = total.astype(jnp.bfloat16)

        self.add_loop((g.nz,), body)
        for z in h.zs:
            send(self.own.at[self.at(h.y, h.x, z, None)], self.last.at[h.z], s.at[6], s.at[7], h.on_z(z))

    def finish(self):
        h, s, g = self.h, self.sems, self.h.grid
        wait_bytes(self.last.at[pl.ds(0, g.nz - 1)], s.at[7])
        total = self.own[self.at(h.y, h.x, h.z, None)].astype(jnp.float32)
        for z in h.zs:
            total += self.last[z].astype(jnp.float32)
        self.result[pl.ds(self.start, self.rows)] = total

    stages = ("stage_core", "stage_one", "stage_two", "stage_three", "finish")

    def drain_z(self):
        wait_bytes(self.last.at[pl.ds(0, self.h.grid.nz - 1)], self.sems.at[6])

    def drain(self):
        g, s = self.h.grid, self.sems
        wait_bytes(self.other, s.at[0])
        wait_bytes(self.one_a.at[pl.ds(0, g.ny - 1)], s.at[2])
        wait_bytes(self.one_b.at[pl.ds(0, g.nx - 1)], s.at[9])
        wait_bytes(self.two_a.at[pl.ds(0, g.nx - 1)], s.at[4])
        wait_bytes(self.two_b.at[pl.ds(0, g.ny - 1)], s.at[11])
        self.drain_z()


class ColumnReduce(Reduce):
    stages = ("stage_core", "stage_one", "stage_two", "stage_three")

    def stage_three(self):
        h, s, g = self.h, self.sems, self.h.grid
        wait_bytes(self.two_a.at[pl.ds(0, g.nx - 1)], s.at[5])
        wait_bytes(self.two_b.at[pl.ds(0, g.ny - 1)], s.at[12])

        def body(place):
            (z,) = place
            total = self.own[self.at(h.y, h.x, z, 0)].astype(jnp.float32)
            for x in h.xs:
                total += self.two_a[x, z].astype(jnp.float32)
            self.result[z, pl.ds(self.start, self.cut)] = total.astype(jnp.bfloat16)
            total = self.own[self.at(h.y, h.x, z, 1)].astype(jnp.float32)
            for y in h.ys:
                total += self.two_b[y, z].astype(jnp.float32)
            self.result[z, pl.ds(self.start + self.cut, self.rows - self.cut)] = total.astype(jnp.bfloat16)

        self.add_loop((g.nz,), body)

    def drain_z(self):
        pass


class Collect:
    def __init__(self, here, column, last, sems):
        self.h, self.column, self.last, self.sems = here, column, last, sems

    def begin(self):
        h, s = self.h, self.sems
        for z in h.zs:
            send(self.column.at[z], self.last.at[h.z], s.at[0], s.at[1], h.on_z(z))

    def end(self):
        h = self.h
        wait_bytes(self.last.at[pl.ds(0, len(h.zs))], self.sems.at[1])
        total = self.column[h.z].astype(jnp.float32)
        for z in h.zs:
            total += self.last[z].astype(jnp.float32)
        return total

    def drain(self):
        wait_bytes(self.last.at[pl.ds(0, len(self.h.zs))], self.sems.at[0])


REDUCE_SEMS = 13
REDUCE_BUFS = 7


class Share:
    def __init__(self, here, value, result, bufs, sems):
        self.h, self.value, self.result, self.sems = here, value, result, sems
        self.bufs = bufs

    @staticmethod
    def scratch(grid, shape):
        return [pltpu.VMEM((n,) + shape, jnp.float32) for n in (2, grid.nx, grid.ny, grid.nz)]

    def axis(self, k):
        h = self.h
        return (
            (h.c, [h.partner], 2),
            (h.x, [h.on_x(x) for x in h.xs], h.grid.nx),
            (h.y, [h.on_y(y) for y in h.ys], h.grid.ny),
            (h.z, [h.on_z(z) for z in h.zs], h.grid.nz),
        )[k]

    def start(self, k):
        me, peers, n = self.axis(k)
        self.bufs[k][me] = self.value[...] if k == 0 else self.total
        for peer in peers:
            send(self.bufs[k].at[me], self.bufs[k].at[me], self.sems.at[2 * k], self.sems.at[2 * k + 1], peer)

    def end(self, k):
        me, peers, n = self.axis(k)
        wait_bytes(self.bufs[k].at[pl.ds(0, n - 1)], self.sems.at[2 * k + 1])
        total = self.bufs[k][0]
        for i in range(1, n):
            total = total + self.bufs[k][i]
        self.total = total
        if k == 3:
            self.result[...] = total

    def drain(self):
        for k in range(4):
            n = self.axis(k)[2]
            wait_bytes(self.bufs[k].at[pl.ds(0, n - 1)], self.sems.at[2 * k])


SHARE_SEMS = 8


def reduce_kernel(grid, z_majors, pieces, shared, *refs):
    n = len(z_majors)
    terms, refs = refs[:n], refs[n:]
    value, refs = (refs[0], refs[1:]) if shared else (None, refs)
    results, refs = refs[:n], refs[n:]
    value_sum, refs = (refs[0], refs[1:]) if shared else (None, refs)
    here = Here(grid)
    greet(here.peers())
    jobs, refs = reduce_jobs(here, terms, results, refs, z_majors, pieces)
    share = None
    if shared:
        share = Share(here, value, value_sum, refs[:4], refs[4])
        share.start(0)
    ticks = pipelined(jobs, len(jobs))
    for k, tick in enumerate(ticks):
        tick()
        if share is not None and k >= len(jobs) and k - len(jobs) < 4:
            step = k - len(jobs)
            share.end(step)
            if step < 3:
                share.start(step + 1)
    if share is not None:
        share.drain()
    for job in jobs:
        job.drain()


def reduce_jobs(here, terms, results, refs, z_majors, pieces):
    n = len(pieces)
    sems = refs[n * REDUCE_BUFS]
    jobs = []
    for k, (i, lead, rows) in enumerate(pieces):
        bufs = refs[k * REDUCE_BUFS : (k + 1) * REDUCE_BUFS]
        term, result, kind = piece_of(terms[i], lead), results[i], Reduce
        deep = len(result.shape) == 3
        if lead is None:
            kind = ColumnReduce if deep else Reduce
        else:
            width = term.shape[-1]
            result = result.at[lead] if deep else result.at[:, pl.ds(lead * width, width)]
        jobs.append(kind(here, term, result, bufs, sems.at[k], z_majors[i], rows))
    return jobs, refs[n * REDUCE_BUFS + 1 :]


def reduce_scratch(grid, terms, z_majors, pieces):
    scratch = []
    for i, _, (_, rows) in pieces:
        scratch += Reduce.scratch(grid, rows, terms[i].shape[-1], z_majors[i])
    return scratch + [pltpu.SemaphoreType.DMA((max(len(pieces), 1), REDUCE_SEMS))]


def split_terms(grid, terms, z_majors):
    split = []
    for term, z_major in zip(terms, z_majors):
        lead = (grid.ny, grid.nx, 2)
        lead = (grid.nz,) + lead if z_major else lead + (grid.nz,)
        split.append(term.reshape(term.shape[:-4] + lead + term.shape[-2:]))
    return split


def reduce_grads(grid, terms, z_majors, value, collective_id):
    shapes = [jax.ShapeDtypeStruct(term.shape[-2:], jnp.float32) for term in terms]
    pieces = chunk_list(terms)
    scratch = reduce_scratch(grid, terms, z_majors, pieces)
    n = len(terms)
    shared = value is not None
    if shared:
        shapes.append(jax.ShapeDtypeStruct(value.shape, jnp.float32))
        scratch += Share.scratch(grid, value.shape)
        scratch.append(pltpu.SemaphoreType.DMA((SHARE_SEMS,)))
    return pl.pallas_call(
        functools.partial(reduce_kernel, grid, tuple(z_majors), pieces, shared),
        out_shape=shapes,
        in_specs=[ANY] * n + [VMEM] * shared,
        out_specs=[VMEM] * len(shapes),
        scratch_shapes=scratch,
        compiler_params=pltpu.CompilerParams(
            collective_id=collective_id, has_side_effects=True, vmem_limit_bytes=62 << 20
        ),
        name="reduce_grads",
    )(*split_terms(grid, terms, z_majors), *([value] if shared else []))


D = 960
QUERY_HEADS = 15
KEY_VALUE_HEADS = 5
GROUP = QUERY_HEADS // KEY_VALUE_HEADS
HEAD = 64
FF = 2560
QKV = (QUERY_HEADS + 2 * KEY_VALUE_HEADS) * HEAD
ADAM_STEP = 10
DOCS = 16
HIDE = -1e30
VALUE_SCALE = 2.0**-9

norm_epsilon = 1e-05
beta_one = 0.9
beta_two = 0.95
adam_epsilon = 1e-08
matrix_rate = 0.03
output_rate = 0.15
gain_rate = 0.5
decay_rate = 0.1

f32 = jnp.float32
bf16 = jnp.bfloat16
DEPTH = 4
SLICE = D // DEPTH


def mm(a, b):
    return lax.dot_general(a, b, (((1,), (0,)), ((), ())), preferred_element_type=f32)


def mm_nt(a, b):
    return lax.dot_general(a, b, (((1,), (1,)), ((), ())), preferred_element_type=f32)


def mm_tn(a, b):
    return lax.dot_general(a, b, (((0,), (0,)), ((), ())), preferred_element_type=f32)


def lanes_below(shape, n):
    return lax.broadcasted_iota(jnp.int32, shape, len(shape) - 1) < n


def inverse_rms(ref):
    total = jnp.zeros((1, ref.shape[1]), f32)
    for k in range(DEPTH):
        x = ref[pl.ds(k * SLICE, SLICE)].astype(f32)
        total += jnp.sum(x * x, axis=0, keepdims=True)
    return lax.rsqrt(total * (1.0 / D) + norm_epsilon)


def three_pieces(row):
    hi = row.astype(bf16).astype(f32)
    mid = (row - hi).astype(bf16).astype(f32)
    low = row - hi - mid
    place = lax.broadcasted_iota(jnp.int32, (16, row.shape[1]), 0)
    block = jnp.where(place == 0, hi, jnp.where(place == 1, mid, jnp.where(place == 2, low, 0.0)))
    return block.astype(bf16)


class KeyChain:
    def __init__(self, here, kv, sems):
        self.h, self.kv, self.sems = here, kv, sems

    def up(self, slot):
        h = self.h
        to = lax.rem(h.z + 1, h.grid.nz)

        @pl.when(h.z < h.grid.nz - 1)
        def _():
            send(self.kv.at[slot], self.kv.at[slot], self.sems.at[0, slot], self.sems.at[1, slot], h.on_z(to))

    def take(self, slot):
        wait_bytes(self.kv.at[slot], self.sems.at[1, slot])
        self.up(slot)

    def drain(self):
        h = self.h
        for s in range(h.grid.nz):

            @pl.when(jnp.logical_and(h.z >= s, h.z < h.grid.nz - 1))
            def _():
                wait_bytes(self.kv.at[h.z - s], self.sems.at[0, h.z - s])


def round_steps(source, rounded, start):
    if len(rounded.shape) == 2:
        rounded[...] = source[...].astype(bf16)
    else:
        for k in range(rounded.shape[0]):
            rounded[k] = source[:, pl.ds((start + k) * WIDTH, WIDTH)].astype(bf16)


def front_kernel(grid, z_majors, pieces, *refs):
    n = len(z_majors)
    shards, refs = refs[:n], refs[n:]
    heads, x, gain, cos, sin, qext, kext = refs[:7]
    refs = refs[7:]
    outs, refs = refs[:n], refs[n:]
    qx, qn, kv, att = refs[:4]
    h1, proj, kx, vt, acc, rounded, sems, kv_sems = refs[4:]
    here = Here(grid)
    tokens = x.shape[1]
    half = tokens // 2
    round_steps(shards[-1], rounded, 0)
    greet(here.peers())
    jobs = gather_jobs(here, [*shards[:-1], rounded], outs, sems, z_majors, pieces)
    ticks = pipelined(jobs, 3)
    for tick in ticks[:3]:
        tick()

    inverse = inverse_rms(x)
    for k in range(DEPTH):
        rows = pl.ds(k * SLICE, SLICE)
        h1[rows] = (x[rows].astype(f32) * inverse * gain[rows, 0:1]).astype(bf16)

    part = QKV // 5

    def project(m, carry):
        rows = pl.ds(pl.multiple_of(m * part, 16), part)
        total = mm(heads[0, rows], h1[pl.ds(0, SLICE)])
        for k in range(1, DEPTH):
            total += mm(heads[k, rows], h1[pl.ds(k * SLICE, SLICE)])
        proj[rows] = total
        return carry

    lax.fori_loop(3, 5, project, 0)

    def turned(h):
        base = h * HEAD
        a = proj[pl.ds(pl.multiple_of(base, 8), HEAD // 2)]
        b = proj[pl.ds(pl.multiple_of(base + HEAD // 2, 8), HEAD // 2)]
        c, s = cos[...], sin[...]
        return a * c - b * s, b * c + a * s

    def keys(g, carry):
        a, b = turned(QUERY_HEADS + g)
        v = proj[pl.ds(pl.multiple_of((QUERY_HEADS + KEY_VALUE_HEADS + g) * HEAD, 8), HEAD)]
        both = jnp.concatenate([a, b, v], axis=0)
        kv[here.z, g] = both.T.astype(bf16)
        return carry

    lax.fori_loop(0, KEY_VALUE_HEADS, keys, 0)
    chain = KeyChain(here, kv, kv_sems)
    chain.up(here.z)
    lax.fori_loop(0, 3, project, 0)

    def queries(h, carry):
        a, b = turned(h)
        scale = HEAD**-0.5
        qx[h, pl.ds(0, 32)] = (a.astype(bf16).astype(f32) * scale).astype(bf16)
        qx[h, pl.ds(32, 32)] = (b.astype(bf16).astype(f32) * scale).astype(bf16)
        qx[h, pl.ds(64, 64)] = qext[...]
        qn[h] = qx[h].astype(f32).T.astype(bf16)
        return carry

    lax.fori_loop(0, QUERY_HEADS, queries, 0)

    def prepare(slot):
        ext = kext[pl.ds(pl.multiple_of(slot * tokens, 16), tokens)]

        def body(g, carry):
            block = kv[slot, g]
            kx[g] = jnp.where(lanes_below(block.shape, HEAD), block, ext)
            turned_block = block.astype(f32).T
            vt[g, pl.ds(0, 16)] = jnp.ones((16, tokens), bf16)
            vt[g, pl.ds(16, HEAD)] = (turned_block[HEAD:] * VALUE_SCALE).astype(bf16)
            return carry

        lax.fori_loop(0, KEY_VALUE_HEADS, body, 0)

    def below(shape, shift):
        return lax.broadcasted_iota(jnp.int32, shape, 0) <= lax.broadcasted_iota(jnp.int32, shape, 1) + shift

    def diagonal(g):
        for i in range(GROUP):
            h = g * GROUP + i
            s = mm(kx[g, pl.ds(0, half)], qx[h, :, pl.ds(0, half)])
            p = jnp.exp(jnp.where(below(s.shape, 0), s, HIDE)).astype(bf16)
            acc[h, :, pl.ds(0, half)] = mm(vt[g, :, pl.ds(0, half)], p)
            s = mm(kx[g], qx[h, :, pl.ds(half, half)])
            p = jnp.exp(jnp.where(below(s.shape, half), s, HIDE)).astype(bf16)
            acc[h, :, pl.ds(half, half)] = mm(vt[g], p)

    def whole(g):
        for i in range(GROUP):
            h = g * GROUP + i
            for k in range(2):
                cols = pl.ds(k * half, half)
                p = jnp.exp(mm(kx[g], qx[h, :, cols])).astype(bf16)
                acc[h, :, cols] += mm(vt[g], p)

    ticks = ticks[3:]

    def micro(t, carry):
        s = t // KEY_VALUE_HEADS
        g = lax.rem(t, KEY_VALUE_HEADS)

        @pl.when(s <= here.z)
        def _():
            slot = here.z - s

            @pl.when(g == 0)
            def _():
                @pl.when(s > 0)
                def _():
                    chain.take(slot)

                prepare(slot)

            @pl.when(s == 0)
            def _():
                diagonal(g)

            @pl.when(s > 0)
            def _():
                whole(g)

        for k, tick in enumerate(ticks):
            pl.when(t == k * (micros - KEY_VALUE_HEADS) // len(ticks))(tick)
        return carry

    micros = grid.nz * KEY_VALUE_HEADS
    lax.fori_loop(0, micros, micro, 0)

    def close(h, carry):
        totals = acc[h, pl.ds(0, 1)]
        scale = (1.0 / VALUE_SCALE) / totals
        att[pl.ds(pl.multiple_of(h * HEAD, 16), HEAD)] = (acc[h, pl.ds(16, HEAD)] * scale).astype(bf16)
        qx[h, pl.ds(HEAD + DOCS, 16)] = three_pieces(-jnp.log(totals))
        return carry

    lax.fori_loop(0, QUERY_HEADS, close, 0)
    for job in jobs:
        job.arrive()
        job.drain()
    chain.drain()


def front(grid, shards, z_majors, leads, heads, x, gain, cos, sin, qext, kext, collective_id):
    tokens = x.shape[1]
    shapes = []
    chosen = leads[-1]
    expand = shards[-1]
    rounded = (len(chosen), SLICE, WIDTH) if chosen else expand.shape
    blocks = [*shards[:-1], jax.ShapeDtypeStruct(rounded, bf16)]
    for block, z_major, chosen in zip(blocks, z_majors, leads):
        lead = (grid.nz, grid.nd) if z_major else (grid.nd, grid.nz)
        lead = (len(chosen),) + lead if chosen else lead
        shapes.append(jax.ShapeDtypeStruct(lead + block.shape[-2:], bf16))
    n = len(shards)
    pieces = chunk_list(blocks, leads)
    shapes += [
        jax.ShapeDtypeStruct((QUERY_HEADS, 128, tokens), bf16),
        jax.ShapeDtypeStruct((QUERY_HEADS, tokens, 128), bf16),
        jax.ShapeDtypeStruct((grid.nz, KEY_VALUE_HEADS, tokens, 128), bf16),
        jax.ShapeDtypeStruct((D, tokens), bf16),
    ]
    return pl.pallas_call(
        functools.partial(front_kernel, grid, tuple(z_majors), pieces),
        out_shape=shapes,
        in_specs=[VMEM] * (n + 7),
        out_specs=[ANY] * n + [VMEM] * 4,
        scratch_shapes=[
            pltpu.VMEM((D, tokens), bf16),
            pltpu.VMEM((QKV, tokens), f32),
            pltpu.VMEM((KEY_VALUE_HEADS, tokens, 128), bf16),
            pltpu.VMEM((KEY_VALUE_HEADS, 80, tokens), bf16),
            pltpu.VMEM((QUERY_HEADS, 80, tokens), f32),
            pltpu.VMEM(rounded, bf16),
            pltpu.SemaphoreType.DMA((max(len(pieces), 1), GATHER_SEMS)),
            pltpu.SemaphoreType.DMA((2, grid.nz)),
        ],
        compiler_params=pltpu.CompilerParams(
            collective_id=collective_id, has_side_effects=True, vmem_limit_bytes=60 << 20
        ),
        name="front",
    )(*shards, heads, x, gain, cos, sin, qext, kext)


STEPS = 5
WIDTH = 128
PARTS = 6


def middle_kernel(grid, ready, summed, *refs):
    att, wo, x, ogt, gain, exp_in, dn_in = refs[:7]
    refs = refs[7:]
    late = STEPS - ready
    if late:
        shard, refs = refs[0], refs[1:]
    out, rg, gsum, dwo, dox, dexp, ddn = refs[:7]
    refs = refs[7:]
    if late:
        exp_late, refs = refs[0], refs[1:]
    if summed:
        gexp, refs = refs[0], refs[1:]
    (res, inv, h2, h2t, og, acc_o, acc_h, mixed, dgate, dup, wg, wu, wd, sg, sd, w_sems, o_sems) = refs[:17]
    refs = refs[17:]
    tokens = x.shape[1]
    half = 2 * WIDTH
    schedule = {}
    gathers, sums = [], []
    if late:
        round_steps(shard, refs[0], ready)
    if late or summed:
        here = Here(grid)
        greet(here.peers())
    if late:
        pieces = [(0, k, (0, SLICE)) for k in range(late)]
        rounded, g_sems, refs = refs[0], refs[1], refs[2:]
        gathers = [
            Gather(here, rounded.at[k], exp_late.at[k], g_sems.at[k], False, (0, SLICE)) for k in range(late)
        ]
        for job in gathers:
            job.stage_z()
        for k, job in enumerate(gathers):
            for i, stage in enumerate(job.stages[1:]):
                schedule.setdefault((k, 4 + 2 * k, 9 + 4 * k)[i], []).append(getattr(job, stage))
            schedule.setdefault((ready + k - 1) * PARTS + 1, []).append(job.arrive)
    if summed:
        pieces = [(0, k, (0, SLICE)) for k in range(summed)]
        sums, refs = reduce_jobs(here, [dexp], [gexp], refs, (False,), pieces)
        for k, job in enumerate(sums):
            for i, stage in enumerate(job.stages):
                place = min((k + 1) * PARTS + 2 + 5 * i, STEPS * PARTS - 1)
                schedule.setdefault(place, []).append(getattr(job, stage))

    def fetch_from(source, index, step, slot, go):
        for d in range(4):
            lanes = pl.ds(d * WIDTH, WIDTH)
            go(pltpu.make_async_copy(source.at[index, d], wg.at[slot, :, :, lanes], w_sems.at[slot, 0]))
            go(pltpu.make_async_copy(source.at[index, 4 + d], wu.at[slot, :, :, lanes], w_sems.at[slot, 1]))
            columns = pl.ds(pl.multiple_of(step * WIDTH, WIDTH), WIDTH)
            go(pltpu.make_async_copy(dn_in.at[d, :, columns], wd.at[slot, :, lanes], w_sems.at[slot, 2]))

    def fetch(step):
        slot = lax.rem(step, 2)

        @pl.when(step < ready)
        def _():
            fetch_from(exp_in, step, step, slot, lambda copy: copy.start())

        if late:

            @pl.when(step >= ready)
            def _():
                fetch_from(exp_late, step - ready, step, slot, lambda copy: copy.start())

    def put_expand(step, go):
        for k in range(2):
            for d in range(4):
                lanes = pl.ds(d * WIDTH, WIDTH)
                to = dexp.at[step, 4 * k + d] if not sums_split else dexp.at[(step,) + sums_place(4 * k + d)]
                go(pltpu.make_async_copy(sg.at[k, :, :, lanes], to, o_sems.at[0]))

    def put_down(step, go):
        for d in range(4):
            columns = pl.ds(pl.multiple_of(step * WIDTH, WIDTH), WIDTH)
            go(pltpu.make_async_copy(sd.at[:, pl.ds(d * WIDTH, WIDTH)], ddn.at[d, :, columns], o_sems.at[1]))

    sums_split = len(dexp.shape) == 7

    def sums_place(d):
        return (d // (2 * grid.nx), d // 2 % grid.nx, d % 2)

    fetch(jnp.int32(0))
    total = jnp.zeros((1, tokens), f32)
    for m in range(DEPTH):
        rows = pl.ds(m * SLICE, SLICE)
        r = x[rows].astype(f32)
        for k in range(DEPTH):
            r += mm(wo[k, rows], att[pl.ds(k * SLICE, SLICE)])
        res[rows] = r
        total += jnp.sum(r * r, axis=0, keepdims=True)
    inverse = lax.rsqrt(total * (1.0 / D) + norm_epsilon)
    inv[...] = inverse
    for m in range(DEPTH):
        rows = pl.ds(m * SLICE, SLICE)
        h2t[rows] = (res[rows] * inverse * gain[rows, 1:2]).astype(bf16)
    h2[...] = h2t[...].astype(f32).T.astype(bf16)
    og[...] = ogt[...].astype(f32).T.astype(bf16)
    acc_o[...] = jnp.zeros_like(acc_o)
    acc_h[...] = jnp.zeros_like(acc_h)

    def activate(slot, k):
        cols = pl.ds(k * half, half)
        gate = mm(h2[...], wg[slot, :, :, cols].reshape(D, half))
        up = mm(h2[...], wu[slot, :, :, cols].reshape(D, half))
        back = mm(og[...], wd[slot, :, cols])
        s = 1.0 / (1.0 + jnp.exp(-gate))
        silu = gate * s
        mixed[:, cols] = (silu * up).astype(bf16)
        dgate[:, cols] = (back * up * s * (1.0 + gate * (1.0 - s))).astype(bf16)
        dup[:, cols] = (back * silu).astype(bf16)

    def micro(t, carry):
        step = t // PARTS
        part = lax.rem(t, PARTS)
        slot = lax.rem(step, 2)

        for place, ticks in schedule.items():

            @pl.when(t == place)
            def _():
                for tick in ticks:
                    tick()

        @pl.when(part == 0)
        def _():
            wait_bytes(wg.at[slot], w_sems.at[slot, 0])
            wait_bytes(wu.at[slot], w_sems.at[slot, 1])
            wait_bytes(wd.at[slot], w_sems.at[slot, 2])
            activate(slot, 0)

        @pl.when(part == 1)
        def _():
            @pl.when(step > 0)
            def _():
                wait_bytes(sg, o_sems.at[0])
                wait_bytes(sd, o_sems.at[1])

            pl.when(step + 1 < STEPS)(lambda: fetch(step + 1))
            activate(slot, 1)

        @pl.when(part == 2)
        def _():
            acc_o[...] += mm_nt(wd[slot], mixed[...])

        @pl.when(part == 3)
        def _():
            for m in range(DEPTH):
                sg[0, m] = mm(h2t[pl.ds(m * SLICE, SLICE)], dgate[...]).astype(bf16)
                sg[1, m] = mm(h2t[pl.ds(m * SLICE, SLICE)], dup[...]).astype(bf16)
            put_expand(step, lambda copy: copy.start())

        @pl.when(part == 4)
        def _():
            sd[...] = mm(ogt[...], mixed[...]).astype(bf16)
            put_down(step, lambda copy: copy.start())

        @pl.when(part == 5)
        def _():
            acc_h[...] += mm_nt(wg[slot].reshape(D, 2 * half), dgate[...])
            acc_h[...] += mm_nt(wu[slot].reshape(D, 2 * half), dup[...])

        return carry

    lax.fori_loop(0, STEPS * PARTS, micro, 0)
    wait_bytes(sg, o_sems.at[0])
    wait_bytes(sd, o_sems.at[1])
    inverse = inv[...]
    total = jnp.zeros((1, tokens), f32)
    for m in range(DEPTH):
        rows = pl.ds(m * SLICE, SLICE)
        out[rows] = (res[rows] + acc_o[rows]).astype(bf16)
        normed = res[rows] * inverse
        up = acc_h[rows]
        gsum[rows] = jnp.sum(up * normed, axis=1, keepdims=True)
        total += jnp.sum(up * gain[rows, 1:2] * normed, axis=0, keepdims=True)
    mean = total * (1.0 / D)
    for m in range(DEPTH):
        rows = pl.ds(m * SLICE, SLICE)
        normed = res[rows] * inverse
        r = ogt[rows].astype(f32) + inverse * (acc_h[rows] * gain[rows, 1:2] - normed * mean)
        rg[rows] = r
        h2t[rows] = r.astype(bf16)
    for k in range(DEPTH):
        rows = pl.ds(k * SLICE, SLICE)
        dwo[k] = mm_nt(h2t[...], att[rows]).astype(bf16)
        acc_h[rows] = mm_tn(wo[k], h2t[...])

    def rows_of(h, carry):
        rows = pl.ds(pl.multiple_of(h * HEAD, 16), HEAD)
        grad = acc_h[rows].astype(bf16)
        dox[h, pl.ds(HEAD, HEAD)] = grad
        delta = jnp.sum(grad.astype(f32) * att[rows].astype(f32), axis=0, keepdims=True)
        dox[h, pl.ds(0, 16)] = three_pieces(-delta)
        dox[h, pl.ds(16, 48)] = jnp.zeros((48, tokens), bf16)
        return carry

    lax.fori_loop(0, QUERY_HEADS, rows_of, 0)
    for job in gathers + sums:
        job.drain()


def middle(grid, att, wo, x, ogt, gain, expand, down, shard, summed, collective_id):
    tokens = x.shape[1]
    ready = expand.shape[0]
    late = STEPS - ready
    blocks = expand.shape[1:]
    if summed:
        grads = (STEPS, grid.ny, grid.nx, 2) + blocks[1:]
    else:
        grads = (STEPS,) + blocks
    shapes = [
        jax.ShapeDtypeStruct((D, tokens), bf16),
        jax.ShapeDtypeStruct((D, tokens), f32),
        jax.ShapeDtypeStruct((D, 1), f32),
        jax.ShapeDtypeStruct((DEPTH, D, SLICE), bf16),
        jax.ShapeDtypeStruct((QUERY_HEADS, 128, tokens), bf16),
        jax.ShapeDtypeStruct(grads, bf16),
        jax.ShapeDtypeStruct(down.shape, bf16),
    ]
    out_specs = [VMEM] * 5 + [ANY] * 2
    inputs = [att, wo, x, ogt, gain, expand, down]
    in_specs = [VMEM] * 5 + [ANY] * 2
    scratch = [
        pltpu.VMEM((D, tokens), f32),
        pltpu.VMEM((1, tokens), f32),
        pltpu.VMEM((tokens, D), bf16),
        pltpu.VMEM((D, tokens), bf16),
        pltpu.VMEM((tokens, D), bf16),
        pltpu.VMEM((D, tokens), f32),
        pltpu.VMEM((D, tokens), f32),
        pltpu.VMEM((tokens, 4 * WIDTH), bf16),
        pltpu.VMEM((tokens, 4 * WIDTH), bf16),
        pltpu.VMEM((tokens, 4 * WIDTH), bf16),
        pltpu.VMEM((2, DEPTH, SLICE, 4 * WIDTH), bf16),
        pltpu.VMEM((2, DEPTH, SLICE, 4 * WIDTH), bf16),
        pltpu.VMEM((2, D, 4 * WIDTH), bf16),
        pltpu.VMEM((2, DEPTH, SLICE, 4 * WIDTH), bf16),
        pltpu.VMEM((D, 4 * WIDTH), bf16),
        pltpu.SemaphoreType.DMA((2, 3)),
        pltpu.SemaphoreType.DMA((2,)),
    ]
    if late:
        inputs.append(shard)
        in_specs.append(VMEM)
        shapes.append(jax.ShapeDtypeStruct((late,) + blocks, bf16))
        out_specs.append(ANY)
        scratch.append(pltpu.VMEM((late, SLICE, WIDTH), bf16))
        scratch.append(pltpu.SemaphoreType.DMA((late, GATHER_SEMS)))
    if summed:
        shapes.append(jax.ShapeDtypeStruct((summed,) + blocks[2:], f32))
        out_specs.append(VMEM)
        pieces = [(0, k, (0, SLICE)) for k in range(summed)]
        term = jax.ShapeDtypeStruct(blocks, bf16)
        scratch += reduce_scratch(grid, [term], (False,), pieces)
    params = dict(collective_id=collective_id, has_side_effects=True) if late or summed else {}
    return pl.pallas_call(
        functools.partial(middle_kernel, grid, ready, summed),
        out_shape=shapes,
        in_specs=in_specs,
        out_specs=out_specs,
        scratch_shapes=scratch,
        compiler_params=pltpu.CompilerParams(vmem_limit_bytes=62 << 20, **params),
        name="middle",
    )(*inputs)


class GradChain:
    def __init__(self, here, part, sent, got, sems):
        self.h, self.part, self.sent, self.got, self.sems = here, part, sent, got, sems

    def summed(self, slot, g, write):
        h = self.h

        @pl.when(h.z < h.grid.nz - 1)
        def _():
            wait_bytes(self.got.at[slot, g], self.sems.at[1, slot, g])
            write(g, self.part[slot, g] + self.got[slot, g].astype(f32))

        @pl.when(h.z == h.grid.nz - 1)
        def _():
            write(g, self.part[slot, g])

    def relay(self, slot, g):
        h = self.h

        def write(g, value):
            self.sent[slot, g] = value.astype(bf16)

        self.summed(slot, g, write)
        to = lax.rem(h.z + h.grid.nz - 1, h.grid.nz)
        sems = self.sems
        send(self.sent.at[slot, g], self.got.at[slot, g], sems.at[0, slot, g], sems.at[1, slot, g], h.on_z(to))

    def drain(self):
        h = self.h

        def body(t, carry):
            slot, g = t // KEY_VALUE_HEADS, lax.rem(t, KEY_VALUE_HEADS)
            wait_bytes(self.sent.at[slot, g], self.sems.at[0, slot, g])
            return carry

        lax.fori_loop(0, h.z * KEY_VALUE_HEADS, body, 0)


def back_kernel(grid, z_majors, pieces, early, *refs):
    n = len(z_majors)
    terms, refs = refs[:n], refs[n:]
    qx, qn, dox, kv, kext, cos, sin = refs[:7]
    refs = refs[7:]
    if early:
        first, refs = refs[0], refs[1:]
    results, refs = refs[:n], refs[n:]
    for k in range(early):
        results[1][:, pl.ds(k * WIDTH, WIDTH)] = first[k]
    hd, refs = refs[0], refs[1:]
    here = Here(grid)
    jobs, refs = reduce_jobs(here, terms, results, refs, z_majors, pieces)
    don, kx, vx, kt, dq, part, sent, got, kv_sems = refs
    tokens = dox.shape[2]
    half = tokens // 2
    greet(here.peers())
    ticks = pipelined(jobs, len(jobs))
    for tick in ticks[: len(jobs)]:
        tick()
    ticks = ticks[len(jobs) :]

    def gather_queries(h, carry):
        dq[h] = jnp.zeros((HEAD, tokens), f32)
        don[h] = dox[h].astype(f32).T.astype(bf16)
        return carry

    lax.fori_loop(0, QUERY_HEADS, gather_queries, 0)

    def prepare(slot):
        ext = kext[pl.ds(pl.multiple_of(slot * tokens, 16), tokens)]

        def body(g, carry):
            block = kv[slot, g]
            low = lanes_below(block.shape, HEAD)
            kx[g] = jnp.where(low, block, ext)
            ones = jnp.where(lanes_below(block.shape, 3), 1.0, 0.0).astype(bf16)
            vx[g] = jnp.where(low, ones, block)
            kt[g] = block.astype(f32).T[:HEAD].astype(bf16)
            return carry

        lax.fori_loop(0, KEY_VALUE_HEADS, body, 0)

    def tile(g, h, count, k, masked):
        keys, cols = pl.ds(0, count), pl.ds(k * half, half)
        s = mm(kx[g, keys], qx[h, :, cols])
        if masked:
            row = lax.broadcasted_iota(jnp.int32, s.shape, 0)
            col = lax.broadcasted_iota(jnp.int32, s.shape, 1) + k * half
            s = jnp.where(row <= col, s, HIDE)
        p = jnp.exp(s)
        ds = (p * mm(vx[g, keys], dox[h, :, cols])).astype(bf16)
        dq[h, :, cols] += mm(kt[g, :, keys], ds)
        dk = mm(ds, qn[h, cols])
        dv = mm(p.astype(bf16), don[h, cols])
        return jnp.where(lanes_below(dk.shape, HEAD), dk, dv)

    def whole(slot, g):
        total = None
        for i in range(GROUP):
            for k in range(2):
                new = tile(g, g * GROUP + i, tokens, k, False)
                total = new if total is None else total + new
        part[slot, g] = total

    def diagonal(g):
        total = None
        for i in range(GROUP):
            new = tile(g, g * GROUP + i, tokens, 1, True)
            total = new if total is None else total + new
        part[here.z, g] = total
        total = part[here.z, g, pl.ds(0, half)]
        for i in range(GROUP):
            total += tile(g, g * GROUP + i, half, 0, True)
        part[here.z, g, pl.ds(0, half)] = total

    chain = GradChain(here, part, sent, got, kv_sems)
    micros = grid.nz * KEY_VALUE_HEADS
    top = here.z == grid.nz - 1

    def micro(t, carry):
        slot = t // KEY_VALUE_HEADS
        g = lax.rem(t, KEY_VALUE_HEADS)

        @pl.when(slot <= here.z)
        def _():
            pl.when(g == 0)(lambda: prepare(slot))

            @pl.when(slot < here.z)
            def _():
                whole(slot, g)
                pl.when(top)(lambda: chain.relay(slot, g))

            pl.when(slot == here.z)(lambda: diagonal(g))

        @pl.when(jnp.logical_and(jnp.logical_not(top), jnp.logical_and(slot >= 1, slot <= here.z)))
        def _():
            chain.relay(slot - 1, g)

        for k, tick in enumerate(ticks):
            pl.when(t == k * micros // len(ticks))(tick)
        return carry

    lax.fori_loop(0, micros, micro, 0)

    def turn_back(a, b):
        c, s = cos[...], sin[...]
        return a * c + b * s, b * c - a * s

    def queries(h, carry):
        scale = HEAD**-0.5
        a, b = turn_back(dq[h, pl.ds(0, 32)] * scale, dq[h, pl.ds(32, 32)] * scale)
        hd[pl.ds(pl.multiple_of(h * HEAD, 16), 32)] = a.astype(bf16)
        hd[pl.ds(pl.multiple_of(h * HEAD + 32, 16), 32)] = b.astype(bf16)
        return carry

    lax.fori_loop(0, QUERY_HEADS, queries, 0)

    def write(g, value):
        turned = value.T
        a, b = turn_back(turned[:32], turned[32:64])
        base = (QUERY_HEADS + g) * HEAD
        hd[pl.ds(pl.multiple_of(base, 16), 32)] = a.astype(bf16)
        hd[pl.ds(pl.multiple_of(base + 32, 16), 32)] = b.astype(bf16)
        base = (QUERY_HEADS + KEY_VALUE_HEADS + g) * HEAD
        hd[pl.ds(pl.multiple_of(base, 16), HEAD)] = turned[64:].astype(bf16)

    def close(g, carry):
        chain.summed(here.z, g, write)
        return carry

    lax.fori_loop(0, KEY_VALUE_HEADS, close, 0)
    chain.drain()
    for job in jobs:
        job.drain()


def back(grid, terms, z_majors, leads, early, qx, qn, dox, kv, kext, cos, sin, collective_id):
    tokens = dox.shape[2]
    n = len(terms)
    pieces = chunk_list(terms, leads)
    shapes = []
    for k, (term, chosen) in enumerate(zip(terms, leads)):
        rows, cols = term.shape[-2:]
        if k == 1:
            shapes.append(jax.ShapeDtypeStruct((rows, cols * term.shape[0] if chosen else cols), f32))
        else:
            shapes.append(jax.ShapeDtypeStruct((grid.nz, rows, cols), bf16))
    scratch = reduce_scratch(grid, terms, z_majors, pieces)
    shapes.append(jax.ShapeDtypeStruct((QKV, tokens), bf16))
    blocks = (grid.nz, KEY_VALUE_HEADS, tokens, 128)
    scratch += [
        pltpu.VMEM((QUERY_HEADS, tokens, 128), bf16),
        pltpu.VMEM((KEY_VALUE_HEADS, tokens, 128), bf16),
        pltpu.VMEM((KEY_VALUE_HEADS, tokens, 128), bf16),
        pltpu.VMEM((KEY_VALUE_HEADS, HEAD, tokens), bf16),
        pltpu.VMEM((QUERY_HEADS, HEAD, tokens), f32),
        pltpu.VMEM(blocks, f32),
        pltpu.VMEM((grid.nz - 1,) + blocks[1:], bf16),
        pltpu.VMEM(blocks, bf16),
        pltpu.SemaphoreType.DMA((2, grid.nz, KEY_VALUE_HEADS)),
    ]
    return pl.pallas_call(
        functools.partial(back_kernel, grid, tuple(z_majors), pieces, 0 if early is None else early.shape[0]),
        out_shape=shapes,
        in_specs=[ANY] * n + [VMEM] * (7 + (early is not None)),
        out_specs=[VMEM] * (n + 1),
        scratch_shapes=scratch,
        compiler_params=pltpu.CompilerParams(
            collective_id=collective_id, has_side_effects=True, vmem_limit_bytes=63 << 20
        ),
        name="back",
    )(*split_terms(grid, terms, z_majors), qx, qn, dox, kv, kext, cos, sin, *([] if early is None else [early]))


def adamw(weight, grad, first, second, rate, decay):
    first_new = beta_one * first + (1.0 - beta_one) * grad
    second_new = beta_two * second + (1.0 - beta_two) * grad * grad
    first_hat = first_new / (1.0 - beta_one**ADAM_STEP)
    second_hat = second_new / (1.0 - beta_two**ADAM_STEP)
    weight_new = weight - rate * (
        first_hat / (jnp.sqrt(second_hat) + adam_epsilon) + decay * weight
    )
    return (weight_new, first_new, second_new)


def finish_kernel(grid, pieces, *refs):
    hd, heads, x, gain, rg, gain_two, down, output, ig, gheads, ggains, gdown, goutput = refs[:13]
    h1, og, flat, wide, terms, value, last_down, last_output, last_sems = refs[13:22]
    here = Here(grid)
    greet(here.peers())
    columns = [Collect(here, down, last_down, last_sems.at[0]), Collect(here, output, last_output, last_sems.at[1])]
    for column in columns:
        column.begin()
    jobs, refs = reduce_jobs(here, [terms], [gheads], refs[22:], (True,), pieces)
    share = Share(here, value, ggains, refs[:4], refs[4])
    tokens = x.shape[1]
    inverse = inverse_rms(x)
    for k in range(DEPTH):
        rows = pl.ds(k * SLICE, SLICE)
        h1[rows] = (x[rows].astype(f32) * inverse * gain[rows, 0:1]).astype(bf16)
    rows = terms.shape[-2]
    for k in range(DEPTH):
        flat[...] = mm_nt(hd[...], h1[pl.ds(k * SLICE, SLICE)])
        for d in range(grid.nd):
            place = (k, d // (2 * grid.nx), d // 2 % grid.nx, d % 2)
            terms[place] = flat[pl.ds(d * rows, rows)].astype(bf16)
    ticks = pipelined(jobs, len(jobs))
    for tick in ticks[: len(jobs)]:
        tick()
    ticks = ticks[len(jobs) :]

    def turn(count=1):
        for _ in range(count):
            if ticks:
                ticks.pop(0)()

    for k in range(DEPTH):
        og[pl.ds(k * SLICE, SLICE)] = mm_tn(heads[k], hd[...])
        if k == 1:
            turn()
    turn()
    total = jnp.zeros((1, tokens), f32)
    for k in range(DEPTH):
        rows = pl.ds(k * SLICE, SLICE)
        normed = x[rows].astype(f32) * inverse
        sums = jnp.sum(og[rows] * normed, axis=1, keepdims=True)
        place = lax.broadcasted_iota(jnp.int32, (SLICE, 128), 1)
        wide[rows] = jnp.where(place == 0, sums, jnp.where(place == 1, gain_two[rows], 0.0))
        total += jnp.sum(og[rows] * gain[rows, 0:1] * normed, axis=0, keepdims=True)
    value[...] = wide[...].T[:8]
    share.start(0)
    turn()
    mean = total * (1.0 / D)
    for k in range(DEPTH):
        rows = pl.ds(k * SLICE, SLICE)
        normed = x[rows].astype(f32) * inverse
        ig[rows] = rg[rows] + inverse * (og[rows] * gain[rows, 0:1] - normed * mean)
    turn()
    gdown[...] = columns[0].end()
    goutput[...] = columns[1].end().T
    for k in range(4):
        share.end(k)
        if k < 3:
            share.start(k + 1)
        turn(2)
    turn(len(ticks))
    share.drain()
    for job in jobs + columns:
        job.drain()


def finish(grid, hd, heads, x, gain, rg, gain_two, down, output, collective_id):
    tokens = x.shape[1]
    rows = QKV // grid.nd
    term = jax.ShapeDtypeStruct((rows, SLICE), bf16)
    pieces = chunk_list([term])
    scratch = [
        pltpu.VMEM((D, tokens), bf16),
        pltpu.VMEM((D, tokens), f32),
        pltpu.VMEM((QKV, SLICE), f32),
        pltpu.VMEM((D, 128), f32),
        pltpu.VMEM((grid.nz, grid.ny, grid.nx, 2, rows, SLICE), bf16),
        pltpu.VMEM((8, D), f32),
        pltpu.VMEM(down.shape, bf16),
        pltpu.VMEM(output.shape, bf16),
        pltpu.SemaphoreType.DMA((2, 2)),
    ]
    scratch += reduce_scratch(grid, [term], (True,), pieces)
    scratch += Share.scratch(grid, (8, D))
    scratch.append(pltpu.SemaphoreType.DMA((SHARE_SEMS,)))
    return pl.pallas_call(
        functools.partial(finish_kernel, grid, pieces),
        out_shape=[
            jax.ShapeDtypeStruct((D, tokens), f32),
            jax.ShapeDtypeStruct((rows, SLICE), f32),
            jax.ShapeDtypeStruct((8, D), f32),
            jax.ShapeDtypeStruct(down.shape[1:], f32),
            jax.ShapeDtypeStruct(output.shape[:0:-1], f32),
        ],
        in_specs=[VMEM] * 8,
        out_specs=[VMEM] * 5,
        scratch_shapes=scratch,
        compiler_params=pltpu.CompilerParams(
            collective_id=collective_id, has_side_effects=True, vmem_limit_bytes=62 << 20
        ),
        name="finish",
    )(hd, heads, x, gain, rg, gain_two, down, output)


READY = 3
SUMMED = 1


def local(
    grid,
    hidden_in,
    out_grad,
    seg_ids,
    doc_start,
    norm_gains,
    heads_weight,
    output_weight,
    expand_weight,
    down_weight,
    gains_first,
    gains_second,
    heads_first,
    heads_second,
    output_first,
    output_second,
    expand_first,
    expand_second,
    down_first,
    down_second,
):
    tokens = hidden_in.shape[0]
    first_row = lax.axis_index("shard") * tokens
    positions = first_row + jnp.arange(tokens, dtype=jnp.int32)
    freq = jnp.power(10000.0, -jnp.arange(HEAD // 2).astype(f32) / (HEAD // 2))
    angle = (positions - doc_start).astype(f32)[None, :] * freq[:, None]
    cos, sin = jnp.cos(angle), jnp.sin(angle)
    seg_row = seg_ids[0]
    seg_query = lax.dynamic_slice_in_dim(seg_row, first_row, tokens)
    doc = jnp.arange(HEAD, dtype=jnp.int32)
    qext = jnp.where((doc[:, None] < DOCS) & (seg_query[None, :] == doc[:, None]), HIDE, 0.0).astype(bf16)
    lane = jnp.arange(128, dtype=jnp.int32) - HEAD
    other_doc = (lane[None, :] >= 0) & (lane[None, :] < DOCS) & (seg_row[:, None] != lane[None, :])
    kext = jnp.where(other_doc | ((lane >= DOCS) & (lane < DOCS + 3))[None, :], 1.0, 0.0).astype(bf16)
    x, ogt = hidden_in.T, out_grad.T
    gain = norm_gains.T

    heads_stack, *columns = gather_weights(
        grid, [heads_weight.T], (True,), [output_weight, down_weight.T], (False, True, False), 1
    )
    heads = heads_stack.reshape(DEPTH, QKV, SLICE)
    stepped = expand_weight.shape[1] == STEPS * WIDTH
    leads = [None, None, list(range(READY)) if stepped else None]
    shards = [*columns, expand_weight]
    output_stack, down_stack, expand_stack, qx, qn, kv, att = front(
        grid, shards, (True, True, False), leads, heads, x, gain, cos, sin, qext, kext, 2
    )
    wo = output_stack.reshape(DEPTH, D, SLICE)
    down = down_stack.reshape(DEPTH, D, FF // DEPTH)
    blocks = (8, DEPTH, SLICE)
    if stepped:
        late = middle(grid, att, wo, x, ogt, gain, expand_stack, down, expand_weight, SUMMED, 5)
        out, rg, gain_two_term, dwo, dox, dexpand, ddn, *late = late
        early_exp = late[-1] if SUMMED else None
    else:
        expand = expand_stack.transpose(1, 2, 0, 3).reshape(DEPTH, SLICE, 8, STEPS, WIDTH)
        expand = expand.transpose(3, 2, 0, 1, 4)
        out, rg, gain_two_term, dwo, dox, dexpand, ddn = middle(
            grid, att, wo, x, ogt, gain, expand, down, None, 0, 5
        )
        early_exp = None
        dexpand = dexpand.transpose(2, 3, 1, 0, 4).reshape(DEPTH, SLICE, grid.nd, -1).transpose(2, 0, 1, 3)
    if stepped:
        dexpand = dexpand.reshape((STEPS, grid.nd, grid.nz, SLICE, WIDTH))
    terms = [ddn.reshape(down_stack.shape), dexpand, dwo.reshape(output_stack.shape)]
    leads = [None, list(range(SUMMED, STEPS)) if stepped else None, None]
    down_column, expand_grad, output_column, hd = back(
        grid, terms, (True, False, True), leads, early_exp, qx, qn, dox, kv, kext, cos, sin, 3
    )
    ig, heads_grad, gains_grad, down_grad, output_grad = finish(
        grid, hd, heads, x, gain, rg, gain_two_term, down_column, output_column, 4
    )
    heads_grad, down_grad, gains_grad = heads_grad.T, down_grad.T, gains_grad[:2]
    hidden_out, input_grad = out.T, ig.T
    gains_new, gains_first_new, gains_second_new = adamw(
        norm_gains, gains_grad, gains_first, gains_second, gain_rate, 0.0
    )
    heads_new, heads_first_new, heads_second_new = adamw(
        heads_weight, heads_grad, heads_first, heads_second, matrix_rate, decay_rate
    )
    output_new, output_first_new, output_second_new = adamw(
        output_weight, output_grad, output_first, output_second, output_rate, decay_rate
    )
    expand_new, expand_first_new, expand_second_new = adamw(
        expand_weight, expand_grad, expand_first, expand_second, matrix_rate, decay_rate
    )
    down_new, down_first_new, down_second_new = adamw(
        down_weight, down_grad, down_first, down_second, matrix_rate, decay_rate
    )
    return (
        hidden_out,
        input_grad,
        gains_grad,
        heads_grad,
        output_grad,
        expand_grad,
        down_grad,
        gains_new,
        heads_new,
        output_new,
        expand_new,
        down_new,
        gains_first_new,
        gains_second_new,
        heads_first_new,
        heads_second_new,
        output_first_new,
        output_second_new,
        expand_first_new,
        expand_second_new,
        down_first_new,
        down_second_new,
    )


def solution(mesh):
    return jax.shard_map(
        functools.partial(local, Grid(mesh)),
        mesh=mesh,
        in_specs=(
            P(("dp", "shard"), None),
            P(("dp", "shard"), None),
            P("dp", None),
            P(("dp", "shard")),
            P(),
            P("shard", "dp"),
            P("shard", "dp"),
            P("shard", "dp"),
            P("shard", "dp"),
            P(),
            P(),
            P("shard", "dp"),
            P("shard", "dp"),
            P("shard", "dp"),
            P("shard", "dp"),
            P("shard", "dp"),
            P("shard", "dp"),
            P("shard", "dp"),
            P("shard", "dp"),
        ),
        out_specs=(
            P(("dp", "shard"), None),
            P(("dp", "shard"), None),
            P(),
            P("shard", "dp"),
            P("shard", "dp"),
            P("shard", "dp"),
            P("shard", "dp"),
            P(),
            P("shard", "dp"),
            P("shard", "dp"),
            P("shard", "dp"),
            P("shard", "dp"),
            P(),
            P(),
            P("shard", "dp"),
            P("shard", "dp"),
            P("shard", "dp"),
            P("shard", "dp"),
            P("shard", "dp"),
            P("shard", "dp"),
            P("shard", "dp"),
            P("shard", "dp"),
        ),
        check_vma=False,
    )
```

```python
import functools
import math

import jax
import jax.numpy as jnp
from jax import lax
from jax.experimental import pallas as pl
from jax.experimental.pallas import tpu as pltpu
from jax.sharding import PartitionSpec as P

MESH = pl.DeviceIdType.MESH
ANY = pl.BlockSpec(memory_space=pl.ANY)
VMEM = pl.BlockSpec(memory_space=pltpu.VMEM)


class Grid:
    def __init__(self, mesh):
        self.nd = mesh.shape["dp"]
        self.nz = mesh.shape["shard"]
        self.nx = math.isqrt(self.nd // 2)
        self.ny = self.nd // 2 // self.nx
        assert self.nx == self.ny and self.nx * self.ny * 2 == self.nd

    def dp(self, y, x, c):
        return (y * self.nx + x) * 2 + c


class Here:
    def __init__(self, grid):
        self.grid = grid
        d = lax.axis_index("dp")
        self.z = lax.axis_index("shard")
        self.d = d
        self.c = lax.rem(d, 2)
        self.x = lax.rem(d // 2, grid.nx)
        self.y = d // (2 * grid.nx)
        g = grid
        self.xs = [lax.rem(self.x + k, g.nx) for k in range(1, g.nx)]
        self.ys = [lax.rem(self.y + k, g.ny) for k in range(1, g.ny)]
        self.zs = [lax.rem(self.z + k, g.nz) for k in range(1, g.nz)]
        self.partner = (g.dp(self.y, self.x, 1 - self.c), self.z)

    def on_x(self, x):
        return (self.grid.dp(self.y, x, self.c), self.z)

    def on_y(self, y):
        return (self.grid.dp(y, self.x, self.c), self.z)

    def on_z(self, z):
        return (self.d, z)

    def peers(self):
        return (
            [self.partner]
            + [self.on_x(x) for x in self.xs]
            + [self.on_y(y) for y in self.ys]
            + [self.on_z(z) for z in self.zs]
        )


def greet(peers):
    barrier = pltpu.get_barrier_semaphore()
    for peer in peers:
        pl.semaphore_signal(barrier, inc=1, device_id=peer, device_id_type=MESH)
    pl.semaphore_wait(barrier, len(peers))


def send(src, dst, send_sem, recv_sem, device):
    pltpu.make_async_remote_copy(
        src_ref=src,
        dst_ref=dst,
        send_sem=send_sem,
        recv_sem=recv_sem,
        device_id=device,
        device_id_type=MESH,
    ).start()


def wait_bytes(ref, sem):
    pltpu.make_async_copy(ref, ref, sem).wait()


def half_rows(rows):
    return max(16, int(rows / 32 + 0.5) * 16)


def chunks_of(rows, size=64):
    starts = list(range(0, rows, size))
    if len(starts) > 1 and rows - starts[-1] < size // 2:
        starts.pop()
    return [(start, stop - start) for start, stop in zip(starts, starts[1:] + [rows])]


class Gather:
    def __init__(self, here, shard, out, sems, z_major, rows):
        self.h, self.shard, self.out, self.sems, self.z_major = here, shard, out, sems, z_major
        self.start, self.rows = rows
        self.cut = half_rows(self.rows)

    def span(self, half=None):
        if half is None:
            return pl.ds(self.start, self.rows)
        return pl.ds(self.start, self.cut) if half == 0 else pl.ds(self.start + self.cut, self.rows - self.cut)

    def column(self, d, half=None):
        return self.out.at[:, d, self.span(half)] if self.z_major else self.out.at[d, :, self.span(half)]

    def block(self, d, z):
        return self.out.at[z, d, self.span()] if self.z_major else self.out.at[d, z, self.span()]

    def columns(self, count):
        some = pl.ds(0, count)
        return self.out.at[:, some, self.span()] if self.z_major else self.out.at[some, :, self.span()]

    def blocks(self, count):
        some = pl.ds(0, count)
        return self.out.at[some, 0, self.span()] if self.z_major else self.out.at[0, some, self.span()]

    def own(self):
        h = self.h
        return pltpu.make_async_copy(self.shard.at[self.span()], self.block(h.d, h.z), self.sems.at[8])

    def stage_z(self):
        h, s = self.h, self.sems
        for z in h.zs:
            send(self.shard.at[self.span()], self.block(h.d, h.z), s.at[0], s.at[1], h.on_z(z))
        self.own().start()

    def await_z(self):
        wait_bytes(self.blocks(len(self.h.zs)), self.sems.at[1])

    def drain_z(self):
        wait_bytes(self.blocks(len(self.h.zs)), self.sems.at[0])

    def stage_one(self):
        h, s = self.h, self.sems
        self.await_z()
        self.own().wait()
        for x in h.xs:
            send(self.column(h.d, 0), self.column(h.d, 0), s.at[2], s.at[3], h.on_x(x))
        for y in h.ys:
            send(self.column(h.d, 1), self.column(h.d, 1), s.at[2], s.at[3], h.on_y(y))
        send(self.column(h.d), self.column(h.d), s.at[6], s.at[7], h.partner)

    def stage_two(self):
        h, s, g = self.h, self.sems, self.h.grid
        wait_bytes(self.columns(len(h.xs)), s.at[3])
        for y in h.ys:
            for x in [h.x] + h.xs:
                col = self.column(g.dp(h.y, x, h.c), 0)
                send(col, col, s.at[4], s.at[5], h.on_y(y))
        for x in h.xs:
            for y in [h.y] + h.ys:
                col = self.column(g.dp(y, h.x, h.c), 1)
                send(col, col, s.at[4], s.at[5], h.on_x(x))
        for x in h.xs:
            col = self.column(g.dp(h.y, x, h.c), 0)
            send(col, col, s.at[6], s.at[7], h.partner)
        for y in h.ys:
            col = self.column(g.dp(y, h.x, h.c), 1)
            send(col, col, s.at[6], s.at[7], h.partner)

    def stage_three(self):
        h, s, g = self.h, self.sems, self.h.grid
        wait_bytes(self.columns(g.nx * len(h.ys)), s.at[5])
        for y in h.ys:
            for x in [h.x] + h.xs:
                col = self.column(g.dp(y, x, h.c), 0)
                send(col, col, s.at[6], s.at[7], h.partner)
        for x in h.xs:
            for y in [h.y] + h.ys:
                col = self.column(g.dp(y, x, h.c), 1)
                send(col, col, s.at[6], s.at[7], h.partner)

    def arrive(self):
        g = self.h.grid
        wait_bytes(self.columns(g.nd // 2), self.sems.at[7])

    def drain(self):
        h, s, g = self.h, self.sems, self.h.grid
        self.drain_z()
        wait_bytes(self.columns(len(h.xs)), s.at[2])
        wait_bytes(self.columns(g.nx * len(h.ys)), s.at[4])
        wait_bytes(self.columns(g.nd // 2), s.at[6])

    stages = ("stage_z", "stage_one", "stage_two", "stage_three")


class ColumnGather(Gather):
    def own(self):
        return pltpu.make_async_copy(self.shard.at[:, self.span()], self.column(self.h.d), self.sems.at[8])

    def stage_z(self):
        self.own().start()

    def await_z(self):
        pass

    def drain_z(self):
        pass


class Spread:
    def __init__(self, here, shard, out, sems):
        self.h, self.shard, self.out, self.sems = here, shard, out, sems

    def own(self):
        return pltpu.make_async_copy(self.shard, self.out.at[self.h.z], self.sems.at[2])

    def begin(self):
        h, s = self.h, self.sems
        for z in h.zs:
            send(self.shard, self.out.at[h.z], s.at[0], s.at[1], h.on_z(z))
        self.own().start()

    def end(self):
        some = self.out.at[pl.ds(0, len(self.h.zs))]
        wait_bytes(some, self.sems.at[1])
        wait_bytes(some, self.sems.at[0])
        self.own().wait()


def pipelined(jobs, ahead=0):
    ticks = [getattr(job, job.stages[0]) for job in jobs[:ahead]]
    depth = max((len(job.stages) for job in jobs), default=0)
    for step in range(len(jobs) + depth - 1):
        for k in range(depth):
            i = step - k
            if 0 <= i < len(jobs) and k < len(jobs[i].stages) and not (k == 0 and i < ahead):
                ticks.append(getattr(jobs[i], jobs[i].stages[k]))
    return ticks


def chunk_list(shards, leads=None):
    pieces = []
    for i, shard in enumerate(shards):
        if leads is not None and leads[i]:
            pieces += [(i, k, (0, shard.shape[-2])) for k in leads[i]]
        else:
            pieces += [(i, None, rows) for rows in chunks_of(shard.shape[-2])]
    return pieces


def piece_of(ref, lead):
    return ref if lead is None else ref.at[lead]


def gather_jobs(here, shards, outs, sems, z_majors, pieces):
    jobs = []
    for k, (i, lead, rows) in enumerate(pieces):
        kind = ColumnGather if lead is None and len(shards[i].shape) == 3 else Gather
        job = kind(here, piece_of(shards[i], lead), piece_of(outs[i], lead), sems.at[k], z_majors[i], rows)
        jobs.append(job)
    return jobs


GATHER_SEMS = 9


def gather_kernel(grid, z_majors, pieces, turns, *refs):
    n, spreads = len(z_majors), len(turns) - len(z_majors)
    given, refs = refs[: n + spreads], refs[n + spreads :]
    outs, refs = refs[:n], refs[n:]
    columns, refs = refs[:spreads], refs[spreads:]
    rounded, (sems, spread_sems) = refs[: n + spreads], refs[n + spreads :]
    for source, half, turn in zip(given, rounded, turns):
        half[...] = (source[...].T if turn else source[...]).astype(jnp.bfloat16)
    shards, singles = rounded[:n], rounded[n:]
    here = Here(grid)
    greet(here.peers())
    jobs = gather_jobs(here, shards, outs, sems, z_majors, pieces)
    ticks = pipelined(jobs, len(jobs))
    for tick in ticks[: len(jobs)]:
        tick()
    others = [Spread(here, singles[k], columns[k], spread_sems.at[k]) for k in range(spreads)]
    for other in others:
        other.begin()
    for tick in ticks[len(jobs) :]:
        tick()
    for job in jobs:
        job.arrive()
        job.drain()
    for other in others:
        other.end()


def gather_weights(grid, shards, z_majors, singles, turns, collective_id):
    blocks = []
    for value, turn in zip([*shards, *singles], turns):
        blocks.append(jax.ShapeDtypeStruct(value.shape[::-1] if turn else value.shape, jnp.bfloat16))
    n = len(shards)
    shapes = []
    for block, z_major in zip(blocks, z_majors):
        lead = (grid.nz, grid.nd) if z_major else (grid.nd, grid.nz)
        shapes.append(jax.ShapeDtypeStruct(lead + block.shape, block.dtype))
    for block in blocks[n:]:
        shapes.append(jax.ShapeDtypeStruct((grid.nz,) + block.shape, block.dtype))
    pieces = chunk_list(blocks[:n])
    return pl.pallas_call(
        functools.partial(gather_kernel, grid, tuple(z_majors), pieces, tuple(turns)),
        out_shape=shapes,
        in_specs=[VMEM] * len(blocks),
        out_specs=[ANY] * len(shapes),
        scratch_shapes=[pltpu.VMEM(block.shape, block.dtype) for block in blocks]
        + [
            pltpu.SemaphoreType.DMA((len(pieces), GATHER_SEMS)),
            pltpu.SemaphoreType.DMA((len(singles), 3)),
        ],
        compiler_params=pltpu.CompilerParams(collective_id=collective_id, has_side_effects=True),
        name="gather_weights",
    )(*shards, *singles)


class Reduce:
    def __init__(self, here, terms, result, bufs, sems, z_major, rows):
        self.h, self.terms, self.result, self.sems, self.z_major = here, terms, result, sems, z_major
        self.own, self.other, self.one_a, self.one_b, self.two_a, self.two_b, self.last = bufs
        self.start, self.rows = rows
        self.cut = half_rows(self.rows)

    @staticmethod
    def scratch(grid, rows, cols, z_major):
        cut = half_rows(rows)
        ny, nx, nz = grid.ny, grid.nx, grid.nz
        full = (nz, ny, nx) if z_major else (ny, nx, nz)
        row = (nz, nx) if z_major else (nx, nz)
        bf = jnp.bfloat16
        return [
            pltpu.VMEM(full + (rows, cols), bf),
            pltpu.VMEM(full + (rows, cols), bf),
            pltpu.VMEM((ny,) + row + (cut, cols), bf),
            pltpu.VMEM((nx,) + row + (rows - cut, cols), bf),
            pltpu.VMEM((nx, nz, cut, cols), bf),
            pltpu.VMEM((ny, nz, rows - cut, cols), bf),
            pltpu.VMEM((nz, rows, cols), bf),
        ]

    def span(self, half):
        return {None: slice(None), 0: pl.ds(0, self.cut), 1: pl.ds(self.cut, self.rows - self.cut)}[half]

    def at(self, y, x, z, half):
        y, x, z = (slice(None) if v is None else v for v in (y, x, z))
        return (z, y, x, self.span(half)) if self.z_major else (y, x, z, self.span(half))

    def side(self, c):
        rows = pl.ds(self.start, self.rows)
        return self.terms.at[:, :, :, c, rows] if self.z_major else self.terms.at[:, :, c, :, rows]

    def load(self):
        return pltpu.make_async_copy(self.side(self.h.c), self.own, self.sems.at[8])

    def stage_core(self):
        h, s = self.h, self.sems
        send(self.side(1 - h.c), self.other, s.at[0], s.at[1], h.partner)
        self.load().start()

    def add_loop(self, shape, body):
        total = math.prod(shape)

        def step(i, carry):
            place = []
            rest = i
            for size in reversed(shape):
                place.append(lax.rem(rest, size))
                rest = rest // size
            body(tuple(reversed(place)))
            return carry

        lax.fori_loop(0, total, step, 0)

    def stage_one(self):
        h, s, g = self.h, self.sems, self.h.grid
        self.load().wait()
        wait_bytes(self.other, s.at[1])

        def body(place):
            self.own[place] = self.own[place] + self.other[place]

        self.add_loop(self.own.shape[:3], body)
        for y in h.ys:
            send(self.own.at[self.at(y, None, None, 0)], self.one_a.at[h.y], s.at[2], s.at[3], h.on_y(y))
        for x in h.xs:
            send(self.own.at[self.at(None, x, None, 1)], self.one_b.at[h.x], s.at[9], s.at[10], h.on_x(x))

    def stage_two(self):
        h, s, g = self.h, self.sems, self.h.grid
        wait_bytes(self.one_a.at[pl.ds(0, g.ny - 1)], s.at[3])
        wait_bytes(self.one_b.at[pl.ds(0, g.nx - 1)], s.at[10])

        def body_a(place):
            where = (place[1], place[0]) if self.z_major else place
            spot = self.at(h.y, where[0], where[1], 0)
            total = self.own[spot].astype(jnp.float32)
            for y in h.ys:
                total += self.one_a[(y,) + place].astype(jnp.float32)
            self.own[spot] = total.astype(jnp.bfloat16)

        self.add_loop(self.one_a.shape[1:3], body_a)

        def body_b(place):
            where = (place[1], place[0]) if self.z_major else place
            spot = self.at(where[0], h.x, where[1], 1)
            total = self.own[spot].astype(jnp.float32)
            for x in h.xs:
                total += self.one_b[(x,) + place].astype(jnp.float32)
            self.own[spot] = total.astype(jnp.bfloat16)

        self.add_loop(self.one_b.shape[1:3], body_b)
        for x in h.xs:
            send(self.own.at[self.at(h.y, x, None, 0)], self.two_a.at[h.x], s.at[4], s.at[5], h.on_x(x))
        for y in h.ys:
            send(self.own.at[self.at(y, h.x, None, 1)], self.two_b.at[h.y], s.at[11], s.at[12], h.on_y(y))

    def stage_three(self):
        h, s, g = self.h, self.sems, self.h.grid
        wait_bytes(self.two_a.at[pl.ds(0, g.nx - 1)], s.at[5])
        wait_bytes(self.two_b.at[pl.ds(0, g.ny - 1)], s.at[12])

        def body(place):
            (z,) = place
            spot = self.at(h.y, h.x, z, 0)
            total = self.own[spot].astype(jnp.float32)
            for x in h.xs:
                total += self.two_a[x, z].astype(jnp.float32)
            self.own[spot] = total.astype(jnp.bfloat16)
            spot = self.at(h.y, h.x, z, 1)
            total = self.own[spot].astype(jnp.float32)
            for y in h.ys:
                total += self.two_b[y, z].astype(jnp.float32)
            self.own[spot] = total.astype(jnp.bfloat16)

        self.add_loop((g.nz,), body)
        for z in h.zs:
            send(self.own.at[self.at(h.y, h.x, z, None)], self.last.at[h.z], s.at[6], s.at[7], h.on_z(z))

    def finish(self):
        h, s, g = self.h, self.sems, self.h.grid
        wait_bytes(self.last.at[pl.ds(0, g.nz - 1)], s.at[7])
        total = self.own[self.at(h.y, h.x, h.z, None)].astype(jnp.float32)
        for z in h.zs:
            total += self.last[z].astype(jnp.float32)
        self.result[pl.ds(self.start, self.rows)] = total

    stages = ("stage_core", "stage_one", "stage_two", "stage_three", "finish")

    def drain_z(self):
        wait_bytes(self.last.at[pl.ds(0, self.h.grid.nz - 1)], self.sems.at[6])

    def drain(self):
        g, s = self.h.grid, self.sems
        wait_bytes(self.other, s.at[0])
        wait_bytes(self.one_a.at[pl.ds(0, g.ny - 1)], s.at[2])
        wait_bytes(self.one_b.at[pl.ds(0, g.nx - 1)], s.at[9])
        wait_bytes(self.two_a.at[pl.ds(0, g.nx - 1)], s.at[4])
        wait_bytes(self.two_b.at[pl.ds(0, g.ny - 1)], s.at[11])
        self.drain_z()


class ColumnReduce(Reduce):
    stages = ("stage_core", "stage_one", "stage_two", "stage_three")

    def stage_three(self):
        h, s, g = self.h, self.sems, self.h.grid
        wait_bytes(self.two_a.at[pl.ds(0, g.nx - 1)], s.at[5])
        wait_bytes(self.two_b.at[pl.ds(0, g.ny - 1)], s.at[12])

        def body(place):
            (z,) = place
            total = self.own[self.at(h.y, h.x, z, 0)].astype(jnp.float32)
            for x in h.xs:
                total += self.two_a[x, z].astype(jnp.float32)
            self.result[z, pl.ds(self.start, self.cut)] = total.astype(jnp.bfloat16)
            total = self.own[self.at(h.y, h.x, z, 1)].astype(jnp.float32)
            for y in h.ys:
                total += self.two_b[y, z].astype(jnp.float32)
            self.result[z, pl.ds(self.start + self.cut, self.rows - self.cut)] = total.astype(jnp.bfloat16)

        self.add_loop((g.nz,), body)

    def drain_z(self):
        pass


class Collect:
    def __init__(self, here, column, last, sems):
        self.h, self.column, self.last, self.sems = here, column, last, sems

    def begin(self):
        h, s = self.h, self.sems
        for z in h.zs:
            send(self.column.at[z], self.last.at[h.z], s.at[0], s.at[1], h.on_z(z))

    def end(self):
        h = self.h
        wait_bytes(self.last.at[pl.ds(0, len(h.zs))], self.sems.at[1])
        total = self.column[h.z].astype(jnp.float32)
        for z in h.zs:
            total += self.last[z].astype(jnp.float32)
        return total

    def drain(self):
        wait_bytes(self.last.at[pl.ds(0, len(self.h.zs))], self.sems.at[0])


REDUCE_SEMS = 13
REDUCE_BUFS = 7


class Share:
    def __init__(self, here, value, result, bufs, sems):
        self.h, self.value, self.result, self.sems = here, value, result, sems
        self.bufs = bufs

    @staticmethod
    def scratch(grid, shape):
        return [pltpu.VMEM((n,) + shape, jnp.float32) for n in (2, grid.nx, grid.ny, grid.nz)]

    def axis(self, k):
        h = self.h
        return (
            (h.c, [h.partner], 2),
            (h.x, [h.on_x(x) for x in h.xs], h.grid.nx),
            (h.y, [h.on_y(y) for y in h.ys], h.grid.ny),
            (h.z, [h.on_z(z) for z in h.zs], h.grid.nz),
        )[k]

    def start(self, k):
        me, peers, n = self.axis(k)
        self.bufs[k][me] = self.value[...] if k == 0 else self.total
        for peer in peers:
            send(self.bufs[k].at[me], self.bufs[k].at[me], self.sems.at[2 * k], self.sems.at[2 * k + 1], peer)

    def end(self, k):
        me, peers, n = self.axis(k)
        wait_bytes(self.bufs[k].at[pl.ds(0, n - 1)], self.sems.at[2 * k + 1])
        total = self.bufs[k][0]
        for i in range(1, n):
            total = total + self.bufs[k][i]
        self.total = total
        if k == 3:
            self.result[...] = total

    def drain(self):
        for k in range(4):
            n = self.axis(k)[2]
            wait_bytes(self.bufs[k].at[pl.ds(0, n - 1)], self.sems.at[2 * k])


SHARE_SEMS = 8


def reduce_kernel(grid, z_majors, pieces, shared, *refs):
    n = len(z_majors)
    terms, refs = refs[:n], refs[n:]
    value, refs = (refs[0], refs[1:]) if shared else (None, refs)
    results, refs = refs[:n], refs[n:]
    value_sum, refs = (refs[0], refs[1:]) if shared else (None, refs)
    here = Here(grid)
    greet(here.peers())
    jobs, refs = reduce_jobs(here, terms, results, refs, z_majors, pieces)
    share = None
    if shared:
        share = Share(here, value, value_sum, refs[:4], refs[4])
        share.start(0)
    ticks = pipelined(jobs, len(jobs))
    for k, tick in enumerate(ticks):
        tick()
        if share is not None and k >= len(jobs) and k - len(jobs) < 4:
            step = k - len(jobs)
            share.end(step)
            if step < 3:
                share.start(step + 1)
    if share is not None:
        share.drain()
    for job in jobs:
        job.drain()


def reduce_jobs(here, terms, results, refs, z_majors, pieces):
    n = len(pieces)
    sems = refs[n * REDUCE_BUFS]
    jobs = []
    for k, (i, lead, rows) in enumerate(pieces):
        bufs = refs[k * REDUCE_BUFS : (k + 1) * REDUCE_BUFS]
        term, result, kind = piece_of(terms[i], lead), results[i], Reduce
        deep = len(result.shape) == 3
        if lead is None:
            kind = ColumnReduce if deep else Reduce
        else:
            width = term.shape[-1]
            result = result.at[lead] if deep else result.at[:, pl.ds(lead * width, width)]
        jobs.append(kind(here, term, result, bufs, sems.at[k], z_majors[i], rows))
    return jobs, refs[n * REDUCE_BUFS + 1 :]


def reduce_scratch(grid, terms, z_majors, pieces):
    scratch = []
    for i, _, (_, rows) in pieces:
        scratch += Reduce.scratch(grid, rows, terms[i].shape[-1], z_majors[i])
    return scratch + [pltpu.SemaphoreType.DMA((max(len(pieces), 1), REDUCE_SEMS))]


def split_terms(grid, terms, z_majors):
    split = []
    for term, z_major in zip(terms, z_majors):
        lead = (grid.ny, grid.nx, 2)
        lead = (grid.nz,) + lead if z_major else lead + (grid.nz,)
        split.append(term.reshape(term.shape[:-4] + lead + term.shape[-2:]))
    return split


def reduce_grads(grid, terms, z_majors, value, collective_id):
    shapes = [jax.ShapeDtypeStruct(term.shape[-2:], jnp.float32) for term in terms]
    pieces = chunk_list(terms)
    scratch = reduce_scratch(grid, terms, z_majors, pieces)
    n = len(terms)
    shared = value is not None
    if shared:
        shapes.append(jax.ShapeDtypeStruct(value.shape, jnp.float32))
        scratch += Share.scratch(grid, value.shape)
        scratch.append(pltpu.SemaphoreType.DMA((SHARE_SEMS,)))
    return pl.pallas_call(
        functools.partial(reduce_kernel, grid, tuple(z_majors), pieces, shared),
        out_shape=shapes,
        in_specs=[ANY] * n + [VMEM] * shared,
        out_specs=[VMEM] * len(shapes),
        scratch_shapes=scratch,
        compiler_params=pltpu.CompilerParams(
            collective_id=collective_id, has_side_effects=True, vmem_limit_bytes=62 << 20
        ),
        name="reduce_grads",
    )(*split_terms(grid, terms, z_majors), *([value] if shared else []))


D = 960
QUERY_HEADS = 15
KEY_VALUE_HEADS = 5
GROUP = QUERY_HEADS // KEY_VALUE_HEADS
HEAD = 64
FF = 2560
QKV = (QUERY_HEADS + 2 * KEY_VALUE_HEADS) * HEAD
ADAM_STEP = 10
DOCS = 16
HIDE = -1e30
VALUE_SCALE = 2.0**-9

norm_epsilon = 1e-05
beta_one = 0.9
beta_two = 0.95
adam_epsilon = 1e-08
matrix_rate = 0.03
output_rate = 0.15
gain_rate = 0.5
decay_rate = 0.1

f32 = jnp.float32
bf16 = jnp.bfloat16
DEPTH = 4
SLICE = D // DEPTH


def mm(a, b):
    return lax.dot_general(a, b, (((1,), (0,)), ((), ())), preferred_element_type=f32)


def mm_nt(a, b):
    return lax.dot_general(a, b, (((1,), (1,)), ((), ())), preferred_element_type=f32)


def mm_tn(a, b):
    return lax.dot_general(a, b, (((0,), (0,)), ((), ())), preferred_element_type=f32)


def lanes_below(shape, n):
    return lax.broadcasted_iota(jnp.int32, shape, len(shape) - 1) < n


def inverse_rms(ref):
    total = jnp.zeros((1, ref.shape[1]), f32)
    for k in range(DEPTH):
        x = ref[pl.ds(k * SLICE, SLICE)].astype(f32)
        total += jnp.sum(x * x, axis=0, keepdims=True)
    return lax.rsqrt(total * (1.0 / D) + norm_epsilon)


def three_pieces(row):
    hi = row.astype(bf16).astype(f32)
    mid = (row - hi).astype(bf16).astype(f32)
    low = row - hi - mid
    place = lax.broadcasted_iota(jnp.int32, (16, row.shape[1]), 0)
    block = jnp.where(place == 0, hi, jnp.where(place == 1, mid, jnp.where(place == 2, low, 0.0)))
    return block.astype(bf16)


class KeyChain:
    def __init__(self, here, kv, sems):
        self.h, self.kv, self.sems = here, kv, sems

    def up(self, slot):
        h = self.h
        to = lax.rem(h.z + 1, h.grid.nz)

        @pl.when(h.z < h.grid.nz - 1)
        def _():
            send(self.kv.at[slot], self.kv.at[slot], self.sems.at[0, slot], self.sems.at[1, slot], h.on_z(to))

    def take(self, slot):
        wait_bytes(self.kv.at[slot], self.sems.at[1, slot])
        self.up(slot)

    def drain(self):
        h = self.h
        for s in range(h.grid.nz):

            @pl.when(jnp.logical_and(h.z >= s, h.z < h.grid.nz - 1))
            def _():
                wait_bytes(self.kv.at[h.z - s], self.sems.at[0, h.z - s])


def round_steps(source, rounded, start):
    if len(rounded.shape) == 2:
        rounded[...] = source[...].astype(bf16)
    else:
        for k in range(rounded.shape[0]):
            rounded[k] = source[:, pl.ds((start + k) * WIDTH, WIDTH)].astype(bf16)


def front_kernel(grid, z_majors, pieces, late, *refs):
    n = len(z_majors)
    shards, refs = refs[:n], refs[n:]
    heads, x, gain, cos, sin, qext, kext = refs[:7]
    refs = refs[7:]
    outs, refs = refs[:n], refs[n:]
    qx, qn, kv, att = refs[:4]
    refs = refs[4:]
    if late:
        columns, refs = refs[0], refs[1:]
    h1, proj, kx, vt, acc, rounded, sems, kv_sems = refs[:8]
    here = Here(grid)
    tokens = x.shape[1]
    half = tokens // 2
    round_steps(shards[-1], rounded, 0)
    spreads = []
    if late:
        late_rounded, late_sems = refs[8:]
        round_steps(shards[-1], late_rounded, STEPS - late)
        spreads = [Spread(here, late_rounded.at[k], columns.at[k], late_sems.at[k]) for k in range(late)]
    greet(here.peers())
    jobs = gather_jobs(here, [*shards[:-1], rounded], outs, sems, z_majors, pieces)
    ticks = pipelined(jobs, 3)
    for tick in ticks[:3]:
        tick()

    inverse = inverse_rms(x)
    for k in range(DEPTH):
        rows = pl.ds(k * SLICE, SLICE)
        h1[rows] = (x[rows].astype(f32) * inverse * gain[rows, 0:1]).astype(bf16)

    part = QKV // 5

    def project(m, carry):
        rows = pl.ds(pl.multiple_of(m * part, 16), part)
        total = mm(heads[0, rows], h1[pl.ds(0, SLICE)])
        for k in range(1, DEPTH):
            total += mm(heads[k, rows], h1[pl.ds(k * SLICE, SLICE)])
        proj[rows] = total
        return carry

    lax.fori_loop(3, 5, project, 0)

    def turned(h):
        base = h * HEAD
        a = proj[pl.ds(pl.multiple_of(base, 8), HEAD // 2)]
        b = proj[pl.ds(pl.multiple_of(base + HEAD // 2, 8), HEAD // 2)]
        c, s = cos[...], sin[...]
        return a * c - b * s, b * c + a * s

    def keys(g, carry):
        a, b = turned(QUERY_HEADS + g)
        v = proj[pl.ds(pl.multiple_of((QUERY_HEADS + KEY_VALUE_HEADS + g) * HEAD, 8), HEAD)]
        both = jnp.concatenate([a, b, v], axis=0)
        kv[here.z, g] = both.T.astype(bf16)
        return carry

    lax.fori_loop(0, KEY_VALUE_HEADS, keys, 0)
    chain = KeyChain(here, kv, kv_sems)
    chain.up(here.z)
    lax.fori_loop(0, 3, project, 0)

    def queries(h, carry):
        a, b = turned(h)
        scale = HEAD**-0.5
        qx[h, pl.ds(0, 32)] = (a.astype(bf16).astype(f32) * scale).astype(bf16)
        qx[h, pl.ds(32, 32)] = (b.astype(bf16).astype(f32) * scale).astype(bf16)
        qx[h, pl.ds(64, 64)] = qext[...]
        qn[h] = qx[h].astype(f32).T.astype(bf16)
        return carry

    lax.fori_loop(0, QUERY_HEADS, queries, 0)

    def prepare(slot):
        ext = kext[pl.ds(pl.multiple_of(slot * tokens, 16), tokens)]

        def body(g, carry):
            block = kv[slot, g]
            kx[g] = jnp.where(lanes_below(block.shape, HEAD), block, ext)
            turned_block = block.astype(f32).T
            vt[g, pl.ds(0, 16)] = jnp.ones((16, tokens), bf16)
            vt[g, pl.ds(16, HEAD)] = (turned_block[HEAD:] * VALUE_SCALE).astype(bf16)
            return carry

        lax.fori_loop(0, KEY_VALUE_HEADS, body, 0)

    def below(shape, shift):
        return lax.broadcasted_iota(jnp.int32, shape, 0) <= lax.broadcasted_iota(jnp.int32, shape, 1) + shift

    def diagonal(g):
        for i in range(GROUP):
            h = g * GROUP + i
            s = mm(kx[g, pl.ds(0, half)], qx[h, :, pl.ds(0, half)])
            p = jnp.exp(jnp.where(below(s.shape, 0), s, HIDE)).astype(bf16)
            acc[h, :, pl.ds(0, half)] = mm(vt[g, :, pl.ds(0, half)], p)
            s = mm(kx[g], qx[h, :, pl.ds(half, half)])
            p = jnp.exp(jnp.where(below(s.shape, half), s, HIDE)).astype(bf16)
            acc[h, :, pl.ds(half, half)] = mm(vt[g], p)

    def whole(g):
        for i in range(GROUP):
            h = g * GROUP + i
            for k in range(2):
                cols = pl.ds(k * half, half)
                p = jnp.exp(mm(kx[g], qx[h, :, cols])).astype(bf16)
                acc[h, :, cols] += mm(vt[g], p)

    ticks = ticks[3:]

    def micro(t, carry):
        s = t // KEY_VALUE_HEADS
        g = lax.rem(t, KEY_VALUE_HEADS)

        @pl.when(s <= here.z)
        def _():
            slot = here.z - s

            @pl.when(g == 0)
            def _():
                @pl.when(s > 0)
                def _():
                    chain.take(slot)

                prepare(slot)

            @pl.when(s == 0)
            def _():
                diagonal(g)

            @pl.when(s > 0)
            def _():
                whole(g)

        for k, tick in enumerate(ticks):
            pl.when(t == k * (micros - KEY_VALUE_HEADS) // len(ticks))(tick)
        for spread in spreads:
            pl.when(t == micros - 2 * KEY_VALUE_HEADS + 1)(spread.begin)
        return carry

    micros = grid.nz * KEY_VALUE_HEADS
    lax.fori_loop(0, micros, micro, 0)

    def close(h, carry):
        totals = acc[h, pl.ds(0, 1)]
        scale = (1.0 / VALUE_SCALE) / totals
        att[pl.ds(pl.multiple_of(h * HEAD, 16), HEAD)] = (acc[h, pl.ds(16, HEAD)] * scale).astype(bf16)
        qx[h, pl.ds(HEAD + DOCS, 16)] = three_pieces(-jnp.log(totals))
        return carry

    lax.fori_loop(0, QUERY_HEADS, close, 0)
    for job in jobs:
        job.arrive()
        job.drain()
    for spread in spreads:
        spread.end()
    chain.drain()


def front(grid, shards, z_majors, leads, heads, x, gain, cos, sin, qext, kext, collective_id):
    tokens = x.shape[1]
    shapes = []
    chosen = leads[-1]
    expand = shards[-1]
    rounded = (len(chosen), SLICE, WIDTH) if chosen else expand.shape
    blocks = [*shards[:-1], jax.ShapeDtypeStruct(rounded, bf16)]
    for block, z_major, chosen in zip(blocks, z_majors, leads):
        lead = (grid.nz, grid.nd) if z_major else (grid.nd, grid.nz)
        lead = (len(chosen),) + lead if chosen else lead
        shapes.append(jax.ShapeDtypeStruct(lead + block.shape[-2:], bf16))
    n = len(shards)
    pieces = chunk_list(blocks, leads)
    shapes += [
        jax.ShapeDtypeStruct((QUERY_HEADS, 128, tokens), bf16),
        jax.ShapeDtypeStruct((QUERY_HEADS, tokens, 128), bf16),
        jax.ShapeDtypeStruct((grid.nz, KEY_VALUE_HEADS, tokens, 128), bf16),
        jax.ShapeDtypeStruct((D, tokens), bf16),
    ]
    late = STEPS - len(leads[-1]) if leads[-1] else 0
    last = []
    if late:
        shapes.append(jax.ShapeDtypeStruct((late, grid.nz, SLICE, WIDTH), bf16))
        last = [pltpu.VMEM((late, SLICE, WIDTH), bf16), pltpu.SemaphoreType.DMA((late, 3))]
    return pl.pallas_call(
        functools.partial(front_kernel, grid, tuple(z_majors), pieces, late),
        out_shape=shapes,
        in_specs=[VMEM] * (n + 7),
        out_specs=[ANY] * n + [VMEM] * 4 + [ANY] * (late > 0),
        scratch_shapes=[
            pltpu.VMEM((D, tokens), bf16),
            pltpu.VMEM((QKV, tokens), f32),
            pltpu.VMEM((KEY_VALUE_HEADS, tokens, 128), bf16),
            pltpu.VMEM((KEY_VALUE_HEADS, 80, tokens), bf16),
            pltpu.VMEM((QUERY_HEADS, 80, tokens), f32),
            pltpu.VMEM(rounded, bf16),
            pltpu.SemaphoreType.DMA((max(len(pieces), 1), GATHER_SEMS)),
            pltpu.SemaphoreType.DMA((2, grid.nz)),
            *last,
        ],
        compiler_params=pltpu.CompilerParams(
            collective_id=collective_id, has_side_effects=True, vmem_limit_bytes=60 << 20
        ),
        name="front",
    )(*shards, heads, x, gain, cos, sin, qext, kext)


STEPS = 5
WIDTH = 128
PARTS = 6


def middle_kernel(grid, ready, summed, *refs):
    att, wo, x, ogt, gain, exp_in, dn_in = refs[:7]
    refs = refs[7:]
    late = STEPS - ready
    if late:
        shard, refs = refs[0], refs[1:]
    out, rg, gsum, dwo, dox, dexp, ddn = refs[:7]
    refs = refs[7:]
    if late:
        exp_late, refs = refs[0], refs[1:]
    if summed:
        gexp, refs = refs[0], refs[1:]
    (res, inv, h2, h2t, og, acc_o, acc_h, mixed, dgate, dup, wg, wu, wd, sg, sd, w_sems, o_sems) = refs[:17]
    refs = refs[17:]
    tokens = x.shape[1]
    half = 2 * WIDTH
    schedule = {}
    gathers, sums = [], []
    if late or summed:
        here = Here(grid)
        greet(here.peers())
    if late:
        pieces = [(0, k, (0, SLICE)) for k in range(late)]
        g_sems, refs = refs[0], refs[1:]
        gathers = [
            ColumnGather(here, shard.at[k], exp_late.at[k], g_sems.at[k], False, (0, SLICE)) for k in range(late)
        ]
        for job in gathers:
            job.stage_z()
        for job in gathers:
            job.stage_one()
        for k, job in enumerate(gathers):
            for i, stage in enumerate(job.stages[2:]):
                schedule.setdefault((2 * k, 6 + 4 * k)[i], []).append(getattr(job, stage))
            schedule.setdefault((ready + k - 1) * PARTS + 1, []).append(job.arrive)
    if summed:
        pieces = [(0, k, (0, SLICE)) for k in range(summed)]
        sums, refs = reduce_jobs(here, [dexp], [gexp], refs, (False,), pieces)
        for k, job in enumerate(sums):
            for i, stage in enumerate(job.stages):
                place = min((k + 1) * PARTS + 2 + 5 * i, STEPS * PARTS - 1)
                schedule.setdefault(place, []).append(getattr(job, stage))

    def fetch_from(source, index, step, slot, go):
        for d in range(4):
            lanes = pl.ds(d * WIDTH, WIDTH)
            go(pltpu.make_async_copy(source.at[index, d], wg.at[slot, :, :, lanes], w_sems.at[slot, 0]))
            go(pltpu.make_async_copy(source.at[index, 4 + d], wu.at[slot, :, :, lanes], w_sems.at[slot, 1]))
            columns = pl.ds(pl.multiple_of(step * WIDTH, WIDTH), WIDTH)
            go(pltpu.make_async_copy(dn_in.at[d, :, columns], wd.at[slot, :, lanes], w_sems.at[slot, 2]))

    def fetch(step):
        slot = lax.rem(step, 2)

        @pl.when(step < ready)
        def _():
            fetch_from(exp_in, step, step, slot, lambda copy: copy.start())

        if late:

            @pl.when(step >= ready)
            def _():
                fetch_from(exp_late, step - ready, step, slot, lambda copy: copy.start())

    def put_expand(step, go):
        for k in range(2):
            for d in range(4):
                lanes = pl.ds(d * WIDTH, WIDTH)
                to = dexp.at[step, 4 * k + d] if not sums_split else dexp.at[(step,) + sums_place(4 * k + d)]
                go(pltpu.make_async_copy(sg.at[k, :, :, lanes], to, o_sems.at[0]))

    def put_down(step, go):
        for d in range(4):
            columns = pl.ds(pl.multiple_of(step * WIDTH, WIDTH), WIDTH)
            go(pltpu.make_async_copy(sd.at[:, pl.ds(d * WIDTH, WIDTH)], ddn.at[d, :, columns], o_sems.at[1]))

    sums_split = len(dexp.shape) == 7

    def sums_place(d):
        return (d // (2 * grid.nx), d // 2 % grid.nx, d % 2)

    fetch(jnp.int32(0))
    total = jnp.zeros((1, tokens), f32)
    for m in range(DEPTH):
        rows = pl.ds(m * SLICE, SLICE)
        r = x[rows].astype(f32)
        for k in range(DEPTH):
            r += mm(wo[k, rows], att[pl.ds(k * SLICE, SLICE)])
        res[rows] = r
        total += jnp.sum(r * r, axis=0, keepdims=True)
    inverse = lax.rsqrt(total * (1.0 / D) + norm_epsilon)
    inv[...] = inverse
    for m in range(DEPTH):
        rows = pl.ds(m * SLICE, SLICE)
        h2t[rows] = (res[rows] * inverse * gain[rows, 1:2]).astype(bf16)
    h2[...] = h2t[...].astype(f32).T.astype(bf16)
    og[...] = ogt[...].astype(f32).T.astype(bf16)
    acc_o[...] = jnp.zeros_like(acc_o)
    acc_h[...] = jnp.zeros_like(acc_h)

    def activate(slot, k):
        cols = pl.ds(k * half, half)
        gate = mm(h2[...], wg[slot, :, :, cols].reshape(D, half))
        up = mm(h2[...], wu[slot, :, :, cols].reshape(D, half))
        back = mm(og[...], wd[slot, :, cols])
        s = 1.0 / (1.0 + jnp.exp(-gate))
        silu = gate * s
        mixed[:, cols] = (silu * up).astype(bf16)
        dgate[:, cols] = (back * up * s * (1.0 + gate * (1.0 - s))).astype(bf16)
        dup[:, cols] = (back * silu).astype(bf16)

    def micro(t, carry):
        step = t // PARTS
        part = lax.rem(t, PARTS)
        slot = lax.rem(step, 2)

        for place, ticks in schedule.items():

            @pl.when(t == place)
            def _():
                for tick in ticks:
                    tick()

        @pl.when(part == 0)
        def _():
            wait_bytes(wg.at[slot], w_sems.at[slot, 0])
            wait_bytes(wu.at[slot], w_sems.at[slot, 1])
            wait_bytes(wd.at[slot], w_sems.at[slot, 2])
            activate(slot, 0)

        @pl.when(part == 1)
        def _():
            @pl.when(step > 0)
            def _():
                wait_bytes(sg, o_sems.at[0])
                wait_bytes(sd, o_sems.at[1])

            pl.when(step + 1 < STEPS)(lambda: fetch(step + 1))
            activate(slot, 1)

        @pl.when(part == 2)
        def _():
            acc_o[...] += mm_nt(wd[slot], mixed[...])

        @pl.when(part == 3)
        def _():
            for m in range(DEPTH):
                sg[0, m] = mm(h2t[pl.ds(m * SLICE, SLICE)], dgate[...]).astype(bf16)
                sg[1, m] = mm(h2t[pl.ds(m * SLICE, SLICE)], dup[...]).astype(bf16)
            put_expand(step, lambda copy: copy.start())

        @pl.when(part == 4)
        def _():
            sd[...] = mm(ogt[...], mixed[...]).astype(bf16)
            put_down(step, lambda copy: copy.start())

        @pl.when(part == 5)
        def _():
            acc_h[...] += mm_nt(wg[slot].reshape(D, 2 * half), dgate[...])
            acc_h[...] += mm_nt(wu[slot].reshape(D, 2 * half), dup[...])

        return carry

    lax.fori_loop(0, STEPS * PARTS, micro, 0)
    wait_bytes(sg, o_sems.at[0])
    wait_bytes(sd, o_sems.at[1])
    inverse = inv[...]
    total = jnp.zeros((1, tokens), f32)
    for m in range(DEPTH):
        rows = pl.ds(m * SLICE, SLICE)
        out[rows] = (res[rows] + acc_o[rows]).astype(bf16)
        normed = res[rows] * inverse
        up = acc_h[rows]
        gsum[rows] = jnp.sum(up * normed, axis=1, keepdims=True)
        total += jnp.sum(up * gain[rows, 1:2] * normed, axis=0, keepdims=True)
    mean = total * (1.0 / D)
    for m in range(DEPTH):
        rows = pl.ds(m * SLICE, SLICE)
        normed = res[rows] * inverse
        r = ogt[rows].astype(f32) + inverse * (acc_h[rows] * gain[rows, 1:2] - normed * mean)
        rg[rows] = r
        h2t[rows] = r.astype(bf16)
    for k in range(DEPTH):
        rows = pl.ds(k * SLICE, SLICE)
        dwo[k] = mm_nt(h2t[...], att[rows]).astype(bf16)
        acc_h[rows] = mm_tn(wo[k], h2t[...])

    def rows_of(h, carry):
        rows = pl.ds(pl.multiple_of(h * HEAD, 16), HEAD)
        grad = acc_h[rows].astype(bf16)
        dox[h, pl.ds(HEAD, HEAD)] = grad
        delta = jnp.sum(grad.astype(f32) * att[rows].astype(f32), axis=0, keepdims=True)
        dox[h, pl.ds(0, 16)] = three_pieces(-delta)
        dox[h, pl.ds(16, 48)] = jnp.zeros((48, tokens), bf16)
        return carry

    lax.fori_loop(0, QUERY_HEADS, rows_of, 0)
    for job in gathers + sums:
        job.drain()


def middle(grid, att, wo, x, ogt, gain, expand, down, shard, summed, collective_id):
    tokens = x.shape[1]
    ready = expand.shape[0]
    late = STEPS - ready
    blocks = expand.shape[1:]
    if summed:
        grads = (STEPS, grid.ny, grid.nx, 2) + blocks[1:]
    else:
        grads = (STEPS,) + blocks
    shapes = [
        jax.ShapeDtypeStruct((D, tokens), bf16),
        jax.ShapeDtypeStruct((D, tokens), f32),
        jax.ShapeDtypeStruct((D, 1), f32),
        jax.ShapeDtypeStruct((DEPTH, D, SLICE), bf16),
        jax.ShapeDtypeStruct((QUERY_HEADS, 128, tokens), bf16),
        jax.ShapeDtypeStruct(grads, bf16),
        jax.ShapeDtypeStruct(down.shape, bf16),
    ]
    out_specs = [VMEM] * 5 + [ANY] * 2
    inputs = [att, wo, x, ogt, gain, expand, down]
    in_specs = [VMEM] * 5 + [ANY] * 2
    scratch = [
        pltpu.VMEM((D, tokens), f32),
        pltpu.VMEM((1, tokens), f32),
        pltpu.VMEM((tokens, D), bf16),
        pltpu.VMEM((D, tokens), bf16),
        pltpu.VMEM((tokens, D), bf16),
        pltpu.VMEM((D, tokens), f32),
        pltpu.VMEM((D, tokens), f32),
        pltpu.VMEM((tokens, 4 * WIDTH), bf16),
        pltpu.VMEM((tokens, 4 * WIDTH), bf16),
        pltpu.VMEM((tokens, 4 * WIDTH), bf16),
        pltpu.VMEM((2, DEPTH, SLICE, 4 * WIDTH), bf16),
        pltpu.VMEM((2, DEPTH, SLICE, 4 * WIDTH), bf16),
        pltpu.VMEM((2, D, 4 * WIDTH), bf16),
        pltpu.VMEM((2, DEPTH, SLICE, 4 * WIDTH), bf16),
        pltpu.VMEM((D, 4 * WIDTH), bf16),
        pltpu.SemaphoreType.DMA((2, 3)),
        pltpu.SemaphoreType.DMA((2,)),
    ]
    if late:
        inputs.append(shard)
        in_specs.append(VMEM)
        shapes.append(jax.ShapeDtypeStruct((late,) + blocks, bf16))
        out_specs.append(ANY)
        scratch.append(pltpu.SemaphoreType.DMA((late, GATHER_SEMS)))
    if summed:
        shapes.append(jax.ShapeDtypeStruct((summed,) + blocks[2:], f32))
        out_specs.append(VMEM)
        pieces = [(0, k, (0, SLICE)) for k in range(summed)]
        term = jax.ShapeDtypeStruct(blocks, bf16)
        scratch += reduce_scratch(grid, [term], (False,), pieces)
    params = dict(collective_id=collective_id, has_side_effects=True) if late or summed else {}
    return pl.pallas_call(
        functools.partial(middle_kernel, grid, ready, summed),
        out_shape=shapes,
        in_specs=in_specs,
        out_specs=out_specs,
        scratch_shapes=scratch,
        compiler_params=pltpu.CompilerParams(vmem_limit_bytes=62 << 20, **params),
        name="middle",
    )(*inputs)


class GradChain:
    def __init__(self, here, part, sent, got, sems):
        self.h, self.part, self.sent, self.got, self.sems = here, part, sent, got, sems

    def summed(self, slot, g, write):
        h = self.h

        @pl.when(h.z < h.grid.nz - 1)
        def _():
            wait_bytes(self.got.at[slot, g], self.sems.at[1, slot, g])
            write(g, self.part[slot, g] + self.got[slot, g].astype(f32))

        @pl.when(h.z == h.grid.nz - 1)
        def _():
            write(g, self.part[slot, g])

    def relay(self, slot, g):
        h = self.h

        def write(g, value):
            self.sent[slot, g] = value.astype(bf16)

        self.summed(slot, g, write)
        to = lax.rem(h.z + h.grid.nz - 1, h.grid.nz)
        sems = self.sems
        send(self.sent.at[slot, g], self.got.at[slot, g], sems.at[0, slot, g], sems.at[1, slot, g], h.on_z(to))

    def drain(self):
        h = self.h

        def body(t, carry):
            slot, g = t // KEY_VALUE_HEADS, lax.rem(t, KEY_VALUE_HEADS)
            wait_bytes(self.sent.at[slot, g], self.sems.at[0, slot, g])
            return carry

        lax.fori_loop(0, h.z * KEY_VALUE_HEADS, body, 0)


def back_kernel(grid, z_majors, pieces, early, *refs):
    n = len(z_majors)
    terms, refs = refs[:n], refs[n:]
    qx, qn, dox, kv, kext, cos, sin = refs[:7]
    refs = refs[7:]
    if early:
        first, refs = refs[0], refs[1:]
    results, refs = refs[:n], refs[n:]
    for k in range(early):
        results[1][:, pl.ds(k * WIDTH, WIDTH)] = first[k]
    hd, refs = refs[0], refs[1:]
    here = Here(grid)
    jobs, refs = reduce_jobs(here, terms, results, refs, z_majors, pieces)
    don, kx, vx, kt, dq, part, sent, got, kv_sems = refs
    tokens = dox.shape[2]
    half = tokens // 2
    greet(here.peers())
    ticks = pipelined(jobs, len(jobs))
    for tick in ticks[: len(jobs)]:
        tick()
    ticks = ticks[len(jobs) :]

    def gather_queries(h, carry):
        dq[h] = jnp.zeros((HEAD, tokens), f32)
        don[h] = dox[h].astype(f32).T.astype(bf16)
        return carry

    lax.fori_loop(0, QUERY_HEADS, gather_queries, 0)

    def prepare(slot):
        ext = kext[pl.ds(pl.multiple_of(slot * tokens, 16), tokens)]

        def body(g, carry):
            block = kv[slot, g]
            low = lanes_below(block.shape, HEAD)
            kx[g] = jnp.where(low, block, ext)
            ones = jnp.where(lanes_below(block.shape, 3), 1.0, 0.0).astype(bf16)
            vx[g] = jnp.where(low, ones, block)
            kt[g] = block.astype(f32).T[:HEAD].astype(bf16)
            return carry

        lax.fori_loop(0, KEY_VALUE_HEADS, body, 0)

    def tile(g, h, count, k, masked):
        keys, cols = pl.ds(0, count), pl.ds(k * half, half)
        s = mm(kx[g, keys], qx[h, :, cols])
        if masked:
            row = lax.broadcasted_iota(jnp.int32, s.shape, 0)
            col = lax.broadcasted_iota(jnp.int32, s.shape, 1) + k * half
            s = jnp.where(row <= col, s, HIDE)
        p = jnp.exp(s)
        ds = (p * mm(vx[g, keys], dox[h, :, cols])).astype(bf16)
        dq[h, :, cols] += mm(kt[g, :, keys], ds)
        dk = mm(ds, qn[h, cols])
        dv = mm(p.astype(bf16), don[h, cols])
        return jnp.where(lanes_below(dk.shape, HEAD), dk, dv)

    def whole(slot, g):
        total = None
        for i in range(GROUP):
            for k in range(2):
                new = tile(g, g * GROUP + i, tokens, k, False)
                total = new if total is None else total + new
        part[slot, g] = total

    def diagonal(g):
        total = None
        for i in range(GROUP):
            new = tile(g, g * GROUP + i, tokens, 1, True)
            total = new if total is None else total + new
        part[here.z, g] = total
        total = part[here.z, g, pl.ds(0, half)]
        for i in range(GROUP):
            total += tile(g, g * GROUP + i, half, 0, True)
        part[here.z, g, pl.ds(0, half)] = total

    chain = GradChain(here, part, sent, got, kv_sems)
    micros = grid.nz * KEY_VALUE_HEADS
    top = here.z == grid.nz - 1

    def micro(t, carry):
        slot = t // KEY_VALUE_HEADS
        g = lax.rem(t, KEY_VALUE_HEADS)

        @pl.when(slot <= here.z)
        def _():
            pl.when(g == 0)(lambda: prepare(slot))

            @pl.when(slot < here.z)
            def _():
                whole(slot, g)
                pl.when(top)(lambda: chain.relay(slot, g))

            pl.when(slot == here.z)(lambda: diagonal(g))

        @pl.when(jnp.logical_and(jnp.logical_not(top), jnp.logical_and(slot >= 1, slot <= here.z)))
        def _():
            chain.relay(slot - 1, g)

        for k, tick in enumerate(ticks):
            pl.when(t == k * micros // len(ticks))(tick)
        return carry

    lax.fori_loop(0, micros, micro, 0)

    def turn_back(a, b):
        c, s = cos[...], sin[...]
        return a * c + b * s, b * c - a * s

    def queries(h, carry):
        scale = HEAD**-0.5
        a, b = turn_back(dq[h, pl.ds(0, 32)] * scale, dq[h, pl.ds(32, 32)] * scale)
        hd[pl.ds(pl.multiple_of(h * HEAD, 16), 32)] = a.astype(bf16)
        hd[pl.ds(pl.multiple_of(h * HEAD + 32, 16), 32)] = b.astype(bf16)
        return carry

    lax.fori_loop(0, QUERY_HEADS, queries, 0)

    def write(g, value):
        turned = value.T
        a, b = turn_back(turned[:32], turned[32:64])
        base = (QUERY_HEADS + g) * HEAD
        hd[pl.ds(pl.multiple_of(base, 16), 32)] = a.astype(bf16)
        hd[pl.ds(pl.multiple_of(base + 32, 16), 32)] = b.astype(bf16)
        base = (QUERY_HEADS + KEY_VALUE_HEADS + g) * HEAD
        hd[pl.ds(pl.multiple_of(base, 16), HEAD)] = turned[64:].astype(bf16)

    def close(g, carry):
        chain.summed(here.z, g, write)
        return carry

    lax.fori_loop(0, KEY_VALUE_HEADS, close, 0)
    chain.drain()
    for job in jobs:
        job.drain()


def back(grid, terms, z_majors, leads, early, qx, qn, dox, kv, kext, cos, sin, collective_id):
    tokens = dox.shape[2]
    n = len(terms)
    pieces = chunk_list(terms, leads)
    shapes = []
    for k, (term, chosen) in enumerate(zip(terms, leads)):
        rows, cols = term.shape[-2:]
        if k == 1:
            shapes.append(jax.ShapeDtypeStruct((rows, cols * term.shape[0] if chosen else cols), f32))
        else:
            shapes.append(jax.ShapeDtypeStruct((grid.nz, rows, cols), bf16))
    scratch = reduce_scratch(grid, terms, z_majors, pieces)
    shapes.append(jax.ShapeDtypeStruct((QKV, tokens), bf16))
    blocks = (grid.nz, KEY_VALUE_HEADS, tokens, 128)
    scratch += [
        pltpu.VMEM((QUERY_HEADS, tokens, 128), bf16),
        pltpu.VMEM((KEY_VALUE_HEADS, tokens, 128), bf16),
        pltpu.VMEM((KEY_VALUE_HEADS, tokens, 128), bf16),
        pltpu.VMEM((KEY_VALUE_HEADS, HEAD, tokens), bf16),
        pltpu.VMEM((QUERY_HEADS, HEAD, tokens), f32),
        pltpu.VMEM(blocks, f32),
        pltpu.VMEM((grid.nz - 1,) + blocks[1:], bf16),
        pltpu.VMEM(blocks, bf16),
        pltpu.SemaphoreType.DMA((2, grid.nz, KEY_VALUE_HEADS)),
    ]
    return pl.pallas_call(
        functools.partial(back_kernel, grid, tuple(z_majors), pieces, 0 if early is None else early.shape[0]),
        out_shape=shapes,
        in_specs=[ANY] * n + [VMEM] * (7 + (early is not None)),
        out_specs=[VMEM] * (n + 1),
        scratch_shapes=scratch,
        compiler_params=pltpu.CompilerParams(
            collective_id=collective_id, has_side_effects=True, vmem_limit_bytes=63 << 20
        ),
        name="back",
    )(*split_terms(grid, terms, z_majors), qx, qn, dox, kv, kext, cos, sin, *([] if early is None else [early]))


def adamw(weight, grad, first, second, rate, decay):
    first_new = beta_one * first + (1.0 - beta_one) * grad
    second_new = beta_two * second + (1.0 - beta_two) * grad * grad
    first_hat = first_new / (1.0 - beta_one**ADAM_STEP)
    second_hat = second_new / (1.0 - beta_two**ADAM_STEP)
    weight_new = weight - rate * (
        first_hat / (jnp.sqrt(second_hat) + adam_epsilon) + decay * weight
    )
    return (weight_new, first_new, second_new)


def finish_kernel(grid, pieces, *refs):
    hd, heads, x, gain, rg, gain_two, down, output, ig, gheads, ggains, gdown, goutput = refs[:13]
    h1, og, flat, wide, terms, value, last_down, last_output, last_sems = refs[13:22]
    here = Here(grid)
    greet(here.peers())
    columns = [Collect(here, down, last_down, last_sems.at[0]), Collect(here, output, last_output, last_sems.at[1])]
    for column in columns:
        column.begin()
    jobs, refs = reduce_jobs(here, [terms], [gheads], refs[22:], (True,), pieces)
    share = Share(here, value, ggains, refs[:4], refs[4])
    tokens = x.shape[1]
    inverse = inverse_rms(x)
    for k in range(DEPTH):
        rows = pl.ds(k * SLICE, SLICE)
        h1[rows] = (x[rows].astype(f32) * inverse * gain[rows, 0:1]).astype(bf16)
    rows = terms.shape[-2]
    for k in range(DEPTH):
        flat[...] = mm_nt(hd[...], h1[pl.ds(k * SLICE, SLICE)])
        for d in range(grid.nd):
            place = (k, d // (2 * grid.nx), d // 2 % grid.nx, d % 2)
            terms[place] = flat[pl.ds(d * rows, rows)].astype(bf16)
    ticks = pipelined(jobs, len(jobs))
    for tick in ticks[: len(jobs)]:
        tick()
    ticks = ticks[len(jobs) :]

    def turn(count=1):
        for _ in range(count):
            if ticks:
                ticks.pop(0)()

    for k in range(DEPTH):
        og[pl.ds(k * SLICE, SLICE)] = mm_tn(heads[k], hd[...])
        if k == 1:
            turn()
    turn()
    total = jnp.zeros((1, tokens), f32)
    for k in range(DEPTH):
        rows = pl.ds(k * SLICE, SLICE)
        normed = x[rows].astype(f32) * inverse
        sums = jnp.sum(og[rows] * normed, axis=1, keepdims=True)
        place = lax.broadcasted_iota(jnp.int32, (SLICE, 128), 1)
        wide[rows] = jnp.where(place == 0, sums, jnp.where(place == 1, gain_two[rows], 0.0))
        total += jnp.sum(og[rows] * gain[rows, 0:1] * normed, axis=0, keepdims=True)
    value[...] = wide[...].T[:8]
    share.start(0)
    turn()
    mean = total * (1.0 / D)
    for k in range(DEPTH):
        rows = pl.ds(k * SLICE, SLICE)
        normed = x[rows].astype(f32) * inverse
        ig[rows] = rg[rows] + inverse * (og[rows] * gain[rows, 0:1] - normed * mean)
    turn()
    gdown[...] = columns[0].end()
    goutput[...] = columns[1].end().T
    for k in range(4):
        share.end(k)
        if k < 3:
            share.start(k + 1)
        turn(2)
    turn(len(ticks))
    share.drain()
    for job in jobs + columns:
        job.drain()


def finish(grid, hd, heads, x, gain, rg, gain_two, down, output, collective_id):
    tokens = x.shape[1]
    rows = QKV // grid.nd
    term = jax.ShapeDtypeStruct((rows, SLICE), bf16)
    pieces = chunk_list([term])
    scratch = [
        pltpu.VMEM((D, tokens), bf16),
        pltpu.VMEM((D, tokens), f32),
        pltpu.VMEM((QKV, SLICE), f32),
        pltpu.VMEM((D, 128), f32),
        pltpu.VMEM((grid.nz, grid.ny, grid.nx, 2, rows, SLICE), bf16),
        pltpu.VMEM((8, D), f32),
        pltpu.VMEM(down.shape, bf16),
        pltpu.VMEM(output.shape, bf16),
        pltpu.SemaphoreType.DMA((2, 2)),
    ]
    scratch += reduce_scratch(grid, [term], (True,), pieces)
    scratch += Share.scratch(grid, (8, D))
    scratch.append(pltpu.SemaphoreType.DMA((SHARE_SEMS,)))
    return pl.pallas_call(
        functools.partial(finish_kernel, grid, pieces),
        out_shape=[
            jax.ShapeDtypeStruct((D, tokens), f32),
            jax.ShapeDtypeStruct((rows, SLICE), f32),
            jax.ShapeDtypeStruct((8, D), f32),
            jax.ShapeDtypeStruct(down.shape[1:], f32),
            jax.ShapeDtypeStruct(output.shape[:0:-1], f32),
        ],
        in_specs=[VMEM] * 8,
        out_specs=[VMEM] * 5,
        scratch_shapes=scratch,
        compiler_params=pltpu.CompilerParams(
            collective_id=collective_id, has_side_effects=True, vmem_limit_bytes=62 << 20
        ),
        name="finish",
    )(hd, heads, x, gain, rg, gain_two, down, output)


READY = 3
SUMMED = 1


def local(
    grid,
    hidden_in,
    out_grad,
    seg_ids,
    doc_start,
    norm_gains,
    heads_weight,
    output_weight,
    expand_weight,
    down_weight,
    gains_first,
    gains_second,
    heads_first,
    heads_second,
    output_first,
    output_second,
    expand_first,
    expand_second,
    down_first,
    down_second,
):
    tokens = hidden_in.shape[0]
    first_row = lax.axis_index("shard") * tokens
    positions = first_row + jnp.arange(tokens, dtype=jnp.int32)
    freq = jnp.power(10000.0, -jnp.arange(HEAD // 2).astype(f32) / (HEAD // 2))
    angle = (positions - doc_start).astype(f32)[None, :] * freq[:, None]
    cos, sin = jnp.cos(angle), jnp.sin(angle)
    seg_row = seg_ids[0]
    seg_query = lax.dynamic_slice_in_dim(seg_row, first_row, tokens)
    doc = jnp.arange(HEAD, dtype=jnp.int32)
    qext = jnp.where((doc[:, None] < DOCS) & (seg_query[None, :] == doc[:, None]), HIDE, 0.0).astype(bf16)
    lane = jnp.arange(128, dtype=jnp.int32) - HEAD
    other_doc = (lane[None, :] >= 0) & (lane[None, :] < DOCS) & (seg_row[:, None] != lane[None, :])
    kext = jnp.where(other_doc | ((lane >= DOCS) & (lane < DOCS + 3))[None, :], 1.0, 0.0).astype(bf16)
    x, ogt = hidden_in.T, out_grad.T
    gain = norm_gains.T

    heads_stack, *columns = gather_weights(
        grid, [heads_weight.T], (True,), [output_weight, down_weight.T], (False, True, False), 1
    )
    heads = heads_stack.reshape(DEPTH, QKV, SLICE)
    stepped = expand_weight.shape[1] == STEPS * WIDTH
    leads = [None, None, list(range(READY)) if stepped else None]
    shards = [*columns, expand_weight]
    output_stack, down_stack, expand_stack, qx, qn, kv, att, *late_columns = front(
        grid, shards, (True, True, False), leads, heads, x, gain, cos, sin, qext, kext, 2
    )
    wo = output_stack.reshape(DEPTH, D, SLICE)
    down = down_stack.reshape(DEPTH, D, FF // DEPTH)
    blocks = (8, DEPTH, SLICE)
    if stepped:
        late = middle(grid, att, wo, x, ogt, gain, expand_stack, down, late_columns[0], SUMMED, 5)
        out, rg, gain_two_term, dwo, dox, dexpand, ddn, *late = late
        early_exp = late[-1] if SUMMED else None
    else:
        expand = expand_stack.transpose(1, 2, 0, 3).reshape(DEPTH, SLICE, 8, STEPS, WIDTH)
        expand = expand.transpose(3, 2, 0, 1, 4)
        out, rg, gain_two_term, dwo, dox, dexpand, ddn = middle(
            grid, att, wo, x, ogt, gain, expand, down, None, 0, 5
        )
        early_exp = None
        dexpand = dexpand.transpose(2, 3, 1, 0, 4).reshape(DEPTH, SLICE, grid.nd, -1).transpose(2, 0, 1, 3)
    if stepped:
        dexpand = dexpand.reshape((STEPS, grid.nd, grid.nz, SLICE, WIDTH))
    terms = [ddn.reshape(down_stack.shape), dexpand, dwo.reshape(output_stack.shape)]
    leads = [None, list(range(SUMMED, STEPS)) if stepped else None, None]
    down_column, expand_grad, output_column, hd = back(
        grid, terms, (True, False, True), leads, early_exp, qx, qn, dox, kv, kext, cos, sin, 3
    )
    ig, heads_grad, gains_grad, down_grad, output_grad = finish(
        grid, hd, heads, x, gain, rg, gain_two_term, down_column, output_column, 4
    )
    heads_grad, down_grad, gains_grad = heads_grad.T, down_grad.T, gains_grad[:2]
    hidden_out, input_grad = out.T, ig.T
    gains_new, gains_first_new, gains_second_new = adamw(
        norm_gains, gains_grad, gains_first, gains_second, gain_rate, 0.0
    )
    heads_new, heads_first_new, heads_second_new = adamw(
        heads_weight, heads_grad, heads_first, heads_second, matrix_rate, decay_rate
    )
    output_new, output_first_new, output_second_new = adamw(
        output_weight, output_grad, output_first, output_second, output_rate, decay_rate
    )
    expand_new, expand_first_new, expand_second_new = adamw(
        expand_weight, expand_grad, expand_first, expand_second, matrix_rate, decay_rate
    )
    down_new, down_first_new, down_second_new = adamw(
        down_weight, down_grad, down_first, down_second, matrix_rate, decay_rate
    )
    return (
        hidden_out,
        input_grad,
        gains_grad,
        heads_grad,
        output_grad,
        expand_grad,
        down_grad,
        gains_new,
        heads_new,
        output_new,
        expand_new,
        down_new,
        gains_first_new,
        gains_second_new,
        heads_first_new,
        heads_second_new,
        output_first_new,
        output_second_new,
        expand_first_new,
        expand_second_new,
        down_first_new,
        down_second_new,
    )


def solution(mesh):
    return jax.shard_map(
        functools.partial(local, Grid(mesh)),
        mesh=mesh,
        in_specs=(
            P(("dp", "shard"), None),
            P(("dp", "shard"), None),
            P("dp", None),
            P(("dp", "shard")),
            P(),
            P("shard", "dp"),
            P("shard", "dp"),
            P("shard", "dp"),
            P("shard", "dp"),
            P(),
            P(),
            P("shard", "dp"),
            P("shard", "dp"),
            P("shard", "dp"),
            P("shard", "dp"),
            P("shard", "dp"),
            P("shard", "dp"),
            P("shard", "dp"),
            P("shard", "dp"),
        ),
        out_specs=(
            P(("dp", "shard"), None),
            P(("dp", "shard"), None),
            P(),
            P("shard", "dp"),
            P("shard", "dp"),
            P("shard", "dp"),
            P("shard", "dp"),
            P(),
            P("shard", "dp"),
            P("shard", "dp"),
            P("shard", "dp"),
            P("shard", "dp"),
            P(),
            P(),
            P("shard", "dp"),
            P("shard", "dp"),
            P("shard", "dp"),
            P("shard", "dp"),
            P("shard", "dp"),
            P("shard", "dp"),
            P("shard", "dp"),
            P("shard", "dp"),
        ),
        check_vma=False,
    )
```

```python
import functools
import math

import jax
import jax.numpy as jnp
from jax import lax
from jax.experimental import pallas as pl
from jax.experimental.pallas import tpu as pltpu
from jax.sharding import PartitionSpec as P

MESH = pl.DeviceIdType.MESH
ANY = pl.BlockSpec(memory_space=pl.ANY)
VMEM = pl.BlockSpec(memory_space=pltpu.VMEM)


class Grid:
    def __init__(self, mesh):
        self.nd = mesh.shape["dp"]
        self.nz = mesh.shape["shard"]
        self.nx = math.isqrt(self.nd // 2)
        self.ny = self.nd // 2 // self.nx
        assert self.nx == self.ny and self.nx * self.ny * 2 == self.nd

    def dp(self, y, x, c):
        return (y * self.nx + x) * 2 + c


class Here:
    def __init__(self, grid):
        self.grid = grid
        d = lax.axis_index("dp")
        self.z = lax.axis_index("shard")
        self.d = d
        self.c = lax.rem(d, 2)
        self.x = lax.rem(d // 2, grid.nx)
        self.y = d // (2 * grid.nx)
        g = grid
        self.xs = [lax.rem(self.x + k, g.nx) for k in range(1, g.nx)]
        self.ys = [lax.rem(self.y + k, g.ny) for k in range(1, g.ny)]
        self.zs = [lax.rem(self.z + k, g.nz) for k in range(1, g.nz)]
        self.partner = (g.dp(self.y, self.x, 1 - self.c), self.z)

    def on_x(self, x):
        return (self.grid.dp(self.y, x, self.c), self.z)

    def on_y(self, y):
        return (self.grid.dp(y, self.x, self.c), self.z)

    def on_z(self, z):
        return (self.d, z)

    def peers(self):
        return (
            [self.partner]
            + [self.on_x(x) for x in self.xs]
            + [self.on_y(y) for y in self.ys]
            + [self.on_z(z) for z in self.zs]
        )


def greet(peers):
    barrier = pltpu.get_barrier_semaphore()
    for peer in peers:
        pl.semaphore_signal(barrier, inc=1, device_id=peer, device_id_type=MESH)
    pl.semaphore_wait(barrier, len(peers))


def send(src, dst, send_sem, recv_sem, device):
    pltpu.make_async_remote_copy(
        src_ref=src,
        dst_ref=dst,
        send_sem=send_sem,
        recv_sem=recv_sem,
        device_id=device,
        device_id_type=MESH,
    ).start()


def wait_bytes(ref, sem):
    pltpu.make_async_copy(ref, ref, sem).wait()


def half_rows(rows):
    return max(16, int(rows / 32 + 0.5) * 16)


def chunks_of(rows, size=64):
    starts = list(range(0, rows, size))
    if len(starts) > 1 and rows - starts[-1] < size // 2:
        starts.pop()
    return [(start, stop - start) for start, stop in zip(starts, starts[1:] + [rows])]


class Gather:
    def __init__(self, here, shard, out, sems, z_major, rows):
        self.h, self.shard, self.out, self.sems, self.z_major = here, shard, out, sems, z_major
        self.start, self.rows = rows
        self.cut = half_rows(self.rows)

    def span(self, half=None):
        if half is None:
            return pl.ds(self.start, self.rows)
        return pl.ds(self.start, self.cut) if half == 0 else pl.ds(self.start + self.cut, self.rows - self.cut)

    def column(self, d, half=None):
        return self.out.at[:, d, self.span(half)] if self.z_major else self.out.at[d, :, self.span(half)]

    def block(self, d, z):
        return self.out.at[z, d, self.span()] if self.z_major else self.out.at[d, z, self.span()]

    def columns(self, count):
        some = pl.ds(0, count)
        return self.out.at[:, some, self.span()] if self.z_major else self.out.at[some, :, self.span()]

    def blocks(self, count):
        some = pl.ds(0, count)
        return self.out.at[some, 0, self.span()] if self.z_major else self.out.at[0, some, self.span()]

    def own(self):
        h = self.h
        return pltpu.make_async_copy(self.shard.at[self.span()], self.block(h.d, h.z), self.sems.at[8])

    def stage_z(self):
        h, s = self.h, self.sems
        for z in h.zs:
            send(self.shard.at[self.span()], self.block(h.d, h.z), s.at[0], s.at[1], h.on_z(z))
        self.own().start()

    def await_z(self):
        wait_bytes(self.blocks(len(self.h.zs)), self.sems.at[1])

    def drain_z(self):
        wait_bytes(self.blocks(len(self.h.zs)), self.sems.at[0])

    def stage_one(self):
        h, s = self.h, self.sems
        self.await_z()
        self.own().wait()
        for x in h.xs:
            send(self.column(h.d, 0), self.column(h.d, 0), s.at[2], s.at[3], h.on_x(x))
        for y in h.ys:
            send(self.column(h.d, 1), self.column(h.d, 1), s.at[2], s.at[3], h.on_y(y))
        send(self.column(h.d), self.column(h.d), s.at[6], s.at[7], h.partner)

    def stage_two(self):
        h, s, g = self.h, self.sems, self.h.grid
        wait_bytes(self.columns(len(h.xs)), s.at[3])
        for y in h.ys:
            for x in [h.x] + h.xs:
                col = self.column(g.dp(h.y, x, h.c), 0)
                send(col, col, s.at[4], s.at[5], h.on_y(y))
        for x in h.xs:
            for y in [h.y] + h.ys:
                col = self.column(g.dp(y, h.x, h.c), 1)
                send(col, col, s.at[4], s.at[5], h.on_x(x))
        for x in h.xs:
            col = self.column(g.dp(h.y, x, h.c), 0)
            send(col, col, s.at[6], s.at[7], h.partner)
        for y in h.ys:
            col = self.column(g.dp(y, h.x, h.c), 1)
            send(col, col, s.at[6], s.at[7], h.partner)

    def stage_three(self):
        h, s, g = self.h, self.sems, self.h.grid
        wait_bytes(self.columns(g.nx * len(h.ys)), s.at[5])
        for y in h.ys:
            for x in [h.x] + h.xs:
                col = self.column(g.dp(y, x, h.c), 0)
                send(col, col, s.at[6], s.at[7], h.partner)
        for x in h.xs:
            for y in [h.y] + h.ys:
                col = self.column(g.dp(y, x, h.c), 1)
                send(col, col, s.at[6], s.at[7], h.partner)

    def arrive(self):
        g = self.h.grid
        wait_bytes(self.columns(g.nd // 2), self.sems.at[7])

    def drain(self):
        h, s, g = self.h, self.sems, self.h.grid
        self.drain_z()
        wait_bytes(self.columns(len(h.xs)), s.at[2])
        wait_bytes(self.columns(g.nx * len(h.ys)), s.at[4])
        wait_bytes(self.columns(g.nd // 2), s.at[6])

    stages = ("stage_z", "stage_one", "stage_two", "stage_three")


class ColumnGather(Gather):
    def own(self):
        return pltpu.make_async_copy(self.shard.at[:, self.span()], self.column(self.h.d), self.sems.at[8])

    def stage_z(self):
        self.own().start()

    def await_z(self):
        pass

    def drain_z(self):
        pass


class Spread:
    def __init__(self, here, shard, out, sems):
        self.h, self.shard, self.out, self.sems = here, shard, out, sems

    def own(self):
        return pltpu.make_async_copy(self.shard, self.out.at[self.h.z], self.sems.at[2])

    def begin(self):
        h, s = self.h, self.sems
        for z in h.zs:
            send(self.shard, self.out.at[h.z], s.at[0], s.at[1], h.on_z(z))
        self.own().start()

    def end(self):
        some = self.out.at[pl.ds(0, len(self.h.zs))]
        wait_bytes(some, self.sems.at[1])
        wait_bytes(some, self.sems.at[0])
        self.own().wait()


def pipelined(jobs, ahead=0):
    ticks = [getattr(job, job.stages[0]) for job in jobs[:ahead]]
    depth = max((len(job.stages) for job in jobs), default=0)
    for step in range(len(jobs) + depth - 1):
        for k in range(depth):
            i = step - k
            if 0 <= i < len(jobs) and k < len(jobs[i].stages) and not (k == 0 and i < ahead):
                ticks.append(getattr(jobs[i], jobs[i].stages[k]))
    return ticks


def chunk_list(shards, leads=None):
    pieces = []
    for i, shard in enumerate(shards):
        if leads is not None and leads[i]:
            pieces += [(i, k, (0, shard.shape[-2])) for k in leads[i]]
        else:
            pieces += [(i, None, rows) for rows in chunks_of(shard.shape[-2])]
    return pieces


def piece_of(ref, lead):
    return ref if lead is None else ref.at[lead]


def gather_jobs(here, shards, outs, sems, z_majors, pieces):
    jobs = []
    for k, (i, lead, rows) in enumerate(pieces):
        kind = ColumnGather if lead is None and len(shards[i].shape) == 3 else Gather
        job = kind(here, piece_of(shards[i], lead), piece_of(outs[i], lead), sems.at[k], z_majors[i], rows)
        jobs.append(job)
    return jobs


GATHER_SEMS = 9


def gather_kernel(grid, z_majors, pieces, turns, *refs):
    n, spreads = len(z_majors), len(turns) - len(z_majors)
    given, refs = refs[: n + spreads], refs[n + spreads :]
    outs, refs = refs[:n], refs[n:]
    columns, refs = refs[:spreads], refs[spreads:]
    rounded, (sems, spread_sems) = refs[: n + spreads], refs[n + spreads :]
    for source, half, turn in zip(given, rounded, turns):
        half[...] = (source[...].T if turn else source[...]).astype(jnp.bfloat16)
    shards, singles = rounded[:n], rounded[n:]
    here = Here(grid)
    greet(here.peers())
    jobs = gather_jobs(here, shards, outs, sems, z_majors, pieces)
    ticks = pipelined(jobs, len(jobs))
    for tick in ticks[: len(jobs)]:
        tick()
    others = [Spread(here, singles[k], columns[k], spread_sems.at[k]) for k in range(spreads)]
    for other in others:
        other.begin()
    for tick in ticks[len(jobs) :]:
        tick()
    for job in jobs:
        job.arrive()
        job.drain()
    for other in others:
        other.end()


def gather_weights(grid, shards, z_majors, singles, turns, collective_id):
    blocks = []
    for value, turn in zip([*shards, *singles], turns):
        blocks.append(jax.ShapeDtypeStruct(value.shape[::-1] if turn else value.shape, jnp.bfloat16))
    n = len(shards)
    shapes = []
    for block, z_major in zip(blocks, z_majors):
        lead = (grid.nz, grid.nd) if z_major else (grid.nd, grid.nz)
        shapes.append(jax.ShapeDtypeStruct(lead + block.shape, block.dtype))
    for block in blocks[n:]:
        shapes.append(jax.ShapeDtypeStruct((grid.nz,) + block.shape, block.dtype))
    pieces = chunk_list(blocks[:n])
    return pl.pallas_call(
        functools.partial(gather_kernel, grid, tuple(z_majors), pieces, tuple(turns)),
        out_shape=shapes,
        in_specs=[VMEM] * len(blocks),
        out_specs=[ANY] * len(shapes),
        scratch_shapes=[pltpu.VMEM(block.shape, block.dtype) for block in blocks]
        + [
            pltpu.SemaphoreType.DMA((len(pieces), GATHER_SEMS)),
            pltpu.SemaphoreType.DMA((len(singles), 3)),
        ],
        compiler_params=pltpu.CompilerParams(collective_id=collective_id, has_side_effects=True),
        name="gather_weights",
    )(*shards, *singles)


class Reduce:
    def __init__(self, here, terms, result, bufs, sems, z_major, rows):
        self.h, self.terms, self.result, self.sems, self.z_major = here, terms, result, sems, z_major
        self.own, self.other, self.one_a, self.one_b, self.two_a, self.two_b, self.last = bufs
        self.start, self.rows = rows
        self.cut = half_rows(self.rows)

    @staticmethod
    def scratch(grid, rows, cols, z_major):
        cut = half_rows(rows)
        ny, nx, nz = grid.ny, grid.nx, grid.nz
        full = (nz, ny, nx) if z_major else (ny, nx, nz)
        row = (nz, nx) if z_major else (nx, nz)
        bf = jnp.bfloat16
        return [
            pltpu.VMEM(full + (rows, cols), bf),
            pltpu.VMEM(full + (rows, cols), bf),
            pltpu.VMEM((ny,) + row + (cut, cols), bf),
            pltpu.VMEM((nx,) + row + (rows - cut, cols), bf),
            pltpu.VMEM((nx, nz, cut, cols), bf),
            pltpu.VMEM((ny, nz, rows - cut, cols), bf),
            pltpu.VMEM((nz, rows, cols), bf),
        ]

    def span(self, half):
        return {None: slice(None), 0: pl.ds(0, self.cut), 1: pl.ds(self.cut, self.rows - self.cut)}[half]

    def at(self, y, x, z, half):
        y, x, z = (slice(None) if v is None else v for v in (y, x, z))
        return (z, y, x, self.span(half)) if self.z_major else (y, x, z, self.span(half))

    def side(self, c):
        rows = pl.ds(self.start, self.rows)
        return self.terms.at[:, :, :, c, rows] if self.z_major else self.terms.at[:, :, c, :, rows]

    def load(self):
        return pltpu.make_async_copy(self.side(self.h.c), self.own, self.sems.at[8])

    def stage_core(self):
        h, s = self.h, self.sems
        send(self.side(1 - h.c), self.other, s.at[0], s.at[1], h.partner)
        self.load().start()

    def add_loop(self, shape, body):
        total = math.prod(shape)

        def step(i, carry):
            place = []
            rest = i
            for size in reversed(shape):
                place.append(lax.rem(rest, size))
                rest = rest // size
            body(tuple(reversed(place)))
            return carry

        lax.fori_loop(0, total, step, 0)

    def stage_one(self):
        h, s, g = self.h, self.sems, self.h.grid
        self.load().wait()
        wait_bytes(self.other, s.at[1])

        def body(place):
            self.own[place] = self.own[place] + self.other[place]

        self.add_loop(self.own.shape[:3], body)
        for y in h.ys:
            send(self.own.at[self.at(y, None, None, 0)], self.one_a.at[h.y], s.at[2], s.at[3], h.on_y(y))
        for x in h.xs:
            send(self.own.at[self.at(None, x, None, 1)], self.one_b.at[h.x], s.at[9], s.at[10], h.on_x(x))

    def stage_two(self):
        h, s, g = self.h, self.sems, self.h.grid
        wait_bytes(self.one_a.at[pl.ds(0, g.ny - 1)], s.at[3])
        wait_bytes(self.one_b.at[pl.ds(0, g.nx - 1)], s.at[10])

        def body_a(place):
            where = (place[1], place[0]) if self.z_major else place
            spot = self.at(h.y, where[0], where[1], 0)
            total = self.own[spot].astype(jnp.float32)
            for y in h.ys:
                total += self.one_a[(y,) + place].astype(jnp.float32)
            self.own[spot] = total.astype(jnp.bfloat16)

        self.add_loop(self.one_a.shape[1:3], body_a)

        def body_b(place):
            where = (place[1], place[0]) if self.z_major else place
            spot = self.at(where[0], h.x, where[1], 1)
            total = self.own[spot].astype(jnp.float32)
            for x in h.xs:
                total += self.one_b[(x,) + place].astype(jnp.float32)
            self.own[spot] = total.astype(jnp.bfloat16)

        self.add_loop(self.one_b.shape[1:3], body_b)
        for x in h.xs:
            send(self.own.at[self.at(h.y, x, None, 0)], self.two_a.at[h.x], s.at[4], s.at[5], h.on_x(x))
        for y in h.ys:
            send(self.own.at[self.at(y, h.x, None, 1)], self.two_b.at[h.y], s.at[11], s.at[12], h.on_y(y))

    def stage_three(self):
        h, s, g = self.h, self.sems, self.h.grid
        wait_bytes(self.two_a.at[pl.ds(0, g.nx - 1)], s.at[5])
        wait_bytes(self.two_b.at[pl.ds(0, g.ny - 1)], s.at[12])

        def body(place):
            (z,) = place
            spot = self.at(h.y, h.x, z, 0)
            total = self.own[spot].astype(jnp.float32)
            for x in h.xs:
                total += self.two_a[x, z].astype(jnp.float32)
            self.own[spot] = total.astype(jnp.bfloat16)
            spot = self.at(h.y, h.x, z, 1)
            total = self.own[spot].astype(jnp.float32)
            for y in h.ys:
                total += self.two_b[y, z].astype(jnp.float32)
            self.own[spot] = total.astype(jnp.bfloat16)

        self.add_loop((g.nz,), body)
        for z in h.zs:
            send(self.own.at[self.at(h.y, h.x, z, None)], self.last.at[h.z], s.at[6], s.at[7], h.on_z(z))

    def finish(self):
        h, s, g = self.h, self.sems, self.h.grid
        wait_bytes(self.last.at[pl.ds(0, g.nz - 1)], s.at[7])
        total = self.own[self.at(h.y, h.x, h.z, None)].astype(jnp.float32)
        for z in h.zs:
            total += self.last[z].astype(jnp.float32)
        self.result[pl.ds(self.start, self.rows)] = total

    stages = ("stage_core", "stage_one", "stage_two", "stage_three", "finish")

    def drain_z(self):
        wait_bytes(self.last.at[pl.ds(0, self.h.grid.nz - 1)], self.sems.at[6])

    def drain(self):
        g, s = self.h.grid, self.sems
        wait_bytes(self.other, s.at[0])
        wait_bytes(self.one_a.at[pl.ds(0, g.ny - 1)], s.at[2])
        wait_bytes(self.one_b.at[pl.ds(0, g.nx - 1)], s.at[9])
        wait_bytes(self.two_a.at[pl.ds(0, g.nx - 1)], s.at[4])
        wait_bytes(self.two_b.at[pl.ds(0, g.ny - 1)], s.at[11])
        self.drain_z()


class ColumnReduce(Reduce):
    stages = ("stage_core", "stage_one", "stage_two", "stage_three")

    def stage_three(self):
        h, s, g = self.h, self.sems, self.h.grid
        wait_bytes(self.two_a.at[pl.ds(0, g.nx - 1)], s.at[5])
        wait_bytes(self.two_b.at[pl.ds(0, g.ny - 1)], s.at[12])

        def body(place):
            (z,) = place
            total = self.own[self.at(h.y, h.x, z, 0)].astype(jnp.float32)
            for x in h.xs:
                total += self.two_a[x, z].astype(jnp.float32)
            self.result[z, pl.ds(self.start, self.cut)] = total.astype(jnp.bfloat16)
            total = self.own[self.at(h.y, h.x, z, 1)].astype(jnp.float32)
            for y in h.ys:
                total += self.two_b[y, z].astype(jnp.float32)
            self.result[z, pl.ds(self.start + self.cut, self.rows - self.cut)] = total.astype(jnp.bfloat16)

        self.add_loop((g.nz,), body)

    def drain_z(self):
        pass


class Collect:
    def __init__(self, here, column, last, sems):
        self.h, self.column, self.last, self.sems = here, column, last, sems

    def begin(self):
        h, s = self.h, self.sems
        for z in h.zs:
            send(self.column.at[z], self.last.at[h.z], s.at[0], s.at[1], h.on_z(z))

    def end(self):
        h = self.h
        wait_bytes(self.last.at[pl.ds(0, len(h.zs))], self.sems.at[1])
        total = self.column[h.z].astype(jnp.float32)
        for z in h.zs:
            total += self.last[z].astype(jnp.float32)
        return total

    def drain(self):
        wait_bytes(self.last.at[pl.ds(0, len(self.h.zs))], self.sems.at[0])


REDUCE_SEMS = 13
REDUCE_BUFS = 7


class Share:
    def __init__(self, here, value, result, bufs, sems):
        self.h, self.value, self.result, self.sems = here, value, result, sems
        self.bufs = bufs

    @staticmethod
    def scratch(grid, shape):
        return [pltpu.VMEM((n,) + shape, jnp.float32) for n in (2, grid.nx, grid.ny, grid.nz)]

    def axis(self, k):
        h = self.h
        return (
            (h.c, [h.partner], 2),
            (h.x, [h.on_x(x) for x in h.xs], h.grid.nx),
            (h.y, [h.on_y(y) for y in h.ys], h.grid.ny),
            (h.z, [h.on_z(z) for z in h.zs], h.grid.nz),
        )[k]

    def start(self, k):
        me, peers, n = self.axis(k)
        self.bufs[k][me] = self.value[...] if k == 0 else self.total
        for peer in peers:
            send(self.bufs[k].at[me], self.bufs[k].at[me], self.sems.at[2 * k], self.sems.at[2 * k + 1], peer)

    def end(self, k):
        me, peers, n = self.axis(k)
        wait_bytes(self.bufs[k].at[pl.ds(0, n - 1)], self.sems.at[2 * k + 1])
        total = self.bufs[k][0]
        for i in range(1, n):
            total = total + self.bufs[k][i]
        self.total = total
        if k == 3:
            self.result[...] = total

    def drain(self):
        for k in range(4):
            n = self.axis(k)[2]
            wait_bytes(self.bufs[k].at[pl.ds(0, n - 1)], self.sems.at[2 * k])


SHARE_SEMS = 8


def reduce_kernel(grid, z_majors, pieces, shared, *refs):
    n = len(z_majors)
    terms, refs = refs[:n], refs[n:]
    value, refs = (refs[0], refs[1:]) if shared else (None, refs)
    results, refs = refs[:n], refs[n:]
    value_sum, refs = (refs[0], refs[1:]) if shared else (None, refs)
    here = Here(grid)
    greet(here.peers())
    jobs, refs = reduce_jobs(here, terms, results, refs, z_majors, pieces)
    share = None
    if shared:
        share = Share(here, value, value_sum, refs[:4], refs[4])
        share.start(0)
    ticks = pipelined(jobs, len(jobs))
    for k, tick in enumerate(ticks):
        tick()
        if share is not None and k >= len(jobs) and k - len(jobs) < 4:
            step = k - len(jobs)
            share.end(step)
            if step < 3:
                share.start(step + 1)
    if share is not None:
        share.drain()
    for job in jobs:
        job.drain()


def reduce_jobs(here, terms, results, refs, z_majors, pieces):
    n = len(pieces)
    sems = refs[n * REDUCE_BUFS]
    jobs = []
    for k, (i, lead, rows) in enumerate(pieces):
        bufs = refs[k * REDUCE_BUFS : (k + 1) * REDUCE_BUFS]
        term, result, kind = piece_of(terms[i], lead), results[i], Reduce
        deep = len(result.shape) == 3
        if lead is None:
            kind = ColumnReduce if deep else Reduce
        else:
            width = term.shape[-1]
            result = result.at[lead] if deep else result.at[:, pl.ds(lead * width, width)]
        jobs.append(kind(here, term, result, bufs, sems.at[k], z_majors[i], rows))
    return jobs, refs[n * REDUCE_BUFS + 1 :]


def reduce_scratch(grid, terms, z_majors, pieces):
    scratch = []
    for i, _, (_, rows) in pieces:
        scratch += Reduce.scratch(grid, rows, terms[i].shape[-1], z_majors[i])
    return scratch + [pltpu.SemaphoreType.DMA((max(len(pieces), 1), REDUCE_SEMS))]


def split_terms(grid, terms, z_majors):
    split = []
    for term, z_major in zip(terms, z_majors):
        lead = (grid.ny, grid.nx, 2)
        lead = (grid.nz,) + lead if z_major else lead + (grid.nz,)
        split.append(term.reshape(term.shape[:-4] + lead + term.shape[-2:]))
    return split


def reduce_grads(grid, terms, z_majors, value, collective_id):
    shapes = [jax.ShapeDtypeStruct(term.shape[-2:], jnp.float32) for term in terms]
    pieces = chunk_list(terms)
    scratch = reduce_scratch(grid, terms, z_majors, pieces)
    n = len(terms)
    shared = value is not None
    if shared:
        shapes.append(jax.ShapeDtypeStruct(value.shape, jnp.float32))
        scratch += Share.scratch(grid, value.shape)
        scratch.append(pltpu.SemaphoreType.DMA((SHARE_SEMS,)))
    return pl.pallas_call(
        functools.partial(reduce_kernel, grid, tuple(z_majors), pieces, shared),
        out_shape=shapes,
        in_specs=[ANY] * n + [VMEM] * shared,
        out_specs=[VMEM] * len(shapes),
        scratch_shapes=scratch,
        compiler_params=pltpu.CompilerParams(
            collective_id=collective_id, has_side_effects=True, vmem_limit_bytes=62 << 20
        ),
        name="reduce_grads",
    )(*split_terms(grid, terms, z_majors), *([value] if shared else []))


D = 960
QUERY_HEADS = 15
KEY_VALUE_HEADS = 5
GROUP = QUERY_HEADS // KEY_VALUE_HEADS
HEAD = 64
FF = 2560
QKV = (QUERY_HEADS + 2 * KEY_VALUE_HEADS) * HEAD
ADAM_STEP = 10
DOCS = 16
HIDE = -1e30
VALUE_SCALE = 2.0**-9

norm_epsilon = 1e-05
beta_one = 0.9
beta_two = 0.95
adam_epsilon = 1e-08
matrix_rate = 0.03
output_rate = 0.15
gain_rate = 0.5
decay_rate = 0.1

f32 = jnp.float32
bf16 = jnp.bfloat16
DEPTH = 4
SLICE = D // DEPTH


def mm(a, b):
    return lax.dot_general(a, b, (((1,), (0,)), ((), ())), preferred_element_type=f32)


def mm_nt(a, b):
    return lax.dot_general(a, b, (((1,), (1,)), ((), ())), preferred_element_type=f32)


def mm_tn(a, b):
    return lax.dot_general(a, b, (((0,), (0,)), ((), ())), preferred_element_type=f32)


def lanes_below(shape, n):
    return lax.broadcasted_iota(jnp.int32, shape, len(shape) - 1) < n


def inverse_rms(ref):
    total = jnp.zeros((1, ref.shape[1]), f32)
    for k in range(DEPTH):
        x = ref[pl.ds(k * SLICE, SLICE)].astype(f32)
        total += jnp.sum(x * x, axis=0, keepdims=True)
    return lax.rsqrt(total * (1.0 / D) + norm_epsilon)


def three_pieces(row):
    hi = row.astype(bf16).astype(f32)
    mid = (row - hi).astype(bf16).astype(f32)
    low = row - hi - mid
    place = lax.broadcasted_iota(jnp.int32, (16, row.shape[1]), 0)
    block = jnp.where(place == 0, hi, jnp.where(place == 1, mid, jnp.where(place == 2, low, 0.0)))
    return block.astype(bf16)


class KeyChain:
    def __init__(self, here, kv, sems):
        self.h, self.kv, self.sems = here, kv, sems

    def up(self, slot):
        h = self.h
        to = lax.rem(h.z + 1, h.grid.nz)

        @pl.when(h.z < h.grid.nz - 1)
        def _():
            send(self.kv.at[slot], self.kv.at[slot], self.sems.at[0, slot], self.sems.at[1, slot], h.on_z(to))

    def take(self, slot):
        wait_bytes(self.kv.at[slot], self.sems.at[1, slot])
        self.up(slot)

    def drain(self):
        h = self.h
        for s in range(h.grid.nz):

            @pl.when(jnp.logical_and(h.z >= s, h.z < h.grid.nz - 1))
            def _():
                wait_bytes(self.kv.at[h.z - s], self.sems.at[0, h.z - s])


def round_steps(source, rounded, start):
    if len(rounded.shape) == 2:
        rounded[...] = source[...].astype(bf16)
    else:
        for k in range(rounded.shape[0]):
            rounded[k] = source[:, pl.ds((start + k) * WIDTH, WIDTH)].astype(bf16)


def front_kernel(grid, z_majors, pieces, late, *refs):
    n = len(z_majors)
    shards, refs = refs[:n], refs[n:]
    heads, x, gain, cos, sin, qext, kext = refs[:7]
    refs = refs[7:]
    outs, refs = refs[:n], refs[n:]
    qx, qn, kv, att = refs[:4]
    refs = refs[4:]
    if late:
        columns, refs = refs[0], refs[1:]
    h1, proj, kx, vt, acc, rounded, sems, kv_sems = refs[:8]
    here = Here(grid)
    tokens = x.shape[1]
    half = tokens // 2
    round_steps(shards[-1], rounded, 0)
    spreads = []
    if late:
        late_rounded, late_sems = refs[8:]
        round_steps(shards[-1], late_rounded, STEPS - late)
        spreads = [Spread(here, late_rounded.at[k], columns.at[k], late_sems.at[k]) for k in range(late)]
    greet(here.peers())
    jobs = gather_jobs(here, [*shards[:-1], rounded], outs, sems, z_majors, pieces)
    ticks = pipelined(jobs, 3)
    for tick in ticks[:3]:
        tick()

    inverse = inverse_rms(x)
    for k in range(DEPTH):
        rows = pl.ds(k * SLICE, SLICE)
        h1[rows] = (x[rows].astype(f32) * inverse * gain[rows, 0:1]).astype(bf16)

    part = QKV // 5

    def project(m, carry):
        rows = pl.ds(pl.multiple_of(m * part, 16), part)
        total = mm(heads[0, rows], h1[pl.ds(0, SLICE)])
        for k in range(1, DEPTH):
            total += mm(heads[k, rows], h1[pl.ds(k * SLICE, SLICE)])
        proj[rows] = total
        return carry

    lax.fori_loop(3, 5, project, 0)

    def turned(h):
        base = h * HEAD
        a = proj[pl.ds(pl.multiple_of(base, 8), HEAD // 2)]
        b = proj[pl.ds(pl.multiple_of(base + HEAD // 2, 8), HEAD // 2)]
        c, s = cos[...], sin[...]
        return a * c - b * s, b * c + a * s

    def keys(g, carry):
        a, b = turned(QUERY_HEADS + g)
        v = proj[pl.ds(pl.multiple_of((QUERY_HEADS + KEY_VALUE_HEADS + g) * HEAD, 8), HEAD)]
        both = jnp.concatenate([a, b, v], axis=0)
        kv[here.z, g] = both.T.astype(bf16)
        return carry

    lax.fori_loop(0, KEY_VALUE_HEADS, keys, 0)
    chain = KeyChain(here, kv, kv_sems)
    chain.up(here.z)
    lax.fori_loop(0, 3, project, 0)

    def queries(h, carry):
        a, b = turned(h)
        scale = HEAD**-0.5
        qx[h, pl.ds(0, 32)] = (a.astype(bf16).astype(f32) * scale).astype(bf16)
        qx[h, pl.ds(32, 32)] = (b.astype(bf16).astype(f32) * scale).astype(bf16)
        qx[h, pl.ds(64, 64)] = qext[...]
        qn[h] = qx[h].astype(f32).T.astype(bf16)
        return carry

    lax.fori_loop(0, QUERY_HEADS, queries, 0)

    def prepare(slot):
        ext = kext[pl.ds(pl.multiple_of(slot * tokens, 16), tokens)]

        def body(g, carry):
            block = kv[slot, g]
            kx[g] = jnp.where(lanes_below(block.shape, HEAD), block, ext)
            turned_block = block.astype(f32).T
            vt[g, pl.ds(0, 16)] = jnp.ones((16, tokens), bf16)
            vt[g, pl.ds(16, HEAD)] = (turned_block[HEAD:] * VALUE_SCALE).astype(bf16)
            return carry

        lax.fori_loop(0, KEY_VALUE_HEADS, body, 0)

    def below(shape, shift):
        return lax.broadcasted_iota(jnp.int32, shape, 0) <= lax.broadcasted_iota(jnp.int32, shape, 1) + shift

    def diagonal(g):
        for i in range(GROUP):
            h = g * GROUP + i
            s = mm(kx[g, pl.ds(0, half)], qx[h, :, pl.ds(0, half)])
            p = jnp.exp(jnp.where(below(s.shape, 0), s, HIDE)).astype(bf16)
            acc[h, :, pl.ds(0, half)] = mm(vt[g, :, pl.ds(0, half)], p)
            s = mm(kx[g], qx[h, :, pl.ds(half, half)])
            p = jnp.exp(jnp.where(below(s.shape, half), s, HIDE)).astype(bf16)
            acc[h, :, pl.ds(half, half)] = mm(vt[g], p)

    def whole(g):
        for i in range(GROUP):
            h = g * GROUP + i
            for k in range(2):
                cols = pl.ds(k * half, half)
                p = jnp.exp(mm(kx[g], qx[h, :, cols])).astype(bf16)
                acc[h, :, cols] += mm(vt[g], p)

    ticks = ticks[3:]

    def micro(t, carry):
        s = t // KEY_VALUE_HEADS
        g = lax.rem(t, KEY_VALUE_HEADS)

        @pl.when(s <= here.z)
        def _():
            slot = here.z - s

            @pl.when(g == 0)
            def _():
                @pl.when(s > 0)
                def _():
                    chain.take(slot)

                prepare(slot)

            @pl.when(s == 0)
            def _():
                diagonal(g)

            @pl.when(s > 0)
            def _():
                whole(g)

        for k, tick in enumerate(ticks):
            pl.when(t == k * (micros - KEY_VALUE_HEADS) // len(ticks))(tick)
        for spread in spreads:
            pl.when(t == micros - 2 * KEY_VALUE_HEADS + 1)(spread.begin)
        return carry

    micros = grid.nz * KEY_VALUE_HEADS
    lax.fori_loop(0, micros, micro, 0)

    def close(h, carry):
        totals = acc[h, pl.ds(0, 1)]
        scale = (1.0 / VALUE_SCALE) / totals
        att[pl.ds(pl.multiple_of(h * HEAD, 16), HEAD)] = (acc[h, pl.ds(16, HEAD)] * scale).astype(bf16)
        qx[h, pl.ds(HEAD + DOCS, 16)] = three_pieces(-jnp.log(totals))
        return carry

    lax.fori_loop(0, QUERY_HEADS, close, 0)
    for job in jobs:
        job.arrive()
        job.drain()
    for spread in spreads:
        spread.end()
    chain.drain()


def front(grid, shards, z_majors, leads, heads, x, gain, cos, sin, qext, kext, collective_id):
    tokens = x.shape[1]
    shapes = []
    chosen = leads[-1]
    expand = shards[-1]
    rounded = (len(chosen), SLICE, WIDTH) if chosen else expand.shape
    blocks = [*shards[:-1], jax.ShapeDtypeStruct(rounded, bf16)]
    for block, z_major, chosen in zip(blocks, z_majors, leads):
        lead = (grid.nz, grid.nd) if z_major else (grid.nd, grid.nz)
        lead = (len(chosen),) + lead if chosen else lead
        shapes.append(jax.ShapeDtypeStruct(lead + block.shape[-2:], bf16))
    n = len(shards)
    pieces = chunk_list(blocks, leads)
    shapes += [
        jax.ShapeDtypeStruct((QUERY_HEADS, 128, tokens), bf16),
        jax.ShapeDtypeStruct((QUERY_HEADS, tokens, 128), bf16),
        jax.ShapeDtypeStruct((grid.nz, KEY_VALUE_HEADS, tokens, 128), bf16),
        jax.ShapeDtypeStruct((D, tokens), bf16),
    ]
    late = STEPS - len(leads[-1]) if leads[-1] else 0
    last = []
    if late:
        shapes.append(jax.ShapeDtypeStruct((late, grid.nz, SLICE, WIDTH), bf16))
        last = [pltpu.VMEM((late, SLICE, WIDTH), bf16), pltpu.SemaphoreType.DMA((late, 3))]
    return pl.pallas_call(
        functools.partial(front_kernel, grid, tuple(z_majors), pieces, late),
        out_shape=shapes,
        in_specs=[VMEM] * (n + 7),
        out_specs=[ANY] * n + [VMEM] * 4 + [ANY] * (late > 0),
        scratch_shapes=[
            pltpu.VMEM((D, tokens), bf16),
            pltpu.VMEM((QKV, tokens), f32),
            pltpu.VMEM((KEY_VALUE_HEADS, tokens, 128), bf16),
            pltpu.VMEM((KEY_VALUE_HEADS, 80, tokens), bf16),
            pltpu.VMEM((QUERY_HEADS, 80, tokens), f32),
            pltpu.VMEM(rounded, bf16),
            pltpu.SemaphoreType.DMA((max(len(pieces), 1), GATHER_SEMS)),
            pltpu.SemaphoreType.DMA((2, grid.nz)),
            *last,
        ],
        compiler_params=pltpu.CompilerParams(
            collective_id=collective_id, has_side_effects=True, vmem_limit_bytes=60 << 20
        ),
        name="front",
    )(*shards, heads, x, gain, cos, sin, qext, kext)


STEPS = 5
WIDTH = 128
PARTS = 6


def middle_kernel(grid, ready, summed, *refs):
    att, wo, x, ogt, gain, exp_in, dn_in = refs[:7]
    refs = refs[7:]
    late = STEPS - ready
    if late:
        shard, refs = refs[0], refs[1:]
    out, rg, gsum, dwo, dox, dexp, ddn = refs[:7]
    refs = refs[7:]
    if late:
        exp_late, refs = refs[0], refs[1:]
    if summed:
        gexp, refs = refs[0], refs[1:]
    (res, inv, h2, h2t, og, acc_o, acc_h, mixed, dgate, dup, wg, wu, wd, sg, sd, w_sems, o_sems) = refs[:17]
    refs = refs[17:]
    tokens = x.shape[1]
    half = 2 * WIDTH
    schedule = {}
    gathers, sums = [], []
    if late or summed:
        here = Here(grid)
        greet(here.peers())
    if late:
        pieces = [(0, k, (0, SLICE)) for k in range(late)]
        g_sems, refs = refs[0], refs[1:]
        gathers = [
            ColumnGather(here, shard.at[k], exp_late.at[k], g_sems.at[k], False, (0, SLICE)) for k in range(late)
        ]
        for job in gathers:
            job.stage_z()
        for job in gathers:
            job.stage_one()
        for k, job in enumerate(gathers):
            for i, stage in enumerate(job.stages[2:]):
                schedule.setdefault((2 * k, 6 + 4 * k)[i], []).append(getattr(job, stage))
            schedule.setdefault((ready + k - 1) * PARTS + 1, []).append(job.arrive)
    if summed:
        pieces = [(0, k, (0, SLICE)) for k in range(summed)]
        sums, refs = reduce_jobs(here, [dexp], [gexp], refs, (False,), pieces)
        for k, job in enumerate(sums):
            for i, stage in enumerate(job.stages):
                place = min((k + 1) * PARTS + 2 + 5 * i, STEPS * PARTS - 1)
                schedule.setdefault(place, []).append(getattr(job, stage))

    def fetch_from(source, index, step, slot, go):
        for d in range(4):
            lanes = pl.ds(d * WIDTH, WIDTH)
            go(pltpu.make_async_copy(source.at[index, d], wg.at[slot, :, :, lanes], w_sems.at[slot, 0]))
            go(pltpu.make_async_copy(source.at[index, 4 + d], wu.at[slot, :, :, lanes], w_sems.at[slot, 1]))
            columns = pl.ds(pl.multiple_of(step * WIDTH, WIDTH), WIDTH)
            go(pltpu.make_async_copy(dn_in.at[d, :, columns], wd.at[slot, :, lanes], w_sems.at[slot, 2]))

    def fetch(step):
        slot = lax.rem(step, 2)

        @pl.when(step < ready)
        def _():
            fetch_from(exp_in, step, step, slot, lambda copy: copy.start())

        if late:

            @pl.when(step >= ready)
            def _():
                fetch_from(exp_late, step - ready, step, slot, lambda copy: copy.start())

    def put_expand(step, go):
        for k in range(2):
            for d in range(4):
                lanes = pl.ds(d * WIDTH, WIDTH)
                to = dexp.at[step, 4 * k + d] if not sums_split else dexp.at[(step,) + sums_place(4 * k + d)]
                go(pltpu.make_async_copy(sg.at[k, :, :, lanes], to, o_sems.at[0]))

    def put_down(step, go):
        for d in range(4):
            columns = pl.ds(pl.multiple_of(step * WIDTH, WIDTH), WIDTH)
            go(pltpu.make_async_copy(sd.at[:, pl.ds(d * WIDTH, WIDTH)], ddn.at[d, :, columns], o_sems.at[1]))

    sums_split = len(dexp.shape) == 7

    def sums_place(d):
        return (d // (2 * grid.nx), d // 2 % grid.nx, d % 2)

    fetch(jnp.int32(0))
    total = jnp.zeros((1, tokens), f32)
    for m in range(DEPTH):
        rows = pl.ds(m * SLICE, SLICE)
        r = x[rows].astype(f32)
        for k in range(DEPTH):
            r += mm(wo[k, rows], att[pl.ds(k * SLICE, SLICE)])
        res[rows] = r
        total += jnp.sum(r * r, axis=0, keepdims=True)
    inverse = lax.rsqrt(total * (1.0 / D) + norm_epsilon)
    inv[...] = inverse
    for m in range(DEPTH):
        rows = pl.ds(m * SLICE, SLICE)
        h2t[rows] = (res[rows] * inverse * gain[rows, 1:2]).astype(bf16)
    h2[...] = h2t[...].astype(f32).T.astype(bf16)
    og[...] = ogt[...].astype(f32).T.astype(bf16)
    acc_o[...] = jnp.zeros_like(acc_o)
    acc_h[...] = jnp.zeros_like(acc_h)

    def activate(slot, k):
        cols = pl.ds(k * half, half)
        gate = mm(h2[...], wg[slot, :, :, cols].reshape(D, half))
        up = mm(h2[...], wu[slot, :, :, cols].reshape(D, half))
        back = mm(og[...], wd[slot, :, cols])
        s = 1.0 / (1.0 + jnp.exp(-gate))
        silu = gate * s
        mixed[:, cols] = (silu * up).astype(bf16)
        dgate[:, cols] = (back * up * s * (1.0 + gate * (1.0 - s))).astype(bf16)
        dup[:, cols] = (back * silu).astype(bf16)

    def micro(t, carry):
        step = t // PARTS
        part = lax.rem(t, PARTS)
        slot = lax.rem(step, 2)

        for place, ticks in schedule.items():

            @pl.when(t == place)
            def _():
                for tick in ticks:
                    tick()

        @pl.when(part == 0)
        def _():
            wait_bytes(wg.at[slot], w_sems.at[slot, 0])
            wait_bytes(wu.at[slot], w_sems.at[slot, 1])
            wait_bytes(wd.at[slot], w_sems.at[slot, 2])
            activate(slot, 0)

        @pl.when(part == 1)
        def _():
            @pl.when(step > 0)
            def _():
                wait_bytes(sg, o_sems.at[0])
                wait_bytes(sd, o_sems.at[1])

            pl.when(step + 1 < STEPS)(lambda: fetch(step + 1))
            activate(slot, 1)

        @pl.when(part == 2)
        def _():
            acc_o[...] += mm_nt(wd[slot], mixed[...])

        @pl.when(part == 3)
        def _():
            for m in range(DEPTH):
                sg[0, m] = mm(h2t[pl.ds(m * SLICE, SLICE)], dgate[...]).astype(bf16)
                sg[1, m] = mm(h2t[pl.ds(m * SLICE, SLICE)], dup[...]).astype(bf16)
            put_expand(step, lambda copy: copy.start())

        @pl.when(part == 4)
        def _():
            sd[...] = mm(ogt[...], mixed[...]).astype(bf16)
            put_down(step, lambda copy: copy.start())

        @pl.when(part == 5)
        def _():
            acc_h[...] += mm_nt(wg[slot].reshape(D, 2 * half), dgate[...])
            acc_h[...] += mm_nt(wu[slot].reshape(D, 2 * half), dup[...])

        return carry

    lax.fori_loop(0, STEPS * PARTS, micro, 0)
    wait_bytes(sg, o_sems.at[0])
    wait_bytes(sd, o_sems.at[1])
    inverse = inv[...]
    total = jnp.zeros((1, tokens), f32)
    for m in range(DEPTH):
        rows = pl.ds(m * SLICE, SLICE)
        out[rows] = (res[rows] + acc_o[rows]).astype(bf16)
        normed = res[rows] * inverse
        up = acc_h[rows]
        gsum[rows] = jnp.sum(up * normed, axis=1, keepdims=True)
        total += jnp.sum(up * gain[rows, 1:2] * normed, axis=0, keepdims=True)
    mean = total * (1.0 / D)
    for m in range(DEPTH):
        rows = pl.ds(m * SLICE, SLICE)
        normed = res[rows] * inverse
        r = ogt[rows].astype(f32) + inverse * (acc_h[rows] * gain[rows, 1:2] - normed * mean)
        rg[rows] = r
        h2t[rows] = r.astype(bf16)
    for k in range(DEPTH):
        rows = pl.ds(k * SLICE, SLICE)
        dwo[k] = mm_nt(h2t[...], att[rows]).astype(bf16)
        acc_h[rows] = mm_tn(wo[k], h2t[...])

    def rows_of(h, carry):
        rows = pl.ds(pl.multiple_of(h * HEAD, 16), HEAD)
        grad = acc_h[rows].astype(bf16)
        dox[h, pl.ds(HEAD, HEAD)] = grad
        delta = jnp.sum(grad.astype(f32) * att[rows].astype(f32), axis=0, keepdims=True)
        dox[h, pl.ds(0, 16)] = three_pieces(-delta)
        dox[h, pl.ds(16, 48)] = jnp.zeros((48, tokens), bf16)
        return carry

    lax.fori_loop(0, QUERY_HEADS, rows_of, 0)
    for job in gathers + sums:
        job.drain()


def middle(grid, att, wo, x, ogt, gain, expand, down, shard, summed, collective_id):
    tokens = x.shape[1]
    ready = expand.shape[0]
    late = STEPS - ready
    blocks = expand.shape[1:]
    if summed:
        grads = (STEPS, grid.ny, grid.nx, 2) + blocks[1:]
    else:
        grads = (STEPS,) + blocks
    shapes = [
        jax.ShapeDtypeStruct((D, tokens), bf16),
        jax.ShapeDtypeStruct((D, tokens), f32),
        jax.ShapeDtypeStruct((D, 1), f32),
        jax.ShapeDtypeStruct((DEPTH, D, SLICE), bf16),
        jax.ShapeDtypeStruct((QUERY_HEADS, 128, tokens), bf16),
        jax.ShapeDtypeStruct(grads, bf16),
        jax.ShapeDtypeStruct(down.shape, bf16),
    ]
    out_specs = [VMEM] * 5 + [ANY] * 2
    inputs = [att, wo, x, ogt, gain, expand, down]
    in_specs = [VMEM] * 5 + [ANY] * 2
    scratch = [
        pltpu.VMEM((D, tokens), f32),
        pltpu.VMEM((1, tokens), f32),
        pltpu.VMEM((tokens, D), bf16),
        pltpu.VMEM((D, tokens), bf16),
        pltpu.VMEM((tokens, D), bf16),
        pltpu.VMEM((D, tokens), f32),
        pltpu.VMEM((D, tokens), f32),
        pltpu.VMEM((tokens, 4 * WIDTH), bf16),
        pltpu.VMEM((tokens, 4 * WIDTH), bf16),
        pltpu.VMEM((tokens, 4 * WIDTH), bf16),
        pltpu.VMEM((2, DEPTH, SLICE, 4 * WIDTH), bf16),
        pltpu.VMEM((2, DEPTH, SLICE, 4 * WIDTH), bf16),
        pltpu.VMEM((2, D, 4 * WIDTH), bf16),
        pltpu.VMEM((2, DEPTH, SLICE, 4 * WIDTH), bf16),
        pltpu.VMEM((D, 4 * WIDTH), bf16),
        pltpu.SemaphoreType.DMA((2, 3)),
        pltpu.SemaphoreType.DMA((2,)),
    ]
    if late:
        inputs.append(shard)
        in_specs.append(VMEM)
        shapes.append(jax.ShapeDtypeStruct((late,) + blocks, bf16))
        out_specs.append(ANY)
        scratch.append(pltpu.SemaphoreType.DMA((late, GATHER_SEMS)))
    if summed:
        shapes.append(jax.ShapeDtypeStruct((summed,) + blocks[2:], f32))
        out_specs.append(VMEM)
        pieces = [(0, k, (0, SLICE)) for k in range(summed)]
        term = jax.ShapeDtypeStruct(blocks, bf16)
        scratch += reduce_scratch(grid, [term], (False,), pieces)
    params = dict(collective_id=collective_id, has_side_effects=True) if late or summed else {}
    return pl.pallas_call(
        functools.partial(middle_kernel, grid, ready, summed),
        out_shape=shapes,
        in_specs=in_specs,
        out_specs=out_specs,
        scratch_shapes=scratch,
        compiler_params=pltpu.CompilerParams(vmem_limit_bytes=62 << 20, **params),
        name="middle",
    )(*inputs)


class GradChain:
    def __init__(self, here, part, sent, got, sems):
        self.h, self.part, self.sent, self.got, self.sems = here, part, sent, got, sems

    def summed(self, slot, g, write):
        h = self.h

        @pl.when(h.z < h.grid.nz - 1)
        def _():
            wait_bytes(self.got.at[slot, g], self.sems.at[1, slot, g])
            write(g, self.part[slot, g] + self.got[slot, g].astype(f32))

        @pl.when(h.z == h.grid.nz - 1)
        def _():
            write(g, self.part[slot, g])

    def relay(self, slot, g):
        h = self.h

        def write(g, value):
            self.sent[slot, g] = value.astype(bf16)

        self.summed(slot, g, write)
        to = lax.rem(h.z + h.grid.nz - 1, h.grid.nz)
        sems = self.sems
        send(self.sent.at[slot, g], self.got.at[slot, g], sems.at[0, slot, g], sems.at[1, slot, g], h.on_z(to))

    def drain(self):
        h = self.h

        def body(t, carry):
            slot, g = t // KEY_VALUE_HEADS, lax.rem(t, KEY_VALUE_HEADS)
            wait_bytes(self.sent.at[slot, g], self.sems.at[0, slot, g])
            return carry

        lax.fori_loop(0, h.z * KEY_VALUE_HEADS, body, 0)


def back_kernel(grid, z_majors, pieces, early, *refs):
    n = len(z_majors)
    terms, refs = refs[:n], refs[n:]
    qx, qn, dox, kv, kext, cos, sin = refs[:7]
    refs = refs[7:]
    if early:
        first, refs = refs[0], refs[1:]
    results, refs = refs[:n], refs[n:]
    for k in range(early):
        results[1][:, pl.ds(k * WIDTH, WIDTH)] = first[k]
    hd, refs = refs[0], refs[1:]
    here = Here(grid)
    jobs, refs = reduce_jobs(here, terms, results, refs, z_majors, pieces)
    don, kx, vx, kt, dq, part, sent, got, kv_sems = refs
    tokens = dox.shape[2]
    half = tokens // 2
    greet(here.peers())
    ticks = pipelined(jobs, len(jobs))
    for tick in ticks[: len(jobs)]:
        tick()
    ticks = ticks[len(jobs) :]

    def gather_queries(h, carry):
        dq[h] = jnp.zeros((HEAD, tokens), f32)
        don[h] = dox[h].astype(f32).T.astype(bf16)
        return carry

    lax.fori_loop(0, QUERY_HEADS, gather_queries, 0)

    def prepare(slot):
        ext = kext[pl.ds(pl.multiple_of(slot * tokens, 16), tokens)]

        def body(g, carry):
            block = kv[slot, g]
            low = lanes_below(block.shape, HEAD)
            kx[g] = jnp.where(low, block, ext)
            ones = jnp.where(lanes_below(block.shape, 3), 1.0, 0.0).astype(bf16)
            vx[g] = jnp.where(low, ones, block)
            kt[g] = block.astype(f32).T[:HEAD].astype(bf16)
            return carry

        lax.fori_loop(0, KEY_VALUE_HEADS, body, 0)

    def tile(g, h, count, k, masked):
        keys, cols = pl.ds(0, count), pl.ds(k * half, half)
        s = mm(kx[g, keys], qx[h, :, cols])
        if masked:
            row = lax.broadcasted_iota(jnp.int32, s.shape, 0)
            col = lax.broadcasted_iota(jnp.int32, s.shape, 1) + k * half
            s = jnp.where(row <= col, s, HIDE)
        p = jnp.exp(s)
        ds = (p * mm(vx[g, keys], dox[h, :, cols])).astype(bf16)
        dq[h, :, cols] += mm(kt[g, :, keys], ds)
        dk = mm(ds, qn[h, cols])
        dv = mm(p.astype(bf16), don[h, cols])
        return jnp.where(lanes_below(dk.shape, HEAD), dk, dv)

    def whole(slot, g):
        total = None
        for i in range(GROUP):
            for k in range(2):
                new = tile(g, g * GROUP + i, tokens, k, False)
                total = new if total is None else total + new
        part[slot, g] = total

    def diagonal(g):
        total = None
        for i in range(GROUP):
            new = tile(g, g * GROUP + i, tokens, 1, True)
            total = new if total is None else total + new
        part[here.z, g] = total
        total = part[here.z, g, pl.ds(0, half)]
        for i in range(GROUP):
            total += tile(g, g * GROUP + i, half, 0, True)
        part[here.z, g, pl.ds(0, half)] = total

    chain = GradChain(here, part, sent, got, kv_sems)
    micros = grid.nz * KEY_VALUE_HEADS
    top = here.z == grid.nz - 1

    def micro(t, carry):
        slot = t // KEY_VALUE_HEADS
        g = lax.rem(t, KEY_VALUE_HEADS)

        @pl.when(slot <= here.z)
        def _():
            pl.when(g == 0)(lambda: prepare(slot))

            @pl.when(slot < here.z)
            def _():
                whole(slot, g)
                pl.when(top)(lambda: chain.relay(slot, g))

            pl.when(slot == here.z)(lambda: diagonal(g))

        @pl.when(jnp.logical_and(jnp.logical_not(top), jnp.logical_and(slot >= 1, slot <= here.z)))
        def _():
            chain.relay(slot - 1, g)

        for k, tick in enumerate(ticks):
            pl.when(t == k * micros // len(ticks))(tick)
        return carry

    lax.fori_loop(0, micros, micro, 0)

    def turn_back(a, b):
        c, s = cos[...], sin[...]
        return a * c + b * s, b * c - a * s

    def queries(h, carry):
        scale = HEAD**-0.5
        a, b = turn_back(dq[h, pl.ds(0, 32)] * scale, dq[h, pl.ds(32, 32)] * scale)
        hd[pl.ds(pl.multiple_of(h * HEAD, 16), 32)] = a.astype(bf16)
        hd[pl.ds(pl.multiple_of(h * HEAD + 32, 16), 32)] = b.astype(bf16)
        return carry

    lax.fori_loop(0, QUERY_HEADS, queries, 0)

    def write(g, value):
        turned = value.T
        a, b = turn_back(turned[:32], turned[32:64])
        base = (QUERY_HEADS + g) * HEAD
        hd[pl.ds(pl.multiple_of(base, 16), 32)] = a.astype(bf16)
        hd[pl.ds(pl.multiple_of(base + 32, 16), 32)] = b.astype(bf16)
        base = (QUERY_HEADS + KEY_VALUE_HEADS + g) * HEAD
        hd[pl.ds(pl.multiple_of(base, 16), HEAD)] = turned[64:].astype(bf16)

    def close(g, carry):
        chain.summed(here.z, g, write)
        return carry

    lax.fori_loop(0, KEY_VALUE_HEADS, close, 0)
    chain.drain()
    for job in jobs:
        job.drain()


def back(grid, terms, z_majors, leads, early, qx, qn, dox, kv, kext, cos, sin, collective_id):
    tokens = dox.shape[2]
    n = len(terms)
    pieces = chunk_list(terms, leads)
    shapes = []
    for k, (term, chosen) in enumerate(zip(terms, leads)):
        rows, cols = term.shape[-2:]
        if k == 1:
            shapes.append(jax.ShapeDtypeStruct((rows, cols * term.shape[0] if chosen else cols), f32))
        else:
            shapes.append(jax.ShapeDtypeStruct((grid.nz, rows, cols), bf16))
    scratch = reduce_scratch(grid, terms, z_majors, pieces)
    shapes.append(jax.ShapeDtypeStruct((QKV, tokens), bf16))
    blocks = (grid.nz, KEY_VALUE_HEADS, tokens, 128)
    scratch += [
        pltpu.VMEM((QUERY_HEADS, tokens, 128), bf16),
        pltpu.VMEM((KEY_VALUE_HEADS, tokens, 128), bf16),
        pltpu.VMEM((KEY_VALUE_HEADS, tokens, 128), bf16),
        pltpu.VMEM((KEY_VALUE_HEADS, HEAD, tokens), bf16),
        pltpu.VMEM((QUERY_HEADS, HEAD, tokens), f32),
        pltpu.VMEM(blocks, f32),
        pltpu.VMEM((grid.nz - 1,) + blocks[1:], bf16),
        pltpu.VMEM(blocks, bf16),
        pltpu.SemaphoreType.DMA((2, grid.nz, KEY_VALUE_HEADS)),
    ]
    return pl.pallas_call(
        functools.partial(back_kernel, grid, tuple(z_majors), pieces, 0 if early is None else early.shape[0]),
        out_shape=shapes,
        in_specs=[ANY] * n + [VMEM] * (7 + (early is not None)),
        out_specs=[VMEM] * (n + 1),
        scratch_shapes=scratch,
        compiler_params=pltpu.CompilerParams(
            collective_id=collective_id, has_side_effects=True, vmem_limit_bytes=63 << 20
        ),
        name="back",
    )(*split_terms(grid, terms, z_majors), qx, qn, dox, kv, kext, cos, sin, *([] if early is None else [early]))


def adamw(weight, grad, first, second, rate, decay):
    first_new = beta_one * first + (1.0 - beta_one) * grad
    second_new = beta_two * second + (1.0 - beta_two) * grad * grad
    first_hat = first_new / (1.0 - beta_one**ADAM_STEP)
    second_hat = second_new / (1.0 - beta_two**ADAM_STEP)
    weight_new = weight - rate * (
        first_hat / (jnp.sqrt(second_hat) + adam_epsilon) + decay * weight
    )
    return (weight_new, first_new, second_new)


def finish_kernel(grid, pieces, *refs):
    hd, heads, x, gain, rg, gain_two, down, output, ig, gheads, ggains, gdown, goutput = refs[:13]
    h1, og, flat, wide, terms, value, last_down, last_output, last_sems = refs[13:22]
    here = Here(grid)
    greet(here.peers())
    columns = [Collect(here, down, last_down, last_sems.at[0]), Collect(here, output, last_output, last_sems.at[1])]
    for column in columns:
        column.begin()
    jobs, refs = reduce_jobs(here, [terms], [gheads], refs[22:], (True,), pieces)
    share = Share(here, value, ggains, refs[:4], refs[4])
    tokens = x.shape[1]
    inverse = inverse_rms(x)
    for k in range(DEPTH):
        rows = pl.ds(k * SLICE, SLICE)
        h1[rows] = (x[rows].astype(f32) * inverse * gain[rows, 0:1]).astype(bf16)
    rows = terms.shape[-2]
    for k in range(DEPTH):
        flat[...] = mm_nt(hd[...], h1[pl.ds(k * SLICE, SLICE)])
        for d in range(grid.nd):
            place = (k, d // (2 * grid.nx), d // 2 % grid.nx, d % 2)
            terms[place] = flat[pl.ds(d * rows, rows)].astype(bf16)
    ticks = pipelined(jobs, len(jobs))
    for tick in ticks[: len(jobs)]:
        tick()
    ticks = ticks[len(jobs) :]

    def turn(count=1):
        for _ in range(count):
            if ticks:
                ticks.pop(0)()

    for k in range(DEPTH):
        og[pl.ds(k * SLICE, SLICE)] = mm_tn(heads[k], hd[...])
        if k == 1:
            turn()
    turn()
    total = jnp.zeros((1, tokens), f32)
    for k in range(DEPTH):
        rows = pl.ds(k * SLICE, SLICE)
        normed = x[rows].astype(f32) * inverse
        sums = jnp.sum(og[rows] * normed, axis=1, keepdims=True)
        place = lax.broadcasted_iota(jnp.int32, (SLICE, 128), 1)
        wide[rows] = jnp.where(place == 0, sums, jnp.where(place == 1, gain_two[rows], 0.0))
        total += jnp.sum(og[rows] * gain[rows, 0:1] * normed, axis=0, keepdims=True)
    value[...] = wide[...].T[:8]
    share.start(0)
    turn()
    mean = total * (1.0 / D)
    for k in range(DEPTH):
        rows = pl.ds(k * SLICE, SLICE)
        normed = x[rows].astype(f32) * inverse
        ig[rows] = rg[rows] + inverse * (og[rows] * gain[rows, 0:1] - normed * mean)
    turn()
    gdown[...] = columns[0].end()
    goutput[...] = columns[1].end().T
    for k in range(4):
        share.end(k)
        if k < 3:
            share.start(k + 1)
        turn(2)
    turn(len(ticks))
    share.drain()
    for job in jobs + columns:
        job.drain()


def finish(grid, hd, heads, x, gain, rg, gain_two, down, output, collective_id):
    tokens = x.shape[1]
    rows = QKV // grid.nd
    term = jax.ShapeDtypeStruct((rows, SLICE), bf16)
    pieces = chunk_list([term])
    scratch = [
        pltpu.VMEM((D, tokens), bf16),
        pltpu.VMEM((D, tokens), f32),
        pltpu.VMEM((QKV, SLICE), f32),
        pltpu.VMEM((D, 128), f32),
        pltpu.VMEM((grid.nz, grid.ny, grid.nx, 2, rows, SLICE), bf16),
        pltpu.VMEM((8, D), f32),
        pltpu.VMEM(down.shape, bf16),
        pltpu.VMEM(output.shape, bf16),
        pltpu.SemaphoreType.DMA((2, 2)),
    ]
    scratch += reduce_scratch(grid, [term], (True,), pieces)
    scratch += Share.scratch(grid, (8, D))
    scratch.append(pltpu.SemaphoreType.DMA((SHARE_SEMS,)))
    return pl.pallas_call(
        functools.partial(finish_kernel, grid, pieces),
        out_shape=[
            jax.ShapeDtypeStruct((D, tokens), f32),
            jax.ShapeDtypeStruct((rows, SLICE), f32),
            jax.ShapeDtypeStruct((8, D), f32),
            jax.ShapeDtypeStruct(down.shape[1:], f32),
            jax.ShapeDtypeStruct(output.shape[:0:-1], f32),
        ],
        in_specs=[VMEM] * 8,
        out_specs=[VMEM] * 5,
        scratch_shapes=scratch,
        compiler_params=pltpu.CompilerParams(
            collective_id=collective_id, has_side_effects=True, vmem_limit_bytes=62 << 20
        ),
        name="finish",
    )(hd, heads, x, gain, rg, gain_two, down, output)


READY = 2
SUMMED = 1


def local(
    grid,
    hidden_in,
    out_grad,
    seg_ids,
    doc_start,
    norm_gains,
    heads_weight,
    output_weight,
    expand_weight,
    down_weight,
    gains_first,
    gains_second,
    heads_first,
    heads_second,
    output_first,
    output_second,
    expand_first,
    expand_second,
    down_first,
    down_second,
):
    tokens = hidden_in.shape[0]
    first_row = lax.axis_index("shard") * tokens
    positions = first_row + jnp.arange(tokens, dtype=jnp.int32)
    freq = jnp.power(10000.0, -jnp.arange(HEAD // 2).astype(f32) / (HEAD // 2))
    angle = (positions - doc_start).astype(f32)[None, :] * freq[:, None]
    cos, sin = jnp.cos(angle), jnp.sin(angle)
    seg_row = seg_ids[0]
    seg_query = lax.dynamic_slice_in_dim(seg_row, first_row, tokens)
    doc = jnp.arange(HEAD, dtype=jnp.int32)
    qext = jnp.where((doc[:, None] < DOCS) & (seg_query[None, :] == doc[:, None]), HIDE, 0.0).astype(bf16)
    lane = jnp.arange(128, dtype=jnp.int32) - HEAD
    other_doc = (lane[None, :] >= 0) & (lane[None, :] < DOCS) & (seg_row[:, None] != lane[None, :])
    kext = jnp.where(other_doc | ((lane >= DOCS) & (lane < DOCS + 3))[None, :], 1.0, 0.0).astype(bf16)
    x, ogt = hidden_in.T, out_grad.T
    gain = norm_gains.T

    heads_stack, *columns = gather_weights(
        grid, [heads_weight.T], (True,), [output_weight, down_weight.T], (False, True, False), 1
    )
    heads = heads_stack.reshape(DEPTH, QKV, SLICE)
    stepped = expand_weight.shape[1] == STEPS * WIDTH
    leads = [None, None, list(range(READY)) if stepped else None]
    shards = [*columns, expand_weight]
    output_stack, down_stack, expand_stack, qx, qn, kv, att, *late_columns = front(
        grid, shards, (True, True, False), leads, heads, x, gain, cos, sin, qext, kext, 2
    )
    wo = output_stack.reshape(DEPTH, D, SLICE)
    down = down_stack.reshape(DEPTH, D, FF // DEPTH)
    blocks = (8, DEPTH, SLICE)
    if stepped:
        late = middle(grid, att, wo, x, ogt, gain, expand_stack, down, late_columns[0], SUMMED, 5)
        out, rg, gain_two_term, dwo, dox, dexpand, ddn, *late = late
        early_exp = late[-1] if SUMMED else None
    else:
        expand = expand_stack.transpose(1, 2, 0, 3).reshape(DEPTH, SLICE, 8, STEPS, WIDTH)
        expand = expand.transpose(3, 2, 0, 1, 4)
        out, rg, gain_two_term, dwo, dox, dexpand, ddn = middle(
            grid, att, wo, x, ogt, gain, expand, down, None, 0, 5
        )
        early_exp = None
        dexpand = dexpand.transpose(2, 3, 1, 0, 4).reshape(DEPTH, SLICE, grid.nd, -1).transpose(2, 0, 1, 3)
    if stepped:
        dexpand = dexpand.reshape((STEPS, grid.nd, grid.nz, SLICE, WIDTH))
    terms = [ddn.reshape(down_stack.shape), dexpand, dwo.reshape(output_stack.shape)]
    leads = [None, list(range(SUMMED, STEPS)) if stepped else None, None]
    down_column, expand_grad, output_column, hd = back(
        grid, terms, (True, False, True), leads, early_exp, qx, qn, dox, kv, kext, cos, sin, 3
    )
    ig, heads_grad, gains_grad, down_grad, output_grad = finish(
        grid, hd, heads, x, gain, rg, gain_two_term, down_column, output_column, 4
    )
    heads_grad, down_grad, gains_grad = heads_grad.T, down_grad.T, gains_grad[:2]
    hidden_out, input_grad = out.T, ig.T
    gains_new, gains_first_new, gains_second_new = adamw(
        norm_gains, gains_grad, gains_first, gains_second, gain_rate, 0.0
    )
    heads_new, heads_first_new, heads_second_new = adamw(
        heads_weight, heads_grad, heads_first, heads_second, matrix_rate, decay_rate
    )
    output_new, output_first_new, output_second_new = adamw(
        output_weight, output_grad, output_first, output_second, output_rate, decay_rate
    )
    expand_new, expand_first_new, expand_second_new = adamw(
        expand_weight, expand_grad, expand_first, expand_second, matrix_rate, decay_rate
    )
    down_new, down_first_new, down_second_new = adamw(
        down_weight, down_grad, down_first, down_second, matrix_rate, decay_rate
    )
    return (
        hidden_out,
        input_grad,
        gains_grad,
        heads_grad,
        output_grad,
        expand_grad,
        down_grad,
        gains_new,
        heads_new,
        output_new,
        expand_new,
        down_new,
        gains_first_new,
        gains_second_new,
        heads_first_new,
        heads_second_new,
        output_first_new,
        output_second_new,
        expand_first_new,
        expand_second_new,
        down_first_new,
        down_second_new,
    )


def solution(mesh):
    return jax.shard_map(
        functools.partial(local, Grid(mesh)),
        mesh=mesh,
        in_specs=(
            P(("dp", "shard"), None),
            P(("dp", "shard"), None),
            P("dp", None),
            P(("dp", "shard")),
            P(),
            P("shard", "dp"),
            P("shard", "dp"),
            P("shard", "dp"),
            P("shard", "dp"),
            P(),
            P(),
            P("shard", "dp"),
            P("shard", "dp"),
            P("shard", "dp"),
            P("shard", "dp"),
            P("shard", "dp"),
            P("shard", "dp"),
            P("shard", "dp"),
            P("shard", "dp"),
        ),
        out_specs=(
            P(("dp", "shard"), None),
            P(("dp", "shard"), None),
            P(),
            P("shard", "dp"),
            P("shard", "dp"),
            P("shard", "dp"),
            P("shard", "dp"),
            P(),
            P("shard", "dp"),
            P("shard", "dp"),
            P("shard", "dp"),
            P("shard", "dp"),
            P(),
            P(),
            P("shard", "dp"),
            P("shard", "dp"),
            P("shard", "dp"),
            P("shard", "dp"),
            P("shard", "dp"),
            P("shard", "dp"),
            P("shard", "dp"),
            P("shard", "dp"),
        ),
        check_vma=False,
    )
```

```python
import functools
import math

import jax
import jax.numpy as jnp
from jax import lax
from jax.experimental import pallas as pl
from jax.experimental.pallas import tpu as pltpu
from jax.sharding import PartitionSpec as P

MESH = pl.DeviceIdType.MESH
ANY = pl.BlockSpec(memory_space=pl.ANY)
VMEM = pl.BlockSpec(memory_space=pltpu.VMEM)


class Grid:
    def __init__(self, mesh):
        self.nd = mesh.shape["dp"]
        self.nz = mesh.shape["shard"]
        self.nx = math.isqrt(self.nd // 2)
        self.ny = self.nd // 2 // self.nx
        assert self.nx == self.ny and self.nx * self.ny * 2 == self.nd

    def dp(self, y, x, c):
        return (y * self.nx + x) * 2 + c


class Here:
    def __init__(self, grid):
        self.grid = grid
        d = lax.axis_index("dp")
        self.z = lax.axis_index("shard")
        self.d = d
        self.c = lax.rem(d, 2)
        self.x = lax.rem(d // 2, grid.nx)
        self.y = d // (2 * grid.nx)
        g = grid
        self.xs = [lax.rem(self.x + k, g.nx) for k in range(1, g.nx)]
        self.ys = [lax.rem(self.y + k, g.ny) for k in range(1, g.ny)]
        self.zs = [lax.rem(self.z + k, g.nz) for k in range(1, g.nz)]
        self.partner = (g.dp(self.y, self.x, 1 - self.c), self.z)

    def on_x(self, x):
        return (self.grid.dp(self.y, x, self.c), self.z)

    def on_y(self, y):
        return (self.grid.dp(y, self.x, self.c), self.z)

    def on_z(self, z):
        return (self.d, z)

    def peers(self):
        return (
            [self.partner]
            + [self.on_x(x) for x in self.xs]
            + [self.on_y(y) for y in self.ys]
            + [self.on_z(z) for z in self.zs]
        )


def greet(peers):
    barrier = pltpu.get_barrier_semaphore()
    for peer in peers:
        pl.semaphore_signal(barrier, inc=1, device_id=peer, device_id_type=MESH)
    pl.semaphore_wait(barrier, len(peers))


def send(src, dst, send_sem, recv_sem, device):
    pltpu.make_async_remote_copy(
        src_ref=src,
        dst_ref=dst,
        send_sem=send_sem,
        recv_sem=recv_sem,
        device_id=device,
        device_id_type=MESH,
    ).start()


def wait_bytes(ref, sem):
    pltpu.make_async_copy(ref, ref, sem).wait()


def half_rows(rows):
    return max(16, int(rows / 32 + 0.5) * 16)


def chunks_of(rows, size=64):
    starts = list(range(0, rows, size))
    if len(starts) > 1 and rows - starts[-1] < size // 2:
        starts.pop()
    return [(start, stop - start) for start, stop in zip(starts, starts[1:] + [rows])]


class Gather:
    def __init__(self, here, shard, out, sems, z_major, rows):
        self.h, self.shard, self.out, self.sems, self.z_major = here, shard, out, sems, z_major
        self.start, self.rows = rows
        self.cut = half_rows(self.rows)

    def span(self, half=None):
        if half is None:
            return pl.ds(self.start, self.rows)
        return pl.ds(self.start, self.cut) if half == 0 else pl.ds(self.start + self.cut, self.rows - self.cut)

    def column(self, d, half=None):
        return self.out.at[:, d, self.span(half)] if self.z_major else self.out.at[d, :, self.span(half)]

    def block(self, d, z):
        return self.out.at[z, d, self.span()] if self.z_major else self.out.at[d, z, self.span()]

    def columns(self, count):
        some = pl.ds(0, count)
        return self.out.at[:, some, self.span()] if self.z_major else self.out.at[some, :, self.span()]

    def blocks(self, count):
        some = pl.ds(0, count)
        return self.out.at[some, 0, self.span()] if self.z_major else self.out.at[0, some, self.span()]

    def own(self):
        h = self.h
        return pltpu.make_async_copy(self.shard.at[self.span()], self.block(h.d, h.z), self.sems.at[8])

    def stage_z(self):
        h, s = self.h, self.sems
        for z in h.zs:
            send(self.shard.at[self.span()], self.block(h.d, h.z), s.at[0], s.at[1], h.on_z(z))
        self.own().start()

    def await_z(self):
        wait_bytes(self.blocks(len(self.h.zs)), self.sems.at[1])

    def drain_z(self):
        wait_bytes(self.blocks(len(self.h.zs)), self.sems.at[0])

    def stage_one(self):
        h, s = self.h, self.sems
        self.await_z()
        self.own().wait()
        for x in h.xs:
            send(self.column(h.d, 0), self.column(h.d, 0), s.at[2], s.at[3], h.on_x(x))
        for y in h.ys:
            send(self.column(h.d, 1), self.column(h.d, 1), s.at[2], s.at[3], h.on_y(y))
        send(self.column(h.d), self.column(h.d), s.at[6], s.at[7], h.partner)

    def stage_two(self):
        h, s, g = self.h, self.sems, self.h.grid
        wait_bytes(self.columns(len(h.xs)), s.at[3])
        for y in h.ys:
            for x in [h.x] + h.xs:
                col = self.column(g.dp(h.y, x, h.c), 0)
                send(col, col, s.at[4], s.at[5], h.on_y(y))
        for x in h.xs:
            for y in [h.y] + h.ys:
                col = self.column(g.dp(y, h.x, h.c), 1)
                send(col, col, s.at[4], s.at[5], h.on_x(x))
        for x in h.xs:
            col = self.column(g.dp(h.y, x, h.c), 0)
            send(col, col, s.at[6], s.at[7], h.partner)
        for y in h.ys:
            col = self.column(g.dp(y, h.x, h.c), 1)
            send(col, col, s.at[6], s.at[7], h.partner)

    def stage_three(self):
        h, s, g = self.h, self.sems, self.h.grid
        wait_bytes(self.columns(g.nx * len(h.ys)), s.at[5])
        for y in h.ys:
            for x in [h.x] + h.xs:
                col = self.column(g.dp(y, x, h.c), 0)
                send(col, col, s.at[6], s.at[7], h.partner)
        for x in h.xs:
            for y in [h.y] + h.ys:
                col = self.column(g.dp(y, x, h.c), 1)
                send(col, col, s.at[6], s.at[7], h.partner)

    def arrive(self):
        g = self.h.grid
        wait_bytes(self.columns(g.nd // 2), self.sems.at[7])

    def drain(self):
        h, s, g = self.h, self.sems, self.h.grid
        self.drain_z()
        wait_bytes(self.columns(len(h.xs)), s.at[2])
        wait_bytes(self.columns(g.nx * len(h.ys)), s.at[4])
        wait_bytes(self.columns(g.nd // 2), s.at[6])

    stages = ("stage_z", "stage_one", "stage_two", "stage_three")


class ColumnGather(Gather):
    def own(self):
        return pltpu.make_async_copy(self.shard.at[:, self.span()], self.column(self.h.d), self.sems.at[8])

    def stage_z(self):
        self.own().start()

    def await_z(self):
        pass

    def drain_z(self):
        pass


class Spread:
    def __init__(self, here, shard, out, sems):
        self.h, self.shard, self.out, self.sems = here, shard, out, sems

    def own(self):
        return pltpu.make_async_copy(self.shard, self.out.at[self.h.z], self.sems.at[2])

    def begin(self):
        h, s = self.h, self.sems
        for z in h.zs:
            send(self.shard, self.out.at[h.z], s.at[0], s.at[1], h.on_z(z))
        self.own().start()

    def end(self):
        some = self.out.at[pl.ds(0, len(self.h.zs))]
        wait_bytes(some, self.sems.at[1])
        wait_bytes(some, self.sems.at[0])
        self.own().wait()


def pipelined(jobs, ahead=0):
    ticks = [getattr(job, job.stages[0]) for job in jobs[:ahead]]
    depth = max((len(job.stages) for job in jobs), default=0)
    for step in range(len(jobs) + depth - 1):
        for k in range(depth):
            i = step - k
            if 0 <= i < len(jobs) and k < len(jobs[i].stages) and not (k == 0 and i < ahead):
                ticks.append(getattr(jobs[i], jobs[i].stages[k]))
    return ticks


def chunk_list(shards, leads=None):
    pieces = []
    for i, shard in enumerate(shards):
        if leads is not None and leads[i]:
            pieces += [(i, k, (0, shard.shape[-2])) for k in leads[i]]
        else:
            pieces += [(i, None, rows) for rows in chunks_of(shard.shape[-2])]
    return pieces


def piece_of(ref, lead):
    return ref if lead is None else ref.at[lead]


def gather_jobs(here, shards, outs, sems, z_majors, pieces):
    jobs = []
    for k, (i, lead, rows) in enumerate(pieces):
        kind = ColumnGather if lead is None and len(shards[i].shape) == 3 else Gather
        job = kind(here, piece_of(shards[i], lead), piece_of(outs[i], lead), sems.at[k], z_majors[i], rows)
        jobs.append(job)
    return jobs


GATHER_SEMS = 9


def gather_kernel(grid, z_majors, pieces, turns, *refs):
    n, spreads = len(z_majors), len(turns) - len(z_majors)
    given, refs = refs[: n + spreads], refs[n + spreads :]
    outs, refs = refs[:n], refs[n:]
    columns, refs = refs[:spreads], refs[spreads:]
    rounded, (sems, spread_sems) = refs[: n + spreads], refs[n + spreads :]
    for source, half, turn in zip(given, rounded, turns):
        half[...] = (source[...].T if turn else source[...]).astype(jnp.bfloat16)
    shards, singles = rounded[:n], rounded[n:]
    here = Here(grid)
    greet(here.peers())
    jobs = gather_jobs(here, shards, outs, sems, z_majors, pieces)
    ticks = pipelined(jobs, len(jobs))
    for tick in ticks[: len(jobs)]:
        tick()
    others = [Spread(here, singles[k], columns[k], spread_sems.at[k]) for k in range(spreads)]
    for other in others:
        other.begin()
    for tick in ticks[len(jobs) :]:
        tick()
    for job in jobs:
        job.arrive()
        job.drain()
    for other in others:
        other.end()


def gather_weights(grid, shards, z_majors, singles, turns, collective_id):
    blocks = []
    for value, turn in zip([*shards, *singles], turns):
        blocks.append(jax.ShapeDtypeStruct(value.shape[::-1] if turn else value.shape, jnp.bfloat16))
    n = len(shards)
    shapes = []
    for block, z_major in zip(blocks, z_majors):
        lead = (grid.nz, grid.nd) if z_major else (grid.nd, grid.nz)
        shapes.append(jax.ShapeDtypeStruct(lead + block.shape, block.dtype))
    for block in blocks[n:]:
        shapes.append(jax.ShapeDtypeStruct((grid.nz,) + block.shape, block.dtype))
    pieces = chunk_list(blocks[:n])
    return pl.pallas_call(
        functools.partial(gather_kernel, grid, tuple(z_majors), pieces, tuple(turns)),
        out_shape=shapes,
        in_specs=[VMEM] * len(blocks),
        out_specs=[ANY] * len(shapes),
        scratch_shapes=[pltpu.VMEM(block.shape, block.dtype) for block in blocks]
        + [
            pltpu.SemaphoreType.DMA((len(pieces), GATHER_SEMS)),
            pltpu.SemaphoreType.DMA((len(singles), 3)),
        ],
        compiler_params=pltpu.CompilerParams(collective_id=collective_id, has_side_effects=True),
        name="gather_weights",
    )(*shards, *singles)


class Reduce:
    def __init__(self, here, terms, result, bufs, sems, z_major, rows):
        self.h, self.terms, self.result, self.sems, self.z_major = here, terms, result, sems, z_major
        self.own, self.other, self.one_a, self.one_b, self.two_a, self.two_b, self.last = bufs
        self.start, self.rows = rows
        self.cut = half_rows(self.rows)

    @staticmethod
    def scratch(grid, rows, cols, z_major):
        cut = half_rows(rows)
        ny, nx, nz = grid.ny, grid.nx, grid.nz
        full = (nz, ny, nx) if z_major else (ny, nx, nz)
        row = (nz, nx) if z_major else (nx, nz)
        bf = jnp.bfloat16
        return [
            pltpu.VMEM(full + (rows, cols), bf),
            pltpu.VMEM(full + (rows, cols), bf),
            pltpu.VMEM((ny,) + row + (cut, cols), bf),
            pltpu.VMEM((nx,) + row + (rows - cut, cols), bf),
            pltpu.VMEM((nx, nz, cut, cols), bf),
            pltpu.VMEM((ny, nz, rows - cut, cols), bf),
            pltpu.VMEM((nz, rows, cols), bf),
        ]

    def span(self, half):
        return {None: slice(None), 0: pl.ds(0, self.cut), 1: pl.ds(self.cut, self.rows - self.cut)}[half]

    def at(self, y, x, z, half):
        y, x, z = (slice(None) if v is None else v for v in (y, x, z))
        return (z, y, x, self.span(half)) if self.z_major else (y, x, z, self.span(half))

    def side(self, c):
        rows = pl.ds(self.start, self.rows)
        return self.terms.at[:, :, :, c, rows] if self.z_major else self.terms.at[:, :, c, :, rows]

    def load(self):
        return pltpu.make_async_copy(self.side(self.h.c), self.own, self.sems.at[8])

    def stage_core(self):
        h, s = self.h, self.sems
        send(self.side(1 - h.c), self.other, s.at[0], s.at[1], h.partner)
        self.load().start()

    def add_loop(self, shape, body):
        total = math.prod(shape)

        def step(i, carry):
            place = []
            rest = i
            for size in reversed(shape):
                place.append(lax.rem(rest, size))
                rest = rest // size
            body(tuple(reversed(place)))
            return carry

        lax.fori_loop(0, total, step, 0)

    def stage_one(self):
        h, s, g = self.h, self.sems, self.h.grid
        self.load().wait()
        wait_bytes(self.other, s.at[1])

        def body(place):
            self.own[place] = self.own[place] + self.other[place]

        self.add_loop(self.own.shape[:3], body)
        for y in h.ys:
            send(self.own.at[self.at(y, None, None, 0)], self.one_a.at[h.y], s.at[2], s.at[3], h.on_y(y))
        for x in h.xs:
            send(self.own.at[self.at(None, x, None, 1)], self.one_b.at[h.x], s.at[9], s.at[10], h.on_x(x))

    def stage_two(self):
        h, s, g = self.h, self.sems, self.h.grid
        wait_bytes(self.one_a.at[pl.ds(0, g.ny - 1)], s.at[3])
        wait_bytes(self.one_b.at[pl.ds(0, g.nx - 1)], s.at[10])

        def body_a(place):
            where = (place[1], place[0]) if self.z_major else place
            spot = self.at(h.y, where[0], where[1], 0)
            total = self.own[spot].astype(jnp.float32)
            for y in h.ys:
                total += self.one_a[(y,) + place].astype(jnp.float32)
            self.own[spot] = total.astype(jnp.bfloat16)

        self.add_loop(self.one_a.shape[1:3], body_a)

        def body_b(place):
            where = (place[1], place[0]) if self.z_major else place
            spot = self.at(where[0], h.x, where[1], 1)
            total = self.own[spot].astype(jnp.float32)
            for x in h.xs:
                total += self.one_b[(x,) + place].astype(jnp.float32)
            self.own[spot] = total.astype(jnp.bfloat16)

        self.add_loop(self.one_b.shape[1:3], body_b)
        for x in h.xs:
            send(self.own.at[self.at(h.y, x, None, 0)], self.two_a.at[h.x], s.at[4], s.at[5], h.on_x(x))
        for y in h.ys:
            send(self.own.at[self.at(y, h.x, None, 1)], self.two_b.at[h.y], s.at[11], s.at[12], h.on_y(y))

    def stage_three(self):
        h, s, g = self.h, self.sems, self.h.grid
        wait_bytes(self.two_a.at[pl.ds(0, g.nx - 1)], s.at[5])
        wait_bytes(self.two_b.at[pl.ds(0, g.ny - 1)], s.at[12])

        def body(place):
            (z,) = place
            spot = self.at(h.y, h.x, z, 0)
            total = self.own[spot].astype(jnp.float32)
            for x in h.xs:
                total += self.two_a[x, z].astype(jnp.float32)
            self.own[spot] = total.astype(jnp.bfloat16)
            spot = self.at(h.y, h.x, z, 1)
            total = self.own[spot].astype(jnp.float32)
            for y in h.ys:
                total += self.two_b[y, z].astype(jnp.float32)
            self.own[spot] = total.astype(jnp.bfloat16)

        self.add_loop((g.nz,), body)
        for z in h.zs:
            send(self.own.at[self.at(h.y, h.x, z, None)], self.last.at[h.z], s.at[6], s.at[7], h.on_z(z))

    def finish(self):
        h, s, g = self.h, self.sems, self.h.grid
        wait_bytes(self.last.at[pl.ds(0, g.nz - 1)], s.at[7])
        total = self.own[self.at(h.y, h.x, h.z, None)].astype(jnp.float32)
        for z in h.zs:
            total += self.last[z].astype(jnp.float32)
        self.result[pl.ds(self.start, self.rows)] = total

    stages = ("stage_core", "stage_one", "stage_two", "stage_three", "finish")

    def drain_z(self):
        wait_bytes(self.last.at[pl.ds(0, self.h.grid.nz - 1)], self.sems.at[6])

    def drain(self):
        g, s = self.h.grid, self.sems
        wait_bytes(self.other, s.at[0])
        wait_bytes(self.one_a.at[pl.ds(0, g.ny - 1)], s.at[2])
        wait_bytes(self.one_b.at[pl.ds(0, g.nx - 1)], s.at[9])
        wait_bytes(self.two_a.at[pl.ds(0, g.nx - 1)], s.at[4])
        wait_bytes(self.two_b.at[pl.ds(0, g.ny - 1)], s.at[11])
        self.drain_z()


class ColumnReduce(Reduce):
    stages = ("stage_core", "stage_one", "stage_two", "stage_three")

    def stage_three(self):
        h, s, g = self.h, self.sems, self.h.grid
        wait_bytes(self.two_a.at[pl.ds(0, g.nx - 1)], s.at[5])
        wait_bytes(self.two_b.at[pl.ds(0, g.ny - 1)], s.at[12])

        def body(place):
            (z,) = place
            total = self.own[self.at(h.y, h.x, z, 0)].astype(jnp.float32)
            for x in h.xs:
                total += self.two_a[x, z].astype(jnp.float32)
            self.result[z, pl.ds(self.start, self.cut)] = total.astype(jnp.bfloat16)
            total = self.own[self.at(h.y, h.x, z, 1)].astype(jnp.float32)
            for y in h.ys:
                total += self.two_b[y, z].astype(jnp.float32)
            self.result[z, pl.ds(self.start + self.cut, self.rows - self.cut)] = total.astype(jnp.bfloat16)

        self.add_loop((g.nz,), body)

    def drain_z(self):
        pass


class Collect:
    def __init__(self, here, column, last, sems):
        self.h, self.column, self.last, self.sems = here, column, last, sems

    def begin(self):
        h, s = self.h, self.sems
        for z in h.zs:
            send(self.column.at[z], self.last.at[h.z], s.at[0], s.at[1], h.on_z(z))

    def end(self):
        h = self.h
        wait_bytes(self.last.at[pl.ds(0, len(h.zs))], self.sems.at[1])
        total = self.column[h.z].astype(jnp.float32)
        for z in h.zs:
            total += self.last[z].astype(jnp.float32)
        return total

    def drain(self):
        wait_bytes(self.last.at[pl.ds(0, len(self.h.zs))], self.sems.at[0])


REDUCE_SEMS = 13
REDUCE_BUFS = 7


class Share:
    def __init__(self, here, value, result, bufs, sems):
        self.h, self.value, self.result, self.sems = here, value, result, sems
        self.bufs = bufs

    @staticmethod
    def scratch(grid, shape):
        return [pltpu.VMEM((n,) + shape, jnp.float32) for n in (2, grid.nx, grid.ny, grid.nz)]

    def axis(self, k):
        h = self.h
        return (
            (h.c, [h.partner], 2),
            (h.x, [h.on_x(x) for x in h.xs], h.grid.nx),
            (h.y, [h.on_y(y) for y in h.ys], h.grid.ny),
            (h.z, [h.on_z(z) for z in h.zs], h.grid.nz),
        )[k]

    def start(self, k):
        me, peers, n = self.axis(k)
        self.bufs[k][me] = self.value[...] if k == 0 else self.total
        for peer in peers:
            send(self.bufs[k].at[me], self.bufs[k].at[me], self.sems.at[2 * k], self.sems.at[2 * k + 1], peer)

    def end(self, k):
        me, peers, n = self.axis(k)
        wait_bytes(self.bufs[k].at[pl.ds(0, n - 1)], self.sems.at[2 * k + 1])
        total = self.bufs[k][0]
        for i in range(1, n):
            total = total + self.bufs[k][i]
        self.total = total
        if k == 3:
            self.result[...] = total

    def drain(self):
        for k in range(4):
            n = self.axis(k)[2]
            wait_bytes(self.bufs[k].at[pl.ds(0, n - 1)], self.sems.at[2 * k])


SHARE_SEMS = 8


def reduce_kernel(grid, z_majors, pieces, shared, *refs):
    n = len(z_majors)
    terms, refs = refs[:n], refs[n:]
    value, refs = (refs[0], refs[1:]) if shared else (None, refs)
    results, refs = refs[:n], refs[n:]
    value_sum, refs = (refs[0], refs[1:]) if shared else (None, refs)
    here = Here(grid)
    greet(here.peers())
    jobs, refs = reduce_jobs(here, terms, results, refs, z_majors, pieces)
    share = None
    if shared:
        share = Share(here, value, value_sum, refs[:4], refs[4])
        share.start(0)
    ticks = pipelined(jobs, len(jobs))
    for k, tick in enumerate(ticks):
        tick()
        if share is not None and k >= len(jobs) and k - len(jobs) < 4:
            step = k - len(jobs)
            share.end(step)
            if step < 3:
                share.start(step + 1)
    if share is not None:
        share.drain()
    for job in jobs:
        job.drain()


def reduce_jobs(here, terms, results, refs, z_majors, pieces):
    n = len(pieces)
    sems = refs[n * REDUCE_BUFS]
    jobs = []
    for k, (i, lead, rows) in enumerate(pieces):
        bufs = refs[k * REDUCE_BUFS : (k + 1) * REDUCE_BUFS]
        term, result, kind = piece_of(terms[i], lead), results[i], Reduce
        deep = len(result.shape) == 3
        if lead is None:
            kind = ColumnReduce if deep else Reduce
        else:
            width = term.shape[-1]
            result = result.at[lead] if deep else result.at[:, pl.ds(lead * width, width)]
        jobs.append(kind(here, term, result, bufs, sems.at[k], z_majors[i], rows))
    return jobs, refs[n * REDUCE_BUFS + 1 :]


def reduce_scratch(grid, terms, z_majors, pieces):
    scratch = []
    for i, _, (_, rows) in pieces:
        scratch += Reduce.scratch(grid, rows, terms[i].shape[-1], z_majors[i])
    return scratch + [pltpu.SemaphoreType.DMA((max(len(pieces), 1), REDUCE_SEMS))]


def split_terms(grid, terms, z_majors):
    split = []
    for term, z_major in zip(terms, z_majors):
        lead = (grid.ny, grid.nx, 2)
        lead = (grid.nz,) + lead if z_major else lead + (grid.nz,)
        split.append(term.reshape(term.shape[:-4] + lead + term.shape[-2:]))
    return split


def reduce_grads(grid, terms, z_majors, value, collective_id):
    shapes = [jax.ShapeDtypeStruct(term.shape[-2:], jnp.float32) for term in terms]
    pieces = chunk_list(terms)
    scratch = reduce_scratch(grid, terms, z_majors, pieces)
    n = len(terms)
    shared = value is not None
    if shared:
        shapes.append(jax.ShapeDtypeStruct(value.shape, jnp.float32))
        scratch += Share.scratch(grid, value.shape)
        scratch.append(pltpu.SemaphoreType.DMA((SHARE_SEMS,)))
    return pl.pallas_call(
        functools.partial(reduce_kernel, grid, tuple(z_majors), pieces, shared),
        out_shape=shapes,
        in_specs=[ANY] * n + [VMEM] * shared,
        out_specs=[VMEM] * len(shapes),
        scratch_shapes=scratch,
        compiler_params=pltpu.CompilerParams(
            collective_id=collective_id, has_side_effects=True, vmem_limit_bytes=62 << 20
        ),
        name="reduce_grads",
    )(*split_terms(grid, terms, z_majors), *([value] if shared else []))


D = 960
QUERY_HEADS = 15
KEY_VALUE_HEADS = 5
GROUP = QUERY_HEADS // KEY_VALUE_HEADS
HEAD = 64
FF = 2560
QKV = (QUERY_HEADS + 2 * KEY_VALUE_HEADS) * HEAD
ADAM_STEP = 10
DOCS = 16
HIDE = -1e30
VALUE_SCALE = 2.0**-9

norm_epsilon = 1e-05
beta_one = 0.9
beta_two = 0.95
adam_epsilon = 1e-08
matrix_rate = 0.03
output_rate = 0.15
gain_rate = 0.5
decay_rate = 0.1

f32 = jnp.float32
bf16 = jnp.bfloat16
DEPTH = 4
SLICE = D // DEPTH


def mm(a, b):
    return lax.dot_general(a, b, (((1,), (0,)), ((), ())), preferred_element_type=f32)


def mm_nt(a, b):
    return lax.dot_general(a, b, (((1,), (1,)), ((), ())), preferred_element_type=f32)


def mm_tn(a, b):
    return lax.dot_general(a, b, (((0,), (0,)), ((), ())), preferred_element_type=f32)


def lanes_below(shape, n):
    return lax.broadcasted_iota(jnp.int32, shape, len(shape) - 1) < n


def inverse_rms(ref):
    total = jnp.zeros((1, ref.shape[1]), f32)
    for k in range(DEPTH):
        x = ref[pl.ds(k * SLICE, SLICE)].astype(f32)
        total += jnp.sum(x * x, axis=0, keepdims=True)
    return lax.rsqrt(total * (1.0 / D) + norm_epsilon)


def three_pieces(row):
    hi = row.astype(bf16).astype(f32)
    mid = (row - hi).astype(bf16).astype(f32)
    low = row - hi - mid
    place = lax.broadcasted_iota(jnp.int32, (16, row.shape[1]), 0)
    block = jnp.where(place == 0, hi, jnp.where(place == 1, mid, jnp.where(place == 2, low, 0.0)))
    return block.astype(bf16)


class KeyChain:
    def __init__(self, here, kv, sems):
        self.h, self.kv, self.sems = here, kv, sems

    def up(self, slot):
        h = self.h
        to = lax.rem(h.z + 1, h.grid.nz)

        @pl.when(h.z < h.grid.nz - 1)
        def _():
            send(self.kv.at[slot], self.kv.at[slot], self.sems.at[0, slot], self.sems.at[1, slot], h.on_z(to))

    def take(self, slot):
        wait_bytes(self.kv.at[slot], self.sems.at[1, slot])
        self.up(slot)

    def drain(self):
        h = self.h
        for s in range(h.grid.nz):

            @pl.when(jnp.logical_and(h.z >= s, h.z < h.grid.nz - 1))
            def _():
                wait_bytes(self.kv.at[h.z - s], self.sems.at[0, h.z - s])


def round_steps(source, rounded, start):
    if len(rounded.shape) == 2:
        rounded[...] = source[...].astype(bf16)
    else:
        for k in range(rounded.shape[0]):
            rounded[k] = source[:, pl.ds((start + k) * WIDTH, WIDTH)].astype(bf16)


def front_kernel(grid, z_majors, pieces, *refs):
    n = len(z_majors)
    shards, refs = refs[:n], refs[n:]
    heads, x, gain, cos, sin, qext, kext = refs[:7]
    refs = refs[7:]
    outs, refs = refs[:n], refs[n:]
    qx, qn, kv, att = refs[:4]
    h1, proj, kx, vt, acc, rounded, sems, kv_sems = refs[4:]
    here = Here(grid)
    tokens = x.shape[1]
    half = tokens // 2
    round_steps(shards[-1], rounded, 0)
    greet(here.peers())
    jobs = gather_jobs(here, [*shards[:-1], rounded], outs, sems, z_majors, pieces)
    ticks = pipelined(jobs, 3)
    for tick in ticks[:3]:
        tick()

    inverse = inverse_rms(x)
    for k in range(DEPTH):
        rows = pl.ds(k * SLICE, SLICE)
        h1[rows] = (x[rows].astype(f32) * inverse * gain[rows, 0:1]).astype(bf16)

    part = QKV // 5

    def project(m, carry):
        rows = pl.ds(pl.multiple_of(m * part, 16), part)
        total = mm(heads[0, rows], h1[pl.ds(0, SLICE)])
        for k in range(1, DEPTH):
            total += mm(heads[k, rows], h1[pl.ds(k * SLICE, SLICE)])
        proj[rows] = total
        return carry

    lax.fori_loop(3, 5, project, 0)

    def turned(h):
        base = h * HEAD
        a = proj[pl.ds(pl.multiple_of(base, 8), HEAD // 2)]
        b = proj[pl.ds(pl.multiple_of(base + HEAD // 2, 8), HEAD // 2)]
        c, s = cos[...], sin[...]
        return a * c - b * s, b * c + a * s

    def keys(g, carry):
        a, b = turned(QUERY_HEADS + g)
        v = proj[pl.ds(pl.multiple_of((QUERY_HEADS + KEY_VALUE_HEADS + g) * HEAD, 8), HEAD)]
        both = jnp.concatenate([a, b, v], axis=0)
        kv[here.z, g] = both.T.astype(bf16)
        return carry

    lax.fori_loop(0, KEY_VALUE_HEADS, keys, 0)
    chain = KeyChain(here, kv, kv_sems)
    chain.up(here.z)
    lax.fori_loop(0, 3, project, 0)

    def queries(h, carry):
        a, b = turned(h)
        scale = HEAD**-0.5
        qx[h, pl.ds(0, 32)] = (a.astype(bf16).astype(f32) * scale).astype(bf16)
        qx[h, pl.ds(32, 32)] = (b.astype(bf16).astype(f32) * scale).astype(bf16)
        qx[h, pl.ds(64, 64)] = qext[...]
        qn[h] = qx[h].astype(f32).T.astype(bf16)
        return carry

    lax.fori_loop(0, QUERY_HEADS, queries, 0)

    def prepare(slot):
        ext = kext[pl.ds(pl.multiple_of(slot * tokens, 16), tokens)]

        def body(g, carry):
            block = kv[slot, g]
            kx[g] = jnp.where(lanes_below(block.shape, HEAD), block, ext)
            turned_block = block.astype(f32).T
            vt[g, pl.ds(0, 16)] = jnp.ones((16, tokens), bf16)
            vt[g, pl.ds(16, HEAD)] = (turned_block[HEAD:] * VALUE_SCALE).astype(bf16)
            return carry

        lax.fori_loop(0, KEY_VALUE_HEADS, body, 0)

    def below(shape, shift):
        return lax.broadcasted_iota(jnp.int32, shape, 0) <= lax.broadcasted_iota(jnp.int32, shape, 1) + shift

    def diagonal(g):
        for i in range(GROUP):
            h = g * GROUP + i
            s = mm(kx[g, pl.ds(0, half)], qx[h, :, pl.ds(0, half)])
            p = jnp.exp(jnp.where(below(s.shape, 0), s, HIDE)).astype(bf16)
            acc[h, :, pl.ds(0, half)] = mm(vt[g, :, pl.ds(0, half)], p)
            s = mm(kx[g], qx[h, :, pl.ds(half, half)])
            p = jnp.exp(jnp.where(below(s.shape, half), s, HIDE)).astype(bf16)
            acc[h, :, pl.ds(half, half)] = mm(vt[g], p)

    def whole(g):
        for i in range(GROUP):
            h = g * GROUP + i
            for k in range(2):
                cols = pl.ds(k * half, half)
                p = jnp.exp(mm(kx[g], qx[h, :, cols])).astype(bf16)
                acc[h, :, cols] += mm(vt[g], p)

    ticks = ticks[3:]

    def micro(t, carry):
        s = t // KEY_VALUE_HEADS
        g = lax.rem(t, KEY_VALUE_HEADS)

        @pl.when(s <= here.z)
        def _():
            slot = here.z - s

            @pl.when(g == 0)
            def _():
                @pl.when(s > 0)
                def _():
                    chain.take(slot)

                prepare(slot)

            @pl.when(s == 0)
            def _():
                diagonal(g)

            @pl.when(s > 0)
            def _():
                whole(g)

        for k, tick in enumerate(ticks):
            pl.when(t == k * (micros - KEY_VALUE_HEADS) // len(ticks))(tick)
        return carry

    micros = grid.nz * KEY_VALUE_HEADS
    lax.fori_loop(0, micros, micro, 0)

    def close(h, carry):
        totals = acc[h, pl.ds(0, 1)]
        scale = (1.0 / VALUE_SCALE) / totals
        att[pl.ds(pl.multiple_of(h * HEAD, 16), HEAD)] = (acc[h, pl.ds(16, HEAD)] * scale).astype(bf16)
        qx[h, pl.ds(HEAD + DOCS, 16)] = three_pieces(-jnp.log(totals))
        return carry

    lax.fori_loop(0, QUERY_HEADS, close, 0)
    for job in jobs:
        job.arrive()
        job.drain()
    chain.drain()


def front(grid, shards, z_majors, leads, heads, x, gain, cos, sin, qext, kext, collective_id):
    tokens = x.shape[1]
    shapes = []
    chosen = leads[-1]
    expand = shards[-1]
    rounded = (len(chosen), SLICE, WIDTH) if chosen else expand.shape
    blocks = [*shards[:-1], jax.ShapeDtypeStruct(rounded, bf16)]
    for block, z_major, chosen in zip(blocks, z_majors, leads):
        lead = (grid.nz, grid.nd) if z_major else (grid.nd, grid.nz)
        lead = (len(chosen),) + lead if chosen else lead
        shapes.append(jax.ShapeDtypeStruct(lead + block.shape[-2:], bf16))
    n = len(shards)
    pieces = chunk_list(blocks, leads)
    shapes += [
        jax.ShapeDtypeStruct((QUERY_HEADS, 128, tokens), bf16),
        jax.ShapeDtypeStruct((QUERY_HEADS, tokens, 128), bf16),
        jax.ShapeDtypeStruct((grid.nz, KEY_VALUE_HEADS, tokens, 128), bf16),
        jax.ShapeDtypeStruct((D, tokens), bf16),
    ]
    return pl.pallas_call(
        functools.partial(front_kernel, grid, tuple(z_majors), pieces),
        out_shape=shapes,
        in_specs=[VMEM] * (n + 7),
        out_specs=[ANY] * n + [VMEM] * 4,
        scratch_shapes=[
            pltpu.VMEM((D, tokens), bf16),
            pltpu.VMEM((QKV, tokens), f32),
            pltpu.VMEM((KEY_VALUE_HEADS, tokens, 128), bf16),
            pltpu.VMEM((KEY_VALUE_HEADS, 80, tokens), bf16),
            pltpu.VMEM((QUERY_HEADS, 80, tokens), f32),
            pltpu.VMEM(rounded, bf16),
            pltpu.SemaphoreType.DMA((max(len(pieces), 1), GATHER_SEMS)),
            pltpu.SemaphoreType.DMA((2, grid.nz)),
        ],
        compiler_params=pltpu.CompilerParams(
            collective_id=collective_id, has_side_effects=True, vmem_limit_bytes=60 << 20
        ),
        name="front",
    )(*shards, heads, x, gain, cos, sin, qext, kext)


STEPS = 5
WIDTH = 128
PARTS = 6


def middle_kernel(grid, ready, summed, *refs):
    att, wo, x, ogt, gain, exp_in, dn_in = refs[:7]
    refs = refs[7:]
    late = STEPS - ready
    if late:
        shard, refs = refs[0], refs[1:]
    out, rg, gsum, dwo, dox, dexp, ddn = refs[:7]
    refs = refs[7:]
    if late:
        exp_late, refs = refs[0], refs[1:]
    if summed:
        gexp, refs = refs[0], refs[1:]
    (res, inv, h2, h2t, og, acc_o, acc_h, mixed, dgate, dup, wg, wu, wd, sg, sd, w_sems, o_sems) = refs[:17]
    refs = refs[17:]
    tokens = x.shape[1]
    half = 2 * WIDTH
    schedule = {}
    gathers, sums = [], []
    if late:
        round_steps(shard, refs[0], ready)
    if late or summed:
        here = Here(grid)
        greet(here.peers())
    if late:
        pieces = [(0, k, (0, SLICE)) for k in range(late)]
        rounded, g_sems, refs = refs[0], refs[1], refs[2:]
        gathers = [
            Gather(here, rounded.at[k], exp_late.at[k], g_sems.at[k], False, (0, SLICE)) for k in range(late)
        ]
        for job in gathers:
            job.stage_z()
        for k, job in enumerate(gathers):
            for i, stage in enumerate(job.stages[1:]):
                schedule.setdefault((k, 4 + 2 * k, 9 + 4 * k)[i], []).append(getattr(job, stage))
            schedule.setdefault((ready + k - 1) * PARTS + 1, []).append(job.arrive)
    if summed:
        pieces = [(0, k, (0, SLICE)) for k in range(summed)]
        sums, refs = reduce_jobs(here, [dexp], [gexp], refs, (False,), pieces)
        for k, job in enumerate(sums):
            for i, stage in enumerate(job.stages):
                place = min((k + 1) * PARTS + 2 + 5 * i, STEPS * PARTS - 1)
                schedule.setdefault(place, []).append(getattr(job, stage))

    def fetch_from(source, index, step, slot, go):
        for d in range(4):
            lanes = pl.ds(d * WIDTH, WIDTH)
            go(pltpu.make_async_copy(source.at[index, d], wg.at[slot, :, :, lanes], w_sems.at[slot, 0]))
            go(pltpu.make_async_copy(source.at[index, 4 + d], wu.at[slot, :, :, lanes], w_sems.at[slot, 1]))
            columns = pl.ds(pl.multiple_of(step * WIDTH, WIDTH), WIDTH)
            go(pltpu.make_async_copy(dn_in.at[d, :, columns], wd.at[slot, :, lanes], w_sems.at[slot, 2]))

    def fetch(step):
        slot = lax.rem(step, 2)

        @pl.when(step < ready)
        def _():
            fetch_from(exp_in, step, step, slot, lambda copy: copy.start())

        if late:

            @pl.when(step >= ready)
            def _():
                fetch_from(exp_late, step - ready, step, slot, lambda copy: copy.start())

    def put_expand(step, go):
        for k in range(2):
            for d in range(4):
                lanes = pl.ds(d * WIDTH, WIDTH)
                to = dexp.at[step, 4 * k + d] if not sums_split else dexp.at[(step,) + sums_place(4 * k + d)]
                go(pltpu.make_async_copy(sg.at[k, :, :, lanes], to, o_sems.at[0]))

    def put_down(step, go):
        for d in range(4):
            columns = pl.ds(pl.multiple_of(step * WIDTH, WIDTH), WIDTH)
            go(pltpu.make_async_copy(sd.at[:, pl.ds(d * WIDTH, WIDTH)], ddn.at[d, :, columns], o_sems.at[1]))

    sums_split = len(dexp.shape) == 7

    def sums_place(d):
        return (d // (2 * grid.nx), d // 2 % grid.nx, d % 2)

    fetch(jnp.int32(0))
    total = jnp.zeros((1, tokens), f32)
    for m in range(DEPTH):
        rows = pl.ds(m * SLICE, SLICE)
        r = x[rows].astype(f32)
        for k in range(DEPTH):
            r += mm(wo[k, rows], att[pl.ds(k * SLICE, SLICE)])
        res[rows] = r
        total += jnp.sum(r * r, axis=0, keepdims=True)
    inverse = lax.rsqrt(total * (1.0 / D) + norm_epsilon)
    inv[...] = inverse
    for m in range(DEPTH):
        rows = pl.ds(m * SLICE, SLICE)
        h2t[rows] = (res[rows] * inverse * gain[rows, 1:2]).astype(bf16)
    h2[...] = h2t[...].astype(f32).T.astype(bf16)
    og[...] = ogt[...].astype(f32).T.astype(bf16)
    acc_o[...] = jnp.zeros_like(acc_o)
    acc_h[...] = jnp.zeros_like(acc_h)

    def activate(slot, k):
        cols = pl.ds(k * half, half)
        gate = mm(h2[...], wg[slot, :, :, cols].reshape(D, half))
        up = mm(h2[...], wu[slot, :, :, cols].reshape(D, half))
        back = mm(og[...], wd[slot, :, cols])
        s = 1.0 / (1.0 + jnp.exp(-gate))
        silu = gate * s
        mixed[:, cols] = (silu * up).astype(bf16)
        dgate[:, cols] = (back * up * s * (1.0 + gate * (1.0 - s))).astype(bf16)
        dup[:, cols] = (back * silu).astype(bf16)

    def micro(t, carry):
        step = t // PARTS
        part = lax.rem(t, PARTS)
        slot = lax.rem(step, 2)

        for place, ticks in schedule.items():

            @pl.when(t == place)
            def _():
                for tick in ticks:
                    tick()

        @pl.when(part == 0)
        def _():
            wait_bytes(wg.at[slot], w_sems.at[slot, 0])
            wait_bytes(wu.at[slot], w_sems.at[slot, 1])
            wait_bytes(wd.at[slot], w_sems.at[slot, 2])
            activate(slot, 0)

        @pl.when(part == 1)
        def _():
            @pl.when(step > 0)
            def _():
                wait_bytes(sg, o_sems.at[0])
                wait_bytes(sd, o_sems.at[1])

            pl.when(step + 1 < STEPS)(lambda: fetch(step + 1))
            activate(slot, 1)

        @pl.when(part == 2)
        def _():
            acc_o[...] += mm_nt(wd[slot], mixed[...])

        @pl.when(part == 3)
        def _():
            for m in range(DEPTH):
                sg[0, m] = mm(h2t[pl.ds(m * SLICE, SLICE)], dgate[...]).astype(bf16)
                sg[1, m] = mm(h2t[pl.ds(m * SLICE, SLICE)], dup[...]).astype(bf16)
            put_expand(step, lambda copy: copy.start())

        @pl.when(part == 4)
        def _():
            sd[...] = mm(ogt[...], mixed[...]).astype(bf16)
            put_down(step, lambda copy: copy.start())

        @pl.when(part == 5)
        def _():
            acc_h[...] += mm_nt(wg[slot].reshape(D, 2 * half), dgate[...])
            acc_h[...] += mm_nt(wu[slot].reshape(D, 2 * half), dup[...])

        return carry

    lax.fori_loop(0, STEPS * PARTS, micro, 0)
    wait_bytes(sg, o_sems.at[0])
    wait_bytes(sd, o_sems.at[1])
    inverse = inv[...]
    total = jnp.zeros((1, tokens), f32)
    for m in range(DEPTH):
        rows = pl.ds(m * SLICE, SLICE)
        out[rows] = (res[rows] + acc_o[rows]).astype(bf16)
        normed = res[rows] * inverse
        up = acc_h[rows]
        gsum[rows] = jnp.sum(up * normed, axis=1, keepdims=True)
        total += jnp.sum(up * gain[rows, 1:2] * normed, axis=0, keepdims=True)
    mean = total * (1.0 / D)
    for m in range(DEPTH):
        rows = pl.ds(m * SLICE, SLICE)
        normed = res[rows] * inverse
        r = ogt[rows].astype(f32) + inverse * (acc_h[rows] * gain[rows, 1:2] - normed * mean)
        rg[rows] = r
        h2t[rows] = r.astype(bf16)
    for k in range(DEPTH):
        rows = pl.ds(k * SLICE, SLICE)
        dwo[k] = mm_nt(h2t[...], att[rows]).astype(bf16)
        acc_h[rows] = mm_tn(wo[k], h2t[...])

    def rows_of(h, carry):
        rows = pl.ds(pl.multiple_of(h * HEAD, 16), HEAD)
        grad = acc_h[rows].astype(bf16)
        dox[h, pl.ds(HEAD, HEAD)] = grad
        delta = jnp.sum(grad.astype(f32) * att[rows].astype(f32), axis=0, keepdims=True)
        dox[h, pl.ds(0, 16)] = three_pieces(-delta)
        dox[h, pl.ds(16, 48)] = jnp.zeros((48, tokens), bf16)
        return carry

    lax.fori_loop(0, QUERY_HEADS, rows_of, 0)
    for job in gathers + sums:
        job.drain()


def middle(grid, att, wo, x, ogt, gain, expand, down, shard, summed, collective_id):
    tokens = x.shape[1]
    ready = expand.shape[0]
    late = STEPS - ready
    blocks = expand.shape[1:]
    if summed:
        grads = (STEPS, grid.ny, grid.nx, 2) + blocks[1:]
    else:
        grads = (STEPS,) + blocks
    shapes = [
        jax.ShapeDtypeStruct((D, tokens), bf16),
        jax.ShapeDtypeStruct((D, tokens), f32),
        jax.ShapeDtypeStruct((D, 1), f32),
        jax.ShapeDtypeStruct((DEPTH, D, SLICE), bf16),
        jax.ShapeDtypeStruct((QUERY_HEADS, 128, tokens), bf16),
        jax.ShapeDtypeStruct(grads, bf16),
        jax.ShapeDtypeStruct(down.shape, bf16),
    ]
    out_specs = [VMEM] * 5 + [ANY] * 2
    inputs = [att, wo, x, ogt, gain, expand, down]
    in_specs = [VMEM] * 5 + [ANY] * 2
    scratch = [
        pltpu.VMEM((D, tokens), f32),
        pltpu.VMEM((1, tokens), f32),
        pltpu.VMEM((tokens, D), bf16),
        pltpu.VMEM((D, tokens), bf16),
        pltpu.VMEM((tokens, D), bf16),
        pltpu.VMEM((D, tokens), f32),
        pltpu.VMEM((D, tokens), f32),
        pltpu.VMEM((tokens, 4 * WIDTH), bf16),
        pltpu.VMEM((tokens, 4 * WIDTH), bf16),
        pltpu.VMEM((tokens, 4 * WIDTH), bf16),
        pltpu.VMEM((2, DEPTH, SLICE, 4 * WIDTH), bf16),
        pltpu.VMEM((2, DEPTH, SLICE, 4 * WIDTH), bf16),
        pltpu.VMEM((2, D, 4 * WIDTH), bf16),
        pltpu.VMEM((2, DEPTH, SLICE, 4 * WIDTH), bf16),
        pltpu.VMEM((D, 4 * WIDTH), bf16),
        pltpu.SemaphoreType.DMA((2, 3)),
        pltpu.SemaphoreType.DMA((2,)),
    ]
    if late:
        inputs.append(shard)
        in_specs.append(VMEM)
        shapes.append(jax.ShapeDtypeStruct((late,) + blocks, bf16))
        out_specs.append(ANY)
        scratch.append(pltpu.VMEM((late, SLICE, WIDTH), bf16))
        scratch.append(pltpu.SemaphoreType.DMA((late, GATHER_SEMS)))
    if summed:
        shapes.append(jax.ShapeDtypeStruct((summed,) + blocks[2:], f32))
        out_specs.append(VMEM)
        pieces = [(0, k, (0, SLICE)) for k in range(summed)]
        term = jax.ShapeDtypeStruct(blocks, bf16)
        scratch += reduce_scratch(grid, [term], (False,), pieces)
    params = dict(collective_id=collective_id, has_side_effects=True) if late or summed else {}
    return pl.pallas_call(
        functools.partial(middle_kernel, grid, ready, summed),
        out_shape=shapes,
        in_specs=in_specs,
        out_specs=out_specs,
        scratch_shapes=scratch,
        compiler_params=pltpu.CompilerParams(vmem_limit_bytes=62 << 20, **params),
        name="middle",
    )(*inputs)


class GradChain:
    def __init__(self, here, part, sent, got, sems):
        self.h, self.part, self.sent, self.got, self.sems = here, part, sent, got, sems

    def summed(self, slot, g, write):
        h = self.h

        @pl.when(h.z < h.grid.nz - 1)
        def _():
            wait_bytes(self.got.at[slot, g], self.sems.at[1, slot, g])
            write(g, self.part[slot, g] + self.got[slot, g].astype(f32))

        @pl.when(h.z == h.grid.nz - 1)
        def _():
            write(g, self.part[slot, g])

    def relay(self, slot, g):
        h = self.h

        def write(g, value):
            self.sent[slot, g] = value.astype(bf16)

        self.summed(slot, g, write)
        to = lax.rem(h.z + h.grid.nz - 1, h.grid.nz)
        sems = self.sems
        send(self.sent.at[slot, g], self.got.at[slot, g], sems.at[0, slot, g], sems.at[1, slot, g], h.on_z(to))

    def drain(self):
        h = self.h

        def body(t, carry):
            slot, g = t // KEY_VALUE_HEADS, lax.rem(t, KEY_VALUE_HEADS)
            wait_bytes(self.sent.at[slot, g], self.sems.at[0, slot, g])
            return carry

        lax.fori_loop(0, h.z * KEY_VALUE_HEADS, body, 0)


def back_kernel(grid, z_majors, pieces, early, *refs):
    n = len(z_majors)
    terms, refs = refs[:n], refs[n:]
    qx, qn, dox, kv, kext, cos, sin = refs[:7]
    refs = refs[7:]
    if early:
        first, refs = refs[0], refs[1:]
    results, refs = refs[:n], refs[n:]
    for k in range(early):
        results[1][:, pl.ds(k * WIDTH, WIDTH)] = first[k]
    hd, refs = refs[0], refs[1:]
    here = Here(grid)
    jobs, refs = reduce_jobs(here, terms, results, refs, z_majors, pieces)
    don, kx, vx, kt, dq, part, sent, got, kv_sems = refs
    tokens = dox.shape[2]
    half = tokens // 2
    greet(here.peers())
    ticks = pipelined(jobs, len(jobs))
    for tick in ticks[: len(jobs)]:
        tick()
    ticks = ticks[len(jobs) :]

    def gather_queries(h, carry):
        dq[h] = jnp.zeros((HEAD, tokens), f32)
        don[h] = dox[h].astype(f32).T.astype(bf16)
        return carry

    lax.fori_loop(0, QUERY_HEADS, gather_queries, 0)

    def prepare(slot):
        ext = kext[pl.ds(pl.multiple_of(slot * tokens, 16), tokens)]

        def body(g, carry):
            block = kv[slot, g]
            low = lanes_below(block.shape, HEAD)
            kx[g] = jnp.where(low, block, ext)
            ones = jnp.where(lanes_below(block.shape, 3), 1.0, 0.0).astype(bf16)
            vx[g] = jnp.where(low, ones, block)
            kt[g] = block.astype(f32).T[:HEAD].astype(bf16)
            return carry

        lax.fori_loop(0, KEY_VALUE_HEADS, body, 0)

    def tile(g, h, count, k, masked):
        keys, cols = pl.ds(0, count), pl.ds(k * half, half)
        s = mm(kx[g, keys], qx[h, :, cols])
        if masked:
            row = lax.broadcasted_iota(jnp.int32, s.shape, 0)
            col = lax.broadcasted_iota(jnp.int32, s.shape, 1) + k * half
            s = jnp.where(row <= col, s, HIDE)
        p = jnp.exp(s)
        ds = (p * mm(vx[g, keys], dox[h, :, cols])).astype(bf16)
        dq[h, :, cols] += mm(kt[g, :, keys], ds)
        dk = mm(ds, qn[h, cols])
        dv = mm(p.astype(bf16), don[h, cols])
        return jnp.where(lanes_below(dk.shape, HEAD), dk, dv)

    def whole(slot, g):
        total = None
        for i in range(GROUP):
            for k in range(2):
                new = tile(g, g * GROUP + i, tokens, k, False)
                total = new if total is None else total + new
        part[slot, g] = total

    def diagonal(g):
        total = None
        for i in range(GROUP):
            new = tile(g, g * GROUP + i, tokens, 1, True)
            total = new if total is None else total + new
        part[here.z, g] = total
        total = part[here.z, g, pl.ds(0, half)]
        for i in range(GROUP):
            total += tile(g, g * GROUP + i, half, 0, True)
        part[here.z, g, pl.ds(0, half)] = total

    chain = GradChain(here, part, sent, got, kv_sems)
    micros = grid.nz * KEY_VALUE_HEADS
    top = here.z == grid.nz - 1

    def micro(t, carry):
        slot = t // KEY_VALUE_HEADS
        g = lax.rem(t, KEY_VALUE_HEADS)

        @pl.when(slot <= here.z)
        def _():
            pl.when(g == 0)(lambda: prepare(slot))

            @pl.when(slot < here.z)
            def _():
                whole(slot, g)
                pl.when(top)(lambda: chain.relay(slot, g))

            pl.when(slot == here.z)(lambda: diagonal(g))

        @pl.when(jnp.logical_and(jnp.logical_not(top), jnp.logical_and(slot >= 1, slot <= here.z)))
        def _():
            chain.relay(slot - 1, g)

        for k, tick in enumerate(ticks):
            pl.when(t == k * (micros - 3) // len(ticks))(tick)
        return carry

    lax.fori_loop(0, micros, micro, 0)

    def turn_back(a, b):
        c, s = cos[...], sin[...]
        return a * c + b * s, b * c - a * s

    def queries(h, carry):
        scale = HEAD**-0.5
        a, b = turn_back(dq[h, pl.ds(0, 32)] * scale, dq[h, pl.ds(32, 32)] * scale)
        hd[pl.ds(pl.multiple_of(h * HEAD, 16), 32)] = a.astype(bf16)
        hd[pl.ds(pl.multiple_of(h * HEAD + 32, 16), 32)] = b.astype(bf16)
        return carry

    lax.fori_loop(0, QUERY_HEADS, queries, 0)

    def write(g, value):
        turned = value.T
        a, b = turn_back(turned[:32], turned[32:64])
        base = (QUERY_HEADS + g) * HEAD
        hd[pl.ds(pl.multiple_of(base, 16), 32)] = a.astype(bf16)
        hd[pl.ds(pl.multiple_of(base + 32, 16), 32)] = b.astype(bf16)
        base = (QUERY_HEADS + KEY_VALUE_HEADS + g) * HEAD
        hd[pl.ds(pl.multiple_of(base, 16), HEAD)] = turned[64:].astype(bf16)

    def close(g, carry):
        chain.summed(here.z, g, write)
        return carry

    lax.fori_loop(0, KEY_VALUE_HEADS, close, 0)
    chain.drain()
    for job in jobs:
        job.drain()


def back(grid, terms, z_majors, leads, early, qx, qn, dox, kv, kext, cos, sin, collective_id):
    tokens = dox.shape[2]
    n = len(terms)
    pieces = chunk_list(terms, leads)
    shapes = []
    for k, (term, chosen) in enumerate(zip(terms, leads)):
        rows, cols = term.shape[-2:]
        if k == 1:
            shapes.append(jax.ShapeDtypeStruct((rows, cols * term.shape[0] if chosen else cols), f32))
        else:
            shapes.append(jax.ShapeDtypeStruct((grid.nz, rows, cols), bf16))
    scratch = reduce_scratch(grid, terms, z_majors, pieces)
    shapes.append(jax.ShapeDtypeStruct((QKV, tokens), bf16))
    blocks = (grid.nz, KEY_VALUE_HEADS, tokens, 128)
    scratch += [
        pltpu.VMEM((QUERY_HEADS, tokens, 128), bf16),
        pltpu.VMEM((KEY_VALUE_HEADS, tokens, 128), bf16),
        pltpu.VMEM((KEY_VALUE_HEADS, tokens, 128), bf16),
        pltpu.VMEM((KEY_VALUE_HEADS, HEAD, tokens), bf16),
        pltpu.VMEM((QUERY_HEADS, HEAD, tokens), f32),
        pltpu.VMEM(blocks, f32),
        pltpu.VMEM((grid.nz - 1,) + blocks[1:], bf16),
        pltpu.VMEM(blocks, bf16),
        pltpu.SemaphoreType.DMA((2, grid.nz, KEY_VALUE_HEADS)),
    ]
    return pl.pallas_call(
        functools.partial(back_kernel, grid, tuple(z_majors), pieces, 0 if early is None else early.shape[0]),
        out_shape=shapes,
        in_specs=[ANY] * n + [VMEM] * (7 + (early is not None)),
        out_specs=[VMEM] * (n + 1),
        scratch_shapes=scratch,
        compiler_params=pltpu.CompilerParams(
            collective_id=collective_id, has_side_effects=True, vmem_limit_bytes=63 << 20
        ),
        name="back",
    )(*split_terms(grid, terms, z_majors), qx, qn, dox, kv, kext, cos, sin, *([] if early is None else [early]))


def adamw(weight, grad, first, second, rate, decay):
    first_new = beta_one * first + (1.0 - beta_one) * grad
    second_new = beta_two * second + (1.0 - beta_two) * grad * grad
    first_hat = first_new / (1.0 - beta_one**ADAM_STEP)
    second_hat = second_new / (1.0 - beta_two**ADAM_STEP)
    weight_new = weight - rate * (
        first_hat / (jnp.sqrt(second_hat) + adam_epsilon) + decay * weight
    )
    return (weight_new, first_new, second_new)


def finish_kernel(grid, pieces, *refs):
    hd, heads, x, gain, rg, gain_two, down, output, ig, gheads, ggains, gdown, goutput = refs[:13]
    h1, og, flat, wide, terms, value, last_down, last_output, last_sems = refs[13:22]
    here = Here(grid)
    greet(here.peers())
    columns = [Collect(here, down, last_down, last_sems.at[0]), Collect(here, output, last_output, last_sems.at[1])]
    for column in columns:
        column.begin()
    jobs, refs = reduce_jobs(here, [terms], [gheads], refs[22:], (True,), pieces)
    share = Share(here, value, ggains, refs[:4], refs[4])
    tokens = x.shape[1]
    inverse = inverse_rms(x)
    for k in range(DEPTH):
        rows = pl.ds(k * SLICE, SLICE)
        h1[rows] = (x[rows].astype(f32) * inverse * gain[rows, 0:1]).astype(bf16)
    rows = terms.shape[-2]
    for k in range(DEPTH):
        flat[...] = mm_nt(hd[...], h1[pl.ds(k * SLICE, SLICE)])
        for d in range(grid.nd):
            place = (k, d // (2 * grid.nx), d // 2 % grid.nx, d % 2)
            terms[place] = flat[pl.ds(d * rows, rows)].astype(bf16)
    ticks = pipelined(jobs, len(jobs))
    for tick in ticks[: len(jobs)]:
        tick()
    ticks = ticks[len(jobs) :]

    def turn(count=1):
        for _ in range(count):
            if ticks:
                ticks.pop(0)()

    for k in range(DEPTH):
        og[pl.ds(k * SLICE, SLICE)] = mm_tn(heads[k], hd[...])
        if k == 1:
            turn()
    turn()
    total = jnp.zeros((1, tokens), f32)
    for k in range(DEPTH):
        rows = pl.ds(k * SLICE, SLICE)
        normed = x[rows].astype(f32) * inverse
        sums = jnp.sum(og[rows] * normed, axis=1, keepdims=True)
        place = lax.broadcasted_iota(jnp.int32, (SLICE, 128), 1)
        wide[rows] = jnp.where(place == 0, sums, jnp.where(place == 1, gain_two[rows], 0.0))
        total += jnp.sum(og[rows] * gain[rows, 0:1] * normed, axis=0, keepdims=True)
    value[...] = wide[...].T[:8]
    share.start(0)
    turn()
    mean = total * (1.0 / D)
    for k in range(DEPTH):
        rows = pl.ds(k * SLICE, SLICE)
        normed = x[rows].astype(f32) * inverse
        ig[rows] = rg[rows] + inverse * (og[rows] * gain[rows, 0:1] - normed * mean)
    turn()
    gdown[...] = columns[0].end()
    goutput[...] = columns[1].end().T
    for k in range(4):
        share.end(k)
        if k < 3:
            share.start(k + 1)
        turn(2)
    turn(len(ticks))
    share.drain()
    for job in jobs + columns:
        job.drain()


def finish(grid, hd, heads, x, gain, rg, gain_two, down, output, collective_id):
    tokens = x.shape[1]
    rows = QKV // grid.nd
    term = jax.ShapeDtypeStruct((rows, SLICE), bf16)
    pieces = chunk_list([term])
    scratch = [
        pltpu.VMEM((D, tokens), bf16),
        pltpu.VMEM((D, tokens), f32),
        pltpu.VMEM((QKV, SLICE), f32),
        pltpu.VMEM((D, 128), f32),
        pltpu.VMEM((grid.nz, grid.ny, grid.nx, 2, rows, SLICE), bf16),
        pltpu.VMEM((8, D), f32),
        pltpu.VMEM(down.shape, bf16),
        pltpu.VMEM(output.shape, bf16),
        pltpu.SemaphoreType.DMA((2, 2)),
    ]
    scratch += reduce_scratch(grid, [term], (True,), pieces)
    scratch += Share.scratch(grid, (8, D))
    scratch.append(pltpu.SemaphoreType.DMA((SHARE_SEMS,)))
    return pl.pallas_call(
        functools.partial(finish_kernel, grid, pieces),
        out_shape=[
            jax.ShapeDtypeStruct((D, tokens), f32),
            jax.ShapeDtypeStruct((rows, SLICE), f32),
            jax.ShapeDtypeStruct((8, D), f32),
            jax.ShapeDtypeStruct(down.shape[1:], f32),
            jax.ShapeDtypeStruct(output.shape[:0:-1], f32),
        ],
        in_specs=[VMEM] * 8,
        out_specs=[VMEM] * 5,
        scratch_shapes=scratch,
        compiler_params=pltpu.CompilerParams(
            collective_id=collective_id, has_side_effects=True, vmem_limit_bytes=62 << 20
        ),
        name="finish",
    )(hd, heads, x, gain, rg, gain_two, down, output)


READY = 3
SUMMED = 1


def local(
    grid,
    hidden_in,
    out_grad,
    seg_ids,
    doc_start,
    norm_gains,
    heads_weight,
    output_weight,
    expand_weight,
    down_weight,
    gains_first,
    gains_second,
    heads_first,
    heads_second,
    output_first,
    output_second,
    expand_first,
    expand_second,
    down_first,
    down_second,
):
    tokens = hidden_in.shape[0]
    first_row = lax.axis_index("shard") * tokens
    positions = first_row + jnp.arange(tokens, dtype=jnp.int32)
    freq = jnp.power(10000.0, -jnp.arange(HEAD // 2).astype(f32) / (HEAD // 2))
    angle = (positions - doc_start).astype(f32)[None, :] * freq[:, None]
    cos, sin = jnp.cos(angle), jnp.sin(angle)
    seg_row = seg_ids[0]
    seg_query = lax.dynamic_slice_in_dim(seg_row, first_row, tokens)
    doc = jnp.arange(HEAD, dtype=jnp.int32)
    qext = jnp.where((doc[:, None] < DOCS) & (seg_query[None, :] == doc[:, None]), HIDE, 0.0).astype(bf16)
    lane = jnp.arange(128, dtype=jnp.int32) - HEAD
    other_doc = (lane[None, :] >= 0) & (lane[None, :] < DOCS) & (seg_row[:, None] != lane[None, :])
    kext = jnp.where(other_doc | ((lane >= DOCS) & (lane < DOCS + 3))[None, :], 1.0, 0.0).astype(bf16)
    x, ogt = hidden_in.T, out_grad.T
    gain = norm_gains.T

    heads_stack, *columns = gather_weights(
        grid, [heads_weight.T], (True,), [output_weight, down_weight.T], (False, True, False), 1
    )
    heads = heads_stack.reshape(DEPTH, QKV, SLICE)
    stepped = expand_weight.shape[1] == STEPS * WIDTH
    leads = [None, None, list(range(READY)) if stepped else None]
    shards = [*columns, expand_weight]
    output_stack, down_stack, expand_stack, qx, qn, kv, att = front(
        grid, shards, (True, True, False), leads, heads, x, gain, cos, sin, qext, kext, 2
    )
    wo = output_stack.reshape(DEPTH, D, SLICE)
    down = down_stack.reshape(DEPTH, D, FF // DEPTH)
    blocks = (8, DEPTH, SLICE)
    if stepped:
        late = middle(grid, att, wo, x, ogt, gain, expand_stack, down, expand_weight, SUMMED, 5)
        out, rg, gain_two_term, dwo, dox, dexpand, ddn, *late = late
        early_exp = late[-1] if SUMMED else None
    else:
        expand = expand_stack.transpose(1, 2, 0, 3).reshape(DEPTH, SLICE, 8, STEPS, WIDTH)
        expand = expand.transpose(3, 2, 0, 1, 4)
        out, rg, gain_two_term, dwo, dox, dexpand, ddn = middle(
            grid, att, wo, x, ogt, gain, expand, down, None, 0, 5
        )
        early_exp = None
        dexpand = dexpand.transpose(2, 3, 1, 0, 4).reshape(DEPTH, SLICE, grid.nd, -1).transpose(2, 0, 1, 3)
    if stepped:
        dexpand = dexpand.reshape((STEPS, grid.nd, grid.nz, SLICE, WIDTH))
    terms = [ddn.reshape(down_stack.shape), dexpand, dwo.reshape(output_stack.shape)]
    leads = [None, list(range(SUMMED, STEPS)) if stepped else None, None]
    down_column, expand_grad, output_column, hd = back(
        grid, terms, (True, False, True), leads, early_exp, qx, qn, dox, kv, kext, cos, sin, 3
    )
    ig, heads_grad, gains_grad, down_grad, output_grad = finish(
        grid, hd, heads, x, gain, rg, gain_two_term, down_column, output_column, 4
    )
    heads_grad, down_grad, gains_grad = heads_grad.T, down_grad.T, gains_grad[:2]
    hidden_out, input_grad = out.T, ig.T
    gains_new, gains_first_new, gains_second_new = adamw(
        norm_gains, gains_grad, gains_first, gains_second, gain_rate, 0.0
    )
    heads_new, heads_first_new, heads_second_new = adamw(
        heads_weight, heads_grad, heads_first, heads_second, matrix_rate, decay_rate
    )
    output_new, output_first_new, output_second_new = adamw(
        output_weight, output_grad, output_first, output_second, output_rate, decay_rate
    )
    expand_new, expand_first_new, expand_second_new = adamw(
        expand_weight, expand_grad, expand_first, expand_second, matrix_rate, decay_rate
    )
    down_new, down_first_new, down_second_new = adamw(
        down_weight, down_grad, down_first, down_second, matrix_rate, decay_rate
    )
    return (
        hidden_out,
        input_grad,
        gains_grad,
        heads_grad,
        output_grad,
        expand_grad,
        down_grad,
        gains_new,
        heads_new,
        output_new,
        expand_new,
        down_new,
        gains_first_new,
        gains_second_new,
        heads_first_new,
        heads_second_new,
        output_first_new,
        output_second_new,
        expand_first_new,
        expand_second_new,
        down_first_new,
        down_second_new,
    )


def solution(mesh):
    return jax.shard_map(
        functools.partial(local, Grid(mesh)),
        mesh=mesh,
        in_specs=(
            P(("dp", "shard"), None),
            P(("dp", "shard"), None),
            P("dp", None),
            P(("dp", "shard")),
            P(),
            P("shard", "dp"),
            P("shard", "dp"),
            P("shard", "dp"),
            P("shard", "dp"),
            P(),
            P(),
            P("shard", "dp"),
            P("shard", "dp"),
            P("shard", "dp"),
            P("shard", "dp"),
            P("shard", "dp"),
            P("shard", "dp"),
            P("shard", "dp"),
            P("shard", "dp"),
        ),
        out_specs=(
            P(("dp", "shard"), None),
            P(("dp", "shard"), None),
            P(),
            P("shard", "dp"),
            P("shard", "dp"),
            P("shard", "dp"),
            P("shard", "dp"),
            P(),
            P("shard", "dp"),
            P("shard", "dp"),
            P("shard", "dp"),
            P("shard", "dp"),
            P(),
            P(),
            P("shard", "dp"),
            P("shard", "dp"),
            P("shard", "dp"),
            P("shard", "dp"),
            P("shard", "dp"),
            P("shard", "dp"),
            P("shard", "dp"),
            P("shard", "dp"),
        ),
        check_vma=False,
    )
```
